32 devices in a mesh: shard: 8 (over z, core), context: 2 (over x), tensor: 2 (over y).
Axes of the slice: x: 2, y: 2, z: 4, core: 2. Of those that a mesh axis runs over, the one named last changes fastest.
Arguments:
- inputs: bfloat16 [32, 1024, 768], P('shard', 'context'), may hold values from -6 to 6
- out_grad: bfloat16 [32, 1024, 768], P('shard', 'context'), may hold values from -6 to 6
- picture_starts: int32 [32, 2], P('shard'), may hold values from 0 to 768, as said below
- segment_offsets: int32 [12, 5], P('tensor'), may hold values from 0 to 1023
- dilation_offsets: int32 [12, 5], P('tensor'), may hold values from 0 to 11
- norm_gains: bfloat16 [2, 768], P(None, 'shard'), may hold values from 0.5 to 1.5
- w_qkv: bfloat16 [3, 768, 768], P(None, 'shard', 'tensor'), may hold values from -0.21875 to 0.21875
- head_biases: bfloat16 [2, 12, 64], P(None, 'tensor', 'shard'), may hold values from -3 to 3
- head_gain: bfloat16 [12, 64], P('tensor', 'shard'), may hold values from 0.5 to 1.5
- w_out: bfloat16 [768, 768], P('tensor', 'shard'), may hold values from -0.21875 to 0.21875
- out_biases: bfloat16 [2, 768], P(None, 'shard'), may hold values from -3 to 3
- w_up: bfloat16 [768, 3072], P('shard', 'tensor'), may hold values from -0.21875 to 0.21875
- unit_bias: bfloat16 [48, 64], P('tensor', 'shard'), may hold values from -3 to 3
- unit_gain: bfloat16 [48, 64], P('tensor', 'shard'), may hold values from 0.5 to 1.5
- w_down: bfloat16 [3072, 768], P('tensor', 'shard'), may hold values from -0.109375 to 0.109375
Outputs:
- layer_out: bfloat16 [32, 1024, 768], P('shard', 'context')
- input_grad: bfloat16 [32, 1024, 768], P('shard', 'context')
- norm_gains_grad: float32 [2, 768], P(None, 'shard')
- w_qkv_grad: float32 [3, 768, 768], P(None, 'shard', 'tensor')
- head_biases_grad: float32 [2, 12, 64], P(None, 'tensor', 'shard')
- head_gain_grad: float32 [12, 64], P('tensor', 'shard')
- w_out_grad: float32 [768, 768], P('tensor', 'shard')
- out_biases_grad: float32 [2, 768], P(None, 'shard')
- w_up_grad: float32 [768, 3072], P('shard', 'tensor')
- unit_bias_grad: float32 [48, 64], P('tensor', 'shard')
- unit_gain_grad: float32 [48, 64], P('tensor', 'shard')
- w_down_grad: float32 [3072, 768], P('tensor', 'shard')
The draws below stay inside these ranges and needn't reach their ends.
Inputs may be any that keep to these rules, and one draw needn't show every extreme that they name: `picture_starts`: in every sequence, piece k (k = 0 to 1) covers 256 positions from its start, which lies between k * 512 and that plus 1024 // 2 - 256, on a multiple of 32; pieces never intersect. `segment_offsets`: used modulo each pattern's segment span. `dilation_offsets`: used modulo each pattern's dilation.
All inputs are finite; a program needn't handle non-finite values.
Results may differ from the reference program's by a relative error of at most 0.018.
Values may be sent and summed in bfloat16 or wider, within the bound.
A program may use at most 320 MiB of HBM per device.

```python
import jax
import jax.numpy as jnp
from jax import lax

D = 768
H = 12
HD = 64
FF = 3072
SEQUENCE_TOKENS = 1024
PIECE = 256
PIECES = 2
PATTERNS = 5
SEQS = 32
UNIT_ROWS = 48


def draw_picture_starts(key, part):
    piece_span = SEQUENCE_TOKENS // PIECES
    grain = SEQUENCE_TOKENS // 32
    choices_count = (piece_span - PIECE) // grain + 1
    picks = jax.random.randint(key, (SEQS, PIECES), 0, choices_count)
    bases = jnp.arange(PIECES, dtype=jnp.int32)[None, :] * piece_span
    return (bases + picks * grain).astype(jnp.int32)


def place_ends(values, own_key, low, top_value):
    index_at = [jax.random.randint(jax.random.fold_in(own_key, axis), (), 0, length) for axis, length in enumerate(values.shape)]
    widest = values.shape.index(max(values.shape))
    beside = index_at[:widest] + [(index_at[widest] + 1) % values.shape[widest]] + index_at[widest + 1:]
    return values.at[tuple(index_at)].set(low).at[tuple(beside)].set(top_value)


def block_scale(stream_key, extent, split, smallest, largest):
    def one(position, parts):
        draws = jax.random.uniform(jax.random.fold_in(jax.random.fold_in(stream_key, 6), position), (parts,), jnp.float32, smallest / len(split), largest / len(split))
        return jnp.repeat(jnp.exp(draws), extent[position] // parts).reshape((-1,) + (1,) * (len(extent) - position - 1))

    gain = one(*split[0])
    for cut in split[1:]:
        gain = gain * one(*cut)
    return gain


def gaussian(stream_key, extent, scale, most, split=(), kind=jnp.bfloat16):
    gain = block_scale(stream_key, extent, split, -0.22, 0.18) if split else 1.0
    entries = jax.random.normal(stream_key, extent, jnp.float32) * scale * gain
    return jnp.minimum(jnp.maximum(entries, -most), most).astype(kind)


def setup_inputs(seed: int = 0) -> dict:
    streams_of = jax.random.split(jax.random.key(seed), 16)
    return {
        "inputs": gaussian(streams_of[0], (SEQS, SEQUENCE_TOKENS, D), 1.0, 6.0, ((0, 8), (1, 2))),
        "out_grad": gaussian(streams_of[1], (SEQS, SEQUENCE_TOKENS, D), 1.0, 6.0, ((0, 8), (1, 2))),
        "picture_starts": draw_picture_starts(jax.random.fold_in(streams_of[15], 71), 0),
        "segment_offsets": place_ends(jax.random.randint(streams_of[3], (H, PATTERNS), 0, SEQUENCE_TOKENS), jax.random.fold_in(streams_of[3], 1), 0, SEQUENCE_TOKENS - 1).astype(jnp.int32),
        "dilation_offsets": place_ends(jax.random.randint(streams_of[4], (H, PATTERNS), 0, 12), jax.random.fold_in(streams_of[4], 1), 0, 11).astype(jnp.int32),
        "norm_gains": jnp.clip(1.0 + 0.1 * jax.random.normal(streams_of[5], (2, D), jnp.float32), 0.5, 1.5).astype(jnp.bfloat16),
        "w_qkv": gaussian(streams_of[6], (3, D, D), D ** -0.5, 0.21875, ((1, 8), (2, 2))),
        "head_biases": gaussian(streams_of[7], (2, H, HD), 0.5, 3.0, ((1, 2), (2, 8))),
        "head_gain": jnp.clip(1.0 + 0.1 * jax.random.normal(streams_of[8], (H, HD), jnp.float32), 0.5, 1.5).astype(jnp.bfloat16),
        "w_out": gaussian(streams_of[9], (D, D), D ** -0.5, 0.21875, ((0, 2), (1, 8))),
        "out_biases": gaussian(streams_of[10], (2, D), 0.5, 3.0, ((1, 8),)),
        "w_up": gaussian(streams_of[11], (D, FF), D ** -0.5, 0.21875, ((0, 8), (1, 2))),
        "unit_bias": gaussian(streams_of[12], (UNIT_ROWS, HD), 0.5, 3.0, ((0, 2), (1, 8))),
        "unit_gain": jnp.clip(1.0 + 0.1 * jax.random.normal(streams_of[13], (UNIT_ROWS, HD), jnp.float32), 0.5, 1.5).astype(jnp.bfloat16),
        "w_down": gaussian(streams_of[14], (FF, D), FF ** -0.5, 0.109375, ((0, 2), (1, 8))),
    }


epsilon = 1e-05
span_parts = (1, 2, 4, 6, 8)
dilation_rates = (1, 2, 4, 6, 12)
highest = lax.Precision.HIGHEST

@jax.custom_vjp
def low(v):
    return lax.optimization_barrier(v.astype(jnp.bfloat16)).astype(jnp.float32)

@jax.custom_vjp
def low_back(v):
    return v

def low_keep(v):
    return (low(v), None)

def low_pass(kept, grad):
    return (grad,)

def back_keep(v):
    return (v, None)

def back_low(kept, grad):
    return (low(grad),)
low.defvjp(low_keep, low_pass)
low_back.defvjp(back_keep, back_low)

def pattern_total(query_position, key_position, segmented_offsets, dilated_offsets, token_length):
    tallied_total = jnp.zeros((segmented_offsets.shape[0], query_position.shape[0], key_position.shape[0]), jnp.float32)
    for item_number in range(len(span_parts)):
        segmented_span = token_length * span_parts[item_number] // 8
        dilated_stride = dilation_rates[item_number]
        seg_shift = (segmented_offsets[:, item_number] % segmented_span)[:, None, None]
        dilated_phase = (dilated_offsets[:, item_number] % dilated_stride)[:, None, None]
        query_lookup = query_position[None, :, None] + seg_shift
        key_lookup = key_position[None, None, :] + seg_shift
        merged_heads = (query_lookup // segmented_span == key_lookup // segmented_span) & (query_lookup % dilated_stride == dilated_phase) & (key_lookup % dilated_stride == dilated_phase)
        tallied_total = tallied_total + merged_heads.astype(jnp.float32)
    return tallied_total

def picture_index(starts, token_positions):
    marked = jnp.zeros((starts.shape[0], token_positions.shape[0]), jnp.int32)
    for piece_number in range(starts.shape[1]):
        begin_at = starts[:, piece_number][:, None]
        inside = (token_positions[None, :] >= begin_at) & (token_positions[None, :] < begin_at + PIECE)
        marked = marked + (piece_number + 1) * inside.astype(jnp.int32)
    return marked

def allowed_keys(query_pic, key_pic, query_position, key_position):
    causal_ok = key_position[None, None, :] <= query_position[None, :, None]
    same_piece = (query_pic[:, :, None] == key_pic[:, None, :]) & (query_pic[:, :, None] > 0)
    return (causal_ok | same_piece).astype(jnp.float32)

def layer_norm(values, scale_row):
    mean_row = lax.optimization_barrier(jnp.mean(values, -1, keepdims=True))
    centered = values - mean_row
    variance = lax.optimization_barrier(jnp.mean(centered * centered, -1, keepdims=True))
    return centered * lax.rsqrt(variance + epsilon) * scale_row

def forward_layer(flattened_input, layer_parameters, image_list, segmented_offsets, dilated_offsets):
    norm_gains, w_qkv, head_biases, head_gain, w_out, out_biases, w_up, unit_bias, unit_gain, w_down = layer_parameters
    group_seqs = image_list.shape[0]

    def attend_one_head(call_arguments):
        head_queries, head_keys, head_values, segmented_row, dilated_row = call_arguments
        token_positions = jnp.arange(SEQUENCE_TOKENS, dtype=jnp.int32)
        tallied_total = pattern_total(token_positions, token_positions, segmented_row[None, :], dilated_row[None, :], SEQUENCE_TOKENS)[0]
        mask_table = allowed_keys(image_list, image_list, token_positions, token_positions) * tallied_total[None]
        raw_scores = low_back(jnp.einsum('gqd,gkd->gqk', head_queries, head_keys, precision=highest) * HD ** (-0.5))
        masked = jnp.where(mask_table > 0, raw_scores, -1000000000.0)
        row_top = lax.optimization_barrier(jnp.max(masked, -1, keepdims=True))
        exponent = mask_table * jnp.exp(masked - row_top)
        weights_soft = exponent / lax.optimization_barrier(jnp.sum(exponent, -1, keepdims=True))
        return jnp.einsum('gqk,gkd->gqd', low(weights_soft), head_values, precision=highest)

    def per_head_split(head_rows):
        return head_rows.reshape(group_seqs, SEQUENCE_TOKENS, H, HD).transpose(2, 0, 1, 3)
    attn_in = low(layer_norm(flattened_input, norm_gains[0]))
    bias_pair = head_biases.reshape(2, D)
    query_matrix = low_back(low(jnp.dot(attn_in, w_qkv[0], precision=highest) + bias_pair[0]))
    key_matrix = low_back(low(jnp.dot(attn_in, w_qkv[1], precision=highest)))
    value_matrix = low_back(low(jnp.dot(attn_in, w_qkv[2], precision=highest) + bias_pair[1]))
    blended_output = lax.map(jax.checkpoint(attend_one_head), (per_head_split(query_matrix), per_head_split(key_matrix), per_head_split(value_matrix), segmented_offsets, dilated_offsets))
    attended = low_back(blended_output.transpose(1, 2, 0, 3).reshape(group_seqs * SEQUENCE_TOKENS, D))
    sub_in = low(layer_norm(attended, head_gain.reshape(D)))
    branch = low_back(jnp.dot(sub_in, w_out, precision=highest) + out_biases[0])
    middle = flattened_input + branch
    ffn_in = low(layer_norm(middle, norm_gains[1]))
    hidden = low_back(jnp.dot(ffn_in, w_up, precision=highest) + unit_bias.reshape(FF))
    activated = jax.nn.gelu(hidden, approximate=True)
    ffn_mid = low(layer_norm(activated, unit_gain.reshape(FF)))
    result = low_back(jnp.dot(ffn_mid, w_down, precision=highest) + out_biases[1])
    return middle + result

def reference(inputs, out_grad, picture_starts, segment_offsets, dilation_offsets, norm_gains, w_qkv, head_biases, head_gain, w_out, out_biases, w_up, unit_bias, unit_gain, w_down):
    layer_parameters = tuple((item.astype(jnp.float32) for item in (norm_gains, w_qkv, head_biases, head_gain, w_out, out_biases, w_up, unit_bias, unit_gain, w_down)))
    group_seqs = 4
    group_count = SEQS // group_seqs

    def one_group(totals, item_number):
        first_row = (item_number * group_seqs).astype(jnp.int32)
        group_in = lax.dynamic_slice_in_dim(inputs, first_row, group_seqs, 0).astype(jnp.float32).reshape(group_seqs * SEQUENCE_TOKENS, D)
        group_grad = lax.dynamic_slice_in_dim(out_grad, first_row, group_seqs, 0).astype(jnp.float32).reshape(group_seqs * SEQUENCE_TOKENS, D)
        group_pics = lax.dynamic_slice_in_dim(picture_starts, first_row, group_seqs, 0)
        image_list = picture_index(group_pics, jnp.arange(SEQUENCE_TOKENS, dtype=jnp.int32))

        def forward_only(flattened_input, weights):
            return forward_layer(flattened_input, weights, image_list, segment_offsets, dilation_offsets)
        outputs, pullback = jax.vjp(forward_only, group_in, layer_parameters)
        input_grad, param_grads = pullback(group_grad)
        totals = jax.tree.map(jnp.add, totals, param_grads)
        return (totals, (outputs.astype(jnp.bfloat16).reshape(group_seqs, SEQUENCE_TOKENS, D), input_grad.astype(jnp.bfloat16).reshape(group_seqs, SEQUENCE_TOKENS, D)))
    zeros = jax.tree.map(jnp.zeros_like, layer_parameters)
    totals, stacked = lax.scan(one_group, zeros, jnp.arange(group_count, dtype=jnp.int32))
    layer_out = stacked[0].reshape(SEQS, SEQUENCE_TOKENS, D)
    input_grad = stacked[1].reshape(SEQS, SEQUENCE_TOKENS, D)
    return (layer_out, input_grad, totals[0], totals[1], totals[2], totals[3], totals[4], totals[5], totals[6], totals[7], totals[8], totals[9])
```

```python
from functools import partial

import jax
import jax.numpy as jnp
from jax import lax
from jax.sharding import PartitionSpec as P

HD = 64
FF = 3072
PIECE = 256


epsilon = 1e-05
span_parts = (1, 2, 4, 6, 8)
dilation_rates = (1, 2, 4, 6, 12)


def pattern_total(query_position, key_position, segmented_offsets, dilated_offsets, token_length):
    tallied_total = jnp.zeros(
        (segmented_offsets.shape[0], query_position.shape[0], key_position.shape[0]), jnp.float32
    )
    for item_number in range(len(span_parts)):
        segmented_span = token_length * span_parts[item_number] // 8
        dilated_stride = dilation_rates[item_number]
        seg_shift = (segmented_offsets[:, item_number] % segmented_span)[:, None, None]
        dilated_phase = (dilated_offsets[:, item_number] % dilated_stride)[:, None, None]
        query_lookup = query_position[None, :, None] + seg_shift
        key_lookup = key_position[None, None, :] + seg_shift
        merged_heads = (
            (query_lookup // segmented_span == key_lookup // segmented_span)
            & (query_lookup % dilated_stride == dilated_phase)
            & (key_lookup % dilated_stride == dilated_phase)
        )
        tallied_total = tallied_total + merged_heads.astype(jnp.float32)
    return tallied_total


def picture_index(starts, token_positions):
    marked = jnp.zeros((starts.shape[0], token_positions.shape[0]), jnp.int32)
    for piece_number in range(starts.shape[1]):
        begin_at = starts[:, piece_number][:, None]
        inside = (token_positions[None, :] >= begin_at) & (
            token_positions[None, :] < begin_at + PIECE
        )
        marked = marked + (piece_number + 1) * inside.astype(jnp.int32)
    return marked


def allowed_keys(query_pic, key_pic, query_position, key_position):
    causal_ok = key_position[None, None, :] <= query_position[None, :, None]
    same_piece = (query_pic[:, :, None] == key_pic[:, None, :]) & (query_pic[:, :, None] > 0)
    return (causal_ok | same_piece).astype(jnp.float32)


def outer_sum(left_rows, right_rows):
    return lax.dot_general(
        left_rows, right_rows, (((0,), (0,)), ((), ())), preferred_element_type=jnp.float32
    )


def back_dot(left_rows, weight_rows):
    return lax.dot_general(
        left_rows, weight_rows, (((1,), (1,)), ((), ())), preferred_element_type=jnp.float32
    )


def norm_rows(values, scale_row):
    mean_row = jnp.mean(values, -1, keepdims=True)
    centered = values - mean_row
    inv_std = lax.rsqrt(jnp.mean(centered * centered, -1, keepdims=True) + epsilon)
    normed = centered * inv_std
    return (normed, inv_std, normed * scale_row)


def norm_back(normed, inv_std, scale_row, grad_rows):
    scaled = grad_rows * scale_row
    mean_plain = jnp.mean(scaled, -1, keepdims=True)
    mean_cross = jnp.mean(scaled * normed, -1, keepdims=True)
    return (inv_std * (scaled - mean_plain - normed * mean_cross), jnp.sum(grad_rows * normed, 0))


def probabilities(query_heads, key_heads, mask_table):
    raw_scores = jnp.einsum(
        "sqhd,skhd->shqk", query_heads, key_heads, preferred_element_type=jnp.float32
    ) * HD ** (-0.5)
    masked = jnp.where(mask_table > 0, raw_scores, -1000000000.0)
    row_top = jnp.max(masked, -1, keepdims=True)
    exponent = mask_table * jnp.exp(masked - row_top)
    row_total = jnp.sum(exponent, -1, keepdims=True)
    return (exponent / row_total, row_top, row_total)


def gather_weight(local_block, shard_dim, tensor_dim):
    ns = lax.axis_size("shard")
    nt = lax.axis_size("tensor")
    stacked = lax.all_gather(local_block, ("shard", "tensor"), axis=0, tiled=False)
    stacked = stacked.reshape((ns, nt) + local_block.shape)
    rank = local_block.ndim
    order = []
    for dim in range(rank):
        if dim == shard_dim:
            order.append(0)
        if dim == tensor_dim:
            order.append(1)
        order.append(dim + 2)
    moved = stacked.transpose(order)
    full_shape = list(local_block.shape)
    full_shape[shard_dim] *= ns
    full_shape[tensor_dim] *= nt
    return moved.reshape(full_shape)


def scatter_weight(full_grad, shard_dim, tensor_dim):
    ns = lax.axis_size("shard")
    nt = lax.axis_size("tensor")
    rank = full_grad.ndim
    split_shape = []
    positions = {}
    for dim in range(rank):
        size = full_grad.shape[dim]
        if dim == shard_dim:
            positions["s"] = len(split_shape)
            split_shape += [ns, size // ns]
        elif dim == tensor_dim:
            positions["t"] = len(split_shape)
            split_shape += [nt, size // nt]
        else:
            split_shape.append(size)
    pieces = full_grad.astype(jnp.bfloat16).reshape(split_shape)
    rest = [d for d in range(len(split_shape)) if d not in (positions["s"], positions["t"])]
    pieces = pieces.transpose([positions["s"], positions["t"]] + rest)
    pieces = pieces.reshape((ns * nt,) + pieces.shape[2:])
    share = lax.psum_scatter(pieces, ("shard", "tensor"), scatter_dimension=0, tiled=False)
    return lax.psum(share, "context").astype(jnp.float32)


def block_of(full, dims_axes):
    starts = [0] * full.ndim
    sizes = list(full.shape)
    for dim, axis in dims_axes:
        count = lax.axis_size(axis)
        sizes[dim] = full.shape[dim] // count
        starts[dim] = lax.axis_index(axis) * sizes[dim]
    return lax.dynamic_slice(full, starts, sizes)


def forward_pass(block_in, starts, tallied_total, weights, query_position, key_position):
    w_qkv, w_out, w_up, w_down, norm_gains, out_biases, head_biases, head_gain, unit_bias, unit_gain = weights
    seq_count, local_len, model_width = block_in.shape
    seq_len = key_position.shape[0]
    row_count = seq_count * local_len
    heads = model_width // HD
    flattened_input = block_in.reshape(row_count, model_width).astype(jnp.float32)
    first_normed, first_inv, first_out = norm_rows(flattened_input, norm_gains[0])
    attn_in = first_out.astype(jnp.bfloat16)
    projected = jnp.einsum("rd,jde->jre", attn_in, w_qkv, preferred_element_type=jnp.float32)
    query_matrix = (projected[0] + head_biases[0]).astype(jnp.bfloat16)
    keys_local = projected[1].astype(jnp.bfloat16).reshape(seq_count, local_len, model_width)
    values_local = (projected[2] + head_biases[1]).astype(jnp.bfloat16).reshape(
        seq_count, local_len, model_width
    )
    key_all = lax.all_gather(keys_local, "context", axis=1, tiled=True)
    value_all = lax.all_gather(values_local, "context", axis=1, tiled=True)
    query_pic = picture_index(starts, query_position)
    key_pic = picture_index(starts, key_position)
    mask_table = (
        allowed_keys(query_pic, key_pic, query_position, key_position)[:, None] * tallied_total[None]
    )
    query_heads = query_matrix.reshape(seq_count, local_len, heads, HD)
    key_heads = key_all.reshape(seq_count, seq_len, heads, HD)
    value_heads = value_all.reshape(seq_count, seq_len, heads, HD)
    weights_soft = probabilities(query_heads, key_heads, mask_table)[0]
    attended = jnp.einsum(
        "shqk,skhd->sqhd",
        weights_soft.astype(jnp.bfloat16),
        value_heads,
        preferred_element_type=jnp.float32,
    ).reshape(row_count, model_width)
    sub_normed, sub_inv, sub_out = norm_rows(attended, head_gain)
    sub_in = sub_out.astype(jnp.bfloat16)
    middle = flattened_input + (
        jnp.dot(sub_in, w_out, preferred_element_type=jnp.float32) + out_biases[0]
    )
    second_normed, second_inv, second_out = norm_rows(middle, norm_gains[1])
    ffn_in = second_out.astype(jnp.bfloat16)
    hidden = jnp.dot(ffn_in, w_up, preferred_element_type=jnp.float32) + unit_bias
    activated = jax.nn.gelu(hidden, approximate=True)
    unit_normed, unit_inv, unit_out = norm_rows(activated, unit_gain)
    ffn_mid = unit_out.astype(jnp.bfloat16)
    layer_out = (
        middle + (jnp.dot(ffn_mid, w_down, preferred_element_type=jnp.float32) + out_biases[1])
    ).astype(jnp.bfloat16)
    kept_state = (
        attn_in,
        first_normed,
        first_inv,
        query_heads,
        key_heads,
        value_heads,
        mask_table,
        sub_normed,
        sub_inv,
        sub_in,
        second_normed,
        second_inv,
        ffn_in,
        hidden,
        unit_normed,
        unit_inv,
        ffn_mid,
    )
    return (kept_state, layer_out.reshape(seq_count, local_len, model_width))


def backward_pass(kept_state, block_grad, weights):
    w_qkv, w_out, w_up, w_down, norm_gains, out_biases, head_biases, head_gain, unit_bias, unit_gain = weights
    (
        attn_in,
        first_normed,
        first_inv,
        query_heads,
        key_heads,
        value_heads,
        mask_table,
        sub_normed,
        sub_inv,
        sub_in,
        second_normed,
        second_inv,
        ffn_in,
        hidden,
        unit_normed,
        unit_inv,
        ffn_mid,
    ) = kept_state
    seq_count, local_len, model_width = block_grad.shape
    row_count = seq_count * local_len
    seq_len = key_heads.shape[1]
    grad_low = block_grad.reshape(row_count, model_width)
    grad_full = grad_low.astype(jnp.float32)
    down_grad = outer_sum(ffn_mid, grad_low)
    last_bias_grad = jnp.sum(grad_full, 0)
    unit_grad = back_dot(grad_low, w_down)
    activated_grad, unit_gain_grad = norm_back(unit_normed, unit_inv, unit_gain, unit_grad)
    gelu_value, gelu_pull = jax.vjp(partial(jax.nn.gelu, approximate=True), hidden)
    hidden_low = gelu_pull(activated_grad)[0].astype(jnp.bfloat16)
    up_grad = outer_sum(ffn_in, hidden_low)
    unit_bias_grad = jnp.sum(hidden_low, 0, dtype=jnp.float32)
    ffn_in_grad = back_dot(hidden_low, w_up)
    middle_part, second_gain_grad = norm_back(second_normed, second_inv, norm_gains[1], ffn_in_grad)
    middle_grad = grad_full + middle_part
    middle_low = middle_grad.astype(jnp.bfloat16)
    out_weight_grad = outer_sum(sub_in, middle_low)
    first_bias_grad = jnp.sum(middle_low, 0, dtype=jnp.float32)
    sub_grad = back_dot(middle_low, w_out)
    attended_grad, head_gain_grad = norm_back(sub_normed, sub_inv, head_gain, sub_grad)
    attended_low = attended_grad.astype(jnp.bfloat16)
    heads = query_heads.shape[2]
    weights_soft, row_top, row_total = probabilities(query_heads, key_heads, mask_table)
    grad_heads = attended_low.reshape(seq_count, local_len, heads, HD)
    soft_grad = jnp.einsum(
        "sqhd,skhd->shqk", grad_heads, value_heads, preferred_element_type=jnp.float32
    )
    inner_sum = jnp.sum(weights_soft * soft_grad, -1, keepdims=True)
    score_low = (weights_soft * (soft_grad - inner_sum)).astype(jnp.bfloat16)
    root_scale = HD ** (-0.5)
    query_low = (
        (
            jnp.einsum("shqk,skhd->sqhd", score_low, key_heads, preferred_element_type=jnp.float32)
            * root_scale
        )
        .astype(jnp.bfloat16)
        .reshape(row_count, -1)
    )
    key_part = (
        jnp.einsum("shqk,sqhd->skhd", score_low, query_heads, preferred_element_type=jnp.float32)
        * root_scale
    )
    value_part = jnp.einsum(
        "shqk,sqhd->skhd",
        weights_soft.astype(jnp.bfloat16),
        grad_heads,
        preferred_element_type=jnp.float32,
    )
    key_low = lax.psum_scatter(
        key_part.reshape(seq_count, seq_len, -1).astype(jnp.bfloat16),
        "context",
        scatter_dimension=1,
        tiled=True,
    ).reshape(row_count, -1)
    value_low = lax.psum_scatter(
        value_part.reshape(seq_count, seq_len, -1).astype(jnp.bfloat16),
        "context",
        scatter_dimension=1,
        tiled=True,
    ).reshape(row_count, -1)
    stacked = jnp.stack([query_low, key_low, value_low])
    qkv_grad = jnp.einsum("rd,jre->jde", attn_in, stacked, preferred_element_type=jnp.float32)
    head_bias_grad = jnp.stack(
        [jnp.sum(query_low, 0, dtype=jnp.float32), jnp.sum(value_low, 0, dtype=jnp.float32)]
    )
    attn_in_grad = jnp.einsum("jre,jde->rd", stacked, w_qkv, preferred_element_type=jnp.float32)
    input_part, first_gain_grad = norm_back(first_normed, first_inv, norm_gains[0], attn_in_grad)
    input_low = (middle_grad + input_part).astype(jnp.bfloat16)
    big_terms = (qkv_grad, out_weight_grad, up_grad, down_grad)
    small_terms = (
        jnp.stack([first_gain_grad, second_gain_grad]),
        head_bias_grad,
        head_gain_grad,
        jnp.stack([first_bias_grad, last_bias_grad]),
        unit_bias_grad,
        unit_gain_grad,
    )
    return (big_terms, small_terms, input_low.reshape(seq_count, local_len, model_width))


def local(
    inputs,
    out_grad,
    picture_starts,
    segment_offsets,
    dilation_offsets,
    norm_gains,
    w_qkv,
    head_biases,
    head_gain,
    w_out,
    out_biases,
    w_up,
    unit_bias,
    unit_gain,
    w_down,
):
    local_seqs, local_len, model_width = inputs.shape
    tensor_count = lax.axis_size("tensor")
    mine = local_seqs // tensor_count
    first_seq = lax.axis_index("tensor") * mine
    block_in = lax.dynamic_slice_in_dim(inputs, first_seq, mine, 0)
    block_grad = lax.dynamic_slice_in_dim(out_grad, first_seq, mine, 0)
    starts = lax.dynamic_slice_in_dim(picture_starts, first_seq, mine, 0)
    seq_len = local_len * lax.axis_size("context")
    query_position = lax.axis_index("context") * local_len + jnp.arange(local_len, dtype=jnp.int32)
    key_position = jnp.arange(seq_len, dtype=jnp.int32)
    all_segments = lax.all_gather(segment_offsets, "tensor", axis=0, tiled=True)
    all_dilations = lax.all_gather(dilation_offsets, "tensor", axis=0, tiled=True)
    tallied_total = pattern_total(
        query_position, key_position, all_segments, all_dilations, seq_len
    )
    f32 = jnp.float32
    weights = (
        gather_weight(w_qkv, 1, 2),
        gather_weight(w_out, 1, 0),
        gather_weight(w_up, 0, 1),
        gather_weight(w_down, 1, 0),
        lax.all_gather(norm_gains, "shard", axis=1, tiled=True).astype(f32),
        lax.all_gather(out_biases, "shard", axis=1, tiled=True).astype(f32),
        gather_weight(head_biases, 2, 1).reshape(2, model_width).astype(f32),
        gather_weight(head_gain, 1, 0).reshape(model_width).astype(f32),
        gather_weight(unit_bias, 1, 0).reshape(-1).astype(f32),
        gather_weight(unit_gain, 1, 0).reshape(-1).astype(f32),
    )
    kept_state, layer_block = forward_pass(
        block_in, starts, tallied_total, weights, query_position, key_position
    )
    layer_out = lax.all_gather(layer_block, "tensor", axis=0, tiled=True)
    big_terms, small_terms, input_block = backward_pass(kept_state, block_grad, weights)
    input_grad = lax.all_gather(input_block, "tensor", axis=0, tiled=True)
    qkv_grad, out_weight_grad, up_grad, down_grad = big_terms
    down_share = scatter_weight(down_grad, 1, 0)
    up_share = scatter_weight(up_grad, 0, 1)
    out_share = scatter_weight(out_weight_grad, 1, 0)
    qkv_share = scatter_weight(qkv_grad, 1, 2)
    packed = jnp.concatenate([term.reshape(-1) for term in small_terms])
    packed = lax.psum(packed, ("shard", "context", "tensor"))
    unpacked = []
    offset = 0
    for term in small_terms:
        unpacked.append(packed[offset : offset + term.size].reshape(term.shape))
        offset += term.size
    gains_full, head_bias_full, head_gain_full, out_bias_full, unit_bias_full, unit_gain_full = unpacked
    heads = model_width // HD
    unit_rows = unit_bias_full.shape[0] // HD
    gains_share = block_of(gains_full, ((1, "shard"),))
    head_bias_share = block_of(head_bias_full.reshape(2, heads, HD), ((1, "tensor"), (2, "shard")))
    head_gain_share = block_of(head_gain_full.reshape(heads, HD), ((0, "tensor"), (1, "shard")))
    out_bias_share = block_of(out_bias_full, ((1, "shard"),))
    unit_bias_share = block_of(unit_bias_full.reshape(unit_rows, HD), ((0, "tensor"), (1, "shard")))
    unit_gain_share = block_of(unit_gain_full.reshape(unit_rows, HD), ((0, "tensor"), (1, "shard")))
    return (
        layer_out,
        input_grad,
        gains_share,
        qkv_share,
        head_bias_share,
        head_gain_share,
        out_share,
        out_bias_share,
        up_share,
        unit_bias_share,
        unit_gain_share,
        down_share,
    )


def solution(mesh):
    placed = (
        P("shard", "context", None),
        P("shard", "context", None),
        P("shard", None),
        P("tensor", None),
        P("tensor", None),
        P(None, "shard"),
        P(None, "shard", "tensor"),
        P(None, "tensor", "shard"),
        P("tensor", "shard"),
        P("tensor", "shard"),
        P(None, "shard"),
        P("shard", "tensor"),
        P("tensor", "shard"),
        P("tensor", "shard"),
        P("tensor", "shard"),
    )
    return jax.shard_map(
        local,
        mesh=mesh,
        in_specs=placed,
        out_specs=(
            P("shard", "context", None),
            P("shard", "context", None),
            P(None, "shard"),
            P(None, "shard", "tensor"),
            P(None, "tensor", "shard"),
            P("tensor", "shard"),
            P("tensor", "shard"),
            P(None, "shard"),
            P("shard", "tensor"),
            P("tensor", "shard"),
            P("tensor", "shard"),
            P("tensor", "shard"),
        ),
        check_vma=False,
    )
```

```python
from functools import partial

import jax
import jax.numpy as jnp
from jax import lax
from jax.sharding import PartitionSpec as P

HD = 64
FF = 3072
PIECE = 256


epsilon = 1e-05
span_parts = (1, 2, 4, 6, 8)
dilation_rates = (1, 2, 4, 6, 12)


def pattern_total(query_position, key_position, segmented_offsets, dilated_offsets, token_length):
    tallied_total = jnp.zeros(
        (segmented_offsets.shape[0], query_position.shape[0], key_position.shape[0]), jnp.float32
    )
    for item_number in range(len(span_parts)):
        segmented_span = token_length * span_parts[item_number] // 8
        dilated_stride = dilation_rates[item_number]
        seg_shift = (segmented_offsets[:, item_number] % segmented_span)[:, None, None]
        dilated_phase = (dilated_offsets[:, item_number] % dilated_stride)[:, None, None]
        query_lookup = query_position[None, :, None] + seg_shift
        key_lookup = key_position[None, None, :] + seg_shift
        merged_heads = (
            (query_lookup // segmented_span == key_lookup // segmented_span)
            & (query_lookup % dilated_stride == dilated_phase)
            & (key_lookup % dilated_stride == dilated_phase)
        )
        tallied_total = tallied_total + merged_heads.astype(jnp.float32)
    return tallied_total


def picture_index(starts, token_positions):
    marked = jnp.zeros((starts.shape[0], token_positions.shape[0]), jnp.int32)
    for piece_number in range(starts.shape[1]):
        begin_at = starts[:, piece_number][:, None]
        inside = (token_positions[None, :] >= begin_at) & (
            token_positions[None, :] < begin_at + PIECE
        )
        marked = marked + (piece_number + 1) * inside.astype(jnp.int32)
    return marked


def allowed_keys(query_pic, key_pic, query_position, key_position):
    causal_ok = key_position[None, None, :] <= query_position[None, :, None]
    same_piece = (query_pic[:, :, None] == key_pic[:, None, :]) & (query_pic[:, :, None] > 0)
    return (causal_ok | same_piece).astype(jnp.float32)


def outer_sum(left_rows, right_rows):
    return lax.dot_general(
        left_rows, right_rows, (((0,), (0,)), ((), ())), preferred_element_type=jnp.float32
    )


def back_dot(left_rows, weight_rows):
    return lax.dot_general(
        left_rows, weight_rows, (((1,), (1,)), ((), ())), preferred_element_type=jnp.float32
    )


def norm_rows(values, scale_row):
    mean_row = jnp.mean(values, -1, keepdims=True)
    centered = values - mean_row
    inv_std = lax.rsqrt(jnp.mean(centered * centered, -1, keepdims=True) + epsilon)
    normed = centered * inv_std
    return (normed, inv_std, normed * scale_row)


def norm_back(normed, inv_std, scale_row, grad_rows):
    scaled = grad_rows * scale_row
    mean_plain = jnp.mean(scaled, -1, keepdims=True)
    mean_cross = jnp.mean(scaled * normed, -1, keepdims=True)
    return (inv_std * (scaled - mean_plain - normed * mean_cross), jnp.sum(grad_rows * normed, 0))


def probabilities(query_heads, key_heads, mask_table):
    raw_scores = jnp.einsum(
        "sqhd,skhd->shqk", query_heads, key_heads, preferred_element_type=jnp.float32
    ) * HD ** (-0.5)
    masked = jnp.where(mask_table > 0, raw_scores, -1000000000.0)
    row_top = jnp.max(masked, -1, keepdims=True)
    exponent = mask_table * jnp.exp(masked - row_top)
    row_total = jnp.sum(exponent, -1, keepdims=True)
    return (exponent / row_total, row_top, row_total)


def assemble(stacked, shard_dim, tensor_dim):
    ns, nt = stacked.shape[0], stacked.shape[1]
    if shard_dim is None:
        stacked = stacked[:1]
    if tensor_dim is None:
        stacked = stacked[:, :1]
    local_shape = stacked.shape[2:]
    order = []
    for dim in range(len(local_shape)):
        if dim == shard_dim:
            order.append(0)
        if dim == tensor_dim:
            order.append(1)
        order.append(dim + 2)
    if shard_dim is None:
        order = [0] + order
    if tensor_dim is None:
        order = [1] + order
    moved = stacked.transpose(order)
    full_shape = list(local_shape)
    if shard_dim is not None:
        full_shape[shard_dim] *= ns
    if tensor_dim is not None:
        full_shape[tensor_dim] *= nt
    return moved.reshape(full_shape)


def gather_weight(local_block, shard_dim, tensor_dim):
    ns = lax.axis_size("shard")
    nt = lax.axis_size("tensor")
    stacked = lax.all_gather(local_block, ("shard", "tensor"), axis=0, tiled=False)
    return assemble(stacked.reshape((ns, nt) + local_block.shape), shard_dim, tensor_dim)


def gather_packed(blocks):
    ns = lax.axis_size("shard")
    nt = lax.axis_size("tensor")
    flat = jnp.concatenate([block.reshape(-1) for block, _, _ in blocks])
    padded = -flat.size % 2048
    flat = jnp.pad(flat, (0, padded)).reshape(-1, 128)
    stacked = lax.all_gather(flat, ("shard", "tensor"), axis=0, tiled=False).reshape(ns, nt, -1)
    pieces = []
    offset = 0
    for block, shard_dim, tensor_dim in blocks:
        part = stacked[:, :, offset : offset + block.size].reshape((ns, nt) + block.shape)
        pieces.append(assemble(part, shard_dim, tensor_dim))
        offset += block.size
    return pieces


def pair_gather(block, axis_name, dim):
    if lax.axis_size(axis_name) != 2:
        return lax.all_gather(block, axis_name, axis=dim, tiled=True)
    other = lax.ppermute(block, axis_name, perm=[(0, 1), (1, 0)])
    first = lax.axis_index(axis_name) == 0
    return jnp.where(
        first, jnp.concatenate([block, other], dim), jnp.concatenate([other, block], dim)
    )


def pair_reduce(full, axis_name, dim):
    if lax.axis_size(axis_name) != 2:
        return lax.psum_scatter(
            full.astype(jnp.bfloat16), axis_name, scatter_dimension=dim, tiled=True
        ).astype(jnp.float32)
    half = full.shape[dim] // 2
    me = lax.axis_index(axis_name)
    kept = lax.dynamic_slice_in_dim(full, me * half, half, dim)
    sent = lax.dynamic_slice_in_dim(full, (1 - me) * half, half, dim).astype(jnp.bfloat16)
    received = lax.ppermute(sent, axis_name, perm=[(0, 1), (1, 0)])
    return kept + received.astype(jnp.float32)


def scatter_weight(full_grad, shard_dim, tensor_dim):
    ns = lax.axis_size("shard")
    nt = lax.axis_size("tensor")
    rank = full_grad.ndim
    split_shape = []
    positions = {}
    for dim in range(rank):
        size = full_grad.shape[dim]
        if dim == shard_dim:
            positions["s"] = len(split_shape)
            split_shape += [ns, size // ns]
        elif dim == tensor_dim:
            positions["t"] = len(split_shape)
            split_shape += [nt, size // nt]
        else:
            split_shape.append(size)
    pieces = full_grad.astype(jnp.bfloat16).reshape(split_shape)
    rest = [d for d in range(len(split_shape)) if d not in (positions["s"], positions["t"])]
    pieces = pieces.transpose([positions["s"], positions["t"]] + rest)
    pieces = pieces.reshape((ns * nt,) + pieces.shape[2:])
    share = lax.psum_scatter(pieces, ("shard", "tensor"), scatter_dimension=0, tiled=False)
    return lax.psum(share, "context").astype(jnp.float32)


def block_of(full, dims_axes):
    starts = [0] * full.ndim
    sizes = list(full.shape)
    for dim, axis in dims_axes:
        count = lax.axis_size(axis)
        sizes[dim] = full.shape[dim] // count
        starts[dim] = lax.axis_index(axis) * sizes[dim]
    return lax.dynamic_slice(full, starts, sizes)


def forward_pass(block_in, starts, tallied_total, weights, query_position, key_position):
    w_qkv, w_out, w_up, w_down, norm_gains, out_biases, head_biases, head_gain, unit_bias, unit_gain = weights
    seq_count, local_len, model_width = block_in.shape
    seq_len = key_position.shape[0]
    row_count = seq_count * local_len
    heads = model_width // HD
    flattened_input = block_in.reshape(row_count, model_width).astype(jnp.float32)
    first_normed, first_inv, first_out = norm_rows(flattened_input, norm_gains[0])
    attn_in = first_out.astype(jnp.bfloat16)
    projected = jnp.einsum("rd,jde->jre", attn_in, w_qkv, preferred_element_type=jnp.float32)
    query_matrix = (projected[0] + head_biases[0]).astype(jnp.bfloat16)
    keys_local = projected[1].astype(jnp.bfloat16).reshape(seq_count, local_len, model_width)
    values_local = (projected[2] + head_biases[1]).astype(jnp.bfloat16).reshape(
        seq_count, local_len, model_width
    )
    key_all = pair_gather(keys_local, "context", 1)
    value_all = pair_gather(values_local, "context", 1)
    query_pic = picture_index(starts, query_position)
    key_pic = picture_index(starts, key_position)
    mask_table = (
        allowed_keys(query_pic, key_pic, query_position, key_position)[:, None] * tallied_total[None]
    )
    query_heads = query_matrix.reshape(seq_count, local_len, heads, HD)
    key_heads = key_all.reshape(seq_count, seq_len, heads, HD)
    value_heads = value_all.reshape(seq_count, seq_len, heads, HD)
    weights_soft = probabilities(query_heads, key_heads, mask_table)[0]
    attended = jnp.einsum(
        "shqk,skhd->sqhd",
        weights_soft.astype(jnp.bfloat16),
        value_heads,
        preferred_element_type=jnp.float32,
    ).reshape(row_count, model_width)
    sub_normed, sub_inv, sub_out = norm_rows(attended, head_gain)
    sub_in = sub_out.astype(jnp.bfloat16)
    middle = flattened_input + (
        jnp.dot(sub_in, w_out, preferred_element_type=jnp.float32) + out_biases[0]
    )
    second_normed, second_inv, second_out = norm_rows(middle, norm_gains[1])
    ffn_in = second_out.astype(jnp.bfloat16)
    hidden = jnp.dot(ffn_in, w_up, preferred_element_type=jnp.float32) + unit_bias
    activated = jax.nn.gelu(hidden, approximate=True)
    unit_normed, unit_inv, unit_out = norm_rows(activated, unit_gain)
    ffn_mid = unit_out.astype(jnp.bfloat16)
    layer_out = (
        middle + (jnp.dot(ffn_mid, w_down, preferred_element_type=jnp.float32) + out_biases[1])
    ).astype(jnp.bfloat16)
    kept_state = (
        attn_in,
        first_normed,
        first_inv,
        query_heads,
        key_heads,
        value_heads,
        mask_table,
        sub_normed,
        sub_inv,
        sub_in,
        second_normed,
        second_inv,
        ffn_in,
        hidden,
        unit_normed,
        unit_inv,
        ffn_mid,
    )
    return (kept_state, layer_out.reshape(seq_count, local_len, model_width))


def backward_pass(kept_state, block_grad, weights):
    w_qkv, w_out, w_up, w_down, norm_gains, out_biases, head_biases, head_gain, unit_bias, unit_gain = weights
    (
        attn_in,
        first_normed,
        first_inv,
        query_heads,
        key_heads,
        value_heads,
        mask_table,
        sub_normed,
        sub_inv,
        sub_in,
        second_normed,
        second_inv,
        ffn_in,
        hidden,
        unit_normed,
        unit_inv,
        ffn_mid,
    ) = kept_state
    seq_count, local_len, model_width = block_grad.shape
    row_count = seq_count * local_len
    seq_len = key_heads.shape[1]
    grad_low = block_grad.reshape(row_count, model_width)
    grad_full = grad_low.astype(jnp.float32)
    down_grad = outer_sum(ffn_mid, grad_low)
    last_bias_grad = jnp.sum(grad_full, 0)
    unit_grad = back_dot(grad_low, w_down)
    activated_grad, unit_gain_grad = norm_back(unit_normed, unit_inv, unit_gain, unit_grad)
    gelu_value, gelu_pull = jax.vjp(partial(jax.nn.gelu, approximate=True), hidden)
    hidden_low = gelu_pull(activated_grad)[0].astype(jnp.bfloat16)
    up_grad = outer_sum(ffn_in, hidden_low)
    unit_bias_grad = jnp.sum(hidden_low, 0, dtype=jnp.float32)
    ffn_in_grad = back_dot(hidden_low, w_up)
    middle_part, second_gain_grad = norm_back(second_normed, second_inv, norm_gains[1], ffn_in_grad)
    middle_grad = grad_full + middle_part
    middle_low = middle_grad.astype(jnp.bfloat16)
    out_weight_grad = outer_sum(sub_in, middle_low)
    first_bias_grad = jnp.sum(middle_low, 0, dtype=jnp.float32)
    sub_grad = back_dot(middle_low, w_out)
    attended_grad, head_gain_grad = norm_back(sub_normed, sub_inv, head_gain, sub_grad)
    attended_low = attended_grad.astype(jnp.bfloat16)
    heads = query_heads.shape[2]
    weights_soft, row_top, row_total = probabilities(query_heads, key_heads, mask_table)
    grad_heads = attended_low.reshape(seq_count, local_len, heads, HD)
    soft_grad = jnp.einsum(
        "sqhd,skhd->shqk", grad_heads, value_heads, preferred_element_type=jnp.float32
    )
    inner_sum = jnp.sum(weights_soft * soft_grad, -1, keepdims=True)
    score_low = (weights_soft * (soft_grad - inner_sum)).astype(jnp.bfloat16)
    root_scale = HD ** (-0.5)
    query_low = (
        (
            jnp.einsum("shqk,skhd->sqhd", score_low, key_heads, preferred_element_type=jnp.float32)
            * root_scale
        )
        .astype(jnp.bfloat16)
        .reshape(row_count, -1)
    )
    key_part = (
        jnp.einsum("shqk,sqhd->skhd", score_low, query_heads, preferred_element_type=jnp.float32)
        * root_scale
    )
    value_part = jnp.einsum(
        "shqk,sqhd->skhd",
        weights_soft.astype(jnp.bfloat16),
        grad_heads,
        preferred_element_type=jnp.float32,
    )
    key_low = (
        pair_reduce(key_part.reshape(seq_count, seq_len, -1), "context", 1)
        .astype(jnp.bfloat16)
        .reshape(row_count, -1)
    )
    value_low = (
        pair_reduce(value_part.reshape(seq_count, seq_len, -1), "context", 1)
        .astype(jnp.bfloat16)
        .reshape(row_count, -1)
    )
    stacked = jnp.stack([query_low, key_low, value_low])
    qkv_grad = jnp.einsum("rd,jre->jde", attn_in, stacked, preferred_element_type=jnp.float32)
    head_bias_grad = jnp.stack(
        [jnp.sum(query_low, 0, dtype=jnp.float32), jnp.sum(value_low, 0, dtype=jnp.float32)]
    )
    attn_in_grad = jnp.einsum("jre,jde->rd", stacked, w_qkv, preferred_element_type=jnp.float32)
    input_part, first_gain_grad = norm_back(first_normed, first_inv, norm_gains[0], attn_in_grad)
    input_low = (middle_grad + input_part).astype(jnp.bfloat16)
    big_terms = (qkv_grad, out_weight_grad, up_grad, down_grad)
    small_terms = (
        jnp.stack([first_gain_grad, second_gain_grad]),
        head_bias_grad,
        head_gain_grad,
        jnp.stack([first_bias_grad, last_bias_grad]),
        unit_bias_grad,
        unit_gain_grad,
    )
    return (big_terms, small_terms, input_low.reshape(seq_count, local_len, model_width))


def local(
    inputs,
    out_grad,
    picture_starts,
    segment_offsets,
    dilation_offsets,
    norm_gains,
    w_qkv,
    head_biases,
    head_gain,
    w_out,
    out_biases,
    w_up,
    unit_bias,
    unit_gain,
    w_down,
):
    local_seqs, local_len, model_width = inputs.shape
    tensor_count = lax.axis_size("tensor")
    mine = local_seqs // tensor_count
    first_seq = lax.axis_index("tensor") * mine
    block_in = lax.dynamic_slice_in_dim(inputs, first_seq, mine, 0)
    block_grad = lax.dynamic_slice_in_dim(out_grad, first_seq, mine, 0)
    starts = lax.dynamic_slice_in_dim(picture_starts, first_seq, mine, 0)
    seq_len = local_len * lax.axis_size("context")
    query_position = lax.axis_index("context") * local_len + jnp.arange(local_len, dtype=jnp.int32)
    key_position = jnp.arange(seq_len, dtype=jnp.int32)
    spans = jnp.array([seq_len * part // 8 for part in span_parts], jnp.int32)
    rates = jnp.array(dilation_rates, jnp.int32)
    segment_kept = segment_offsets % spans
    dilation_kept = dilation_offsets % rates
    offset_digits = jnp.concatenate(
        [segment_kept // 32, segment_kept % 32, dilation_kept], 1
    ).astype(jnp.bfloat16)
    f32 = jnp.float32
    (
        w_qkv_full,
        gains_full,
        out_bias_full,
        head_bias_full,
        head_gain_full,
        unit_bias_full,
        unit_gain_full,
        digits_full,
    ) = gather_packed(
        (
            (w_qkv, 1, 2),
            (norm_gains, 1, None),
            (out_biases, 1, None),
            (head_biases, 2, 1),
            (head_gain, 1, 0),
            (unit_bias, 1, 0),
            (unit_gain, 1, 0),
            (offset_digits, None, 0),
        )
    )
    patterns = len(span_parts)
    digits_full = digits_full.astype(jnp.int32)
    all_segments = digits_full[:, :patterns] * 32 + digits_full[:, patterns : 2 * patterns]
    all_dilations = digits_full[:, 2 * patterns :]
    tallied_total = pattern_total(
        query_position, key_position, all_segments, all_dilations, seq_len
    )
    weights = (
        w_qkv_full,
        gather_weight(w_out, 1, 0),
        gather_weight(w_up, 0, 1),
        gather_weight(w_down, 1, 0),
        gains_full.astype(f32),
        out_bias_full.astype(f32),
        head_bias_full.reshape(2, model_width).astype(f32),
        head_gain_full.reshape(model_width).astype(f32),
        unit_bias_full.reshape(-1).astype(f32),
        unit_gain_full.reshape(-1).astype(f32),
    )
    kept_state, layer_block = forward_pass(
        block_in, starts, tallied_total, weights, query_position, key_position
    )
    layer_out = pair_gather(layer_block, "tensor", 0)
    big_terms, small_terms, input_block = backward_pass(kept_state, block_grad, weights)
    input_grad = pair_gather(input_block, "tensor", 0)
    qkv_grad, out_weight_grad, up_grad, down_grad = big_terms
    down_share = scatter_weight(down_grad, 1, 0)
    up_share = scatter_weight(up_grad, 0, 1)
    out_share = scatter_weight(out_weight_grad, 1, 0)
    qkv_share = scatter_weight(qkv_grad, 1, 2)
    packed = jnp.concatenate([term.reshape(-1) for term in small_terms])
    packed = lax.psum(packed, ("shard", "context", "tensor"))
    unpacked = []
    offset = 0
    for term in small_terms:
        unpacked.append(packed[offset : offset + term.size].reshape(term.shape))
        offset += term.size
    gains_full, head_bias_full, head_gain_full, out_bias_full, unit_bias_full, unit_gain_full = unpacked
    heads = model_width // HD
    unit_rows = unit_bias_full.shape[0] // HD
    gains_share = block_of(gains_full, ((1, "shard"),))
    head_bias_share = block_of(head_bias_full.reshape(2, heads, HD), ((1, "tensor"), (2, "shard")))
    head_gain_share = block_of(head_gain_full.reshape(heads, HD), ((0, "tensor"), (1, "shard")))
    out_bias_share = block_of(out_bias_full, ((1, "shard"),))
    unit_bias_share = block_of(unit_bias_full.reshape(unit_rows, HD), ((0, "tensor"), (1, "shard")))
    unit_gain_share = block_of(unit_gain_full.reshape(unit_rows, HD), ((0, "tensor"), (1, "shard")))
    return (
        layer_out,
        input_grad,
        gains_share,
        qkv_share,
        head_bias_share,
        head_gain_share,
        out_share,
        out_bias_share,
        up_share,
        unit_bias_share,
        unit_gain_share,
        down_share,
    )


def solution(mesh):
    placed = (
        P("shard", "context", None),
        P("shard", "context", None),
        P("shard", None),
        P("tensor", None),
        P("tensor", None),
        P(None, "shard"),
        P(None, "shard", "tensor"),
        P(None, "tensor", "shard"),
        P("tensor", "shard"),
        P("tensor", "shard"),
        P(None, "shard"),
        P("shard", "tensor"),
        P("tensor", "shard"),
        P("tensor", "shard"),
        P("tensor", "shard"),
    )
    return jax.shard_map(
        local,
        mesh=mesh,
        in_specs=placed,
        out_specs=(
            P("shard", "context", None),
            P("shard", "context", None),
            P(None, "shard"),
            P(None, "shard", "tensor"),
            P(None, "tensor", "shard"),
            P("tensor", "shard"),
            P("tensor", "shard"),
            P(None, "shard"),
            P("shard", "tensor"),
            P("tensor", "shard"),
            P("tensor", "shard"),
            P("tensor", "shard"),
        ),
        check_vma=False,
    )
```

```python
from functools import partial

import jax
import jax.numpy as jnp
from jax import lax
from jax.sharding import PartitionSpec as P

HD = 64
FF = 3072
PIECE = 256


epsilon = 1e-05
span_parts = (1, 2, 4, 6, 8)
dilation_rates = (1, 2, 4, 6, 12)


def pattern_total(query_position, key_position, segmented_offsets, dilated_offsets, token_length):
    tallied_total = jnp.zeros(
        (segmented_offsets.shape[0], query_position.shape[0], key_position.shape[0]), jnp.float32
    )
    for item_number in range(len(span_parts)):
        segmented_span = token_length * span_parts[item_number] // 8
        dilated_stride = dilation_rates[item_number]
        seg_shift = (segmented_offsets[:, item_number] % segmented_span)[:, None, None]
        dilated_phase = (dilated_offsets[:, item_number] % dilated_stride)[:, None, None]
        query_lookup = query_position[None, :, None] + seg_shift
        key_lookup = key_position[None, None, :] + seg_shift
        merged_heads = (
            (query_lookup // segmented_span == key_lookup // segmented_span)
            & (query_lookup % dilated_stride == dilated_phase)
            & (key_lookup % dilated_stride == dilated_phase)
        )
        tallied_total = tallied_total + merged_heads.astype(jnp.float32)
    return tallied_total


def picture_index(starts, token_positions):
    marked = jnp.zeros((starts.shape[0], token_positions.shape[0]), jnp.int32)
    for piece_number in range(starts.shape[1]):
        begin_at = starts[:, piece_number][:, None]
        inside = (token_positions[None, :] >= begin_at) & (
            token_positions[None, :] < begin_at + PIECE
        )
        marked = marked + (piece_number + 1) * inside.astype(jnp.int32)
    return marked


def allowed_keys(query_pic, key_pic, query_position, key_position):
    causal_ok = key_position[None, None, :] <= query_position[None, :, None]
    same_piece = (query_pic[:, :, None] == key_pic[:, None, :]) & (query_pic[:, :, None] > 0)
    return (causal_ok | same_piece).astype(jnp.float32)


def outer_sum(left_rows, right_rows):
    return lax.dot_general(
        left_rows, right_rows, (((0,), (0,)), ((), ())), preferred_element_type=jnp.float32
    )


def back_dot(left_rows, weight_rows):
    return lax.dot_general(
        left_rows, weight_rows, (((1,), (1,)), ((), ())), preferred_element_type=jnp.float32
    )


def norm_rows(values, scale_row):
    mean_row = jnp.mean(values, -1, keepdims=True)
    centered = values - mean_row
    inv_std = lax.rsqrt(jnp.mean(centered * centered, -1, keepdims=True) + epsilon)
    normed = centered * inv_std
    return (normed, inv_std, normed * scale_row)


def norm_back(normed, inv_std, scale_row, grad_rows):
    scaled = grad_rows * scale_row
    mean_plain = jnp.mean(scaled, -1, keepdims=True)
    mean_cross = jnp.mean(scaled * normed, -1, keepdims=True)
    return (inv_std * (scaled - mean_plain - normed * mean_cross), jnp.sum(grad_rows * normed, 0))


def probabilities(query_heads, key_heads, mask_table):
    raw_scores = jnp.einsum(
        "sqhd,skhd->shqk", query_heads, key_heads, preferred_element_type=jnp.float32
    ) * HD ** (-0.5)
    masked = jnp.where(mask_table > 0, raw_scores, -1000000000.0)
    row_top = jnp.max(masked, -1, keepdims=True)
    exponent = mask_table * jnp.exp(masked - row_top)
    row_total = jnp.sum(exponent, -1, keepdims=True)
    return (exponent / row_total, row_top, row_total)


def assemble(stacked, shard_dim, tensor_dim):
    ns, nt = stacked.shape[0], stacked.shape[1]
    if shard_dim is None:
        stacked = stacked[:1]
    if tensor_dim is None:
        stacked = stacked[:, :1]
    local_shape = stacked.shape[2:]
    order = []
    for dim in range(len(local_shape)):
        if dim == shard_dim:
            order.append(0)
        if dim == tensor_dim:
            order.append(1)
        order.append(dim + 2)
    if shard_dim is None:
        order = [0] + order
    if tensor_dim is None:
        order = [1] + order
    moved = stacked.transpose(order)
    full_shape = list(local_shape)
    if shard_dim is not None:
        full_shape[shard_dim] *= ns
    if tensor_dim is not None:
        full_shape[tensor_dim] *= nt
    return moved.reshape(full_shape)


def gather_weight(local_block, shard_dim, tensor_dim):
    ns = lax.axis_size("shard")
    nt = lax.axis_size("tensor")
    stacked = lax.all_gather(local_block, ("shard", "tensor"), axis=0, tiled=False)
    return assemble(stacked.reshape((ns, nt) + local_block.shape), shard_dim, tensor_dim)


def gather_packed(blocks):
    ns = lax.axis_size("shard")
    nt = lax.axis_size("tensor")
    flat = jnp.concatenate([block.reshape(-1) for block, _, _ in blocks])
    padded = -flat.size % 2048
    flat = jnp.pad(flat, (0, padded)).reshape(-1, 128)
    stacked = lax.all_gather(flat, ("shard", "tensor"), axis=0, tiled=False).reshape(ns, nt, -1)
    pieces = []
    offset = 0
    for block, shard_dim, tensor_dim in blocks:
        part = stacked[:, :, offset : offset + block.size].reshape((ns, nt) + block.shape)
        pieces.append(assemble(part, shard_dim, tensor_dim))
        offset += block.size
    return pieces


def pair_gather(block, axis_name, dim):
    if lax.axis_size(axis_name) != 2:
        return lax.all_gather(block, axis_name, axis=dim, tiled=True)
    other = lax.ppermute(block, axis_name, perm=[(0, 1), (1, 0)])
    first = lax.axis_index(axis_name) == 0
    return jnp.where(
        first, jnp.concatenate([block, other], dim), jnp.concatenate([other, block], dim)
    )


def pair_reduce(full, axis_name, dim):
    if lax.axis_size(axis_name) != 2:
        return lax.psum_scatter(
            full.astype(jnp.bfloat16), axis_name, scatter_dimension=dim, tiled=True
        ).astype(jnp.float32)
    half = full.shape[dim] // 2
    me = lax.axis_index(axis_name)
    kept = lax.dynamic_slice_in_dim(full, me * half, half, dim)
    sent = lax.dynamic_slice_in_dim(full, (1 - me) * half, half, dim).astype(jnp.bfloat16)
    received = lax.ppermute(sent, axis_name, perm=[(0, 1), (1, 0)])
    return kept + received.astype(jnp.float32)


def pair_sum(share, axis_name):
    if lax.axis_size(axis_name) != 2:
        return lax.psum(share, axis_name).astype(jnp.float32)
    received = lax.ppermute(share, axis_name, perm=[(0, 1), (1, 0)])
    return share.astype(jnp.float32) + received.astype(jnp.float32)


def disassemble(full, shard_dim, tensor_dim):
    ns = lax.axis_size("shard")
    nt = lax.axis_size("tensor")
    split_shape = []
    positions = {}
    for dim, size in enumerate(full.shape):
        if dim == shard_dim:
            positions["s"] = len(split_shape)
            split_shape += [ns, size // ns]
        elif dim == tensor_dim:
            positions["t"] = len(split_shape)
            split_shape += [nt, size // nt]
        else:
            split_shape.append(size)
    pieces = full.reshape(split_shape)
    lead = [positions[key] for key in ("s", "t") if key in positions]
    rest = [d for d in range(len(split_shape)) if d not in lead]
    pieces = pieces.transpose(lead + rest)
    if "s" not in positions:
        pieces = jnp.broadcast_to(pieces[None], (ns,) + pieces.shape)
    if "t" not in positions:
        pieces = jnp.broadcast_to(pieces[:, None], (ns, nt) + pieces.shape[1:])
    return pieces.reshape(ns * nt, -1)


def pack_rows(terms):
    rows = jnp.concatenate(
        [disassemble(full.astype(jnp.bfloat16), shard_dim, tensor_dim) for full, shard_dim, tensor_dim in terms],
        1,
    )
    width = rows.shape[1]
    return jnp.pad(rows, ((0, 0), (0, -width % 1024))).reshape(rows.shape[0], -1, 128)


def scatter_rows(rows):
    return lax.psum_scatter(rows, ("shard", "tensor"), scatter_dimension=0, tiled=False)


def unpack_share(share, terms):
    total = pair_sum(share, "context").reshape(-1)
    pieces = []
    offset = 0
    ns = lax.axis_size("shard")
    nt = lax.axis_size("tensor")
    for full, shard_dim, tensor_dim in terms:
        local_shape = list(full.shape)
        if shard_dim is not None:
            local_shape[shard_dim] //= ns
        if tensor_dim is not None:
            local_shape[tensor_dim] //= nt
        count = 1
        for size in local_shape:
            count *= size
        pieces.append(total[offset : offset + count].reshape(local_shape))
        offset += count
    return pieces


def forward_pass(block_in, starts, tallied_total, weights, query_position, key_position):
    w_qkv, w_out, w_up, w_down, norm_gains, out_biases, head_biases, head_gain, unit_bias, unit_gain = weights
    seq_count, local_len, model_width = block_in.shape
    seq_len = key_position.shape[0]
    row_count = seq_count * local_len
    heads = model_width // HD
    flattened_input = block_in.reshape(row_count, model_width).astype(jnp.float32)
    first_normed, first_inv, first_out = norm_rows(flattened_input, norm_gains[0])
    attn_in = first_out.astype(jnp.bfloat16)
    projected = jnp.einsum("rd,jde->jre", attn_in, w_qkv, preferred_element_type=jnp.float32)
    query_matrix = (projected[0] + head_biases[0]).astype(jnp.bfloat16)
    keys_local = projected[1].astype(jnp.bfloat16).reshape(seq_count, local_len, model_width)
    values_local = (projected[2] + head_biases[1]).astype(jnp.bfloat16).reshape(
        seq_count, local_len, model_width
    )
    key_all = pair_gather(keys_local, "context", 1)
    value_all = pair_gather(values_local, "context", 1)
    query_pic = picture_index(starts, query_position)
    key_pic = picture_index(starts, key_position)
    mask_table = (
        allowed_keys(query_pic, key_pic, query_position, key_position)[:, None] * tallied_total[None]
    )
    query_heads = query_matrix.reshape(seq_count, local_len, heads, HD)
    key_heads = key_all.reshape(seq_count, seq_len, heads, HD)
    value_heads = value_all.reshape(seq_count, seq_len, heads, HD)
    weights_soft = probabilities(query_heads, key_heads, mask_table)[0]
    attended = jnp.einsum(
        "shqk,skhd->sqhd",
        weights_soft.astype(jnp.bfloat16),
        value_heads,
        preferred_element_type=jnp.float32,
    ).reshape(row_count, model_width)
    sub_normed, sub_inv, sub_out = norm_rows(attended, head_gain)
    sub_in = sub_out.astype(jnp.bfloat16)
    middle = flattened_input + (
        jnp.dot(sub_in, w_out, preferred_element_type=jnp.float32) + out_biases[0]
    )
    second_normed, second_inv, second_out = norm_rows(middle, norm_gains[1])
    ffn_in = second_out.astype(jnp.bfloat16)
    hidden = jnp.dot(ffn_in, w_up, preferred_element_type=jnp.float32) + unit_bias
    activated = jax.nn.gelu(hidden, approximate=True)
    unit_normed, unit_inv, unit_out = norm_rows(activated, unit_gain)
    ffn_mid = unit_out.astype(jnp.bfloat16)
    layer_out = (
        middle + (jnp.dot(ffn_mid, w_down, preferred_element_type=jnp.float32) + out_biases[1])
    ).astype(jnp.bfloat16)
    kept_state = (
        attn_in,
        first_normed,
        first_inv,
        query_heads,
        key_heads,
        value_heads,
        mask_table,
        sub_normed,
        sub_inv,
        sub_in,
        second_normed,
        second_inv,
        ffn_in,
        hidden,
        unit_normed,
        unit_inv,
        ffn_mid,
    )
    return (kept_state, layer_out.reshape(seq_count, local_len, model_width))


def backward_pass(kept_state, block_grad, weights):
    w_qkv, w_out, w_up, w_down, norm_gains, out_biases, head_biases, head_gain, unit_bias, unit_gain = weights
    (
        attn_in,
        first_normed,
        first_inv,
        query_heads,
        key_heads,
        value_heads,
        mask_table,
        sub_normed,
        sub_inv,
        sub_in,
        second_normed,
        second_inv,
        ffn_in,
        hidden,
        unit_normed,
        unit_inv,
        ffn_mid,
    ) = kept_state
    seq_count, local_len, model_width = block_grad.shape
    row_count = seq_count * local_len
    seq_len = key_heads.shape[1]
    grad_low = block_grad.reshape(row_count, model_width)
    grad_full = grad_low.astype(jnp.float32)
    down_grad = outer_sum(ffn_mid, grad_low)
    last_bias_grad = jnp.sum(grad_full, 0)
    unit_grad = back_dot(grad_low, w_down)
    activated_grad, unit_gain_grad = norm_back(unit_normed, unit_inv, unit_gain, unit_grad)
    gelu_value, gelu_pull = jax.vjp(partial(jax.nn.gelu, approximate=True), hidden)
    hidden_low = gelu_pull(activated_grad)[0].astype(jnp.bfloat16)
    up_grad = outer_sum(ffn_in, hidden_low)
    unit_bias_grad = jnp.sum(hidden_low, 0, dtype=jnp.float32)
    ffn_in_grad = back_dot(hidden_low, w_up)
    middle_part, second_gain_grad = norm_back(second_normed, second_inv, norm_gains[1], ffn_in_grad)
    middle_grad = grad_full + middle_part
    middle_low = middle_grad.astype(jnp.bfloat16)
    out_weight_grad = outer_sum(sub_in, middle_low)
    first_bias_grad = jnp.sum(middle_low, 0, dtype=jnp.float32)
    sub_grad = back_dot(middle_low, w_out)
    attended_grad, head_gain_grad = norm_back(sub_normed, sub_inv, head_gain, sub_grad)
    attended_low = attended_grad.astype(jnp.bfloat16)
    early_terms = ((down_grad, 1, 0), (up_grad, 0, 1))
    middle_terms = ((out_weight_grad, 1, 0),)
    early_rows, middle_rows, attended_low = lax.optimization_barrier(
        (pack_rows(early_terms), pack_rows(middle_terms), attended_low)
    )
    early_share = scatter_rows(early_rows)
    middle_share = scatter_rows(middle_rows)
    heads = query_heads.shape[2]
    weights_soft, row_top, row_total = probabilities(query_heads, key_heads, mask_table)
    grad_heads = attended_low.reshape(seq_count, local_len, heads, HD)
    soft_grad = jnp.einsum(
        "sqhd,skhd->shqk", grad_heads, value_heads, preferred_element_type=jnp.float32
    )
    inner_sum = jnp.sum(weights_soft * soft_grad, -1, keepdims=True)
    score_low = (weights_soft * (soft_grad - inner_sum)).astype(jnp.bfloat16)
    root_scale = HD ** (-0.5)
    query_low = (
        (
            jnp.einsum("shqk,skhd->sqhd", score_low, key_heads, preferred_element_type=jnp.float32)
            * root_scale
        )
        .astype(jnp.bfloat16)
        .reshape(row_count, -1)
    )
    key_part = (
        jnp.einsum("shqk,sqhd->skhd", score_low, query_heads, preferred_element_type=jnp.float32)
        * root_scale
    )
    value_part = jnp.einsum(
        "shqk,sqhd->skhd",
        weights_soft.astype(jnp.bfloat16),
        grad_heads,
        preferred_element_type=jnp.float32,
    )
    key_low = (
        pair_reduce(key_part.reshape(seq_count, seq_len, -1), "context", 1)
        .astype(jnp.bfloat16)
        .reshape(row_count, -1)
    )
    value_low = (
        pair_reduce(value_part.reshape(seq_count, seq_len, -1), "context", 1)
        .astype(jnp.bfloat16)
        .reshape(row_count, -1)
    )
    stacked = jnp.stack([query_low, key_low, value_low])
    early_share, stacked = lax.optimization_barrier((early_share, stacked))
    qkv_grad = jnp.einsum("rd,jre->jde", attn_in, stacked, preferred_element_type=jnp.float32)
    head_bias_grad = jnp.stack(
        [jnp.sum(query_low, 0, dtype=jnp.float32), jnp.sum(value_low, 0, dtype=jnp.float32)]
    )
    attn_in_grad = jnp.einsum("jre,jde->rd", stacked, w_qkv, preferred_element_type=jnp.float32)
    input_part, first_gain_grad = norm_back(first_normed, first_inv, norm_gains[0], attn_in_grad)
    input_low = (middle_grad + input_part).astype(jnp.bfloat16)
    heads = model_width // HD
    unit_rows = unit_bias_grad.shape[0] // HD
    late_terms = (
        (qkv_grad, 1, 2),
        (jnp.stack([first_gain_grad, second_gain_grad]), 1, None),
        (jnp.stack([first_bias_grad, last_bias_grad]), 1, None),
        (head_bias_grad.reshape(2, heads, HD), 2, 1),
        (head_gain_grad.reshape(heads, HD), 1, 0),
        (unit_bias_grad.reshape(unit_rows, HD), 1, 0),
        (unit_gain_grad.reshape(unit_rows, HD), 1, 0),
    )
    late_share = scatter_rows(pack_rows(late_terms))
    grad_shares = (
        unpack_share(early_share, early_terms)
        + unpack_share(middle_share, middle_terms)
        + unpack_share(late_share, late_terms)
    )
    return (grad_shares, input_low.reshape(seq_count, local_len, model_width))


def local(
    inputs,
    out_grad,
    picture_starts,
    segment_offsets,
    dilation_offsets,
    norm_gains,
    w_qkv,
    head_biases,
    head_gain,
    w_out,
    out_biases,
    w_up,
    unit_bias,
    unit_gain,
    w_down,
):
    local_seqs, local_len, model_width = inputs.shape
    tensor_count = lax.axis_size("tensor")
    mine = local_seqs // tensor_count
    first_seq = lax.axis_index("tensor") * mine
    block_in = lax.dynamic_slice_in_dim(inputs, first_seq, mine, 0)
    block_grad = lax.dynamic_slice_in_dim(out_grad, first_seq, mine, 0)
    starts = lax.dynamic_slice_in_dim(picture_starts, first_seq, mine, 0)
    seq_len = local_len * lax.axis_size("context")
    query_position = lax.axis_index("context") * local_len + jnp.arange(local_len, dtype=jnp.int32)
    key_position = jnp.arange(seq_len, dtype=jnp.int32)
    spans = jnp.array([seq_len * part // 8 for part in span_parts], jnp.int32)
    rates = jnp.array(dilation_rates, jnp.int32)
    segment_kept = segment_offsets % spans
    dilation_kept = dilation_offsets % rates
    offset_digits = jnp.concatenate(
        [segment_kept // 32, segment_kept % 32, dilation_kept], 1
    ).astype(jnp.bfloat16)
    f32 = jnp.float32
    (
        w_qkv_full,
        gains_full,
        out_bias_full,
        head_bias_full,
        head_gain_full,
        unit_bias_full,
        unit_gain_full,
        digits_full,
    ) = gather_packed(
        (
            (w_qkv, 1, 2),
            (norm_gains, 1, None),
            (out_biases, 1, None),
            (head_biases, 2, 1),
            (head_gain, 1, 0),
            (unit_bias, 1, 0),
            (unit_gain, 1, 0),
            (offset_digits, None, 0),
        )
    )
    patterns = len(span_parts)
    digits_full = digits_full.astype(jnp.int32)
    all_segments = digits_full[:, :patterns] * 32 + digits_full[:, patterns : 2 * patterns]
    all_dilations = digits_full[:, 2 * patterns :]
    tallied_total = pattern_total(
        query_position, key_position, all_segments, all_dilations, seq_len
    )
    w_out, w_up, w_down, w_qkv_full = lax.optimization_barrier((w_out, w_up, w_down, w_qkv_full))
    weights = (
        w_qkv_full,
        gather_weight(w_out, 1, 0),
        gather_weight(w_up, 0, 1),
        gather_weight(w_down, 1, 0),
        gains_full.astype(f32),
        out_bias_full.astype(f32),
        head_bias_full.reshape(2, model_width).astype(f32),
        head_gain_full.reshape(model_width).astype(f32),
        unit_bias_full.reshape(-1).astype(f32),
        unit_gain_full.reshape(-1).astype(f32),
    )
    kept_state, layer_block = forward_pass(
        block_in, starts, tallied_total, weights, query_position, key_position
    )
    layer_out = pair_gather(layer_block, "tensor", 0)
    grad_shares, input_block = backward_pass(kept_state, block_grad, weights)
    input_grad = pair_gather(input_block, "tensor", 0)
    (
        down_share,
        up_share,
        out_share,
        qkv_share,
        gains_share,
        out_bias_share,
        head_bias_share,
        head_gain_share,
        unit_bias_share,
        unit_gain_share,
    ) = grad_shares
    return (
        layer_out,
        input_grad,
        gains_share,
        qkv_share,
        head_bias_share,
        head_gain_share,
        out_share,
        out_bias_share,
        up_share,
        unit_bias_share,
        unit_gain_share,
        down_share,
    )


def solution(mesh):
    placed = (
        P("shard", "context", None),
        P("shard", "context", None),
        P("shard", None),
        P("tensor", None),
        P("tensor", None),
        P(None, "shard"),
        P(None, "shard", "tensor"),
        P(None, "tensor", "shard"),
        P("tensor", "shard"),
        P("tensor", "shard"),
        P(None, "shard"),
        P("shard", "tensor"),
        P("tensor", "shard"),
        P("tensor", "shard"),
        P("tensor", "shard"),
    )
    return jax.shard_map(
        local,
        mesh=mesh,
        in_specs=placed,
        out_specs=(
            P("shard", "context", None),
            P("shard", "context", None),
            P(None, "shard"),
            P(None, "shard", "tensor"),
            P(None, "tensor", "shard"),
            P("tensor", "shard"),
            P("tensor", "shard"),
            P(None, "shard"),
            P("shard", "tensor"),
            P("tensor", "shard"),
            P("tensor", "shard"),
            P("tensor", "shard"),
        ),
        check_vma=False,
    )
```

```python
from functools import partial

import jax
import jax.numpy as jnp
from jax import lax
from jax.experimental import pallas as pl
from jax.experimental.pallas import tpu as pltpu
from jax.sharding import PartitionSpec as P

HD = 64
FF = 3072
PIECE = 256


epsilon = 1e-05
span_parts = (1, 2, 4, 6, 8)
dilation_rates = (1, 2, 4, 6, 12)


def pattern_total(query_position, key_position, segmented_offsets, dilated_offsets, token_length):
    tallied_total = jnp.zeros(
        (segmented_offsets.shape[0], query_position.shape[0], key_position.shape[0]), jnp.float32
    )
    for item_number in range(len(span_parts)):
        segmented_span = token_length * span_parts[item_number] // 8
        dilated_stride = dilation_rates[item_number]
        seg_shift = (segmented_offsets[:, item_number] % segmented_span)[:, None, None]
        dilated_phase = (dilated_offsets[:, item_number] % dilated_stride)[:, None, None]
        query_lookup = query_position[None, :, None] + seg_shift
        key_lookup = key_position[None, None, :] + seg_shift
        merged_heads = (
            (query_lookup // segmented_span == key_lookup // segmented_span)
            & (query_lookup % dilated_stride == dilated_phase)
            & (key_lookup % dilated_stride == dilated_phase)
        )
        tallied_total = tallied_total + merged_heads.astype(jnp.float32)
    return tallied_total


def picture_index(starts, token_positions):
    marked = jnp.zeros((starts.shape[0], token_positions.shape[0]), jnp.int32)
    for piece_number in range(starts.shape[1]):
        begin_at = starts[:, piece_number][:, None]
        inside = (token_positions[None, :] >= begin_at) & (
            token_positions[None, :] < begin_at + PIECE
        )
        marked = marked + (piece_number + 1) * inside.astype(jnp.int32)
    return marked


def allowed_keys(query_pic, key_pic, query_position, key_position):
    causal_ok = key_position[None, None, :] <= query_position[None, :, None]
    same_piece = (query_pic[:, :, None] == key_pic[:, None, :]) & (query_pic[:, :, None] > 0)
    return (causal_ok | same_piece).astype(jnp.float32)


def outer_sum(left_rows, right_rows):
    return lax.dot_general(
        left_rows, right_rows, (((0,), (0,)), ((), ())), preferred_element_type=jnp.float32
    )


def back_dot(left_rows, weight_rows):
    return lax.dot_general(
        left_rows, weight_rows, (((1,), (1,)), ((), ())), preferred_element_type=jnp.float32
    )


def norm_rows(values, scale_row):
    mean_row = jnp.mean(values, -1, keepdims=True)
    centered = values - mean_row
    inv_std = lax.rsqrt(jnp.mean(centered * centered, -1, keepdims=True) + epsilon)
    normed = centered * inv_std
    return (normed, inv_std, normed * scale_row)


def norm_back(normed, inv_std, scale_row, grad_rows):
    scaled = grad_rows * scale_row
    mean_plain = jnp.mean(scaled, -1, keepdims=True)
    mean_cross = jnp.mean(scaled * normed, -1, keepdims=True)
    return (inv_std * (scaled - mean_plain - normed * mean_cross), jnp.sum(grad_rows * normed, 0))


def probabilities(query_heads, key_heads, mask_table):
    raw_scores = jnp.einsum(
        "sqhd,skhd->shqk", query_heads, key_heads, preferred_element_type=jnp.float32
    ) * HD ** (-0.5)
    masked = jnp.where(mask_table > 0, raw_scores, -1000000000.0)
    row_top = jnp.max(masked, -1, keepdims=True)
    exponent = mask_table * jnp.exp(masked - row_top)
    row_total = jnp.sum(exponent, -1, keepdims=True)
    return (exponent / row_total, row_top, row_total)


SCALE = HD ** (-0.5)
HIDDEN = -1000000000.0
PAIR = 2
CODE_WIDTH = 8


def pair_masks(patq_ref, patk_ref, pcq_ref, pck_ref):
    first_q = patq_ref[0]
    first_k = patk_ref[0]
    row = first_q[:, 5:6]
    col = first_k[5:6, :]
    piece_q = pcq_ref[0][:, 0:1]
    piece_k = pck_ref[0][0:1, :]
    allowed = (col <= row) | (piece_q == piece_k)
    masks = []
    for head in range(PAIR):
        codes_q = patq_ref[head]
        codes_k = patk_ref[head]
        tally = (codes_q[:, 0:1] == codes_k[0:1, :]).astype(jnp.float32)
        for pattern in range(1, len(span_parts)):
            tally = tally + (
                codes_q[:, pattern : pattern + 1] == codes_k[pattern : pattern + 1, :]
            ).astype(jnp.float32)
        masks.append(jnp.where(allowed, tally, 0.0))
    return masks


def soft_rows(query_part, key_block, mask):
    scores = (
        lax.dot_general(
            query_part, key_block, (((1,), (1,)), ((), ())), preferred_element_type=jnp.float32
        )
        * SCALE
    )
    masked = jnp.where(mask > 0, scores, HIDDEN)
    top = jnp.max(masked, axis=1, keepdims=True)
    exponent = mask * jnp.exp(masked - top)
    return exponent / jnp.sum(exponent, axis=1, keepdims=True)


def attention_fwd_kernel(q_ref, k_ref, v_ref, patq_ref, patk_ref, pcq_ref, pck_ref, o_ref):
    query = q_ref[0]
    key_block = k_ref[0]
    value_block = v_ref[0]
    first = lax.broadcasted_iota(jnp.int32, query.shape, 1) < HD
    masks = pair_masks(patq_ref, patk_ref, pcq_ref, pck_ref)
    result = None
    for head in range(PAIR):
        keep = first if head == 0 else jnp.logical_not(first)
        query_part = jnp.where(keep, query, jnp.zeros_like(query))
        probs = soft_rows(query_part, key_block, masks[head])
        mixed = jnp.dot(
            probs.astype(jnp.bfloat16), value_block, preferred_element_type=jnp.float32
        )
        result = mixed if result is None else jnp.where(first, result, mixed)
    o_ref[0] = result


def attention_bwd_kernel(
    q_ref, k_ref, v_ref, do_ref, patq_ref, patk_ref, pcq_ref, pck_ref, dq_ref, dk_ref, dv_ref
):
    @pl.when(pl.program_id(2) == 0)
    def _():
        dk_ref[...] = jnp.zeros_like(dk_ref)
        dv_ref[...] = jnp.zeros_like(dv_ref)

    query = q_ref[0]
    key_block = k_ref[0]
    value_block = v_ref[0]
    grad_out = do_ref[0]
    first = lax.broadcasted_iota(jnp.int32, query.shape, 1) < HD
    masks = pair_masks(patq_ref, patk_ref, pcq_ref, pck_ref)
    query_grad = None
    key_grad = dk_ref[0]
    value_grad = dv_ref[0]
    for head in range(PAIR):
        keep = first if head == 0 else jnp.logical_not(first)
        query_part = jnp.where(keep, query, jnp.zeros_like(query))
        grad_part = jnp.where(keep, grad_out, jnp.zeros_like(grad_out))
        probs = soft_rows(query_part, key_block, masks[head])
        prob_grad = lax.dot_general(
            grad_part, value_block, (((1,), (1,)), ((), ())), preferred_element_type=jnp.float32
        )
        inner = jnp.sum(probs * prob_grad, axis=1, keepdims=True)
        score_low = (probs * (prob_grad - inner)).astype(jnp.bfloat16)
        part = jnp.dot(score_low, key_block, preferred_element_type=jnp.float32)
        query_grad = part if query_grad is None else jnp.where(first, query_grad, part)
        key_grad = key_grad + SCALE * lax.dot_general(
            score_low, query_part, (((0,), (0,)), ((), ())), preferred_element_type=jnp.float32
        )
        value_grad = value_grad + lax.dot_general(
            probs.astype(jnp.bfloat16),
            grad_part,
            (((0,), (0,)), ((), ())),
            preferred_element_type=jnp.float32,
        )
    dq_ref[0] = (query_grad * SCALE).astype(jnp.bfloat16)
    dk_ref[0] = key_grad
    dv_ref[0] = value_grad


def attention_specs(seq_count, local_len, seq_len, block_q):
    lanes = PAIR * HD
    query_spec = pl.BlockSpec((1, block_q, lanes), lambda s, g, b: (s, b, g))
    key_spec = pl.BlockSpec((1, seq_len, lanes), lambda s, g, b: (s, 0, g))
    patq_spec = pl.BlockSpec((PAIR, block_q, CODE_WIDTH), lambda s, g, b: (g, b, 0))
    patk_spec = pl.BlockSpec((PAIR, CODE_WIDTH, seq_len), lambda s, g, b: (g, 0, 0))
    pcq_spec = pl.BlockSpec((1, block_q, CODE_WIDTH), lambda s, g, b: (s, b, 0))
    pck_spec = pl.BlockSpec((1, CODE_WIDTH, seq_len), lambda s, g, b: (s, 0, 0))
    return query_spec, key_spec, patq_spec, patk_spec, pcq_spec, pck_spec


def attention_forward(query, keys, values, codes):
    seq_count, local_len, width = query.shape
    seq_len = keys.shape[1]
    block_q = min(256, local_len)
    grid = (seq_count, width // (PAIR * HD), local_len // block_q)
    query_spec, key_spec, patq_spec, patk_spec, pcq_spec, pck_spec = attention_specs(
        seq_count, local_len, seq_len, block_q
    )
    flops = 8 * seq_count * local_len * seq_len * width
    return pl.pallas_call(
        attention_fwd_kernel,
        grid=grid,
        in_specs=[query_spec, key_spec, key_spec, patq_spec, patk_spec, pcq_spec, pck_spec],
        out_specs=query_spec,
        out_shape=jax.ShapeDtypeStruct((seq_count, local_len, width), jnp.float32),
        compiler_params=pltpu.CompilerParams(
            dimension_semantics=("parallel", "parallel", "arbitrary"),
            vmem_limit_bytes=48 * 1024 * 1024,
        ),
        cost_estimate=pl.CostEstimate(
            flops=flops,
            transcendentals=seq_count * local_len * seq_len * width // HD,
            bytes_accessed=2 * query.size + 2 * keys.size * 2 * (local_len // block_q) + 4 * query.size,
        ),
    )(query, keys, values, *codes)


def attention_backward(query, keys, values, grad_out, codes):
    seq_count, local_len, width = query.shape
    seq_len = keys.shape[1]
    block_q = min(256, local_len)
    grid = (seq_count, width // (PAIR * HD), local_len // block_q)
    query_spec, key_spec, patq_spec, patk_spec, pcq_spec, pck_spec = attention_specs(
        seq_count, local_len, seq_len, block_q
    )
    flops = 20 * seq_count * local_len * seq_len * width
    return pl.pallas_call(
        attention_bwd_kernel,
        grid=grid,
        in_specs=[
            query_spec,
            key_spec,
            key_spec,
            query_spec,
            patq_spec,
            patk_spec,
            pcq_spec,
            pck_spec,
        ],
        out_specs=[query_spec, key_spec, key_spec],
        out_shape=[
            jax.ShapeDtypeStruct((seq_count, local_len, width), jnp.bfloat16),
            jax.ShapeDtypeStruct((seq_count, seq_len, width), jnp.float32),
            jax.ShapeDtypeStruct((seq_count, seq_len, width), jnp.float32),
        ],
        compiler_params=pltpu.CompilerParams(
            dimension_semantics=("parallel", "parallel", "arbitrary"),
            vmem_limit_bytes=48 * 1024 * 1024,
        ),
        cost_estimate=pl.CostEstimate(
            flops=flops,
            transcendentals=seq_count * local_len * seq_len * width // HD,
            bytes_accessed=4 * query.size + 2 * keys.size * 2 * (local_len // block_q) + 16 * keys.size,
        ),
    )(query, keys, values, grad_out, *codes)


def mask_codes(starts, query_position, key_position, segment_offsets, dilation_offsets, seq_len):
    heads = segment_offsets.shape[0]
    query_codes = []
    key_codes = []
    for pattern in range(len(span_parts)):
        span = seq_len * span_parts[pattern] // 8
        rate = dilation_rates[pattern]
        shift = (segment_offsets[:, pattern] % span)[:, None]
        phase = (dilation_offsets[:, pattern] % rate)[:, None]
        query_at = query_position[None, :] + shift
        key_at = key_position[None, :] + shift
        query_codes.append(jnp.where(query_at % rate == phase, query_at // span, -1))
        key_codes.append(jnp.where(key_at % rate == phase, key_at // span, -2))
    patterns = len(span_parts)
    query_codes.append(jnp.broadcast_to(query_position[None, :], (heads, query_position.shape[0])))
    key_codes.append(jnp.broadcast_to(key_position[None, :], (heads, key_position.shape[0])))
    filler = CODE_WIDTH - patterns - 1
    query_codes += [jnp.zeros((heads, query_position.shape[0]), jnp.int32)] * filler
    key_codes += [jnp.zeros((heads, key_position.shape[0]), jnp.int32)] * filler
    patq = jnp.stack(query_codes, 2).astype(jnp.int32)
    patk = jnp.stack(key_codes, 1).astype(jnp.int32)
    query_pic = picture_index(starts, query_position)
    key_pic = picture_index(starts, key_position)
    pcq = jnp.where(query_pic > 0, query_pic, -1)[:, :, None]
    pcq = jnp.pad(pcq, ((0, 0), (0, 0), (0, CODE_WIDTH - 1)))
    pck = jnp.where(key_pic > 0, key_pic, -2)[:, None, :]
    pck = jnp.pad(pck, ((0, 0), (0, CODE_WIDTH - 1), (0, 0)))
    return (patq, patk, pcq.astype(jnp.int32), pck.astype(jnp.int32))


def assemble(stacked, shard_dim, tensor_dim):
    ns, nt = stacked.shape[0], stacked.shape[1]
    if shard_dim is None:
        stacked = stacked[:1]
    if tensor_dim is None:
        stacked = stacked[:, :1]
    local_shape = stacked.shape[2:]
    order = []
    for dim in range(len(local_shape)):
        if dim == shard_dim:
            order.append(0)
        if dim == tensor_dim:
            order.append(1)
        order.append(dim + 2)
    if shard_dim is None:
        order = [0] + order
    if tensor_dim is None:
        order = [1] + order
    moved = stacked.transpose(order)
    full_shape = list(local_shape)
    if shard_dim is not None:
        full_shape[shard_dim] *= ns
    if tensor_dim is not None:
        full_shape[tensor_dim] *= nt
    return moved.reshape(full_shape)


def gather_weight(local_block, shard_dim, tensor_dim):
    ns = lax.axis_size("shard")
    nt = lax.axis_size("tensor")
    stacked = lax.all_gather(local_block, ("shard", "tensor"), axis=0, tiled=False)
    return assemble(stacked.reshape((ns, nt) + local_block.shape), shard_dim, tensor_dim)


def gather_packed(blocks):
    ns = lax.axis_size("shard")
    nt = lax.axis_size("tensor")
    flat = jnp.concatenate([block.reshape(-1) for block, _, _ in blocks])
    padded = -flat.size % 2048
    flat = jnp.pad(flat, (0, padded)).reshape(-1, 128)
    stacked = lax.all_gather(flat, ("shard", "tensor"), axis=0, tiled=False).reshape(ns, nt, -1)
    pieces = []
    offset = 0
    for block, shard_dim, tensor_dim in blocks:
        part = stacked[:, :, offset : offset + block.size].reshape((ns, nt) + block.shape)
        pieces.append(assemble(part, shard_dim, tensor_dim))
        offset += block.size
    return pieces


def pair_gather(block, axis_name, dim):
    if lax.axis_size(axis_name) != 2:
        return lax.all_gather(block, axis_name, axis=dim, tiled=True)
    other = lax.ppermute(block, axis_name, perm=[(0, 1), (1, 0)])
    first = lax.axis_index(axis_name) == 0
    return jnp.where(
        first, jnp.concatenate([block, other], dim), jnp.concatenate([other, block], dim)
    )


def pair_reduce(full, axis_name, dim):
    if lax.axis_size(axis_name) != 2:
        return lax.psum_scatter(
            full.astype(jnp.bfloat16), axis_name, scatter_dimension=dim, tiled=True
        ).astype(jnp.float32)
    half = full.shape[dim] // 2
    me = lax.axis_index(axis_name)
    kept = lax.dynamic_slice_in_dim(full, me * half, half, dim)
    sent = lax.dynamic_slice_in_dim(full, (1 - me) * half, half, dim).astype(jnp.bfloat16)
    received = lax.ppermute(sent, axis_name, perm=[(0, 1), (1, 0)])
    return kept + received.astype(jnp.float32)


def pair_sum(share, axis_name):
    if lax.axis_size(axis_name) != 2:
        return lax.psum(share, axis_name).astype(jnp.float32)
    received = lax.ppermute(share, axis_name, perm=[(0, 1), (1, 0)])
    return share.astype(jnp.float32) + received.astype(jnp.float32)


def disassemble(full, shard_dim, tensor_dim):
    ns = lax.axis_size("shard")
    nt = lax.axis_size("tensor")
    split_shape = []
    positions = {}
    for dim, size in enumerate(full.shape):
        if dim == shard_dim:
            positions["s"] = len(split_shape)
            split_shape += [ns, size // ns]
        elif dim == tensor_dim:
            positions["t"] = len(split_shape)
            split_shape += [nt, size // nt]
        else:
            split_shape.append(size)
    pieces = full.reshape(split_shape)
    lead = [positions[key] for key in ("s", "t") if key in positions]
    rest = [d for d in range(len(split_shape)) if d not in lead]
    pieces = pieces.transpose(lead + rest)
    if "s" not in positions:
        pieces = jnp.broadcast_to(pieces[None], (ns,) + pieces.shape)
    if "t" not in positions:
        pieces = jnp.broadcast_to(pieces[:, None], (ns, nt) + pieces.shape[1:])
    return pieces.reshape(ns * nt, -1)


def pack_rows(terms):
    rows = jnp.concatenate(
        [disassemble(full.astype(jnp.bfloat16), shard_dim, tensor_dim) for full, shard_dim, tensor_dim in terms],
        1,
    )
    width = rows.shape[1]
    return jnp.pad(rows, ((0, 0), (0, -width % 1024))).reshape(rows.shape[0], -1, 128)


def scatter_rows(rows):
    return lax.psum_scatter(rows, ("shard", "tensor"), scatter_dimension=0, tiled=False)


def unpack_share(share, terms):
    total = pair_sum(share, "context").reshape(-1)
    pieces = []
    offset = 0
    ns = lax.axis_size("shard")
    nt = lax.axis_size("tensor")
    for full, shard_dim, tensor_dim in terms:
        local_shape = list(full.shape)
        if shard_dim is not None:
            local_shape[shard_dim] //= ns
        if tensor_dim is not None:
            local_shape[tensor_dim] //= nt
        count = 1
        for size in local_shape:
            count *= size
        pieces.append(total[offset : offset + count].reshape(local_shape))
        offset += count
    return pieces


def forward_pass(block_in, codes, weights):
    w_qkv, w_out, w_up, w_down, norm_gains, out_biases, head_biases, head_gain, unit_bias, unit_gain = weights
    seq_count, local_len, model_width = block_in.shape
    row_count = seq_count * local_len
    flattened_input = block_in.reshape(row_count, model_width).astype(jnp.float32)
    first_normed, first_inv, first_out = norm_rows(flattened_input, norm_gains[0])
    attn_in = first_out.astype(jnp.bfloat16)
    projected = jnp.einsum("rd,jde->jre", attn_in, w_qkv, preferred_element_type=jnp.float32)
    query_matrix = (projected[0] + head_biases[0]).astype(jnp.bfloat16)
    keys_local = projected[1].astype(jnp.bfloat16).reshape(seq_count, local_len, model_width)
    values_local = (projected[2] + head_biases[1]).astype(jnp.bfloat16).reshape(
        seq_count, local_len, model_width
    )
    key_all = pair_gather(keys_local, "context", 1)
    value_all = pair_gather(values_local, "context", 1)
    attended = attention_forward(
        query_matrix.reshape(seq_count, local_len, model_width), key_all, value_all, codes
    ).reshape(row_count, model_width)
    sub_normed, sub_inv, sub_out = norm_rows(attended, head_gain)
    sub_in = sub_out.astype(jnp.bfloat16)
    middle = flattened_input + (
        jnp.dot(sub_in, w_out, preferred_element_type=jnp.float32) + out_biases[0]
    )
    second_normed, second_inv, second_out = norm_rows(middle, norm_gains[1])
    ffn_in = second_out.astype(jnp.bfloat16)
    hidden = jnp.dot(ffn_in, w_up, preferred_element_type=jnp.float32) + unit_bias
    activated = jax.nn.gelu(hidden, approximate=True)
    unit_normed, unit_inv, unit_out = norm_rows(activated, unit_gain)
    ffn_mid = unit_out.astype(jnp.bfloat16)
    layer_out = (
        middle + (jnp.dot(ffn_mid, w_down, preferred_element_type=jnp.float32) + out_biases[1])
    ).astype(jnp.bfloat16)
    kept_state = (
        attn_in,
        first_normed,
        first_inv,
        query_matrix,
        key_all,
        value_all,
        codes,
        sub_normed,
        sub_inv,
        sub_in,
        second_normed,
        second_inv,
        ffn_in,
        hidden,
        unit_normed,
        unit_inv,
        ffn_mid,
    )
    return (kept_state, layer_out.reshape(seq_count, local_len, model_width))


def backward_pass(kept_state, block_grad, weights):
    w_qkv, w_out, w_up, w_down, norm_gains, out_biases, head_biases, head_gain, unit_bias, unit_gain = weights
    (
        attn_in,
        first_normed,
        first_inv,
        query_matrix,
        key_all,
        value_all,
        codes,
        sub_normed,
        sub_inv,
        sub_in,
        second_normed,
        second_inv,
        ffn_in,
        hidden,
        unit_normed,
        unit_inv,
        ffn_mid,
    ) = kept_state
    seq_count, local_len, model_width = block_grad.shape
    row_count = seq_count * local_len
    seq_len = key_all.shape[1]
    grad_low = block_grad.reshape(row_count, model_width)
    grad_full = grad_low.astype(jnp.float32)
    down_grad = outer_sum(ffn_mid, grad_low)
    last_bias_grad = jnp.sum(grad_full, 0)
    unit_grad = back_dot(grad_low, w_down)
    activated_grad, unit_gain_grad = norm_back(unit_normed, unit_inv, unit_gain, unit_grad)
    gelu_value, gelu_pull = jax.vjp(partial(jax.nn.gelu, approximate=True), hidden)
    hidden_low = gelu_pull(activated_grad)[0].astype(jnp.bfloat16)
    up_grad = outer_sum(ffn_in, hidden_low)
    unit_bias_grad = jnp.sum(hidden_low, 0, dtype=jnp.float32)
    ffn_in_grad = back_dot(hidden_low, w_up)
    middle_part, second_gain_grad = norm_back(second_normed, second_inv, norm_gains[1], ffn_in_grad)
    middle_grad = grad_full + middle_part
    middle_low = middle_grad.astype(jnp.bfloat16)
    out_weight_grad = outer_sum(sub_in, middle_low)
    first_bias_grad = jnp.sum(middle_low, 0, dtype=jnp.float32)
    sub_grad = back_dot(middle_low, w_out)
    attended_grad, head_gain_grad = norm_back(sub_normed, sub_inv, head_gain, sub_grad)
    attended_low = attended_grad.astype(jnp.bfloat16)
    early_terms = ((down_grad, 1, 0), (up_grad, 0, 1))
    middle_terms = ((out_weight_grad, 1, 0),)
    early_rows, middle_rows, attended_low = lax.optimization_barrier(
        (pack_rows(early_terms), pack_rows(middle_terms), attended_low)
    )
    early_share = scatter_rows(early_rows)
    middle_share = scatter_rows(middle_rows)
    query_grad, key_part, value_part = attention_backward(
        query_matrix.reshape(seq_count, local_len, model_width),
        key_all,
        value_all,
        attended_low.reshape(seq_count, local_len, model_width),
        codes,
    )
    query_low = query_grad.reshape(row_count, model_width)
    key_low = (
        pair_reduce(key_part, "context", 1).astype(jnp.bfloat16).reshape(row_count, model_width)
    )
    value_low = (
        pair_reduce(value_part, "context", 1).astype(jnp.bfloat16).reshape(row_count, model_width)
    )
    stacked = jnp.stack([query_low, key_low, value_low])
    early_share, stacked = lax.optimization_barrier((early_share, stacked))
    qkv_grad = jnp.einsum("rd,jre->jde", attn_in, stacked, preferred_element_type=jnp.float32)
    head_bias_grad = jnp.stack(
        [jnp.sum(query_low, 0, dtype=jnp.float32), jnp.sum(value_low, 0, dtype=jnp.float32)]
    )
    attn_in_grad = jnp.einsum("jre,jde->rd", stacked, w_qkv, preferred_element_type=jnp.float32)
    input_part, first_gain_grad = norm_back(first_normed, first_inv, norm_gains[0], attn_in_grad)
    input_low = (middle_grad + input_part).astype(jnp.bfloat16)
    heads = model_width // HD
    unit_rows = unit_bias_grad.shape[0] // HD
    late_terms = (
        (qkv_grad, 1, 2),
        (jnp.stack([first_gain_grad, second_gain_grad]), 1, None),
        (jnp.stack([first_bias_grad, last_bias_grad]), 1, None),
        (head_bias_grad.reshape(2, heads, HD), 2, 1),
        (head_gain_grad.reshape(heads, HD), 1, 0),
        (unit_bias_grad.reshape(unit_rows, HD), 1, 0),
        (unit_gain_grad.reshape(unit_rows, HD), 1, 0),
    )
    late_share = scatter_rows(pack_rows(late_terms))
    grad_shares = (
        unpack_share(early_share, early_terms)
        + unpack_share(middle_share, middle_terms)
        + unpack_share(late_share, late_terms)
    )
    return (grad_shares, input_low.reshape(seq_count, local_len, model_width))


def local(
    inputs,
    out_grad,
    picture_starts,
    segment_offsets,
    dilation_offsets,
    norm_gains,
    w_qkv,
    head_biases,
    head_gain,
    w_out,
    out_biases,
    w_up,
    unit_bias,
    unit_gain,
    w_down,
):
    local_seqs, local_len, model_width = inputs.shape
    tensor_count = lax.axis_size("tensor")
    mine = local_seqs // tensor_count
    first_seq = lax.axis_index("tensor") * mine
    block_in = lax.dynamic_slice_in_dim(inputs, first_seq, mine, 0)
    block_grad = lax.dynamic_slice_in_dim(out_grad, first_seq, mine, 0)
    starts = lax.dynamic_slice_in_dim(picture_starts, first_seq, mine, 0)
    seq_len = local_len * lax.axis_size("context")
    query_position = lax.axis_index("context") * local_len + jnp.arange(local_len, dtype=jnp.int32)
    key_position = jnp.arange(seq_len, dtype=jnp.int32)
    spans = jnp.array([seq_len * part // 8 for part in span_parts], jnp.int32)
    rates = jnp.array(dilation_rates, jnp.int32)
    segment_kept = segment_offsets % spans
    dilation_kept = dilation_offsets % rates
    offset_digits = jnp.concatenate(
        [segment_kept // 32, segment_kept % 32, dilation_kept], 1
    ).astype(jnp.bfloat16)
    f32 = jnp.float32
    (
        w_qkv_full,
        gains_full,
        out_bias_full,
        head_bias_full,
        head_gain_full,
        unit_bias_full,
        unit_gain_full,
        digits_full,
    ) = gather_packed(
        (
            (w_qkv, 1, 2),
            (norm_gains, 1, None),
            (out_biases, 1, None),
            (head_biases, 2, 1),
            (head_gain, 1, 0),
            (unit_bias, 1, 0),
            (unit_gain, 1, 0),
            (offset_digits, None, 0),
        )
    )
    patterns = len(span_parts)
    digits_full = digits_full.astype(jnp.int32)
    all_segments = digits_full[:, :patterns] * 32 + digits_full[:, patterns : 2 * patterns]
    all_dilations = digits_full[:, 2 * patterns :]
    codes = mask_codes(starts, query_position, key_position, all_segments, all_dilations, seq_len)
    w_out, w_up, w_down, w_qkv_full = lax.optimization_barrier((w_out, w_up, w_down, w_qkv_full))
    weights = (
        w_qkv_full,
        gather_weight(w_out, 1, 0),
        gather_weight(w_up, 0, 1),
        gather_weight(w_down, 1, 0),
        gains_full.astype(f32),
        out_bias_full.astype(f32),
        head_bias_full.reshape(2, model_width).astype(f32),
        head_gain_full.reshape(model_width).astype(f32),
        unit_bias_full.reshape(-1).astype(f32),
        unit_gain_full.reshape(-1).astype(f32),
    )
    kept_state, layer_block = forward_pass(block_in, codes, weights)
    layer_out = pair_gather(layer_block, "tensor", 0)
    grad_shares, input_block = backward_pass(kept_state, block_grad, weights)
    input_grad = pair_gather(input_block, "tensor", 0)
    (
        down_share,
        up_share,
        out_share,
        qkv_share,
        gains_share,
        out_bias_share,
        head_bias_share,
        head_gain_share,
        unit_bias_share,
        unit_gain_share,
    ) = grad_shares
    return (
        layer_out,
        input_grad,
        gains_share,
        qkv_share,
        head_bias_share,
        head_gain_share,
        out_share,
        out_bias_share,
        up_share,
        unit_bias_share,
        unit_gain_share,
        down_share,
    )


def solution(mesh):
    placed = (
        P("shard", "context", None),
        P("shard", "context", None),
        P("shard", None),
        P("tensor", None),
        P("tensor", None),
        P(None, "shard"),
        P(None, "shard", "tensor"),
        P(None, "tensor", "shard"),
        P("tensor", "shard"),
        P("tensor", "shard"),
        P(None, "shard"),
        P("shard", "tensor"),
        P("tensor", "shard"),
        P("tensor", "shard"),
        P("tensor", "shard"),
    )
    return jax.shard_map(
        local,
        mesh=mesh,
        in_specs=placed,
        out_specs=(
            P("shard", "context", None),
            P("shard", "context", None),
            P(None, "shard"),
            P(None, "shard", "tensor"),
            P(None, "tensor", "shard"),
            P("tensor", "shard"),
            P("tensor", "shard"),
            P(None, "shard"),
            P("shard", "tensor"),
            P("tensor", "shard"),
            P("tensor", "shard"),
            P("tensor", "shard"),
        ),
        check_vma=False,
    )
```

```python
from functools import partial

import jax
import jax.numpy as jnp
from jax import lax
from jax.experimental import pallas as pl
from jax.experimental.pallas import tpu as pltpu
from jax.sharding import PartitionSpec as P

HD = 64
FF = 3072
PIECE = 256
PIECES = 2


epsilon = 1e-05
span_parts = (1, 2, 4, 6, 8)
dilation_rates = (1, 2, 4, 6, 12)


def pattern_total(query_position, key_position, segmented_offsets, dilated_offsets, token_length):
    tallied_total = jnp.zeros(
        (segmented_offsets.shape[0], query_position.shape[0], key_position.shape[0]), jnp.float32
    )
    for item_number in range(len(span_parts)):
        segmented_span = token_length * span_parts[item_number] // 8
        dilated_stride = dilation_rates[item_number]
        seg_shift = (segmented_offsets[:, item_number] % segmented_span)[:, None, None]
        dilated_phase = (dilated_offsets[:, item_number] % dilated_stride)[:, None, None]
        query_lookup = query_position[None, :, None] + seg_shift
        key_lookup = key_position[None, None, :] + seg_shift
        merged_heads = (
            (query_lookup // segmented_span == key_lookup // segmented_span)
            & (query_lookup % dilated_stride == dilated_phase)
            & (key_lookup % dilated_stride == dilated_phase)
        )
        tallied_total = tallied_total + merged_heads.astype(jnp.float32)
    return tallied_total


def picture_index(starts, token_positions):
    marked = jnp.zeros((starts.shape[0], token_positions.shape[0]), jnp.int32)
    for piece_number in range(starts.shape[1]):
        begin_at = starts[:, piece_number][:, None]
        inside = (token_positions[None, :] >= begin_at) & (
            token_positions[None, :] < begin_at + PIECE
        )
        marked = marked + (piece_number + 1) * inside.astype(jnp.int32)
    return marked


def allowed_keys(query_pic, key_pic, query_position, key_position):
    causal_ok = key_position[None, None, :] <= query_position[None, :, None]
    same_piece = (query_pic[:, :, None] == key_pic[:, None, :]) & (query_pic[:, :, None] > 0)
    return (causal_ok | same_piece).astype(jnp.float32)


def outer_sum(left_rows, right_rows):
    return lax.dot_general(
        left_rows, right_rows, (((0,), (0,)), ((), ())), preferred_element_type=jnp.float32
    )


def back_dot(left_rows, weight_rows):
    return lax.dot_general(
        left_rows, weight_rows, (((1,), (1,)), ((), ())), preferred_element_type=jnp.float32
    )


def norm_rows(values, scale_row):
    mean_row = jnp.mean(values, -1, keepdims=True)
    centered = values - mean_row
    inv_std = lax.rsqrt(jnp.mean(centered * centered, -1, keepdims=True) + epsilon)
    normed = centered * inv_std
    return (normed, inv_std, normed * scale_row)


def norm_back(normed, inv_std, scale_row, grad_rows):
    scaled = grad_rows * scale_row
    mean_plain = jnp.mean(scaled, -1, keepdims=True)
    mean_cross = jnp.mean(scaled * normed, -1, keepdims=True)
    return (inv_std * (scaled - mean_plain - normed * mean_cross), jnp.sum(grad_rows * normed, 0))


def probabilities(query_heads, key_heads, mask_table):
    raw_scores = jnp.einsum(
        "sqhd,skhd->shqk", query_heads, key_heads, preferred_element_type=jnp.float32
    ) * HD ** (-0.5)
    masked = jnp.where(mask_table > 0, raw_scores, -1000000000.0)
    row_top = jnp.max(masked, -1, keepdims=True)
    exponent = mask_table * jnp.exp(masked - row_top)
    row_total = jnp.sum(exponent, -1, keepdims=True)
    return (exponent / row_total, row_top, row_total)


SCALE = HD ** (-0.5)
HIDDEN = -1000000000.0
PAIR = 2
CODE_WIDTH = 8


def pair_masks(patq_ref, patk_ref, pcq_ref, pck_ref):
    first_q = patq_ref[0]
    first_k = patk_ref[0]
    row = first_q[:, 5:6]
    col = first_k[5:6, :]
    piece_q = pcq_ref[0][:, 0:1]
    piece_k = pck_ref[0][0:1, :]
    allowed = (col <= row) | (piece_q == piece_k)
    masks = []
    for head in range(PAIR):
        codes_q = patq_ref[head]
        codes_k = patk_ref[head]
        tally = (codes_q[:, 0:1] == codes_k[0:1, :]).astype(jnp.float32)
        for pattern in range(1, len(span_parts)):
            tally = tally + (
                codes_q[:, pattern : pattern + 1] == codes_k[pattern : pattern + 1, :]
            ).astype(jnp.float32)
        masks.append(jnp.where(allowed, tally, 0.0))
    return masks


def soft_rows(query_part, key_block, mask):
    scores = (
        lax.dot_general(
            query_part, key_block, (((1,), (1,)), ((), ())), preferred_element_type=jnp.float32
        )
        * SCALE
    )
    masked = jnp.where(mask > 0, scores, HIDDEN)
    top = jnp.max(masked, axis=1, keepdims=True)
    exponent = mask * jnp.exp(masked - top)
    return exponent / jnp.sum(exponent, axis=1, keepdims=True)


def attention_fwd_kernel(q_ref, k_ref, v_ref, patq_ref, patk_ref, pcq_ref, pck_ref, o_ref):
    query = q_ref[0]
    key_block = k_ref[0]
    value_block = v_ref[0]
    first = lax.broadcasted_iota(jnp.int32, query.shape, 1) < HD
    masks = pair_masks(patq_ref, patk_ref, pcq_ref, pck_ref)
    result = None
    for head in range(PAIR):
        keep = first if head == 0 else jnp.logical_not(first)
        query_part = jnp.where(keep, query, jnp.zeros_like(query))
        probs = soft_rows(query_part, key_block, masks[head])
        mixed = jnp.dot(
            probs.astype(jnp.bfloat16), value_block, preferred_element_type=jnp.float32
        )
        result = mixed if result is None else jnp.where(first, result, mixed)
    o_ref[0] = result


def attention_bwd_kernel(
    q_ref, k_ref, v_ref, do_ref, patq_ref, patk_ref, pcq_ref, pck_ref, dq_ref, dk_ref, dv_ref
):
    @pl.when(pl.program_id(2) == 0)
    def _():
        dk_ref[...] = jnp.zeros_like(dk_ref)
        dv_ref[...] = jnp.zeros_like(dv_ref)

    query = q_ref[0]
    key_block = k_ref[0]
    value_block = v_ref[0]
    grad_out = do_ref[0]
    first = lax.broadcasted_iota(jnp.int32, query.shape, 1) < HD
    masks = pair_masks(patq_ref, patk_ref, pcq_ref, pck_ref)
    query_grad = None
    key_grad = dk_ref[0]
    value_grad = dv_ref[0]
    for head in range(PAIR):
        keep = first if head == 0 else jnp.logical_not(first)
        query_part = jnp.where(keep, query, jnp.zeros_like(query))
        grad_part = jnp.where(keep, grad_out, jnp.zeros_like(grad_out))
        probs = soft_rows(query_part, key_block, masks[head])
        prob_grad = lax.dot_general(
            grad_part, value_block, (((1,), (1,)), ((), ())), preferred_element_type=jnp.float32
        )
        inner = jnp.sum(probs * prob_grad, axis=1, keepdims=True)
        score_low = (probs * (prob_grad - inner)).astype(jnp.bfloat16)
        part = jnp.dot(score_low, key_block, preferred_element_type=jnp.float32)
        query_grad = part if query_grad is None else jnp.where(first, query_grad, part)
        key_grad = key_grad + SCALE * lax.dot_general(
            score_low, query_part, (((0,), (0,)), ((), ())), preferred_element_type=jnp.float32
        )
        value_grad = value_grad + lax.dot_general(
            probs.astype(jnp.bfloat16),
            grad_part,
            (((0,), (0,)), ((), ())),
            preferred_element_type=jnp.float32,
        )
    dq_ref[0] = (query_grad * SCALE).astype(jnp.bfloat16)
    dk_ref[0] = key_grad
    dv_ref[0] = value_grad


def attention_specs(seq_count, local_len, seq_len, block_q):
    lanes = PAIR * HD
    query_spec = pl.BlockSpec((1, block_q, lanes), lambda s, g, b: (s, b, g))
    key_spec = pl.BlockSpec((1, seq_len, lanes), lambda s, g, b: (s, 0, g))
    patq_spec = pl.BlockSpec((PAIR, block_q, CODE_WIDTH), lambda s, g, b: (g, b, 0))
    patk_spec = pl.BlockSpec((PAIR, CODE_WIDTH, seq_len), lambda s, g, b: (g, 0, 0))
    pcq_spec = pl.BlockSpec((1, block_q, CODE_WIDTH), lambda s, g, b: (s, b, 0))
    pck_spec = pl.BlockSpec((1, CODE_WIDTH, seq_len), lambda s, g, b: (s, 0, 0))
    return query_spec, key_spec, patq_spec, patk_spec, pcq_spec, pck_spec


def attention_forward(query, keys, values, codes):
    seq_count, local_len, width = query.shape
    seq_len = keys.shape[1]
    block_q = min(256, local_len)
    grid = (seq_count, width // (PAIR * HD), local_len // block_q)
    query_spec, key_spec, patq_spec, patk_spec, pcq_spec, pck_spec = attention_specs(
        seq_count, local_len, seq_len, block_q
    )
    flops = 8 * seq_count * local_len * seq_len * width
    return pl.pallas_call(
        attention_fwd_kernel,
        grid=grid,
        in_specs=[query_spec, key_spec, key_spec, patq_spec, patk_spec, pcq_spec, pck_spec],
        out_specs=query_spec,
        out_shape=jax.ShapeDtypeStruct((seq_count, local_len, width), jnp.float32),
        compiler_params=pltpu.CompilerParams(
            dimension_semantics=("parallel", "parallel", "arbitrary"),
            vmem_limit_bytes=48 * 1024 * 1024,
        ),
        cost_estimate=pl.CostEstimate(
            flops=flops,
            transcendentals=seq_count * local_len * seq_len * width // HD,
            bytes_accessed=2 * query.size + 2 * keys.size * 2 * (local_len // block_q) + 4 * query.size,
        ),
    )(query, keys, values, *codes)


def attention_backward(query, keys, values, grad_out, codes):
    seq_count, local_len, width = query.shape
    seq_len = keys.shape[1]
    block_q = min(256, local_len)
    grid = (seq_count, width // (PAIR * HD), local_len // block_q)
    query_spec, key_spec, patq_spec, patk_spec, pcq_spec, pck_spec = attention_specs(
        seq_count, local_len, seq_len, block_q
    )
    flops = 20 * seq_count * local_len * seq_len * width
    return pl.pallas_call(
        attention_bwd_kernel,
        grid=grid,
        in_specs=[
            query_spec,
            key_spec,
            key_spec,
            query_spec,
            patq_spec,
            patk_spec,
            pcq_spec,
            pck_spec,
        ],
        out_specs=[query_spec, key_spec, key_spec],
        out_shape=[
            jax.ShapeDtypeStruct((seq_count, local_len, width), jnp.bfloat16),
            jax.ShapeDtypeStruct((seq_count, seq_len, width), jnp.float32),
            jax.ShapeDtypeStruct((seq_count, seq_len, width), jnp.float32),
        ],
        compiler_params=pltpu.CompilerParams(
            dimension_semantics=("parallel", "parallel", "arbitrary"),
            vmem_limit_bytes=48 * 1024 * 1024,
        ),
        cost_estimate=pl.CostEstimate(
            flops=flops,
            transcendentals=seq_count * local_len * seq_len * width // HD,
            bytes_accessed=4 * query.size + 2 * keys.size * 2 * (local_len // block_q) + 16 * keys.size,
        ),
    )(query, keys, values, grad_out, *codes)


def mask_codes(starts, query_position, key_position, segment_offsets, dilation_offsets, seq_len):
    heads = segment_offsets.shape[0]
    query_codes = []
    key_codes = []
    for pattern in range(len(span_parts)):
        span = seq_len * span_parts[pattern] // 8
        rate = dilation_rates[pattern]
        shift = (segment_offsets[:, pattern] % span)[:, None]
        phase = (dilation_offsets[:, pattern] % rate)[:, None]
        query_at = query_position[None, :] + shift
        key_at = key_position[None, :] + shift
        query_codes.append(jnp.where(query_at % rate == phase, query_at // span, -1))
        key_codes.append(jnp.where(key_at % rate == phase, key_at // span, -2))
    patterns = len(span_parts)
    query_codes.append(jnp.broadcast_to(query_position[None, :], (heads, query_position.shape[0])))
    key_codes.append(jnp.broadcast_to(key_position[None, :], (heads, key_position.shape[0])))
    filler = CODE_WIDTH - patterns - 1
    query_codes += [jnp.zeros((heads, query_position.shape[0]), jnp.int32)] * filler
    key_codes += [jnp.zeros((heads, key_position.shape[0]), jnp.int32)] * filler
    patq = jnp.stack(query_codes, 2).astype(jnp.int32)
    patk = jnp.stack(key_codes, 1).astype(jnp.int32)
    query_pic = picture_index(starts, query_position)
    key_pic = picture_index(starts, key_position)
    pcq = jnp.where(query_pic > 0, query_pic, -1)[:, :, None]
    pcq = jnp.pad(pcq, ((0, 0), (0, 0), (0, CODE_WIDTH - 1)))
    pck = jnp.where(key_pic > 0, key_pic, -2)[:, None, :]
    pck = jnp.pad(pck, ((0, 0), (0, CODE_WIDTH - 1), (0, 0)))
    return (patq, patk, pcq.astype(jnp.int32), pck.astype(jnp.int32))


def code_part(codes, begin, end, key_end):
    patq, patk, pcq, pck = codes
    return (patq[:, begin:end], patk[:, :, :key_end], pcq[:, begin:end], pck[:, :, :key_end])


def split_attention_forward(query, keys, values, codes, span):
    if span is None:
        return attention_forward(query, keys, values, codes)
    head = attention_forward(
        query[:, :span], keys[:, :span], values[:, :span], code_part(codes, 0, span, span)
    )
    seq_len = keys.shape[1]
    tail = attention_forward(
        query[:, span:], keys, values, code_part(codes, span, query.shape[1], seq_len)
    )
    return jnp.concatenate([head, tail], 1)


def split_attention_backward(query, keys, values, grad_out, codes, span):
    if span is None:
        return attention_backward(query, keys, values, grad_out, codes)
    seq_len = keys.shape[1]
    head_q, head_k, head_v = attention_backward(
        query[:, :span],
        keys[:, :span],
        values[:, :span],
        grad_out[:, :span],
        code_part(codes, 0, span, span),
    )
    tail_q, tail_k, tail_v = attention_backward(
        query[:, span:],
        keys,
        values,
        grad_out[:, span:],
        code_part(codes, span, query.shape[1], seq_len),
    )
    padding = ((0, 0), (0, seq_len - span), (0, 0))
    return (
        jnp.concatenate([head_q, tail_q], 1),
        tail_k + jnp.pad(head_k, padding),
        tail_v + jnp.pad(head_v, padding),
    )


def spread_sequence(block, local_len):
    me_c = lax.axis_index("context")
    me_t = lax.axis_index("tensor")
    swap = [(0, 1), (1, 0)]
    kept = lax.dynamic_slice_in_dim(block, me_c * local_len, local_len, 1)
    other = lax.dynamic_slice_in_dim(block, (1 - me_c) * local_len, local_len, 1)
    from_context = lax.ppermute(other, "context", perm=swap)
    from_tensor = lax.ppermute(kept, "tensor", perm=swap)
    from_corner = lax.ppermute(other, ("context", "tensor"), perm=[(0, 3), (3, 0), (1, 2), (2, 1)])
    first_c = me_c == 0
    own_pair = jnp.where(
        first_c,
        jnp.concatenate([kept, from_context], 0),
        jnp.concatenate([from_context, kept], 0),
    )
    far_pair = jnp.where(
        first_c,
        jnp.concatenate([from_tensor, from_corner], 0),
        jnp.concatenate([from_corner, from_tensor], 0),
    )
    return jnp.where(
        me_t == 0,
        jnp.concatenate([own_pair, far_pair], 0),
        jnp.concatenate([far_pair, own_pair], 0),
    )


def assemble(stacked, shard_dim, tensor_dim):
    ns, nt = stacked.shape[0], stacked.shape[1]
    if shard_dim is None:
        stacked = stacked[:1]
    if tensor_dim is None:
        stacked = stacked[:, :1]
    local_shape = stacked.shape[2:]
    order = []
    for dim in range(len(local_shape)):
        if dim == shard_dim:
            order.append(0)
        if dim == tensor_dim:
            order.append(1)
        order.append(dim + 2)
    if shard_dim is None:
        order = [0] + order
    if tensor_dim is None:
        order = [1] + order
    moved = stacked.transpose(order)
    full_shape = list(local_shape)
    if shard_dim is not None:
        full_shape[shard_dim] *= ns
    if tensor_dim is not None:
        full_shape[tensor_dim] *= nt
    return moved.reshape(full_shape)


def gather_weight(local_block, shard_dim, tensor_dim):
    ns = lax.axis_size("shard")
    nt = lax.axis_size("tensor")
    stacked = lax.all_gather(local_block, ("shard", "tensor"), axis=0, tiled=False)
    return assemble(stacked.reshape((ns, nt) + local_block.shape), shard_dim, tensor_dim)


def gather_packed(blocks):
    ns = lax.axis_size("shard")
    nt = lax.axis_size("tensor")
    flat = jnp.concatenate([block.reshape(-1) for block, _, _ in blocks])
    padded = -flat.size % 2048
    flat = jnp.pad(flat, (0, padded)).reshape(-1, 128)
    stacked = lax.all_gather(flat, ("shard", "tensor"), axis=0, tiled=False).reshape(ns, nt, -1)
    pieces = []
    offset = 0
    for block, shard_dim, tensor_dim in blocks:
        part = stacked[:, :, offset : offset + block.size].reshape((ns, nt) + block.shape)
        pieces.append(assemble(part, shard_dim, tensor_dim))
        offset += block.size
    return pieces


def pair_gather(block, axis_name, dim):
    if lax.axis_size(axis_name) != 2:
        return lax.all_gather(block, axis_name, axis=dim, tiled=True)
    other = lax.ppermute(block, axis_name, perm=[(0, 1), (1, 0)])
    first = lax.axis_index(axis_name) == 0
    return jnp.where(
        first, jnp.concatenate([block, other], dim), jnp.concatenate([other, block], dim)
    )


def pair_reduce(full, axis_name, dim):
    if lax.axis_size(axis_name) != 2:
        return lax.psum_scatter(
            full.astype(jnp.bfloat16), axis_name, scatter_dimension=dim, tiled=True
        ).astype(jnp.float32)
    half = full.shape[dim] // 2
    me = lax.axis_index(axis_name)
    kept = lax.dynamic_slice_in_dim(full, me * half, half, dim)
    sent = lax.dynamic_slice_in_dim(full, (1 - me) * half, half, dim).astype(jnp.bfloat16)
    received = lax.ppermute(sent, axis_name, perm=[(0, 1), (1, 0)])
    return kept + received.astype(jnp.float32)


def pair_sum(share, axis_name):
    if lax.axis_size(axis_name) != 2:
        return lax.psum(share, axis_name).astype(jnp.float32)
    received = lax.ppermute(share, axis_name, perm=[(0, 1), (1, 0)])
    return share.astype(jnp.float32) + received.astype(jnp.float32)


def disassemble(full, shard_dim, tensor_dim):
    ns = lax.axis_size("shard")
    nt = lax.axis_size("tensor")
    split_shape = []
    positions = {}
    for dim, size in enumerate(full.shape):
        if dim == shard_dim:
            positions["s"] = len(split_shape)
            split_shape += [ns, size // ns]
        elif dim == tensor_dim:
            positions["t"] = len(split_shape)
            split_shape += [nt, size // nt]
        else:
            split_shape.append(size)
    pieces = full.reshape(split_shape)
    lead = [positions[key] for key in ("s", "t") if key in positions]
    rest = [d for d in range(len(split_shape)) if d not in lead]
    pieces = pieces.transpose(lead + rest)
    if "s" not in positions:
        pieces = jnp.broadcast_to(pieces[None], (ns,) + pieces.shape)
    if "t" not in positions:
        pieces = jnp.broadcast_to(pieces[:, None], (ns, nt) + pieces.shape[1:])
    return pieces.reshape(ns * nt, -1)


def pack_rows(terms):
    rows = jnp.concatenate(
        [disassemble(full.astype(jnp.bfloat16), shard_dim, tensor_dim) for full, shard_dim, tensor_dim in terms],
        1,
    )
    width = rows.shape[1]
    return jnp.pad(rows, ((0, 0), (0, -width % 1024))).reshape(rows.shape[0], -1, 128)


def scatter_rows(rows):
    return lax.psum_scatter(rows, ("shard", "tensor"), scatter_dimension=0, tiled=False)


def unpack_share(share, terms):
    total = pair_sum(share, "context").reshape(-1)
    pieces = []
    offset = 0
    ns = lax.axis_size("shard")
    nt = lax.axis_size("tensor")
    for full, shard_dim, tensor_dim in terms:
        local_shape = list(full.shape)
        if shard_dim is not None:
            local_shape[shard_dim] //= ns
        if tensor_dim is not None:
            local_shape[tensor_dim] //= nt
        count = 1
        for size in local_shape:
            count *= size
        pieces.append(total[offset : offset + count].reshape(local_shape))
        offset += count
    return pieces


def forward_pass(block_in, codes, weights, span):
    w_qkv, w_out, w_up, w_down, norm_gains, out_biases, head_biases, head_gain, unit_bias, unit_gain = weights
    seq_count, local_len, model_width = block_in.shape
    row_count = seq_count * local_len
    flattened_input = block_in.reshape(row_count, model_width).astype(jnp.float32)
    first_normed, first_inv, first_out = norm_rows(flattened_input, norm_gains[0])
    attn_in = first_out.astype(jnp.bfloat16)
    projected = jnp.einsum("rd,jde->jre", attn_in, w_qkv, preferred_element_type=jnp.float32)
    query_matrix = (projected[0] + head_biases[0]).astype(jnp.bfloat16)
    keys_local = projected[1].astype(jnp.bfloat16).reshape(seq_count, local_len, model_width)
    values_local = (projected[2] + head_biases[1]).astype(jnp.bfloat16).reshape(
        seq_count, local_len, model_width
    )
    if span is None:
        key_all = pair_gather(keys_local, "context", 1)
        value_all = pair_gather(values_local, "context", 1)
    else:
        key_all, value_all = keys_local, values_local
    attended = split_attention_forward(
        query_matrix.reshape(seq_count, local_len, model_width), key_all, value_all, codes, span
    ).reshape(row_count, model_width)
    sub_normed, sub_inv, sub_out = norm_rows(attended, head_gain)
    sub_in = sub_out.astype(jnp.bfloat16)
    middle = flattened_input + (
        jnp.dot(sub_in, w_out, preferred_element_type=jnp.float32) + out_biases[0]
    )
    second_normed, second_inv, second_out = norm_rows(middle, norm_gains[1])
    ffn_in = second_out.astype(jnp.bfloat16)
    hidden = jnp.dot(ffn_in, w_up, preferred_element_type=jnp.float32) + unit_bias
    activated = jax.nn.gelu(hidden, approximate=True)
    unit_normed, unit_inv, unit_out = norm_rows(activated, unit_gain)
    ffn_mid = unit_out.astype(jnp.bfloat16)
    layer_out = (
        middle + (jnp.dot(ffn_mid, w_down, preferred_element_type=jnp.float32) + out_biases[1])
    ).astype(jnp.bfloat16)
    kept_state = (
        attn_in,
        first_normed,
        first_inv,
        query_matrix,
        key_all,
        value_all,
        codes,
        sub_normed,
        sub_inv,
        sub_in,
        second_normed,
        second_inv,
        ffn_in,
        hidden,
        unit_normed,
        unit_inv,
        ffn_mid,
    )
    return (kept_state, layer_out.reshape(seq_count, local_len, model_width))


def backward_pass(kept_state, block_grad, weights, span):
    w_qkv, w_out, w_up, w_down, norm_gains, out_biases, head_biases, head_gain, unit_bias, unit_gain = weights
    (
        attn_in,
        first_normed,
        first_inv,
        query_matrix,
        key_all,
        value_all,
        codes,
        sub_normed,
        sub_inv,
        sub_in,
        second_normed,
        second_inv,
        ffn_in,
        hidden,
        unit_normed,
        unit_inv,
        ffn_mid,
    ) = kept_state
    seq_count, local_len, model_width = block_grad.shape
    row_count = seq_count * local_len
    seq_len = key_all.shape[1]
    grad_low = block_grad.reshape(row_count, model_width)
    grad_full = grad_low.astype(jnp.float32)
    down_grad = outer_sum(ffn_mid, grad_low)
    last_bias_grad = jnp.sum(grad_full, 0)
    unit_grad = back_dot(grad_low, w_down)
    activated_grad, unit_gain_grad = norm_back(unit_normed, unit_inv, unit_gain, unit_grad)
    gelu_value, gelu_pull = jax.vjp(partial(jax.nn.gelu, approximate=True), hidden)
    hidden_low = gelu_pull(activated_grad)[0].astype(jnp.bfloat16)
    up_grad = outer_sum(ffn_in, hidden_low)
    unit_bias_grad = jnp.sum(hidden_low, 0, dtype=jnp.float32)
    ffn_in_grad = back_dot(hidden_low, w_up)
    middle_part, second_gain_grad = norm_back(second_normed, second_inv, norm_gains[1], ffn_in_grad)
    middle_grad = grad_full + middle_part
    middle_low = middle_grad.astype(jnp.bfloat16)
    out_weight_grad = outer_sum(sub_in, middle_low)
    first_bias_grad = jnp.sum(middle_low, 0, dtype=jnp.float32)
    sub_grad = back_dot(middle_low, w_out)
    attended_grad, head_gain_grad = norm_back(sub_normed, sub_inv, head_gain, sub_grad)
    attended_low = attended_grad.astype(jnp.bfloat16)
    early_terms = ((down_grad, 1, 0), (up_grad, 0, 1))
    middle_terms = ((out_weight_grad, 1, 0),)
    early_rows, middle_rows, attended_low = lax.optimization_barrier(
        (pack_rows(early_terms), pack_rows(middle_terms), attended_low)
    )
    early_share = scatter_rows(early_rows)
    middle_share = scatter_rows(middle_rows)
    query_grad, key_part, value_part = split_attention_backward(
        query_matrix.reshape(seq_count, local_len, model_width),
        key_all,
        value_all,
        attended_low.reshape(seq_count, local_len, model_width),
        codes,
        span,
    )
    if span is not None:
        key_part = key_part.reshape(row_count, model_width)
        value_part = value_part.reshape(row_count, model_width)
    query_low = query_grad.reshape(row_count, model_width)
    if span is None:
        key_part = pair_reduce(key_part, "context", 1)
        value_part = pair_reduce(value_part, "context", 1)
    key_low = key_part.astype(jnp.bfloat16).reshape(row_count, model_width)
    value_low = value_part.astype(jnp.bfloat16).reshape(row_count, model_width)
    stacked = jnp.stack([query_low, key_low, value_low])
    early_share, stacked = lax.optimization_barrier((early_share, stacked))
    qkv_grad = jnp.einsum("rd,jre->jde", attn_in, stacked, preferred_element_type=jnp.float32)
    head_bias_grad = jnp.stack(
        [jnp.sum(query_low, 0, dtype=jnp.float32), jnp.sum(value_low, 0, dtype=jnp.float32)]
    )
    attn_in_grad = jnp.einsum("jre,jde->rd", stacked, w_qkv, preferred_element_type=jnp.float32)
    input_part, first_gain_grad = norm_back(first_normed, first_inv, norm_gains[0], attn_in_grad)
    input_low = (middle_grad + input_part).astype(jnp.bfloat16)
    heads = model_width // HD
    unit_rows = unit_bias_grad.shape[0] // HD
    late_terms = (
        (qkv_grad, 1, 2),
        (jnp.stack([first_gain_grad, second_gain_grad]), 1, None),
        (jnp.stack([first_bias_grad, last_bias_grad]), 1, None),
        (head_bias_grad.reshape(2, heads, HD), 2, 1),
        (head_gain_grad.reshape(heads, HD), 1, 0),
        (unit_bias_grad.reshape(unit_rows, HD), 1, 0),
        (unit_gain_grad.reshape(unit_rows, HD), 1, 0),
    )
    late_share = scatter_rows(pack_rows(late_terms))
    grad_shares = (
        unpack_share(early_share, early_terms)
        + unpack_share(middle_share, middle_terms)
        + unpack_share(late_share, late_terms)
    )
    return (grad_shares, input_low.reshape(seq_count, local_len, model_width))


def local(
    inputs,
    out_grad,
    picture_starts,
    segment_offsets,
    dilation_offsets,
    norm_gains,
    w_qkv,
    head_biases,
    head_gain,
    w_out,
    out_biases,
    w_up,
    unit_bias,
    unit_gain,
    w_down,
):
    local_seqs, local_len, model_width = inputs.shape
    tensor_count = lax.axis_size("tensor")
    context_count = lax.axis_size("context")
    seq_len = local_len * context_count
    key_position = jnp.arange(seq_len, dtype=jnp.int32)
    whole = context_count == 2 and tensor_count == 2 and local_seqs == 4
    if whole:
        span = seq_len // PIECES
        me_c = lax.axis_index("context")
        own_seq = lax.axis_index("tensor") * context_count + me_c
        partner_seq = lax.axis_index("tensor") * context_count + 1 - me_c
        swap = [(0, 1), (1, 0)]

        def own_sequence(rows):
            kept = lax.dynamic_slice_in_dim(rows, own_seq, 1, 0)
            sent = lax.dynamic_slice_in_dim(rows, partner_seq, 1, 0)
            received = lax.ppermute(sent, "context", perm=swap)
            return jnp.where(
                me_c == 0,
                jnp.concatenate([kept, received], 1),
                jnp.concatenate([received, kept], 1),
            )

        block_in = own_sequence(inputs)
        block_grad = own_sequence(out_grad)
        starts = lax.dynamic_slice_in_dim(picture_starts, own_seq, 1, 0)
        query_position = key_position
    else:
        span = None
        mine = local_seqs // tensor_count
        first_seq = lax.axis_index("tensor") * mine
        block_in = lax.dynamic_slice_in_dim(inputs, first_seq, mine, 0)
        block_grad = lax.dynamic_slice_in_dim(out_grad, first_seq, mine, 0)
        starts = lax.dynamic_slice_in_dim(picture_starts, first_seq, mine, 0)
        query_position = lax.axis_index("context") * local_len + jnp.arange(
            local_len, dtype=jnp.int32
        )
    spans = jnp.array([seq_len * part // 8 for part in span_parts], jnp.int32)
    rates = jnp.array(dilation_rates, jnp.int32)
    segment_kept = segment_offsets % spans
    dilation_kept = dilation_offsets % rates
    offset_digits = jnp.concatenate(
        [segment_kept // 32, segment_kept % 32, dilation_kept], 1
    ).astype(jnp.bfloat16)
    f32 = jnp.float32
    (
        w_qkv_full,
        gains_full,
        out_bias_full,
        head_bias_full,
        head_gain_full,
        unit_bias_full,
        unit_gain_full,
        digits_full,
    ) = gather_packed(
        (
            (w_qkv, 1, 2),
            (norm_gains, 1, None),
            (out_biases, 1, None),
            (head_biases, 2, 1),
            (head_gain, 1, 0),
            (unit_bias, 1, 0),
            (unit_gain, 1, 0),
            (offset_digits, None, 0),
        )
    )
    patterns = len(span_parts)
    digits_full = digits_full.astype(jnp.int32)
    all_segments = digits_full[:, :patterns] * 32 + digits_full[:, patterns : 2 * patterns]
    all_dilations = digits_full[:, 2 * patterns :]
    codes = mask_codes(starts, query_position, key_position, all_segments, all_dilations, seq_len)
    w_out, w_up, w_down, w_qkv_full = lax.optimization_barrier((w_out, w_up, w_down, w_qkv_full))
    weights = (
        w_qkv_full,
        gather_weight(w_out, 1, 0),
        gather_weight(w_up, 0, 1),
        gather_weight(w_down, 1, 0),
        gains_full.astype(f32),
        out_bias_full.astype(f32),
        head_bias_full.reshape(2, model_width).astype(f32),
        head_gain_full.reshape(model_width).astype(f32),
        unit_bias_full.reshape(-1).astype(f32),
        unit_gain_full.reshape(-1).astype(f32),
    )
    kept_state, layer_block = forward_pass(block_in, codes, weights, span)
    if whole:
        layer_out = spread_sequence(layer_block, local_len)
    else:
        layer_out = pair_gather(layer_block, "tensor", 0)
    grad_shares, input_block = backward_pass(kept_state, block_grad, weights, span)
    if whole:
        input_grad = spread_sequence(input_block, local_len)
    else:
        input_grad = pair_gather(input_block, "tensor", 0)
    (
        down_share,
        up_share,
        out_share,
        qkv_share,
        gains_share,
        out_bias_share,
        head_bias_share,
        head_gain_share,
        unit_bias_share,
        unit_gain_share,
    ) = grad_shares
    return (
        layer_out,
        input_grad,
        gains_share,
        qkv_share,
        head_bias_share,
        head_gain_share,
        out_share,
        out_bias_share,
        up_share,
        unit_bias_share,
        unit_gain_share,
        down_share,
    )


def solution(mesh):
    placed = (
        P("shard", "context", None),
        P("shard", "context", None),
        P("shard", None),
        P("tensor", None),
        P("tensor", None),
        P(None, "shard"),
        P(None, "shard", "tensor"),
        P(None, "tensor", "shard"),
        P("tensor", "shard"),
        P("tensor", "shard"),
        P(None, "shard"),
        P("shard", "tensor"),
        P("tensor", "shard"),
        P("tensor", "shard"),
        P("tensor", "shard"),
    )
    return jax.shard_map(
        local,
        mesh=mesh,
        in_specs=placed,
        out_specs=(
            P("shard", "context", None),
            P("shard", "context", None),
            P(None, "shard"),
            P(None, "shard", "tensor"),
            P(None, "tensor", "shard"),
            P("tensor", "shard"),
            P("tensor", "shard"),
            P(None, "shard"),
            P("shard", "tensor"),
            P("tensor", "shard"),
            P("tensor", "shard"),
            P("tensor", "shard"),
        ),
        check_vma=False,
    )
```

```python
from functools import partial

import jax
import jax.numpy as jnp
from jax import lax
from jax.experimental import pallas as pl
from jax.experimental.pallas import tpu as pltpu
from jax.sharding import PartitionSpec as P

HD = 64
FF = 3072
PIECE = 256
PIECES = 2


epsilon = 1e-05
span_parts = (1, 2, 4, 6, 8)
dilation_rates = (1, 2, 4, 6, 12)


def pattern_total(query_position, key_position, segmented_offsets, dilated_offsets, token_length):
    tallied_total = jnp.zeros(
        (segmented_offsets.shape[0], query_position.shape[0], key_position.shape[0]), jnp.float32
    )
    for item_number in range(len(span_parts)):
        segmented_span = token_length * span_parts[item_number] // 8
        dilated_stride = dilation_rates[item_number]
        seg_shift = (segmented_offsets[:, item_number] % segmented_span)[:, None, None]
        dilated_phase = (dilated_offsets[:, item_number] % dilated_stride)[:, None, None]
        query_lookup = query_position[None, :, None] + seg_shift
        key_lookup = key_position[None, None, :] + seg_shift
        merged_heads = (
            (query_lookup // segmented_span == key_lookup // segmented_span)
            & (query_lookup % dilated_stride == dilated_phase)
            & (key_lookup % dilated_stride == dilated_phase)
        )
        tallied_total = tallied_total + merged_heads.astype(jnp.float32)
    return tallied_total


def picture_index(starts, token_positions):
    marked = jnp.zeros((starts.shape[0], token_positions.shape[0]), jnp.int32)
    for piece_number in range(starts.shape[1]):
        begin_at = starts[:, piece_number][:, None]
        inside = (token_positions[None, :] >= begin_at) & (
            token_positions[None, :] < begin_at + PIECE
        )
        marked = marked + (piece_number + 1) * inside.astype(jnp.int32)
    return marked


def allowed_keys(query_pic, key_pic, query_position, key_position):
    causal_ok = key_position[None, None, :] <= query_position[None, :, None]
    same_piece = (query_pic[:, :, None] == key_pic[:, None, :]) & (query_pic[:, :, None] > 0)
    return (causal_ok | same_piece).astype(jnp.float32)


def outer_sum(left_rows, right_rows):
    return lax.dot_general(
        left_rows, right_rows, (((0,), (0,)), ((), ())), preferred_element_type=jnp.float32
    )


def back_dot(left_rows, weight_rows):
    return lax.dot_general(
        left_rows, weight_rows, (((1,), (1,)), ((), ())), preferred_element_type=jnp.float32
    )


def norm_rows(values, scale_row):
    mean_row = jnp.mean(values, -1, keepdims=True)
    centered = values - mean_row
    inv_std = lax.rsqrt(jnp.mean(centered * centered, -1, keepdims=True) + epsilon)
    normed = centered * inv_std
    return (normed, inv_std, normed * scale_row)


def norm_back(normed, inv_std, scale_row, grad_rows):
    scaled = grad_rows * scale_row
    mean_plain = jnp.mean(scaled, -1, keepdims=True)
    mean_cross = jnp.mean(scaled * normed, -1, keepdims=True)
    return (inv_std * (scaled - mean_plain - normed * mean_cross), jnp.sum(grad_rows * normed, 0))


def probabilities(query_heads, key_heads, mask_table):
    raw_scores = jnp.einsum(
        "sqhd,skhd->shqk", query_heads, key_heads, preferred_element_type=jnp.float32
    ) * HD ** (-0.5)
    masked = jnp.where(mask_table > 0, raw_scores, -1000000000.0)
    row_top = jnp.max(masked, -1, keepdims=True)
    exponent = mask_table * jnp.exp(masked - row_top)
    row_total = jnp.sum(exponent, -1, keepdims=True)
    return (exponent / row_total, row_top, row_total)


SCALE = HD ** (-0.5)
HIDDEN = -1000000000.0
PAIR = 2
CODE_WIDTH = 8


def pair_masks(patq_ref, patk_ref, pcq_ref, pck_ref):
    first_q = patq_ref[0]
    first_k = patk_ref[0]
    row = first_q[:, 5:6]
    col = first_k[5:6, :]
    piece_q = pcq_ref[0][:, 0:1]
    piece_k = pck_ref[0][0:1, :]
    allowed = (col <= row) | (piece_q == piece_k)
    masks = []
    for head in range(PAIR):
        codes_q = patq_ref[head]
        codes_k = patk_ref[head]
        tally = (codes_q[:, 0:1] == codes_k[0:1, :]).astype(jnp.float32)
        for pattern in range(1, len(span_parts)):
            tally = tally + (
                codes_q[:, pattern : pattern + 1] == codes_k[pattern : pattern + 1, :]
            ).astype(jnp.float32)
        masks.append(jnp.where(allowed, tally, 0.0))
    return masks


def soft_rows(query_part, key_block, mask):
    scores = (
        lax.dot_general(
            query_part, key_block, (((1,), (1,)), ((), ())), preferred_element_type=jnp.float32
        )
        * SCALE
    )
    masked = jnp.where(mask > 0, scores, HIDDEN)
    top = jnp.max(masked, axis=1, keepdims=True)
    exponent = mask * jnp.exp(masked - top)
    return exponent / jnp.sum(exponent, axis=1, keepdims=True)


def attention_fwd_kernel(q_ref, k_ref, v_ref, patq_ref, patk_ref, pcq_ref, pck_ref, o_ref):
    query = q_ref[0]
    key_block = k_ref[0]
    value_block = v_ref[0]
    first = lax.broadcasted_iota(jnp.int32, query.shape, 1) < HD
    masks = pair_masks(patq_ref, patk_ref, pcq_ref, pck_ref)
    result = None
    for head in range(PAIR):
        keep = first if head == 0 else jnp.logical_not(first)
        query_part = jnp.where(keep, query, jnp.zeros_like(query))
        probs = soft_rows(query_part, key_block, masks[head])
        mixed = jnp.dot(
            probs.astype(jnp.bfloat16), value_block, preferred_element_type=jnp.float32
        )
        result = mixed if result is None else jnp.where(first, result, mixed)
    o_ref[0] = result


def attention_bwd_kernel(
    q_ref, k_ref, v_ref, do_ref, patq_ref, patk_ref, pcq_ref, pck_ref, dq_ref, dk_ref, dv_ref
):
    @pl.when(pl.program_id(2) == 0)
    def _():
        dk_ref[...] = jnp.zeros_like(dk_ref)
        dv_ref[...] = jnp.zeros_like(dv_ref)

    query = q_ref[0]
    key_block = k_ref[0]
    value_block = v_ref[0]
    grad_out = do_ref[0]
    first = lax.broadcasted_iota(jnp.int32, query.shape, 1) < HD
    masks = pair_masks(patq_ref, patk_ref, pcq_ref, pck_ref)
    query_grad = None
    key_grad = dk_ref[0]
    value_grad = dv_ref[0]
    for head in range(PAIR):
        keep = first if head == 0 else jnp.logical_not(first)
        query_part = jnp.where(keep, query, jnp.zeros_like(query))
        grad_part = jnp.where(keep, grad_out, jnp.zeros_like(grad_out))
        probs = soft_rows(query_part, key_block, masks[head])
        prob_grad = lax.dot_general(
            grad_part, value_block, (((1,), (1,)), ((), ())), preferred_element_type=jnp.float32
        )
        inner = jnp.sum(probs * prob_grad, axis=1, keepdims=True)
        score_low = (probs * (prob_grad - inner)).astype(jnp.bfloat16)
        part = jnp.dot(score_low, key_block, preferred_element_type=jnp.float32)
        query_grad = part if query_grad is None else jnp.where(first, query_grad, part)
        key_grad = key_grad + SCALE * lax.dot_general(
            score_low, query_part, (((0,), (0,)), ((), ())), preferred_element_type=jnp.float32
        )
        value_grad = value_grad + lax.dot_general(
            probs.astype(jnp.bfloat16),
            grad_part,
            (((0,), (0,)), ((), ())),
            preferred_element_type=jnp.float32,
        )
    dq_ref[0] = (query_grad * SCALE).astype(jnp.bfloat16)
    dk_ref[0] = key_grad
    dv_ref[0] = value_grad


def attention_specs(seq_count, local_len, seq_len, block_q):
    lanes = PAIR * HD
    query_spec = pl.BlockSpec((1, block_q, lanes), lambda s, g, b: (s, b, g))
    key_spec = pl.BlockSpec((1, seq_len, lanes), lambda s, g, b: (s, 0, g))
    patq_spec = pl.BlockSpec((PAIR, block_q, CODE_WIDTH), lambda s, g, b: (g, b, 0))
    patk_spec = pl.BlockSpec((PAIR, CODE_WIDTH, seq_len), lambda s, g, b: (g, 0, 0))
    pcq_spec = pl.BlockSpec((1, block_q, CODE_WIDTH), lambda s, g, b: (s, b, 0))
    pck_spec = pl.BlockSpec((1, CODE_WIDTH, seq_len), lambda s, g, b: (s, 0, 0))
    return query_spec, key_spec, patq_spec, patk_spec, pcq_spec, pck_spec


def attention_forward(query, keys, values, codes):
    seq_count, local_len, width = query.shape
    seq_len = keys.shape[1]
    block_q = min(256, local_len)
    grid = (seq_count, width // (PAIR * HD), local_len // block_q)
    query_spec, key_spec, patq_spec, patk_spec, pcq_spec, pck_spec = attention_specs(
        seq_count, local_len, seq_len, block_q
    )
    flops = 8 * seq_count * local_len * seq_len * width
    return pl.pallas_call(
        attention_fwd_kernel,
        grid=grid,
        in_specs=[query_spec, key_spec, key_spec, patq_spec, patk_spec, pcq_spec, pck_spec],
        out_specs=query_spec,
        out_shape=jax.ShapeDtypeStruct((seq_count, local_len, width), jnp.float32),
        compiler_params=pltpu.CompilerParams(
            dimension_semantics=("parallel", "parallel", "arbitrary"),
            vmem_limit_bytes=48 * 1024 * 1024,
        ),
        cost_estimate=pl.CostEstimate(
            flops=flops,
            transcendentals=seq_count * local_len * seq_len * width // HD,
            bytes_accessed=2 * query.size + 2 * keys.size * 2 * (local_len // block_q) + 4 * query.size,
        ),
    )(query, keys, values, *codes)


def attention_backward(query, keys, values, grad_out, codes):
    seq_count, local_len, width = query.shape
    seq_len = keys.shape[1]
    block_q = min(256, local_len)
    grid = (seq_count, width // (PAIR * HD), local_len // block_q)
    query_spec, key_spec, patq_spec, patk_spec, pcq_spec, pck_spec = attention_specs(
        seq_count, local_len, seq_len, block_q
    )
    flops = 20 * seq_count * local_len * seq_len * width
    return pl.pallas_call(
        attention_bwd_kernel,
        grid=grid,
        in_specs=[
            query_spec,
            key_spec,
            key_spec,
            query_spec,
            patq_spec,
            patk_spec,
            pcq_spec,
            pck_spec,
        ],
        out_specs=[query_spec, key_spec, key_spec],
        out_shape=[
            jax.ShapeDtypeStruct((seq_count, local_len, width), jnp.bfloat16),
            jax.ShapeDtypeStruct((seq_count, seq_len, width), jnp.float32),
            jax.ShapeDtypeStruct((seq_count, seq_len, width), jnp.float32),
        ],
        compiler_params=pltpu.CompilerParams(
            dimension_semantics=("parallel", "parallel", "arbitrary"),
            vmem_limit_bytes=48 * 1024 * 1024,
        ),
        cost_estimate=pl.CostEstimate(
            flops=flops,
            transcendentals=seq_count * local_len * seq_len * width // HD,
            bytes_accessed=4 * query.size + 2 * keys.size * 2 * (local_len // block_q) + 16 * keys.size,
        ),
    )(query, keys, values, grad_out, *codes)


def mask_codes(starts, query_position, key_position, segment_offsets, dilation_offsets, seq_len):
    heads = segment_offsets.shape[0]
    query_codes = []
    key_codes = []
    for pattern in range(len(span_parts)):
        span = seq_len * span_parts[pattern] // 8
        rate = dilation_rates[pattern]
        shift = (segment_offsets[:, pattern] % span)[:, None]
        phase = (dilation_offsets[:, pattern] % rate)[:, None]
        query_at = query_position[None, :] + shift
        key_at = key_position[None, :] + shift
        query_codes.append(jnp.where(query_at % rate == phase, query_at // span, -1))
        key_codes.append(jnp.where(key_at % rate == phase, key_at // span, -2))
    patterns = len(span_parts)
    query_codes.append(jnp.broadcast_to(query_position[None, :], (heads, query_position.shape[0])))
    key_codes.append(jnp.broadcast_to(key_position[None, :], (heads, key_position.shape[0])))
    filler = CODE_WIDTH - patterns - 1
    query_codes += [jnp.zeros((heads, query_position.shape[0]), jnp.int32)] * filler
    key_codes += [jnp.zeros((heads, key_position.shape[0]), jnp.int32)] * filler
    patq = jnp.stack(query_codes, 2).astype(jnp.int32)
    patk = jnp.stack(key_codes, 1).astype(jnp.int32)
    query_pic = picture_index(starts, query_position)
    key_pic = picture_index(starts, key_position)
    pcq = jnp.where(query_pic > 0, query_pic, -1)[:, :, None]
    pcq = jnp.pad(pcq, ((0, 0), (0, 0), (0, CODE_WIDTH - 1)))
    pck = jnp.where(key_pic > 0, key_pic, -2)[:, None, :]
    pck = jnp.pad(pck, ((0, 0), (0, CODE_WIDTH - 1), (0, 0)))
    return (patq, patk, pcq.astype(jnp.int32), pck.astype(jnp.int32))


def code_part(codes, begin, end, key_end):
    patq, patk, pcq, pck = codes
    return (patq[:, begin:end], patk[:, :, :key_end], pcq[:, begin:end], pck[:, :, :key_end])


def split_attention_forward(query, keys, values, codes, span):
    if span is None:
        return attention_forward(query, keys, values, codes)
    head = attention_forward(
        query[:, :span], keys[:, :span], values[:, :span], code_part(codes, 0, span, span)
    )
    seq_len = keys.shape[1]
    tail = attention_forward(
        query[:, span:], keys, values, code_part(codes, span, query.shape[1], seq_len)
    )
    return jnp.concatenate([head, tail], 1)


def split_attention_backward(query, keys, values, grad_out, codes, span):
    if span is None:
        return attention_backward(query, keys, values, grad_out, codes)
    seq_len = keys.shape[1]
    head_q, head_k, head_v = attention_backward(
        query[:, :span],
        keys[:, :span],
        values[:, :span],
        grad_out[:, :span],
        code_part(codes, 0, span, span),
    )
    tail_q, tail_k, tail_v = attention_backward(
        query[:, span:],
        keys,
        values,
        grad_out[:, span:],
        code_part(codes, span, query.shape[1], seq_len),
    )
    padding = ((0, 0), (0, seq_len - span), (0, 0))
    return (
        jnp.concatenate([head_q, tail_q], 1),
        tail_k + jnp.pad(head_k, padding),
        tail_v + jnp.pad(head_v, padding),
    )


def spread_sequence(block, local_len):
    me_c = lax.axis_index("context")
    me_t = lax.axis_index("tensor")
    swap = [(0, 1), (1, 0)]
    kept = lax.dynamic_slice_in_dim(block, me_c * local_len, local_len, 1)
    other = lax.dynamic_slice_in_dim(block, (1 - me_c) * local_len, local_len, 1)
    from_context = lax.ppermute(other, "context", perm=swap)
    from_tensor = lax.ppermute(kept, "tensor", perm=swap)
    from_corner = lax.ppermute(other, ("context", "tensor"), perm=[(0, 3), (3, 0), (1, 2), (2, 1)])
    first_c = me_c == 0
    own_pair = jnp.where(
        first_c,
        jnp.concatenate([kept, from_context], 0),
        jnp.concatenate([from_context, kept], 0),
    )
    far_pair = jnp.where(
        first_c,
        jnp.concatenate([from_tensor, from_corner], 0),
        jnp.concatenate([from_corner, from_tensor], 0),
    )
    return jnp.where(
        me_t == 0,
        jnp.concatenate([own_pair, far_pair], 0),
        jnp.concatenate([far_pair, own_pair], 0),
    )


def assemble(stacked, shard_dim, tensor_dim):
    ns, nt = stacked.shape[0], stacked.shape[1]
    if shard_dim is None:
        stacked = stacked[:1]
    if tensor_dim is None:
        stacked = stacked[:, :1]
    local_shape = stacked.shape[2:]
    order = []
    for dim in range(len(local_shape)):
        if dim == shard_dim:
            order.append(0)
        if dim == tensor_dim:
            order.append(1)
        order.append(dim + 2)
    if shard_dim is None:
        order = [0] + order
    if tensor_dim is None:
        order = [1] + order
    moved = stacked.transpose(order)
    full_shape = list(local_shape)
    if shard_dim is not None:
        full_shape[shard_dim] *= ns
    if tensor_dim is not None:
        full_shape[tensor_dim] *= nt
    return moved.reshape(full_shape)


def gather_weight(local_block, shard_dim, tensor_dim):
    ns = lax.axis_size("shard")
    nt = lax.axis_size("tensor")
    stacked = lax.all_gather(local_block, ("shard", "tensor"), axis=0, tiled=False)
    return assemble(stacked.reshape((ns, nt) + local_block.shape), shard_dim, tensor_dim)


def gather_packed(blocks):
    ns = lax.axis_size("shard")
    nt = lax.axis_size("tensor")
    flat = jnp.concatenate([block.reshape(-1) for block, _, _ in blocks])
    padded = -flat.size % 2048
    flat = jnp.pad(flat, (0, padded)).reshape(-1, 128)
    stacked = lax.all_gather(flat, ("shard", "tensor"), axis=0, tiled=False).reshape(ns, nt, -1)
    pieces = []
    offset = 0
    for block, shard_dim, tensor_dim in blocks:
        part = stacked[:, :, offset : offset + block.size].reshape((ns, nt) + block.shape)
        pieces.append(assemble(part, shard_dim, tensor_dim))
        offset += block.size
    return pieces


def pair_gather(block, axis_name, dim):
    if lax.axis_size(axis_name) != 2:
        return lax.all_gather(block, axis_name, axis=dim, tiled=True)
    other = lax.ppermute(block, axis_name, perm=[(0, 1), (1, 0)])
    first = lax.axis_index(axis_name) == 0
    return jnp.where(
        first, jnp.concatenate([block, other], dim), jnp.concatenate([other, block], dim)
    )


def pair_reduce(full, axis_name, dim):
    if lax.axis_size(axis_name) != 2:
        return lax.psum_scatter(
            full.astype(jnp.bfloat16), axis_name, scatter_dimension=dim, tiled=True
        ).astype(jnp.float32)
    half = full.shape[dim] // 2
    me = lax.axis_index(axis_name)
    kept = lax.dynamic_slice_in_dim(full, me * half, half, dim)
    sent = lax.dynamic_slice_in_dim(full, (1 - me) * half, half, dim).astype(jnp.bfloat16)
    received = lax.ppermute(sent, axis_name, perm=[(0, 1), (1, 0)])
    return kept + received.astype(jnp.float32)


def pair_sum(share, axis_name):
    if lax.axis_size(axis_name) != 2:
        return lax.psum(share, axis_name).astype(jnp.float32)
    received = lax.ppermute(share, axis_name, perm=[(0, 1), (1, 0)])
    return share.astype(jnp.float32) + received.astype(jnp.float32)


def disassemble(full, shard_dim, tensor_dim):
    ns = lax.axis_size("shard")
    nt = lax.axis_size("tensor")
    split_shape = []
    positions = {}
    for dim, size in enumerate(full.shape):
        if dim == shard_dim:
            positions["s"] = len(split_shape)
            split_shape += [ns, size // ns]
        elif dim == tensor_dim:
            positions["t"] = len(split_shape)
            split_shape += [nt, size // nt]
        else:
            split_shape.append(size)
    pieces = full.reshape(split_shape)
    lead = [positions[key] for key in ("s", "t") if key in positions]
    rest = [d for d in range(len(split_shape)) if d not in lead]
    pieces = pieces.transpose(lead + rest)
    if "s" not in positions:
        pieces = jnp.broadcast_to(pieces[None], (ns,) + pieces.shape)
    if "t" not in positions:
        pieces = jnp.broadcast_to(pieces[:, None], (ns, nt) + pieces.shape[1:])
    return pieces.reshape(ns * nt, -1)


def pack_rows(terms):
    rows = jnp.concatenate(
        [disassemble(full.astype(jnp.bfloat16), shard_dim, tensor_dim) for full, shard_dim, tensor_dim in terms],
        1,
    )
    width = rows.shape[1]
    return jnp.pad(rows, ((0, 0), (0, -width % 1024))).reshape(rows.shape[0], -1, 128)


def scatter_rows(rows):
    return lax.psum_scatter(rows, ("shard", "tensor"), scatter_dimension=0, tiled=False)


def unpack_share(share, terms):
    total = pair_sum(share, "context").reshape(-1)
    pieces = []
    offset = 0
    ns = lax.axis_size("shard")
    nt = lax.axis_size("tensor")
    for full, shard_dim, tensor_dim in terms:
        local_shape = list(full.shape)
        if shard_dim is not None:
            local_shape[shard_dim] //= ns
        if tensor_dim is not None:
            local_shape[tensor_dim] //= nt
        count = 1
        for size in local_shape:
            count *= size
        pieces.append(total[offset : offset + count].reshape(local_shape))
        offset += count
    return pieces


def shard_stage(grad, dim):
    return lax.psum_scatter(grad.astype(jnp.bfloat16), "shard", scatter_dimension=dim, tiled=True)


def finish_stage(share, tensor_dim):
    summed = pair_reduce(share, "tensor", tensor_dim)
    return pair_sum(summed.astype(jnp.bfloat16), "context")


def forward_pass(block_in, codes, weights, span):
    w_qkv, w_out, w_up, w_down, norm_gains, out_biases, head_biases, head_gain, unit_bias, unit_gain = weights
    seq_count, local_len, model_width = block_in.shape
    row_count = seq_count * local_len
    flattened_input = block_in.reshape(row_count, model_width).astype(jnp.float32)
    first_normed, first_inv, first_out = norm_rows(flattened_input, norm_gains[0])
    attn_in = first_out.astype(jnp.bfloat16)
    projected = jnp.einsum("rd,jde->jre", attn_in, w_qkv, preferred_element_type=jnp.float32)
    query_matrix = (projected[0] + head_biases[0]).astype(jnp.bfloat16)
    keys_local = projected[1].astype(jnp.bfloat16).reshape(seq_count, local_len, model_width)
    values_local = (projected[2] + head_biases[1]).astype(jnp.bfloat16).reshape(
        seq_count, local_len, model_width
    )
    if span is None:
        key_all = pair_gather(keys_local, "context", 1)
        value_all = pair_gather(values_local, "context", 1)
    else:
        key_all, value_all = keys_local, values_local
    attended = split_attention_forward(
        query_matrix.reshape(seq_count, local_len, model_width), key_all, value_all, codes, span
    ).reshape(row_count, model_width)
    sub_normed, sub_inv, sub_out = norm_rows(attended, head_gain)
    sub_in = sub_out.astype(jnp.bfloat16)
    middle = flattened_input + (
        jnp.dot(sub_in, w_out, preferred_element_type=jnp.float32) + out_biases[0]
    )
    second_normed, second_inv, second_out = norm_rows(middle, norm_gains[1])
    ffn_in = second_out.astype(jnp.bfloat16)
    hidden = jnp.dot(ffn_in, w_up, preferred_element_type=jnp.float32) + unit_bias
    activated = jax.nn.gelu(hidden, approximate=True)
    unit_normed, unit_inv, unit_out = norm_rows(activated, unit_gain)
    ffn_mid = unit_out.astype(jnp.bfloat16)
    layer_out = (
        middle + (jnp.dot(ffn_mid, w_down, preferred_element_type=jnp.float32) + out_biases[1])
    ).astype(jnp.bfloat16)
    kept_state = (
        attn_in,
        first_normed,
        first_inv,
        query_matrix,
        key_all,
        value_all,
        codes,
        sub_normed,
        sub_inv,
        sub_in,
        second_normed,
        second_inv,
        ffn_in,
        hidden,
        unit_normed,
        unit_inv,
        ffn_mid,
    )
    return (kept_state, layer_out.reshape(seq_count, local_len, model_width))


def backward_pass(kept_state, block_grad, weights, span):
    w_qkv, w_out, w_up, w_down, norm_gains, out_biases, head_biases, head_gain, unit_bias, unit_gain = weights
    (
        attn_in,
        first_normed,
        first_inv,
        query_matrix,
        key_all,
        value_all,
        codes,
        sub_normed,
        sub_inv,
        sub_in,
        second_normed,
        second_inv,
        ffn_in,
        hidden,
        unit_normed,
        unit_inv,
        ffn_mid,
    ) = kept_state
    seq_count, local_len, model_width = block_grad.shape
    row_count = seq_count * local_len
    seq_len = key_all.shape[1]
    grad_low = block_grad.reshape(row_count, model_width)
    grad_full = grad_low.astype(jnp.float32)
    down_grad = outer_sum(grad_low, ffn_mid)
    last_bias_grad = jnp.sum(grad_full, 0)
    unit_grad = back_dot(grad_low, w_down)
    activated_grad, unit_gain_grad = norm_back(unit_normed, unit_inv, unit_gain, unit_grad)
    gelu_value, gelu_pull = jax.vjp(partial(jax.nn.gelu, approximate=True), hidden)
    hidden_low = gelu_pull(activated_grad)[0].astype(jnp.bfloat16)
    up_grad = outer_sum(ffn_in, hidden_low)
    unit_bias_grad = jnp.sum(hidden_low, 0, dtype=jnp.float32)
    ffn_in_grad = back_dot(hidden_low, w_up)
    middle_part, second_gain_grad = norm_back(second_normed, second_inv, norm_gains[1], ffn_in_grad)
    middle_grad = grad_full + middle_part
    middle_low = middle_grad.astype(jnp.bfloat16)
    out_weight_grad = outer_sum(middle_low, sub_in)
    first_bias_grad = jnp.sum(middle_low, 0, dtype=jnp.float32)
    sub_grad = back_dot(middle_low, w_out)
    attended_grad, head_gain_grad = norm_back(sub_normed, sub_inv, head_gain, sub_grad)
    attended_low = attended_grad.astype(jnp.bfloat16)
    down_grad, up_grad, out_weight_grad, attended_low = lax.optimization_barrier(
        (
            down_grad.astype(jnp.bfloat16),
            up_grad.astype(jnp.bfloat16),
            out_weight_grad.astype(jnp.bfloat16),
            attended_low,
        )
    )
    down_share = shard_stage(down_grad, 0)
    up_share = shard_stage(up_grad, 0)
    out_share = shard_stage(out_weight_grad, 0)
    query_grad, key_part, value_part = split_attention_backward(
        query_matrix.reshape(seq_count, local_len, model_width),
        key_all,
        value_all,
        attended_low.reshape(seq_count, local_len, model_width),
        codes,
        span,
    )
    if span is not None:
        key_part = key_part.reshape(row_count, model_width)
        value_part = value_part.reshape(row_count, model_width)
    query_low = query_grad.reshape(row_count, model_width)
    if span is None:
        key_part = pair_reduce(key_part, "context", 1)
        value_part = pair_reduce(value_part, "context", 1)
    key_low = key_part.astype(jnp.bfloat16).reshape(row_count, model_width)
    value_low = value_part.astype(jnp.bfloat16).reshape(row_count, model_width)
    stacked = jnp.stack([query_low, key_low, value_low])
    down_share, up_share, stacked = lax.optimization_barrier((down_share, up_share, stacked))
    qkv_grad = jnp.einsum("rd,jre->dje", attn_in, stacked, preferred_element_type=jnp.float32)
    head_bias_grad = jnp.stack(
        [jnp.sum(query_low, 0, dtype=jnp.float32), jnp.sum(value_low, 0, dtype=jnp.float32)]
    )
    attn_in_grad = jnp.einsum("jre,jde->rd", stacked, w_qkv, preferred_element_type=jnp.float32)
    input_part, first_gain_grad = norm_back(first_normed, first_inv, norm_gains[0], attn_in_grad)
    input_low = (middle_grad + input_part).astype(jnp.bfloat16)
    heads = model_width // HD
    unit_rows = unit_bias_grad.shape[0] // HD
    small_terms = (
        (jnp.stack([first_gain_grad, second_gain_grad]), 1, None),
        (jnp.stack([first_bias_grad, last_bias_grad]), 1, None),
        (head_bias_grad.reshape(2, heads, HD), 2, 1),
        (head_gain_grad.reshape(heads, HD), 1, 0),
        (unit_bias_grad.reshape(unit_rows, HD), 1, 0),
        (unit_gain_grad.reshape(unit_rows, HD), 1, 0),
    )
    ns = lax.axis_size("shard")
    nt = lax.axis_size("tensor")
    small_rows = jnp.concatenate(
        [disassemble(full, shard_dim, tensor_dim) for full, shard_dim, tensor_dim in small_terms], 1
    )
    small_width = small_rows.shape[1]
    block_rows = model_width // ns
    block_cols = model_width // nt
    small_plane = (
        jnp.pad(small_rows, ((0, 0), (0, block_rows * block_cols - small_width)))
        .reshape(ns, nt, block_rows, block_cols)
        .transpose(0, 2, 1, 3)
        .reshape(model_width, 1, model_width)
    )
    qkv_share = shard_stage(jnp.concatenate([qkv_grad, small_plane], 1), 0)
    qkv_total = finish_stage(qkv_share, 2)
    small_total = qkv_total[:, 3].reshape(-1)[:small_width]
    small_pieces = []
    offset = 0
    for full, shard_dim, tensor_dim in small_terms:
        local_shape = list(full.shape)
        if shard_dim is not None:
            local_shape[shard_dim] //= ns
        if tensor_dim is not None:
            local_shape[tensor_dim] //= nt
        count = 1
        for size in local_shape:
            count *= size
        small_pieces.append(small_total[offset : offset + count].reshape(local_shape))
        offset += count
    grad_shares = (
        finish_stage(down_share, 1).transpose(1, 0),
        finish_stage(up_share, 1),
        finish_stage(out_share, 1).transpose(1, 0),
        qkv_total[:, :3].transpose(1, 0, 2),
    ) + tuple(small_pieces)
    return (grad_shares, input_low.reshape(seq_count, local_len, model_width))


def local(
    inputs,
    out_grad,
    picture_starts,
    segment_offsets,
    dilation_offsets,
    norm_gains,
    w_qkv,
    head_biases,
    head_gain,
    w_out,
    out_biases,
    w_up,
    unit_bias,
    unit_gain,
    w_down,
):
    local_seqs, local_len, model_width = inputs.shape
    tensor_count = lax.axis_size("tensor")
    context_count = lax.axis_size("context")
    seq_len = local_len * context_count
    key_position = jnp.arange(seq_len, dtype=jnp.int32)
    whole = context_count == 2 and tensor_count == 2 and local_seqs == 4
    if whole:
        span = seq_len // PIECES
        me_c = lax.axis_index("context")
        own_seq = lax.axis_index("tensor") * context_count + me_c
        partner_seq = lax.axis_index("tensor") * context_count + 1 - me_c
        swap = [(0, 1), (1, 0)]

        def own_sequence(rows):
            kept = lax.dynamic_slice_in_dim(rows, own_seq, 1, 0)
            sent = lax.dynamic_slice_in_dim(rows, partner_seq, 1, 0)
            received = lax.ppermute(sent, "context", perm=swap)
            return jnp.where(
                me_c == 0,
                jnp.concatenate([kept, received], 1),
                jnp.concatenate([received, kept], 1),
            )

        block_in = own_sequence(inputs)
        block_grad = own_sequence(out_grad)
        starts = lax.dynamic_slice_in_dim(picture_starts, own_seq, 1, 0)
        query_position = key_position
    else:
        span = None
        mine = local_seqs // tensor_count
        first_seq = lax.axis_index("tensor") * mine
        block_in = lax.dynamic_slice_in_dim(inputs, first_seq, mine, 0)
        block_grad = lax.dynamic_slice_in_dim(out_grad, first_seq, mine, 0)
        starts = lax.dynamic_slice_in_dim(picture_starts, first_seq, mine, 0)
        query_position = lax.axis_index("context") * local_len + jnp.arange(
            local_len, dtype=jnp.int32
        )
    spans = jnp.array([seq_len * part // 8 for part in span_parts], jnp.int32)
    rates = jnp.array(dilation_rates, jnp.int32)
    segment_kept = segment_offsets % spans
    dilation_kept = dilation_offsets % rates
    offset_digits = jnp.concatenate(
        [segment_kept // 32, segment_kept % 32, dilation_kept], 1
    ).astype(jnp.bfloat16)
    f32 = jnp.float32
    (
        w_qkv_full,
        gains_full,
        out_bias_full,
        head_bias_full,
        head_gain_full,
        unit_bias_full,
        unit_gain_full,
        digits_full,
    ) = gather_packed(
        (
            (w_qkv, 1, 2),
            (norm_gains, 1, None),
            (out_biases, 1, None),
            (head_biases, 2, 1),
            (head_gain, 1, 0),
            (unit_bias, 1, 0),
            (unit_gain, 1, 0),
            (offset_digits, None, 0),
        )
    )
    patterns = len(span_parts)
    digits_full = digits_full.astype(jnp.int32)
    all_segments = digits_full[:, :patterns] * 32 + digits_full[:, patterns : 2 * patterns]
    all_dilations = digits_full[:, 2 * patterns :]
    codes = mask_codes(starts, query_position, key_position, all_segments, all_dilations, seq_len)
    w_out, w_up, w_down, w_qkv_full = lax.optimization_barrier((w_out, w_up, w_down, w_qkv_full))
    weights = (
        w_qkv_full,
        gather_weight(w_out, 1, 0),
        gather_weight(w_up, 0, 1),
        gather_weight(w_down, 1, 0),
        gains_full.astype(f32),
        out_bias_full.astype(f32),
        head_bias_full.reshape(2, model_width).astype(f32),
        head_gain_full.reshape(model_width).astype(f32),
        unit_bias_full.reshape(-1).astype(f32),
        unit_gain_full.reshape(-1).astype(f32),
    )
    kept_state, layer_block = forward_pass(block_in, codes, weights, span)
    if whole:
        layer_out = spread_sequence(layer_block, local_len)
    else:
        layer_out = pair_gather(layer_block, "tensor", 0)
    grad_shares, input_block = backward_pass(kept_state, block_grad, weights, span)
    if whole:
        input_grad = spread_sequence(input_block, local_len)
    else:
        input_grad = pair_gather(input_block, "tensor", 0)
    (
        down_share,
        up_share,
        out_share,
        qkv_share,
        gains_share,
        out_bias_share,
        head_bias_share,
        head_gain_share,
        unit_bias_share,
        unit_gain_share,
    ) = grad_shares
    return (
        layer_out,
        input_grad,
        gains_share,
        qkv_share,
        head_bias_share,
        head_gain_share,
        out_share,
        out_bias_share,
        up_share,
        unit_bias_share,
        unit_gain_share,
        down_share,
    )


def solution(mesh):
    placed = (
        P("shard", "context", None),
        P("shard", "context", None),
        P("shard", None),
        P("tensor", None),
        P("tensor", None),
        P(None, "shard"),
        P(None, "shard", "tensor"),
        P(None, "tensor", "shard"),
        P("tensor", "shard"),
        P("tensor", "shard"),
        P(None, "shard"),
        P("shard", "tensor"),
        P("tensor", "shard"),
        P("tensor", "shard"),
        P("tensor", "shard"),
    )
    return jax.shard_map(
        local,
        mesh=mesh,
        in_specs=placed,
        out_specs=(
            P("shard", "context", None),
            P("shard", "context", None),
            P(None, "shard"),
            P(None, "shard", "tensor"),
            P(None, "tensor", "shard"),
            P("tensor", "shard"),
            P("tensor", "shard"),
            P(None, "shard"),
            P("shard", "tensor"),
            P("tensor", "shard"),
            P("tensor", "shard"),
            P("tensor", "shard"),
        ),
        check_vma=False,
    )
```

```python
from functools import partial

import jax
import jax.numpy as jnp
from jax import lax
from jax.experimental import pallas as pl
from jax.experimental.pallas import tpu as pltpu
from jax.sharding import PartitionSpec as P

HD = 64
FF = 3072
PIECE = 256
PIECES = 2


epsilon = 1e-05
span_parts = (1, 2, 4, 6, 8)
dilation_rates = (1, 2, 4, 6, 12)


def pattern_total(query_position, key_position, segmented_offsets, dilated_offsets, token_length):
    tallied_total = jnp.zeros(
        (segmented_offsets.shape[0], query_position.shape[0], key_position.shape[0]), jnp.float32
    )
    for item_number in range(len(span_parts)):
        segmented_span = token_length * span_parts[item_number] // 8
        dilated_stride = dilation_rates[item_number]
        seg_shift = (segmented_offsets[:, item_number] % segmented_span)[:, None, None]
        dilated_phase = (dilated_offsets[:, item_number] % dilated_stride)[:, None, None]
        query_lookup = query_position[None, :, None] + seg_shift
        key_lookup = key_position[None, None, :] + seg_shift
        merged_heads = (
            (query_lookup // segmented_span == key_lookup // segmented_span)
            & (query_lookup % dilated_stride == dilated_phase)
            & (key_lookup % dilated_stride == dilated_phase)
        )
        tallied_total = tallied_total + merged_heads.astype(jnp.float32)
    return tallied_total


def picture_index(starts, token_positions):
    marked = jnp.zeros((starts.shape[0], token_positions.shape[0]), jnp.int32)
    for piece_number in range(starts.shape[1]):
        begin_at = starts[:, piece_number][:, None]
        inside = (token_positions[None, :] >= begin_at) & (
            token_positions[None, :] < begin_at + PIECE
        )
        marked = marked + (piece_number + 1) * inside.astype(jnp.int32)
    return marked


def allowed_keys(query_pic, key_pic, query_position, key_position):
    causal_ok = key_position[None, None, :] <= query_position[None, :, None]
    same_piece = (query_pic[:, :, None] == key_pic[:, None, :]) & (query_pic[:, :, None] > 0)
    return (causal_ok | same_piece).astype(jnp.float32)


def outer_sum(left_rows, right_rows):
    return lax.dot_general(
        left_rows, right_rows, (((0,), (0,)), ((), ())), preferred_element_type=jnp.float32
    )


def back_dot(left_rows, weight_rows):
    return lax.dot_general(
        left_rows, weight_rows, (((1,), (1,)), ((), ())), preferred_element_type=jnp.float32
    )


def norm_rows(values, scale_row):
    mean_row = jnp.mean(values, -1, keepdims=True)
    centered = values - mean_row
    inv_std = lax.rsqrt(jnp.mean(centered * centered, -1, keepdims=True) + epsilon)
    normed = centered * inv_std
    return (normed, inv_std, normed * scale_row)


def norm_back(normed, inv_std, scale_row, grad_rows):
    scaled = grad_rows * scale_row
    mean_plain = jnp.mean(scaled, -1, keepdims=True)
    mean_cross = jnp.mean(scaled * normed, -1, keepdims=True)
    return (inv_std * (scaled - mean_plain - normed * mean_cross), jnp.sum(grad_rows * normed, 0))


def probabilities(query_heads, key_heads, mask_table):
    raw_scores = jnp.einsum(
        "sqhd,skhd->shqk", query_heads, key_heads, preferred_element_type=jnp.float32
    ) * HD ** (-0.5)
    masked = jnp.where(mask_table > 0, raw_scores, -1000000000.0)
    row_top = jnp.max(masked, -1, keepdims=True)
    exponent = mask_table * jnp.exp(masked - row_top)
    row_total = jnp.sum(exponent, -1, keepdims=True)
    return (exponent / row_total, row_top, row_total)


SCALE = HD ** (-0.5)
HIDDEN = -1000000000.0
PAIR = 2
CODE_WIDTH = 8


def pair_masks(patq_ref, patk_ref, pcq_ref, pck_ref):
    first_q = patq_ref[0]
    first_k = patk_ref[0]
    row = first_q[:, 5:6]
    col = first_k[5:6, :]
    piece_q = pcq_ref[0][:, 0:1]
    piece_k = pck_ref[0][0:1, :]
    allowed = (col <= row) | (piece_q == piece_k)
    masks = []
    for head in range(PAIR):
        codes_q = patq_ref[head]
        codes_k = patk_ref[head]
        tally = (codes_q[:, 0:1] == codes_k[0:1, :]).astype(jnp.float32)
        for pattern in range(1, len(span_parts)):
            tally = tally + (
                codes_q[:, pattern : pattern + 1] == codes_k[pattern : pattern + 1, :]
            ).astype(jnp.float32)
        masks.append(jnp.where(allowed, tally, 0.0))
    return masks


def soft_rows(query_part, key_block, mask):
    scores = (
        lax.dot_general(
            query_part, key_block, (((1,), (1,)), ((), ())), preferred_element_type=jnp.float32
        )
        * SCALE
    )
    masked = jnp.where(mask > 0, scores, HIDDEN)
    top = jnp.max(masked, axis=1, keepdims=True)
    exponent = mask * jnp.exp(masked - top)
    return exponent / jnp.sum(exponent, axis=1, keepdims=True)


def attention_fwd_kernel(q_ref, k_ref, v_ref, patq_ref, patk_ref, pcq_ref, pck_ref, o_ref):
    query = q_ref[0]
    key_block = k_ref[0]
    value_block = v_ref[0]
    first = lax.broadcasted_iota(jnp.int32, query.shape, 1) < HD
    masks = pair_masks(patq_ref, patk_ref, pcq_ref, pck_ref)
    result = None
    for head in range(PAIR):
        keep = first if head == 0 else jnp.logical_not(first)
        query_part = jnp.where(keep, query, jnp.zeros_like(query))
        probs = soft_rows(query_part, key_block, masks[head])
        mixed = jnp.dot(
            probs.astype(jnp.bfloat16), value_block, preferred_element_type=jnp.float32
        )
        result = mixed if result is None else jnp.where(first, result, mixed)
    o_ref[0] = result


def attention_bwd_kernel(
    q_ref, k_ref, v_ref, do_ref, patq_ref, patk_ref, pcq_ref, pck_ref, dq_ref, dk_ref, dv_ref
):
    @pl.when(pl.program_id(2) == 0)
    def _():
        dk_ref[...] = jnp.zeros_like(dk_ref)
        dv_ref[...] = jnp.zeros_like(dv_ref)

    query = q_ref[0]
    key_block = k_ref[0]
    value_block = v_ref[0]
    grad_out = do_ref[0]
    first = lax.broadcasted_iota(jnp.int32, query.shape, 1) < HD
    masks = pair_masks(patq_ref, patk_ref, pcq_ref, pck_ref)
    query_grad = None
    key_grad = dk_ref[0]
    value_grad = dv_ref[0]
    for head in range(PAIR):
        keep = first if head == 0 else jnp.logical_not(first)
        query_part = jnp.where(keep, query, jnp.zeros_like(query))
        grad_part = jnp.where(keep, grad_out, jnp.zeros_like(grad_out))
        probs = soft_rows(query_part, key_block, masks[head])
        prob_grad = lax.dot_general(
            grad_part, value_block, (((1,), (1,)), ((), ())), preferred_element_type=jnp.float32
        )
        inner = jnp.sum(probs * prob_grad, axis=1, keepdims=True)
        score_low = (probs * (prob_grad - inner)).astype(jnp.bfloat16)
        part = jnp.dot(score_low, key_block, preferred_element_type=jnp.float32)
        query_grad = part if query_grad is None else jnp.where(first, query_grad, part)
        key_grad = key_grad + SCALE * lax.dot_general(
            score_low, query_part, (((0,), (0,)), ((), ())), preferred_element_type=jnp.float32
        )
        value_grad = value_grad + lax.dot_general(
            probs.astype(jnp.bfloat16),
            grad_part,
            (((0,), (0,)), ((), ())),
            preferred_element_type=jnp.float32,
        )
    dq_ref[0] = (query_grad * SCALE).astype(jnp.bfloat16)
    dk_ref[0] = key_grad
    dv_ref[0] = value_grad


def attention_specs(seq_count, local_len, seq_len, block_q):
    lanes = PAIR * HD
    query_spec = pl.BlockSpec((1, block_q, lanes), lambda s, g, b: (s, b, g))
    key_spec = pl.BlockSpec((1, seq_len, lanes), lambda s, g, b: (s, 0, g))
    patq_spec = pl.BlockSpec((PAIR, block_q, CODE_WIDTH), lambda s, g, b: (g, b, 0))
    patk_spec = pl.BlockSpec((PAIR, CODE_WIDTH, seq_len), lambda s, g, b: (g, 0, 0))
    pcq_spec = pl.BlockSpec((1, block_q, CODE_WIDTH), lambda s, g, b: (s, b, 0))
    pck_spec = pl.BlockSpec((1, CODE_WIDTH, seq_len), lambda s, g, b: (s, 0, 0))
    return query_spec, key_spec, patq_spec, patk_spec, pcq_spec, pck_spec


def attention_forward(query, keys, values, codes):
    seq_count, local_len, width = query.shape
    seq_len = keys.shape[1]
    block_q = min(256, local_len)
    grid = (seq_count, width // (PAIR * HD), local_len // block_q)
    query_spec, key_spec, patq_spec, patk_spec, pcq_spec, pck_spec = attention_specs(
        seq_count, local_len, seq_len, block_q
    )
    flops = 8 * seq_count * local_len * seq_len * width
    return pl.pallas_call(
        attention_fwd_kernel,
        grid=grid,
        in_specs=[query_spec, key_spec, key_spec, patq_spec, patk_spec, pcq_spec, pck_spec],
        out_specs=query_spec,
        out_shape=jax.ShapeDtypeStruct((seq_count, local_len, width), jnp.float32),
        compiler_params=pltpu.CompilerParams(
            dimension_semantics=("parallel", "parallel", "arbitrary"),
            vmem_limit_bytes=48 * 1024 * 1024,
        ),
        cost_estimate=pl.CostEstimate(
            flops=flops,
            transcendentals=seq_count * local_len * seq_len * width // HD,
            bytes_accessed=2 * query.size + 2 * keys.size * 2 * (local_len // block_q) + 4 * query.size,
        ),
    )(query, keys, values, *codes)


def attention_backward(query, keys, values, grad_out, codes):
    seq_count, local_len, width = query.shape
    seq_len = keys.shape[1]
    block_q = min(256, local_len)
    grid = (seq_count, width // (PAIR * HD), local_len // block_q)
    query_spec, key_spec, patq_spec, patk_spec, pcq_spec, pck_spec = attention_specs(
        seq_count, local_len, seq_len, block_q
    )
    flops = 20 * seq_count * local_len * seq_len * width
    return pl.pallas_call(
        attention_bwd_kernel,
        grid=grid,
        in_specs=[
            query_spec,
            key_spec,
            key_spec,
            query_spec,
            patq_spec,
            patk_spec,
            pcq_spec,
            pck_spec,
        ],
        out_specs=[query_spec, key_spec, key_spec],
        out_shape=[
            jax.ShapeDtypeStruct((seq_count, local_len, width), jnp.bfloat16),
            jax.ShapeDtypeStruct((seq_count, seq_len, width), jnp.float32),
            jax.ShapeDtypeStruct((seq_count, seq_len, width), jnp.float32),
        ],
        compiler_params=pltpu.CompilerParams(
            dimension_semantics=("parallel", "parallel", "arbitrary"),
            vmem_limit_bytes=48 * 1024 * 1024,
        ),
        cost_estimate=pl.CostEstimate(
            flops=flops,
            transcendentals=seq_count * local_len * seq_len * width // HD,
            bytes_accessed=4 * query.size + 2 * keys.size * 2 * (local_len // block_q) + 16 * keys.size,
        ),
    )(query, keys, values, grad_out, *codes)


def mask_codes(starts, query_position, key_position, segment_offsets, dilation_offsets, seq_len):
    heads = segment_offsets.shape[0]
    query_codes = []
    key_codes = []
    for pattern in range(len(span_parts)):
        span = seq_len * span_parts[pattern] // 8
        rate = dilation_rates[pattern]
        shift = (segment_offsets[:, pattern] % span)[:, None]
        phase = (dilation_offsets[:, pattern] % rate)[:, None]
        query_at = query_position[None, :] + shift
        key_at = key_position[None, :] + shift
        query_codes.append(jnp.where(query_at % rate == phase, query_at // span, -1))
        key_codes.append(jnp.where(key_at % rate == phase, key_at // span, -2))
    patterns = len(span_parts)
    query_codes.append(jnp.broadcast_to(query_position[None, :], (heads, query_position.shape[0])))
    key_codes.append(jnp.broadcast_to(key_position[None, :], (heads, key_position.shape[0])))
    filler = CODE_WIDTH - patterns - 1
    query_codes += [jnp.zeros((heads, query_position.shape[0]), jnp.int32)] * filler
    key_codes += [jnp.zeros((heads, key_position.shape[0]), jnp.int32)] * filler
    patq = jnp.stack(query_codes, 2).astype(jnp.int32)
    patk = jnp.stack(key_codes, 1).astype(jnp.int32)
    query_pic = picture_index(starts, query_position)
    key_pic = picture_index(starts, key_position)
    pcq = jnp.where(query_pic > 0, query_pic, -1)[:, :, None]
    pcq = jnp.pad(pcq, ((0, 0), (0, 0), (0, CODE_WIDTH - 1)))
    pck = jnp.where(key_pic > 0, key_pic, -2)[:, None, :]
    pck = jnp.pad(pck, ((0, 0), (0, CODE_WIDTH - 1), (0, 0)))
    return (patq, patk, pcq.astype(jnp.int32), pck.astype(jnp.int32))


def code_part(codes, begin, end, key_end):
    patq, patk, pcq, pck = codes
    return (patq[:, begin:end], patk[:, :, :key_end], pcq[:, begin:end], pck[:, :, :key_end])


def split_attention_forward(query, keys, values, codes, span):
    if span is None:
        return attention_forward(query, keys, values, codes)
    head = attention_forward(
        query[:, :span], keys[:, :span], values[:, :span], code_part(codes, 0, span, span)
    )
    seq_len = keys.shape[1]
    tail = attention_forward(
        query[:, span:], keys, values, code_part(codes, span, query.shape[1], seq_len)
    )
    return jnp.concatenate([head, tail], 1)


def split_attention_backward(query, keys, values, grad_out, codes, span):
    if span is None:
        return attention_backward(query, keys, values, grad_out, codes)
    seq_len = keys.shape[1]
    head_q, head_k, head_v = attention_backward(
        query[:, :span],
        keys[:, :span],
        values[:, :span],
        grad_out[:, :span],
        code_part(codes, 0, span, span),
    )
    tail_q, tail_k, tail_v = attention_backward(
        query[:, span:],
        keys,
        values,
        grad_out[:, span:],
        code_part(codes, span, query.shape[1], seq_len),
    )
    padding = ((0, 0), (0, seq_len - span), (0, 0))
    return (
        jnp.concatenate([head_q, tail_q], 1),
        tail_k + jnp.pad(head_k, padding),
        tail_v + jnp.pad(head_v, padding),
    )


def spread_sequence(block, local_len):
    me_c = lax.axis_index("context")
    me_t = lax.axis_index("tensor")
    swap = [(0, 1), (1, 0)]
    kept = lax.dynamic_slice_in_dim(block, me_c * local_len, local_len, 1)
    other = lax.dynamic_slice_in_dim(block, (1 - me_c) * local_len, local_len, 1)
    from_context = lax.ppermute(other, "context", perm=swap)
    from_tensor = lax.ppermute(kept, "tensor", perm=swap)
    from_corner = lax.ppermute(other, ("context", "tensor"), perm=[(0, 3), (3, 0), (1, 2), (2, 1)])
    first_c = me_c == 0
    own_pair = jnp.where(
        first_c,
        jnp.concatenate([kept, from_context], 0),
        jnp.concatenate([from_context, kept], 0),
    )
    far_pair = jnp.where(
        first_c,
        jnp.concatenate([from_tensor, from_corner], 0),
        jnp.concatenate([from_corner, from_tensor], 0),
    )
    return jnp.where(
        me_t == 0,
        jnp.concatenate([own_pair, far_pair], 0),
        jnp.concatenate([far_pair, own_pair], 0),
    )


def assemble(stacked, shard_dim, tensor_dim):
    ns, nt = stacked.shape[0], stacked.shape[1]
    if shard_dim is None:
        stacked = stacked[:1]
    if tensor_dim is None:
        stacked = stacked[:, :1]
    local_shape = stacked.shape[2:]
    order = []
    for dim in range(len(local_shape)):
        if dim == shard_dim:
            order.append(0)
        if dim == tensor_dim:
            order.append(1)
        order.append(dim + 2)
    if shard_dim is None:
        order = [0] + order
    if tensor_dim is None:
        order = [1] + order
    moved = stacked.transpose(order)
    full_shape = list(local_shape)
    if shard_dim is not None:
        full_shape[shard_dim] *= ns
    if tensor_dim is not None:
        full_shape[tensor_dim] *= nt
    return moved.reshape(full_shape)


def gather_weight(local_block, shard_dim, tensor_dim):
    ns = lax.axis_size("shard")
    nt = lax.axis_size("tensor")
    stacked = lax.all_gather(local_block, ("shard", "tensor"), axis=0, tiled=False)
    return assemble(stacked.reshape((ns, nt) + local_block.shape), shard_dim, tensor_dim)


def gather_packed(blocks):
    ns = lax.axis_size("shard")
    nt = lax.axis_size("tensor")
    flat = jnp.concatenate([block.reshape(-1) for block, _, _ in blocks])
    padded = -flat.size % 2048
    flat = jnp.pad(flat, (0, padded)).reshape(-1, 128)
    stacked = lax.all_gather(flat, ("shard", "tensor"), axis=0, tiled=False).reshape(ns, nt, -1)
    pieces = []
    offset = 0
    for block, shard_dim, tensor_dim in blocks:
        part = stacked[:, :, offset : offset + block.size].reshape((ns, nt) + block.shape)
        pieces.append(assemble(part, shard_dim, tensor_dim))
        offset += block.size
    return pieces


def pair_gather(block, axis_name, dim):
    if lax.axis_size(axis_name) != 2:
        return lax.all_gather(block, axis_name, axis=dim, tiled=True)
    other = lax.ppermute(block, axis_name, perm=[(0, 1), (1, 0)])
    first = lax.axis_index(axis_name) == 0
    return jnp.where(
        first, jnp.concatenate([block, other], dim), jnp.concatenate([other, block], dim)
    )


def pair_reduce(full, axis_name, dim):
    if lax.axis_size(axis_name) != 2:
        return lax.psum_scatter(
            full.astype(jnp.bfloat16), axis_name, scatter_dimension=dim, tiled=True
        ).astype(jnp.float32)
    half = full.shape[dim] // 2
    me = lax.axis_index(axis_name)
    kept = lax.dynamic_slice_in_dim(full, me * half, half, dim)
    sent = lax.dynamic_slice_in_dim(full, (1 - me) * half, half, dim).astype(jnp.bfloat16)
    received = lax.ppermute(sent, axis_name, perm=[(0, 1), (1, 0)])
    return kept + received.astype(jnp.float32)


def pair_sum(share, axis_name):
    if lax.axis_size(axis_name) != 2:
        return lax.psum(share, axis_name).astype(jnp.float32)
    received = lax.ppermute(share, axis_name, perm=[(0, 1), (1, 0)])
    return share.astype(jnp.float32) + received.astype(jnp.float32)


def disassemble(full, shard_dim, tensor_dim):
    ns = lax.axis_size("shard")
    nt = lax.axis_size("tensor")
    split_shape = []
    positions = {}
    for dim, size in enumerate(full.shape):
        if dim == shard_dim:
            positions["s"] = len(split_shape)
            split_shape += [ns, size // ns]
        elif dim == tensor_dim:
            positions["t"] = len(split_shape)
            split_shape += [nt, size // nt]
        else:
            split_shape.append(size)
    pieces = full.reshape(split_shape)
    lead = [positions[key] for key in ("s", "t") if key in positions]
    rest = [d for d in range(len(split_shape)) if d not in lead]
    pieces = pieces.transpose(lead + rest)
    if "s" not in positions:
        pieces = jnp.broadcast_to(pieces[None], (ns,) + pieces.shape)
    if "t" not in positions:
        pieces = jnp.broadcast_to(pieces[:, None], (ns, nt) + pieces.shape[1:])
    return pieces.reshape(ns * nt, -1)


def pack_rows(terms):
    rows = jnp.concatenate(
        [disassemble(full.astype(jnp.bfloat16), shard_dim, tensor_dim) for full, shard_dim, tensor_dim in terms],
        1,
    )
    width = rows.shape[1]
    return jnp.pad(rows, ((0, 0), (0, -width % 1024))).reshape(rows.shape[0], -1, 128)


def scatter_rows(rows):
    return lax.psum_scatter(rows, ("shard", "tensor"), scatter_dimension=0, tiled=False)


def unpack_share(share, terms):
    total = pair_sum(share, "context").reshape(-1)
    pieces = []
    offset = 0
    ns = lax.axis_size("shard")
    nt = lax.axis_size("tensor")
    for full, shard_dim, tensor_dim in terms:
        local_shape = list(full.shape)
        if shard_dim is not None:
            local_shape[shard_dim] //= ns
        if tensor_dim is not None:
            local_shape[tensor_dim] //= nt
        count = 1
        for size in local_shape:
            count *= size
        pieces.append(total[offset : offset + count].reshape(local_shape))
        offset += count
    return pieces


def shard_stage(grad, dim):
    return lax.psum_scatter(grad.astype(jnp.bfloat16), "shard", scatter_dimension=dim, tiled=True)


def finish_stage(share, tensor_dim):
    summed = pair_reduce(share, "tensor", tensor_dim)
    return pair_sum(summed.astype(jnp.bfloat16), "context")


def forward_pass(block_in, codes, weights, span):
    w_qkv, w_out, w_up, w_down, norm_gains, out_biases, head_biases, head_gain, unit_bias, unit_gain = weights
    seq_count, local_len, model_width = block_in.shape
    row_count = seq_count * local_len
    flattened_input = block_in.reshape(row_count, model_width).astype(jnp.float32)
    first_normed, first_inv, first_out = norm_rows(flattened_input, norm_gains[0])
    attn_in = first_out.astype(jnp.bfloat16)
    projected = jnp.einsum("rd,jde->jre", attn_in, w_qkv, preferred_element_type=jnp.float32)
    query_matrix = (projected[0] + head_biases[0]).astype(jnp.bfloat16)
    keys_local = projected[1].astype(jnp.bfloat16).reshape(seq_count, local_len, model_width)
    values_local = (projected[2] + head_biases[1]).astype(jnp.bfloat16).reshape(
        seq_count, local_len, model_width
    )
    if span is None:
        key_all = pair_gather(keys_local, "context", 1)
        value_all = pair_gather(values_local, "context", 1)
    else:
        key_all, value_all = keys_local, values_local
    attended = split_attention_forward(
        query_matrix.reshape(seq_count, local_len, model_width), key_all, value_all, codes, span
    ).reshape(row_count, model_width)
    sub_normed, sub_inv, sub_out = norm_rows(attended, head_gain)
    sub_in = sub_out.astype(jnp.bfloat16)
    middle = flattened_input + (
        jnp.dot(sub_in, w_out, preferred_element_type=jnp.float32) + out_biases[0]
    )
    second_normed, second_inv, second_out = norm_rows(middle, norm_gains[1])
    ffn_in = second_out.astype(jnp.bfloat16)
    hidden = jnp.dot(ffn_in, w_up, preferred_element_type=jnp.float32) + unit_bias
    activated = jax.nn.gelu(hidden, approximate=True)
    unit_normed, unit_inv, unit_out = norm_rows(activated, unit_gain)
    ffn_mid = unit_out.astype(jnp.bfloat16)
    layer_out = (
        middle + (jnp.dot(ffn_mid, w_down, preferred_element_type=jnp.float32) + out_biases[1])
    ).astype(jnp.bfloat16)
    kept_state = (
        attn_in,
        first_normed,
        first_inv,
        query_matrix,
        key_all,
        value_all,
        codes,
        sub_normed,
        sub_inv,
        sub_in,
        second_normed,
        second_inv,
        ffn_in,
        hidden,
        unit_normed,
        unit_inv,
        ffn_mid,
    )
    return (kept_state, layer_out.reshape(seq_count, local_len, model_width))


def backward_pass(kept_state, block_grad, weights, span):
    w_qkv, w_out, w_up, w_down, norm_gains, out_biases, head_biases, head_gain, unit_bias, unit_gain = weights
    (
        attn_in,
        first_normed,
        first_inv,
        query_matrix,
        key_all,
        value_all,
        codes,
        sub_normed,
        sub_inv,
        sub_in,
        second_normed,
        second_inv,
        ffn_in,
        hidden,
        unit_normed,
        unit_inv,
        ffn_mid,
    ) = kept_state
    seq_count, local_len, model_width = block_grad.shape
    row_count = seq_count * local_len
    seq_len = key_all.shape[1]
    grad_low = block_grad.reshape(row_count, model_width)
    grad_full = grad_low.astype(jnp.float32)
    down_grad = outer_sum(grad_low, ffn_mid)
    last_bias_grad = jnp.sum(grad_full, 0)
    unit_grad = back_dot(grad_low, w_down)
    activated_grad, unit_gain_grad = norm_back(unit_normed, unit_inv, unit_gain, unit_grad)
    gelu_value, gelu_pull = jax.vjp(partial(jax.nn.gelu, approximate=True), hidden)
    hidden_low = gelu_pull(activated_grad)[0].astype(jnp.bfloat16)
    up_grad = outer_sum(ffn_in, hidden_low)
    unit_bias_grad = jnp.sum(hidden_low, 0, dtype=jnp.float32)
    ffn_in_grad = back_dot(hidden_low, w_up)
    middle_part, second_gain_grad = norm_back(second_normed, second_inv, norm_gains[1], ffn_in_grad)
    middle_grad = grad_full + middle_part
    middle_low = middle_grad.astype(jnp.bfloat16)
    out_weight_grad = outer_sum(middle_low, sub_in)
    first_bias_grad = jnp.sum(middle_low, 0, dtype=jnp.float32)
    sub_grad = back_dot(middle_low, w_out)
    attended_grad, head_gain_grad = norm_back(sub_normed, sub_inv, head_gain, sub_grad)
    attended_low = attended_grad.astype(jnp.bfloat16)
    down_grad, up_grad, out_weight_grad, attended_low = lax.optimization_barrier(
        (
            down_grad.astype(jnp.bfloat16),
            up_grad.astype(jnp.bfloat16),
            out_weight_grad.astype(jnp.bfloat16),
            attended_low,
        )
    )
    down_share = shard_stage(down_grad, 0)
    up_share = shard_stage(up_grad, 0)
    out_share = shard_stage(out_weight_grad, 0)
    query_grad, key_part, value_part = split_attention_backward(
        query_matrix.reshape(seq_count, local_len, model_width),
        key_all,
        value_all,
        attended_low.reshape(seq_count, local_len, model_width),
        codes,
        span,
    )
    if span is not None:
        key_part = key_part.reshape(row_count, model_width)
        value_part = value_part.reshape(row_count, model_width)
    query_low = query_grad.reshape(row_count, model_width)
    if span is None:
        key_part = pair_reduce(key_part, "context", 1)
        value_part = pair_reduce(value_part, "context", 1)
    key_low = key_part.astype(jnp.bfloat16).reshape(row_count, model_width)
    value_low = value_part.astype(jnp.bfloat16).reshape(row_count, model_width)
    stacked = jnp.stack([query_low, key_low, value_low])
    down_share, up_share, stacked = lax.optimization_barrier((down_share, up_share, stacked))
    qkv_grad = jnp.einsum("rd,jre->dje", attn_in, stacked, preferred_element_type=jnp.float32)
    head_bias_grad = jnp.stack(
        [jnp.sum(query_low, 0, dtype=jnp.float32), jnp.sum(value_low, 0, dtype=jnp.float32)]
    )
    qkv_grad, stacked = lax.optimization_barrier((qkv_grad, stacked))
    attn_in_grad = jnp.einsum("jre,jde->rd", stacked, w_qkv, preferred_element_type=jnp.float32)
    input_part, first_gain_grad = norm_back(first_normed, first_inv, norm_gains[0], attn_in_grad)
    input_low = (middle_grad + input_part).astype(jnp.bfloat16)
    heads = model_width // HD
    unit_rows = unit_bias_grad.shape[0] // HD
    small_terms = (
        (jnp.stack([first_gain_grad, second_gain_grad]), 1, None),
        (jnp.stack([first_bias_grad, last_bias_grad]), 1, None),
        (head_bias_grad.reshape(2, heads, HD), 2, 1),
        (head_gain_grad.reshape(heads, HD), 1, 0),
        (unit_bias_grad.reshape(unit_rows, HD), 1, 0),
        (unit_gain_grad.reshape(unit_rows, HD), 1, 0),
    )
    ns = lax.axis_size("shard")
    nt = lax.axis_size("tensor")
    small_rows = jnp.concatenate(
        [disassemble(full, shard_dim, tensor_dim) for full, shard_dim, tensor_dim in small_terms], 1
    )
    small_width = small_rows.shape[1]
    block_rows = model_width // ns
    extra_rows = 8
    planes = qkv_grad.shape[1]
    slots = extra_rows * planes * (model_width // nt)
    small_block = (
        jnp.pad(small_rows, ((0, 0), (0, slots - small_width)))
        .reshape(ns, nt, extra_rows, planes, model_width // nt)
        .transpose(0, 2, 3, 1, 4)
        .reshape(ns, extra_rows, planes, model_width)
    )
    widened = jnp.concatenate(
        [qkv_grad.reshape(ns, block_rows, planes, model_width), small_block.astype(qkv_grad.dtype)], 1
    ).reshape(ns * (block_rows + extra_rows), planes, model_width)
    qkv_share = shard_stage(widened, 0)
    qkv_total = finish_stage(qkv_share, 2)
    small_total = qkv_total[block_rows:].reshape(-1)[:small_width]
    small_pieces = []
    offset = 0
    for full, shard_dim, tensor_dim in small_terms:
        local_shape = list(full.shape)
        if shard_dim is not None:
            local_shape[shard_dim] //= ns
        if tensor_dim is not None:
            local_shape[tensor_dim] //= nt
        count = 1
        for size in local_shape:
            count *= size
        small_pieces.append(small_total[offset : offset + count].reshape(local_shape))
        offset += count
    grad_shares = (
        finish_stage(down_share, 1).transpose(1, 0),
        finish_stage(up_share, 1),
        finish_stage(out_share, 1).transpose(1, 0),
        qkv_total[:block_rows].transpose(1, 0, 2),
    ) + tuple(small_pieces)
    return (grad_shares, input_low.reshape(seq_count, local_len, model_width))


def local(
    inputs,
    out_grad,
    picture_starts,
    segment_offsets,
    dilation_offsets,
    norm_gains,
    w_qkv,
    head_biases,
    head_gain,
    w_out,
    out_biases,
    w_up,
    unit_bias,
    unit_gain,
    w_down,
):
    local_seqs, local_len, model_width = inputs.shape
    tensor_count = lax.axis_size("tensor")
    context_count = lax.axis_size("context")
    seq_len = local_len * context_count
    key_position = jnp.arange(seq_len, dtype=jnp.int32)
    whole = context_count == 2 and tensor_count == 2 and local_seqs == 4
    if whole:
        span = seq_len // PIECES
        me_c = lax.axis_index("context")
        own_seq = lax.axis_index("tensor") * context_count + me_c
        partner_seq = lax.axis_index("tensor") * context_count + 1 - me_c
        swap = [(0, 1), (1, 0)]

        def own_sequence(rows):
            kept = lax.dynamic_slice_in_dim(rows, own_seq, 1, 0)
            sent = lax.dynamic_slice_in_dim(rows, partner_seq, 1, 0)
            received = lax.ppermute(sent, "context", perm=swap)
            return jnp.where(
                me_c == 0,
                jnp.concatenate([kept, received], 1),
                jnp.concatenate([received, kept], 1),
            )

        block_in = own_sequence(inputs)
        block_grad = own_sequence(out_grad)
        starts = lax.dynamic_slice_in_dim(picture_starts, own_seq, 1, 0)
        query_position = key_position
    else:
        span = None
        mine = local_seqs // tensor_count
        first_seq = lax.axis_index("tensor") * mine
        block_in = lax.dynamic_slice_in_dim(inputs, first_seq, mine, 0)
        block_grad = lax.dynamic_slice_in_dim(out_grad, first_seq, mine, 0)
        starts = lax.dynamic_slice_in_dim(picture_starts, first_seq, mine, 0)
        query_position = lax.axis_index("context") * local_len + jnp.arange(
            local_len, dtype=jnp.int32
        )
    spans = jnp.array([seq_len * part // 8 for part in span_parts], jnp.int32)
    rates = jnp.array(dilation_rates, jnp.int32)
    segment_kept = segment_offsets % spans
    dilation_kept = dilation_offsets % rates
    offset_digits = jnp.concatenate(
        [segment_kept // 32, segment_kept % 32, dilation_kept], 1
    ).astype(jnp.bfloat16)
    f32 = jnp.float32
    (
        w_qkv_full,
        gains_full,
        out_bias_full,
        head_bias_full,
        head_gain_full,
        unit_bias_full,
        unit_gain_full,
        digits_full,
    ) = gather_packed(
        (
            (w_qkv, 1, 2),
            (norm_gains, 1, None),
            (out_biases, 1, None),
            (head_biases, 2, 1),
            (head_gain, 1, 0),
            (unit_bias, 1, 0),
            (unit_gain, 1, 0),
            (offset_digits, None, 0),
        )
    )
    patterns = len(span_parts)
    digits_full = digits_full.astype(jnp.int32)
    all_segments = digits_full[:, :patterns] * 32 + digits_full[:, patterns : 2 * patterns]
    all_dilations = digits_full[:, 2 * patterns :]
    codes = mask_codes(starts, query_position, key_position, all_segments, all_dilations, seq_len)
    w_out, w_up, w_down, w_qkv_full = lax.optimization_barrier((w_out, w_up, w_down, w_qkv_full))
    weights = (
        w_qkv_full,
        gather_weight(w_out, 1, 0),
        gather_weight(w_up, 0, 1),
        gather_weight(w_down, 1, 0),
        gains_full.astype(f32),
        out_bias_full.astype(f32),
        head_bias_full.reshape(2, model_width).astype(f32),
        head_gain_full.reshape(model_width).astype(f32),
        unit_bias_full.reshape(-1).astype(f32),
        unit_gain_full.reshape(-1).astype(f32),
    )
    kept_state, layer_block = forward_pass(block_in, codes, weights, span)
    if whole:
        layer_out = spread_sequence(layer_block, local_len)
    else:
        layer_out = pair_gather(layer_block, "tensor", 0)
    grad_shares, input_block = backward_pass(kept_state, block_grad, weights, span)
    if whole:
        input_grad = spread_sequence(input_block, local_len)
    else:
        input_grad = pair_gather(input_block, "tensor", 0)
    (
        down_share,
        up_share,
        out_share,
        qkv_share,
        gains_share,
        out_bias_share,
        head_bias_share,
        head_gain_share,
        unit_bias_share,
        unit_gain_share,
    ) = grad_shares
    return (
        layer_out,
        input_grad,
        gains_share,
        qkv_share,
        head_bias_share,
        head_gain_share,
        out_share,
        out_bias_share,
        up_share,
        unit_bias_share,
        unit_gain_share,
        down_share,
    )


def solution(mesh):
    placed = (
        P("shard", "context", None),
        P("shard", "context", None),
        P("shard", None),
        P("tensor", None),
        P("tensor", None),
        P(None, "shard"),
        P(None, "shard", "tensor"),
        P(None, "tensor", "shard"),
        P("tensor", "shard"),
        P("tensor", "shard"),
        P(None, "shard"),
        P("shard", "tensor"),
        P("tensor", "shard"),
        P("tensor", "shard"),
        P("tensor", "shard"),
    )
    return jax.shard_map(
        local,
        mesh=mesh,
        in_specs=placed,
        out_specs=(
            P("shard", "context", None),
            P("shard", "context", None),
            P(None, "shard"),
            P(None, "shard", "tensor"),
            P(None, "tensor", "shard"),
            P("tensor", "shard"),
            P("tensor", "shard"),
            P(None, "shard"),
            P("shard", "tensor"),
            P("tensor", "shard"),
            P("tensor", "shard"),
            P("tensor", "shard"),
        ),
        check_vma=False,
    )
```

```python
from functools import partial

import jax
import jax.numpy as jnp
from jax import lax
from jax.experimental import pallas as pl
from jax.experimental.pallas import tpu as pltpu
from jax.sharding import PartitionSpec as P

HD = 64
FF = 3072
PIECE = 256
PIECES = 2


epsilon = 1e-05
span_parts = (1, 2, 4, 6, 8)
dilation_rates = (1, 2, 4, 6, 12)


def pattern_total(query_position, key_position, segmented_offsets, dilated_offsets, token_length):
    tallied_total = jnp.zeros(
        (segmented_offsets.shape[0], query_position.shape[0], key_position.shape[0]), jnp.float32
    )
    for item_number in range(len(span_parts)):
        segmented_span = token_length * span_parts[item_number] // 8
        dilated_stride = dilation_rates[item_number]
        seg_shift = (segmented_offsets[:, item_number] % segmented_span)[:, None, None]
        dilated_phase = (dilated_offsets[:, item_number] % dilated_stride)[:, None, None]
        query_lookup = query_position[None, :, None] + seg_shift
        key_lookup = key_position[None, None, :] + seg_shift
        merged_heads = (
            (query_lookup // segmented_span == key_lookup // segmented_span)
            & (query_lookup % dilated_stride == dilated_phase)
            & (key_lookup % dilated_stride == dilated_phase)
        )
        tallied_total = tallied_total + merged_heads.astype(jnp.float32)
    return tallied_total


def picture_index(starts, token_positions):
    marked = jnp.zeros((starts.shape[0], token_positions.shape[0]), jnp.int32)
    for piece_number in range(starts.shape[1]):
        begin_at = starts[:, piece_number][:, None]
        inside = (token_positions[None, :] >= begin_at) & (
            token_positions[None, :] < begin_at + PIECE
        )
        marked = marked + (piece_number + 1) * inside.astype(jnp.int32)
    return marked


def allowed_keys(query_pic, key_pic, query_position, key_position):
    causal_ok = key_position[None, None, :] <= query_position[None, :, None]
    same_piece = (query_pic[:, :, None] == key_pic[:, None, :]) & (query_pic[:, :, None] > 0)
    return (causal_ok | same_piece).astype(jnp.float32)


def outer_sum(left_rows, right_rows):
    return lax.dot_general(
        left_rows, right_rows, (((0,), (0,)), ((), ())), preferred_element_type=jnp.float32
    )


def back_dot(left_rows, weight_rows):
    return lax.dot_general(
        left_rows, weight_rows, (((1,), (1,)), ((), ())), preferred_element_type=jnp.float32
    )


def norm_rows(values, scale_row):
    mean_row = jnp.mean(values, -1, keepdims=True)
    centered = values - mean_row
    inv_std = lax.rsqrt(jnp.mean(centered * centered, -1, keepdims=True) + epsilon)
    normed = centered * inv_std
    return (normed, inv_std, normed * scale_row)


def norm_back(normed, inv_std, scale_row, grad_rows):
    scaled = grad_rows * scale_row
    mean_plain = jnp.mean(scaled, -1, keepdims=True)
    mean_cross = jnp.mean(scaled * normed, -1, keepdims=True)
    return (inv_std * (scaled - mean_plain - normed * mean_cross), jnp.sum(grad_rows * normed, 0))


def probabilities(query_heads, key_heads, mask_table):
    raw_scores = jnp.einsum(
        "sqhd,skhd->shqk", query_heads, key_heads, preferred_element_type=jnp.float32
    ) * HD ** (-0.5)
    masked = jnp.where(mask_table > 0, raw_scores, -1000000000.0)
    row_top = jnp.max(masked, -1, keepdims=True)
    exponent = mask_table * jnp.exp(masked - row_top)
    row_total = jnp.sum(exponent, -1, keepdims=True)
    return (exponent / row_total, row_top, row_total)


SCALE = HD ** (-0.5)
HIDDEN = -1000000000.0
PAIR = 2
CODE_WIDTH = 8


def pair_masks(patq_ref, patk_ref, pcq_ref, pck_ref):
    first_q = patq_ref[0]
    first_k = patk_ref[0]
    row = first_q[:, 5:6]
    col = first_k[5:6, :]
    piece_q = pcq_ref[0][:, 0:1]
    piece_k = pck_ref[0][0:1, :]
    allowed = (col <= row) | (piece_q == piece_k)
    masks = []
    for head in range(PAIR):
        codes_q = patq_ref[head]
        codes_k = patk_ref[head]
        tally = (codes_q[:, 0:1] == codes_k[0:1, :]).astype(jnp.float32)
        for pattern in range(1, len(span_parts)):
            tally = tally + (
                codes_q[:, pattern : pattern + 1] == codes_k[pattern : pattern + 1, :]
            ).astype(jnp.float32)
        masks.append(jnp.where(allowed, tally, 0.0))
    return masks


def soft_rows(query_part, key_block, mask):
    scores = (
        lax.dot_general(
            query_part, key_block, (((1,), (1,)), ((), ())), preferred_element_type=jnp.float32
        )
        * SCALE
    )
    masked = jnp.where(mask > 0, scores, HIDDEN)
    top = jnp.max(masked, axis=1, keepdims=True)
    exponent = mask * jnp.exp(masked - top)
    return exponent / jnp.sum(exponent, axis=1, keepdims=True)


def attention_fwd_kernel(q_ref, k_ref, v_ref, patq_ref, patk_ref, pcq_ref, pck_ref, o_ref):
    query = q_ref[0]
    key_block = k_ref[0]
    value_block = v_ref[0]
    first = lax.broadcasted_iota(jnp.int32, query.shape, 1) < HD
    masks = pair_masks(patq_ref, patk_ref, pcq_ref, pck_ref)
    result = None
    for head in range(PAIR):
        keep = first if head == 0 else jnp.logical_not(first)
        query_part = jnp.where(keep, query, jnp.zeros_like(query))
        probs = soft_rows(query_part, key_block, masks[head])
        mixed = jnp.dot(
            probs.astype(jnp.bfloat16), value_block, preferred_element_type=jnp.float32
        )
        result = mixed if result is None else jnp.where(first, result, mixed)
    o_ref[0] = result


def attention_bwd_kernel(
    q_ref, k_ref, v_ref, do_ref, patq_ref, patk_ref, pcq_ref, pck_ref, dq_ref, dk_ref, dv_ref
):
    @pl.when(pl.program_id(2) == 0)
    def _():
        dk_ref[...] = jnp.zeros_like(dk_ref)
        dv_ref[...] = jnp.zeros_like(dv_ref)

    query = q_ref[0]
    key_block = k_ref[0]
    value_block = v_ref[0]
    grad_out = do_ref[0]
    first = lax.broadcasted_iota(jnp.int32, query.shape, 1) < HD
    masks = pair_masks(patq_ref, patk_ref, pcq_ref, pck_ref)
    query_grad = None
    key_grad = dk_ref[0]
    value_grad = dv_ref[0]
    for head in range(PAIR):
        keep = first if head == 0 else jnp.logical_not(first)
        query_part = jnp.where(keep, query, jnp.zeros_like(query))
        grad_part = jnp.where(keep, grad_out, jnp.zeros_like(grad_out))
        probs = soft_rows(query_part, key_block, masks[head])
        prob_grad = lax.dot_general(
            grad_part, value_block, (((1,), (1,)), ((), ())), preferred_element_type=jnp.float32
        )
        inner = jnp.sum(probs * prob_grad, axis=1, keepdims=True)
        score_low = (probs * (prob_grad - inner)).astype(jnp.bfloat16)
        part = jnp.dot(score_low, key_block, preferred_element_type=jnp.float32)
        query_grad = part if query_grad is None else jnp.where(first, query_grad, part)
        key_grad = key_grad + SCALE * lax.dot_general(
            score_low, query_part, (((0,), (0,)), ((), ())), preferred_element_type=jnp.float32
        )
        value_grad = value_grad + lax.dot_general(
            probs.astype(jnp.bfloat16),
            grad_part,
            (((0,), (0,)), ((), ())),
            preferred_element_type=jnp.float32,
        )
    dq_ref[0] = (query_grad * SCALE).astype(jnp.bfloat16)
    dk_ref[0] = key_grad
    dv_ref[0] = value_grad


def attention_specs(seq_count, local_len, seq_len, block_q):
    lanes = PAIR * HD
    query_spec = pl.BlockSpec((1, block_q, lanes), lambda s, g, b: (s, b, g))
    key_spec = pl.BlockSpec((1, seq_len, lanes), lambda s, g, b: (s, 0, g))
    patq_spec = pl.BlockSpec((PAIR, block_q, CODE_WIDTH), lambda s, g, b: (g, b, 0))
    patk_spec = pl.BlockSpec((PAIR, CODE_WIDTH, seq_len), lambda s, g, b: (g, 0, 0))
    pcq_spec = pl.BlockSpec((1, block_q, CODE_WIDTH), lambda s, g, b: (s, b, 0))
    pck_spec = pl.BlockSpec((1, CODE_WIDTH, seq_len), lambda s, g, b: (s, 0, 0))
    return query_spec, key_spec, patq_spec, patk_spec, pcq_spec, pck_spec


def attention_forward(query, keys, values, codes):
    seq_count, local_len, width = query.shape
    seq_len = keys.shape[1]
    block_q = min(256, local_len)
    grid = (seq_count, width // (PAIR * HD), local_len // block_q)
    query_spec, key_spec, patq_spec, patk_spec, pcq_spec, pck_spec = attention_specs(
        seq_count, local_len, seq_len, block_q
    )
    flops = 8 * seq_count * local_len * seq_len * width
    return pl.pallas_call(
        attention_fwd_kernel,
        grid=grid,
        in_specs=[query_spec, key_spec, key_spec, patq_spec, patk_spec, pcq_spec, pck_spec],
        out_specs=query_spec,
        out_shape=jax.ShapeDtypeStruct((seq_count, local_len, width), jnp.float32),
        compiler_params=pltpu.CompilerParams(
            dimension_semantics=("parallel", "parallel", "arbitrary"),
            vmem_limit_bytes=48 * 1024 * 1024,
        ),
        cost_estimate=pl.CostEstimate(
            flops=flops,
            transcendentals=seq_count * local_len * seq_len * width // HD,
            bytes_accessed=2 * query.size + 2 * keys.size * 2 * (local_len // block_q) + 4 * query.size,
        ),
    )(query, keys, values, *codes)


def attention_backward(query, keys, values, grad_out, codes):
    seq_count, local_len, width = query.shape
    seq_len = keys.shape[1]
    block_q = min(256, local_len)
    grid = (seq_count, width // (PAIR * HD), local_len // block_q)
    query_spec, key_spec, patq_spec, patk_spec, pcq_spec, pck_spec = attention_specs(
        seq_count, local_len, seq_len, block_q
    )
    flops = 20 * seq_count * local_len * seq_len * width
    return pl.pallas_call(
        attention_bwd_kernel,
        grid=grid,
        in_specs=[
            query_spec,
            key_spec,
            key_spec,
            query_spec,
            patq_spec,
            patk_spec,
            pcq_spec,
            pck_spec,
        ],
        out_specs=[query_spec, key_spec, key_spec],
        out_shape=[
            jax.ShapeDtypeStruct((seq_count, local_len, width), jnp.bfloat16),
            jax.ShapeDtypeStruct((seq_count, seq_len, width), jnp.float32),
            jax.ShapeDtypeStruct((seq_count, seq_len, width), jnp.float32),
        ],
        compiler_params=pltpu.CompilerParams(
            dimension_semantics=("parallel", "parallel", "arbitrary"),
            vmem_limit_bytes=48 * 1024 * 1024,
        ),
        cost_estimate=pl.CostEstimate(
            flops=flops,
            transcendentals=seq_count * local_len * seq_len * width // HD,
            bytes_accessed=4 * query.size + 2 * keys.size * 2 * (local_len // block_q) + 16 * keys.size,
        ),
    )(query, keys, values, grad_out, *codes)


def mask_codes(starts, query_position, key_position, segment_offsets, dilation_offsets, seq_len):
    heads = segment_offsets.shape[0]
    query_codes = []
    key_codes = []
    for pattern in range(len(span_parts)):
        span = seq_len * span_parts[pattern] // 8
        rate = dilation_rates[pattern]
        shift = (segment_offsets[:, pattern] % span)[:, None]
        phase = (dilation_offsets[:, pattern] % rate)[:, None]
        query_at = query_position[None, :] + shift
        key_at = key_position[None, :] + shift
        query_codes.append(jnp.where(query_at % rate == phase, query_at // span, -1))
        key_codes.append(jnp.where(key_at % rate == phase, key_at // span, -2))
    patterns = len(span_parts)
    query_codes.append(jnp.broadcast_to(query_position[None, :], (heads, query_position.shape[0])))
    key_codes.append(jnp.broadcast_to(key_position[None, :], (heads, key_position.shape[0])))
    filler = CODE_WIDTH - patterns - 1
    query_codes += [jnp.zeros((heads, query_position.shape[0]), jnp.int32)] * filler
    key_codes += [jnp.zeros((heads, key_position.shape[0]), jnp.int32)] * filler
    patq = jnp.stack(query_codes, 2).astype(jnp.int32)
    patk = jnp.stack(key_codes, 1).astype(jnp.int32)
    query_pic = picture_index(starts, query_position)
    key_pic = picture_index(starts, key_position)
    pcq = jnp.where(query_pic > 0, query_pic, -1)[:, :, None]
    pcq = jnp.pad(pcq, ((0, 0), (0, 0), (0, CODE_WIDTH - 1)))
    pck = jnp.where(key_pic > 0, key_pic, -2)[:, None, :]
    pck = jnp.pad(pck, ((0, 0), (0, CODE_WIDTH - 1), (0, 0)))
    return (patq, patk, pcq.astype(jnp.int32), pck.astype(jnp.int32))


def code_part(codes, begin, end, key_end):
    patq, patk, pcq, pck = codes
    return (patq[:, begin:end], patk[:, :, :key_end], pcq[:, begin:end], pck[:, :, :key_end])


def split_attention_forward(query, keys, values, codes, span):
    if span is None:
        return attention_forward(query, keys, values, codes)
    head = attention_forward(
        query[:, :span], keys[:, :span], values[:, :span], code_part(codes, 0, span, span)
    )
    seq_len = keys.shape[1]
    tail = attention_forward(
        query[:, span:], keys, values, code_part(codes, span, query.shape[1], seq_len)
    )
    return jnp.concatenate([head, tail], 1)


def split_attention_backward(query, keys, values, grad_out, codes, span):
    if span is None:
        return attention_backward(query, keys, values, grad_out, codes)
    seq_len = keys.shape[1]
    head_q, head_k, head_v = attention_backward(
        query[:, :span],
        keys[:, :span],
        values[:, :span],
        grad_out[:, :span],
        code_part(codes, 0, span, span),
    )
    tail_q, tail_k, tail_v = attention_backward(
        query[:, span:],
        keys,
        values,
        grad_out[:, span:],
        code_part(codes, span, query.shape[1], seq_len),
    )
    padding = ((0, 0), (0, seq_len - span), (0, 0))
    return (
        jnp.concatenate([head_q, tail_q], 1),
        tail_k + jnp.pad(head_k, padding),
        tail_v + jnp.pad(head_v, padding),
    )


def spread_sequence(block, local_len):
    me_c = lax.axis_index("context")
    me_t = lax.axis_index("tensor")
    swap = [(0, 1), (1, 0)]
    kept = lax.dynamic_slice_in_dim(block, me_c * local_len, local_len, 1)
    other = lax.dynamic_slice_in_dim(block, (1 - me_c) * local_len, local_len, 1)
    from_context = lax.ppermute(other, "context", perm=swap)
    from_tensor = lax.ppermute(kept, "tensor", perm=swap)
    from_corner = lax.ppermute(other, ("context", "tensor"), perm=[(0, 3), (3, 0), (1, 2), (2, 1)])
    first_c = me_c == 0
    own_pair = jnp.where(
        first_c,
        jnp.concatenate([kept, from_context], 0),
        jnp.concatenate([from_context, kept], 0),
    )
    far_pair = jnp.where(
        first_c,
        jnp.concatenate([from_tensor, from_corner], 0),
        jnp.concatenate([from_corner, from_tensor], 0),
    )
    return jnp.where(
        me_t == 0,
        jnp.concatenate([own_pair, far_pair], 0),
        jnp.concatenate([far_pair, own_pair], 0),
    )


def assemble(stacked, shard_dim, tensor_dim):
    ns, nt = stacked.shape[0], stacked.shape[1]
    if shard_dim is None:
        stacked = stacked[:1]
    if tensor_dim is None:
        stacked = stacked[:, :1]
    local_shape = stacked.shape[2:]
    order = []
    for dim in range(len(local_shape)):
        if dim == shard_dim:
            order.append(0)
        if dim == tensor_dim:
            order.append(1)
        order.append(dim + 2)
    if shard_dim is None:
        order = [0] + order
    if tensor_dim is None:
        order = [1] + order
    moved = stacked.transpose(order)
    full_shape = list(local_shape)
    if shard_dim is not None:
        full_shape[shard_dim] *= ns
    if tensor_dim is not None:
        full_shape[tensor_dim] *= nt
    return moved.reshape(full_shape)


def gather_weight(local_block, shard_dim, tensor_dim):
    ns = lax.axis_size("shard")
    nt = lax.axis_size("tensor")
    stacked = lax.all_gather(local_block, ("shard", "tensor"), axis=0, tiled=False)
    return assemble(stacked.reshape((ns, nt) + local_block.shape), shard_dim, tensor_dim)


def gather_packed(blocks):
    ns = lax.axis_size("shard")
    nt = lax.axis_size("tensor")
    flat = jnp.concatenate([block.reshape(-1) for block, _, _ in blocks])
    padded = -flat.size % 2048
    flat = jnp.pad(flat, (0, padded)).reshape(-1, 128)
    stacked = lax.all_gather(flat, ("shard", "tensor"), axis=0, tiled=False).reshape(ns, nt, -1)
    pieces = []
    offset = 0
    for block, shard_dim, tensor_dim in blocks:
        part = stacked[:, :, offset : offset + block.size].reshape((ns, nt) + block.shape)
        pieces.append(assemble(part, shard_dim, tensor_dim))
        offset += block.size
    return pieces


def pair_gather(block, axis_name, dim):
    if lax.axis_size(axis_name) != 2:
        return lax.all_gather(block, axis_name, axis=dim, tiled=True)
    other = lax.ppermute(block, axis_name, perm=[(0, 1), (1, 0)])
    first = lax.axis_index(axis_name) == 0
    return jnp.where(
        first, jnp.concatenate([block, other], dim), jnp.concatenate([other, block], dim)
    )


def pair_reduce(full, axis_name, dim):
    if lax.axis_size(axis_name) != 2:
        return lax.psum_scatter(
            full.astype(jnp.bfloat16), axis_name, scatter_dimension=dim, tiled=True
        ).astype(jnp.float32)
    half = full.shape[dim] // 2
    me = lax.axis_index(axis_name)
    kept = lax.dynamic_slice_in_dim(full, me * half, half, dim)
    sent = lax.dynamic_slice_in_dim(full, (1 - me) * half, half, dim).astype(jnp.bfloat16)
    received = lax.ppermute(sent, axis_name, perm=[(0, 1), (1, 0)])
    return kept + received.astype(jnp.float32)


def pair_sum(share, axis_name):
    if lax.axis_size(axis_name) != 2:
        return lax.psum(share, axis_name).astype(jnp.float32)
    received = lax.ppermute(share, axis_name, perm=[(0, 1), (1, 0)])
    return share.astype(jnp.float32) + received.astype(jnp.float32)


def disassemble(full, shard_dim, tensor_dim):
    ns = lax.axis_size("shard")
    nt = lax.axis_size("tensor")
    split_shape = []
    positions = {}
    for dim, size in enumerate(full.shape):
        if dim == shard_dim:
            positions["s"] = len(split_shape)
            split_shape += [ns, size // ns]
        elif dim == tensor_dim:
            positions["t"] = len(split_shape)
            split_shape += [nt, size // nt]
        else:
            split_shape.append(size)
    pieces = full.reshape(split_shape)
    lead = [positions[key] for key in ("s", "t") if key in positions]
    rest = [d for d in range(len(split_shape)) if d not in lead]
    pieces = pieces.transpose(lead + rest)
    if "s" not in positions:
        pieces = jnp.broadcast_to(pieces[None], (ns,) + pieces.shape)
    if "t" not in positions:
        pieces = jnp.broadcast_to(pieces[:, None], (ns, nt) + pieces.shape[1:])
    return pieces.reshape(ns * nt, -1)


def pack_rows(terms):
    rows = jnp.concatenate(
        [disassemble(full.astype(jnp.bfloat16), shard_dim, tensor_dim) for full, shard_dim, tensor_dim in terms],
        1,
    )
    width = rows.shape[1]
    return jnp.pad(rows, ((0, 0), (0, -width % 1024))).reshape(rows.shape[0], -1, 128)


def scatter_rows(rows):
    return lax.psum_scatter(rows, ("shard", "tensor"), scatter_dimension=0, tiled=False)


def unpack_share(share, terms):
    total = pair_sum(share, "context").reshape(-1)
    pieces = []
    offset = 0
    ns = lax.axis_size("shard")
    nt = lax.axis_size("tensor")
    for full, shard_dim, tensor_dim in terms:
        local_shape = list(full.shape)
        if shard_dim is not None:
            local_shape[shard_dim] //= ns
        if tensor_dim is not None:
            local_shape[tensor_dim] //= nt
        count = 1
        for size in local_shape:
            count *= size
        pieces.append(total[offset : offset + count].reshape(local_shape))
        offset += count
    return pieces


def shard_stage(grad, dim):
    return lax.psum_scatter(grad.astype(jnp.bfloat16), "shard", scatter_dimension=dim, tiled=True)


def finish_stage(share, tensor_dim):
    summed = pair_reduce(share, "tensor", tensor_dim)
    return pair_sum(summed.astype(jnp.bfloat16), "context")


def forward_pass(block_in, codes, weights, span):
    w_qkv, w_out, w_up, w_down, norm_gains, out_biases, head_biases, head_gain, unit_bias, unit_gain = weights
    seq_count, local_len, model_width = block_in.shape
    row_count = seq_count * local_len
    flattened_input = block_in.reshape(row_count, model_width).astype(jnp.float32)
    first_normed, first_inv, first_out = norm_rows(flattened_input, norm_gains[0])
    attn_in = first_out.astype(jnp.bfloat16)
    projected = jnp.einsum("rd,jde->jre", attn_in, w_qkv, preferred_element_type=jnp.float32)
    query_matrix = (projected[0] + head_biases[0]).astype(jnp.bfloat16)
    keys_local = projected[1].astype(jnp.bfloat16).reshape(seq_count, local_len, model_width)
    values_local = (projected[2] + head_biases[1]).astype(jnp.bfloat16).reshape(
        seq_count, local_len, model_width
    )
    if span is None:
        key_all = pair_gather(keys_local, "context", 1)
        value_all = pair_gather(values_local, "context", 1)
    else:
        key_all, value_all = keys_local, values_local
    attended = split_attention_forward(
        query_matrix.reshape(seq_count, local_len, model_width), key_all, value_all, codes, span
    ).reshape(row_count, model_width)
    sub_normed, sub_inv, sub_out = norm_rows(attended, head_gain)
    sub_in = sub_out.astype(jnp.bfloat16)
    middle = flattened_input + (
        jnp.dot(sub_in, w_out, preferred_element_type=jnp.float32) + out_biases[0]
    )
    second_normed, second_inv, second_out = norm_rows(middle, norm_gains[1])
    ffn_in = second_out.astype(jnp.bfloat16)
    hidden = jnp.dot(ffn_in, w_up, preferred_element_type=jnp.float32) + unit_bias
    activated = jax.nn.gelu(hidden, approximate=True)
    unit_normed, unit_inv, unit_out = norm_rows(activated, unit_gain)
    ffn_mid = unit_out.astype(jnp.bfloat16)
    layer_out = (
        middle + (jnp.dot(ffn_mid, w_down, preferred_element_type=jnp.float32) + out_biases[1])
    ).astype(jnp.bfloat16)
    kept_state = (
        attn_in,
        first_normed,
        first_inv,
        query_matrix,
        key_all,
        value_all,
        codes,
        sub_normed,
        sub_inv,
        sub_in,
        second_normed,
        second_inv,
        ffn_in,
        hidden,
        unit_normed,
        unit_inv,
        ffn_mid,
    )
    return (kept_state, layer_out.reshape(seq_count, local_len, model_width))


def backward_pass(kept_state, block_grad, weights, span):
    w_qkv, w_out, w_up, w_down, norm_gains, out_biases, head_biases, head_gain, unit_bias, unit_gain = weights
    (
        attn_in,
        first_normed,
        first_inv,
        query_matrix,
        key_all,
        value_all,
        codes,
        sub_normed,
        sub_inv,
        sub_in,
        second_normed,
        second_inv,
        ffn_in,
        hidden,
        unit_normed,
        unit_inv,
        ffn_mid,
    ) = kept_state
    seq_count, local_len, model_width = block_grad.shape
    row_count = seq_count * local_len
    seq_len = key_all.shape[1]
    grad_low = block_grad.reshape(row_count, model_width)
    grad_full = grad_low.astype(jnp.float32)
    down_grad = outer_sum(grad_low, ffn_mid)
    last_bias_grad = jnp.sum(grad_full, 0)
    unit_grad = back_dot(grad_low, w_down)
    activated_grad, unit_gain_grad = norm_back(unit_normed, unit_inv, unit_gain, unit_grad)
    gelu_value, gelu_pull = jax.vjp(partial(jax.nn.gelu, approximate=True), hidden)
    hidden_low = gelu_pull(activated_grad)[0].astype(jnp.bfloat16)
    up_grad = outer_sum(ffn_in, hidden_low)
    unit_bias_grad = jnp.sum(hidden_low, 0, dtype=jnp.float32)
    ffn_in_grad = back_dot(hidden_low, w_up)
    middle_part, second_gain_grad = norm_back(second_normed, second_inv, norm_gains[1], ffn_in_grad)
    middle_grad = grad_full + middle_part
    middle_low = middle_grad.astype(jnp.bfloat16)
    out_weight_grad = outer_sum(middle_low, sub_in)
    first_bias_grad = jnp.sum(middle_low, 0, dtype=jnp.float32)
    sub_grad = back_dot(middle_low, w_out)
    attended_grad, head_gain_grad = norm_back(sub_normed, sub_inv, head_gain, sub_grad)
    attended_low = attended_grad.astype(jnp.bfloat16)
    down_grad, up_grad, out_weight_grad, attended_low = lax.optimization_barrier(
        (
            down_grad.astype(jnp.bfloat16),
            up_grad.astype(jnp.bfloat16),
            out_weight_grad.astype(jnp.bfloat16),
            attended_low,
        )
    )
    tensor_count = lax.axis_size("tensor")
    early_widths = (down_grad.shape[1], up_grad.shape[1], out_weight_grad.shape[1])
    early_share = shard_stage(
        jnp.concatenate(
            [
                part.reshape(part.shape[0], tensor_count, part.shape[1] // tensor_count)
                for part in (down_grad, up_grad, out_weight_grad)
            ],
            2,
        ),
        0,
    )
    query_grad, key_part, value_part = split_attention_backward(
        query_matrix.reshape(seq_count, local_len, model_width),
        key_all,
        value_all,
        attended_low.reshape(seq_count, local_len, model_width),
        codes,
        span,
    )
    if span is not None:
        key_part = key_part.reshape(row_count, model_width)
        value_part = value_part.reshape(row_count, model_width)
    query_low = query_grad.reshape(row_count, model_width)
    if span is None:
        key_part = pair_reduce(key_part, "context", 1)
        value_part = pair_reduce(value_part, "context", 1)
    key_low = key_part.astype(jnp.bfloat16).reshape(row_count, model_width)
    value_low = value_part.astype(jnp.bfloat16).reshape(row_count, model_width)
    stacked = jnp.stack([query_low, key_low, value_low])
    early_share, stacked = lax.optimization_barrier((early_share, stacked))
    qkv_grad = jnp.einsum("rd,jre->dje", attn_in, stacked, preferred_element_type=jnp.float32)
    head_bias_grad = jnp.stack(
        [jnp.sum(query_low, 0, dtype=jnp.float32), jnp.sum(value_low, 0, dtype=jnp.float32)]
    )
    qkv_grad, stacked = lax.optimization_barrier((qkv_grad, stacked))
    attn_in_grad = jnp.einsum("jre,jde->rd", stacked, w_qkv, preferred_element_type=jnp.float32)
    input_part, first_gain_grad = norm_back(first_normed, first_inv, norm_gains[0], attn_in_grad)
    input_low = (middle_grad + input_part).astype(jnp.bfloat16)
    heads = model_width // HD
    unit_rows = unit_bias_grad.shape[0] // HD
    small_terms = (
        (jnp.stack([first_gain_grad, second_gain_grad]), 1, None),
        (jnp.stack([first_bias_grad, last_bias_grad]), 1, None),
        (head_bias_grad.reshape(2, heads, HD), 2, 1),
        (head_gain_grad.reshape(heads, HD), 1, 0),
        (unit_bias_grad.reshape(unit_rows, HD), 1, 0),
        (unit_gain_grad.reshape(unit_rows, HD), 1, 0),
    )
    ns = lax.axis_size("shard")
    nt = lax.axis_size("tensor")
    small_rows = jnp.concatenate(
        [disassemble(full, shard_dim, tensor_dim) for full, shard_dim, tensor_dim in small_terms], 1
    )
    small_width = small_rows.shape[1]
    block_rows = model_width // ns
    extra_rows = 8
    planes = qkv_grad.shape[1]
    slots = extra_rows * planes * (model_width // nt)
    small_block = (
        jnp.pad(small_rows, ((0, 0), (0, slots - small_width)))
        .reshape(ns, nt, extra_rows, planes, model_width // nt)
        .transpose(0, 2, 3, 1, 4)
        .reshape(ns, extra_rows, planes, model_width)
    )
    widened = jnp.concatenate(
        [qkv_grad.reshape(ns, block_rows, planes, model_width), small_block.astype(qkv_grad.dtype)], 1
    ).reshape(ns * (block_rows + extra_rows), planes, model_width)
    qkv_share = shard_stage(widened, 0)
    qkv_total = finish_stage(qkv_share, 2)
    small_total = qkv_total[block_rows:].reshape(-1)[:small_width]
    small_pieces = []
    offset = 0
    for full, shard_dim, tensor_dim in small_terms:
        local_shape = list(full.shape)
        if shard_dim is not None:
            local_shape[shard_dim] //= ns
        if tensor_dim is not None:
            local_shape[tensor_dim] //= nt
        count = 1
        for size in local_shape:
            count *= size
        small_pieces.append(small_total[offset : offset + count].reshape(local_shape))
        offset += count
    early_total = finish_stage(early_share, 1).reshape(early_share.shape[0], -1)
    down_width = early_widths[0] // nt
    up_width = early_widths[1] // nt
    grad_shares = (
        early_total[:, :down_width].transpose(1, 0),
        early_total[:, down_width : down_width + up_width],
        early_total[:, down_width + up_width :].transpose(1, 0),
        qkv_total[:block_rows].transpose(1, 0, 2),
    ) + tuple(small_pieces)
    return (grad_shares, input_low.reshape(seq_count, local_len, model_width))


def local(
    inputs,
    out_grad,
    picture_starts,
    segment_offsets,
    dilation_offsets,
    norm_gains,
    w_qkv,
    head_biases,
    head_gain,
    w_out,
    out_biases,
    w_up,
    unit_bias,
    unit_gain,
    w_down,
):
    local_seqs, local_len, model_width = inputs.shape
    tensor_count = lax.axis_size("tensor")
    context_count = lax.axis_size("context")
    seq_len = local_len * context_count
    key_position = jnp.arange(seq_len, dtype=jnp.int32)
    whole = context_count == 2 and tensor_count == 2 and local_seqs == 4
    if whole:
        span = seq_len // PIECES
        me_c = lax.axis_index("context")
        own_seq = lax.axis_index("tensor") * context_count + me_c
        partner_seq = lax.axis_index("tensor") * context_count + 1 - me_c
        swap = [(0, 1), (1, 0)]

        def own_sequence(rows):
            kept = lax.dynamic_slice_in_dim(rows, own_seq, 1, 0)
            sent = lax.dynamic_slice_in_dim(rows, partner_seq, 1, 0)
            received = lax.ppermute(sent, "context", perm=swap)
            return jnp.where(
                me_c == 0,
                jnp.concatenate([kept, received], 1),
                jnp.concatenate([received, kept], 1),
            )

        block_in = own_sequence(inputs)
        block_grad = own_sequence(out_grad)
        starts = lax.dynamic_slice_in_dim(picture_starts, own_seq, 1, 0)
        query_position = key_position
    else:
        span = None
        mine = local_seqs // tensor_count
        first_seq = lax.axis_index("tensor") * mine
        block_in = lax.dynamic_slice_in_dim(inputs, first_seq, mine, 0)
        block_grad = lax.dynamic_slice_in_dim(out_grad, first_seq, mine, 0)
        starts = lax.dynamic_slice_in_dim(picture_starts, first_seq, mine, 0)
        query_position = lax.axis_index("context") * local_len + jnp.arange(
            local_len, dtype=jnp.int32
        )
    spans = jnp.array([seq_len * part // 8 for part in span_parts], jnp.int32)
    rates = jnp.array(dilation_rates, jnp.int32)
    segment_kept = segment_offsets % spans
    dilation_kept = dilation_offsets % rates
    offset_digits = jnp.concatenate(
        [segment_kept // 32, segment_kept % 32, dilation_kept], 1
    ).astype(jnp.bfloat16)
    f32 = jnp.float32
    (
        w_qkv_full,
        gains_full,
        out_bias_full,
        head_bias_full,
        head_gain_full,
        unit_bias_full,
        unit_gain_full,
        digits_full,
    ) = gather_packed(
        (
            (w_qkv, 1, 2),
            (norm_gains, 1, None),
            (out_biases, 1, None),
            (head_biases, 2, 1),
            (head_gain, 1, 0),
            (unit_bias, 1, 0),
            (unit_gain, 1, 0),
            (offset_digits, None, 0),
        )
    )
    patterns = len(span_parts)
    digits_full = digits_full.astype(jnp.int32)
    all_segments = digits_full[:, :patterns] * 32 + digits_full[:, patterns : 2 * patterns]
    all_dilations = digits_full[:, 2 * patterns :]
    codes = mask_codes(starts, query_position, key_position, all_segments, all_dilations, seq_len)
    w_out, w_up, w_down, w_qkv_full = lax.optimization_barrier((w_out, w_up, w_down, w_qkv_full))
    weights = (
        w_qkv_full,
        gather_weight(w_out, 1, 0),
        gather_weight(w_up, 0, 1),
        gather_weight(w_down, 1, 0),
        gains_full.astype(f32),
        out_bias_full.astype(f32),
        head_bias_full.reshape(2, model_width).astype(f32),
        head_gain_full.reshape(model_width).astype(f32),
        unit_bias_full.reshape(-1).astype(f32),
        unit_gain_full.reshape(-1).astype(f32),
    )
    kept_state, layer_block = forward_pass(block_in, codes, weights, span)
    if whole:
        layer_out = spread_sequence(layer_block, local_len)
    else:
        layer_out = pair_gather(layer_block, "tensor", 0)
    grad_shares, input_block = backward_pass(kept_state, block_grad, weights, span)
    if whole:
        input_grad = spread_sequence(input_block, local_len)
    else:
        input_grad = pair_gather(input_block, "tensor", 0)
    (
        down_share,
        up_share,
        out_share,
        qkv_share,
        gains_share,
        out_bias_share,
        head_bias_share,
        head_gain_share,
        unit_bias_share,
        unit_gain_share,
    ) = grad_shares
    return (
        layer_out,
        input_grad,
        gains_share,
        qkv_share,
        head_bias_share,
        head_gain_share,
        out_share,
        out_bias_share,
        up_share,
        unit_bias_share,
        unit_gain_share,
        down_share,
    )


def solution(mesh):
    placed = (
        P("shard", "context", None),
        P("shard", "context", None),
        P("shard", None),
        P("tensor", None),
        P("tensor", None),
        P(None, "shard"),
        P(None, "shard", "tensor"),
        P(None, "tensor", "shard"),
        P("tensor", "shard"),
        P("tensor", "shard"),
        P(None, "shard"),
        P("shard", "tensor"),
        P("tensor", "shard"),
        P("tensor", "shard"),
        P("tensor", "shard"),
    )
    return jax.shard_map(
        local,
        mesh=mesh,
        in_specs=placed,
        out_specs=(
            P("shard", "context", None),
            P("shard", "context", None),
            P(None, "shard"),
            P(None, "shard", "tensor"),
            P(None, "tensor", "shard"),
            P("tensor", "shard"),
            P("tensor", "shard"),
            P(None, "shard"),
            P("shard", "tensor"),
            P("tensor", "shard"),
            P("tensor", "shard"),
            P("tensor", "shard"),
        ),
        check_vma=False,
    )
```

```python
from functools import partial

import jax
import jax.numpy as jnp
from jax import lax
from jax.experimental import pallas as pl
from jax.experimental.pallas import tpu as pltpu
from jax.sharding import PartitionSpec as P

HD = 64
FF = 3072
PIECE = 256
PIECES = 2


epsilon = 1e-05
span_parts = (1, 2, 4, 6, 8)
dilation_rates = (1, 2, 4, 6, 12)


def pattern_total(query_position, key_position, segmented_offsets, dilated_offsets, token_length):
    tallied_total = jnp.zeros(
        (segmented_offsets.shape[0], query_position.shape[0], key_position.shape[0]), jnp.float32
    )
    for item_number in range(len(span_parts)):
        segmented_span = token_length * span_parts[item_number] // 8
        dilated_stride = dilation_rates[item_number]
        seg_shift = (segmented_offsets[:, item_number] % segmented_span)[:, None, None]
        dilated_phase = (dilated_offsets[:, item_number] % dilated_stride)[:, None, None]
        query_lookup = query_position[None, :, None] + seg_shift
        key_lookup = key_position[None, None, :] + seg_shift
        merged_heads = (
            (query_lookup // segmented_span == key_lookup // segmented_span)
            & (query_lookup % dilated_stride == dilated_phase)
            & (key_lookup % dilated_stride == dilated_phase)
        )
        tallied_total = tallied_total + merged_heads.astype(jnp.float32)
    return tallied_total


def picture_index(starts, token_positions):
    marked = jnp.zeros((starts.shape[0], token_positions.shape[0]), jnp.int32)
    for piece_number in range(starts.shape[1]):
        begin_at = starts[:, piece_number][:, None]
        inside = (token_positions[None, :] >= begin_at) & (
            token_positions[None, :] < begin_at + PIECE
        )
        marked = marked + (piece_number + 1) * inside.astype(jnp.int32)
    return marked


def allowed_keys(query_pic, key_pic, query_position, key_position):
    causal_ok = key_position[None, None, :] <= query_position[None, :, None]
    same_piece = (query_pic[:, :, None] == key_pic[:, None, :]) & (query_pic[:, :, None] > 0)
    return (causal_ok | same_piece).astype(jnp.float32)


def outer_sum(left_rows, right_rows):
    return lax.dot_general(
        left_rows, right_rows, (((0,), (0,)), ((), ())), preferred_element_type=jnp.float32
    )


def back_dot(left_rows, weight_rows):
    return lax.dot_general(
        left_rows, weight_rows, (((1,), (1,)), ((), ())), preferred_element_type=jnp.float32
    )


def norm_rows(values, scale_row):
    mean_row = jnp.mean(values, -1, keepdims=True)
    centered = values - mean_row
    inv_std = lax.rsqrt(jnp.mean(centered * centered, -1, keepdims=True) + epsilon)
    normed = centered * inv_std
    return (normed, inv_std, normed * scale_row)


def norm_back(normed, inv_std, scale_row, grad_rows):
    scaled = grad_rows * scale_row
    mean_plain = jnp.mean(scaled, -1, keepdims=True)
    mean_cross = jnp.mean(scaled * normed, -1, keepdims=True)
    return (inv_std * (scaled - mean_plain - normed * mean_cross), jnp.sum(grad_rows * normed, 0))


def probabilities(query_heads, key_heads, mask_table):
    raw_scores = jnp.einsum(
        "sqhd,skhd->shqk", query_heads, key_heads, preferred_element_type=jnp.float32
    ) * HD ** (-0.5)
    masked = jnp.where(mask_table > 0, raw_scores, -1000000000.0)
    row_top = jnp.max(masked, -1, keepdims=True)
    exponent = mask_table * jnp.exp(masked - row_top)
    row_total = jnp.sum(exponent, -1, keepdims=True)
    return (exponent / row_total, row_top, row_total)


SCALE = HD ** (-0.5)
HIDDEN = -1000000000.0
PAIR = 2
CODE_WIDTH = 8


def pair_masks(patq_ref, patk_ref, pcq_ref, pck_ref):
    first_q = patq_ref[0]
    first_k = patk_ref[0]
    row = first_q[:, 5:6]
    col = first_k[5:6, :]
    piece_q = pcq_ref[0][:, 0:1]
    piece_k = pck_ref[0][0:1, :]
    allowed = (col <= row) | (piece_q == piece_k)
    masks = []
    for head in range(PAIR):
        codes_q = patq_ref[head]
        codes_k = patk_ref[head]
        tally = (codes_q[:, 0:1] == codes_k[0:1, :]).astype(jnp.float32)
        for pattern in range(1, len(span_parts)):
            tally = tally + (
                codes_q[:, pattern : pattern + 1] == codes_k[pattern : pattern + 1, :]
            ).astype(jnp.float32)
        masks.append(jnp.where(allowed, tally, 0.0))
    return masks


def soft_rows(query_part, key_block, mask):
    scores = (
        lax.dot_general(
            query_part, key_block, (((1,), (1,)), ((), ())), preferred_element_type=jnp.float32
        )
        * SCALE
    )
    masked = jnp.where(mask > 0, scores, HIDDEN)
    top = jnp.max(masked, axis=1, keepdims=True)
    exponent = mask * jnp.exp(masked - top)
    return exponent / jnp.sum(exponent, axis=1, keepdims=True)


def attention_fwd_kernel(q_ref, k_ref, v_ref, patq_ref, patk_ref, pcq_ref, pck_ref, o_ref):
    query = q_ref[0]
    key_block = k_ref[0]
    value_block = v_ref[0]
    first = lax.broadcasted_iota(jnp.int32, query.shape, 1) < HD
    masks = pair_masks(patq_ref, patk_ref, pcq_ref, pck_ref)
    result = None
    for head in range(PAIR):
        keep = first if head == 0 else jnp.logical_not(first)
        query_part = jnp.where(keep, query, jnp.zeros_like(query))
        probs = soft_rows(query_part, key_block, masks[head])
        mixed = jnp.dot(
            probs.astype(jnp.bfloat16), value_block, preferred_element_type=jnp.float32
        )
        result = mixed if result is None else jnp.where(first, result, mixed)
    o_ref[0] = result


def attention_bwd_kernel(
    q_ref, k_ref, v_ref, do_ref, patq_ref, patk_ref, pcq_ref, pck_ref, dq_ref, dk_ref, dv_ref
):
    @pl.when(pl.program_id(2) == 0)
    def _():
        dk_ref[...] = jnp.zeros_like(dk_ref)
        dv_ref[...] = jnp.zeros_like(dv_ref)

    query = q_ref[0]
    key_block = k_ref[0]
    value_block = v_ref[0]
    grad_out = do_ref[0]
    first = lax.broadcasted_iota(jnp.int32, query.shape, 1) < HD
    masks = pair_masks(patq_ref, patk_ref, pcq_ref, pck_ref)
    query_grad = None
    key_grad = dk_ref[0]
    value_grad = dv_ref[0]
    for head in range(PAIR):
        keep = first if head == 0 else jnp.logical_not(first)
        query_part = jnp.where(keep, query, jnp.zeros_like(query))
        grad_part = jnp.where(keep, grad_out, jnp.zeros_like(grad_out))
        probs = soft_rows(query_part, key_block, masks[head])
        prob_grad = lax.dot_general(
            grad_part, value_block, (((1,), (1,)), ((), ())), preferred_element_type=jnp.float32
        )
        inner = jnp.sum(probs * prob_grad, axis=1, keepdims=True)
        score_low = (probs * (prob_grad - inner)).astype(jnp.bfloat16)
        part = jnp.dot(score_low, key_block, preferred_element_type=jnp.float32)
        query_grad = part if query_grad is None else jnp.where(first, query_grad, part)
        key_grad = key_grad + SCALE * lax.dot_general(
            score_low, query_part, (((0,), (0,)), ((), ())), preferred_element_type=jnp.float32
        )
        value_grad = value_grad + lax.dot_general(
            probs.astype(jnp.bfloat16),
            grad_part,
            (((0,), (0,)), ((), ())),
            preferred_element_type=jnp.float32,
        )
    dq_ref[0] = (query_grad * SCALE).astype(jnp.bfloat16)
    dk_ref[0] = key_grad
    dv_ref[0] = value_grad


def attention_specs(seq_count, local_len, seq_len, block_q):
    lanes = PAIR * HD
    query_spec = pl.BlockSpec((1, block_q, lanes), lambda s, g, b: (s, b, g))
    key_spec = pl.BlockSpec((1, seq_len, lanes), lambda s, g, b: (s, 0, g))
    patq_spec = pl.BlockSpec((PAIR, block_q, CODE_WIDTH), lambda s, g, b: (g, b, 0))
    patk_spec = pl.BlockSpec((PAIR, CODE_WIDTH, seq_len), lambda s, g, b: (g, 0, 0))
    pcq_spec = pl.BlockSpec((1, block_q, CODE_WIDTH), lambda s, g, b: (s, b, 0))
    pck_spec = pl.BlockSpec((1, CODE_WIDTH, seq_len), lambda s, g, b: (s, 0, 0))
    return query_spec, key_spec, patq_spec, patk_spec, pcq_spec, pck_spec


def attention_forward(query, keys, values, codes):
    seq_count, local_len, width = query.shape
    seq_len = keys.shape[1]
    block_q = min(256, local_len)
    grid = (seq_count, width // (PAIR * HD), local_len // block_q)
    query_spec, key_spec, patq_spec, patk_spec, pcq_spec, pck_spec = attention_specs(
        seq_count, local_len, seq_len, block_q
    )
    flops = 8 * seq_count * local_len * seq_len * width
    return pl.pallas_call(
        attention_fwd_kernel,
        grid=grid,
        in_specs=[query_spec, key_spec, key_spec, patq_spec, patk_spec, pcq_spec, pck_spec],
        out_specs=query_spec,
        out_shape=jax.ShapeDtypeStruct((seq_count, local_len, width), jnp.float32),
        compiler_params=pltpu.CompilerParams(
            dimension_semantics=("parallel", "parallel", "arbitrary"),
            vmem_limit_bytes=48 * 1024 * 1024,
        ),
        cost_estimate=pl.CostEstimate(
            flops=flops,
            transcendentals=seq_count * local_len * seq_len * width // HD,
            bytes_accessed=2 * query.size + 2 * keys.size * 2 * (local_len // block_q) + 4 * query.size,
        ),
    )(query, keys, values, *codes)


def attention_backward(query, keys, values, grad_out, codes):
    seq_count, local_len, width = query.shape
    seq_len = keys.shape[1]
    block_q = min(256, local_len)
    grid = (seq_count, width // (PAIR * HD), local_len // block_q)
    query_spec, key_spec, patq_spec, patk_spec, pcq_spec, pck_spec = attention_specs(
        seq_count, local_len, seq_len, block_q
    )
    flops = 20 * seq_count * local_len * seq_len * width
    return pl.pallas_call(
        attention_bwd_kernel,
        grid=grid,
        in_specs=[
            query_spec,
            key_spec,
            key_spec,
            query_spec,
            patq_spec,
            patk_spec,
            pcq_spec,
            pck_spec,
        ],
        out_specs=[query_spec, key_spec, key_spec],
        out_shape=[
            jax.ShapeDtypeStruct((seq_count, local_len, width), jnp.bfloat16),
            jax.ShapeDtypeStruct((seq_count, seq_len, width), jnp.float32),
            jax.ShapeDtypeStruct((seq_count, seq_len, width), jnp.float32),
        ],
        compiler_params=pltpu.CompilerParams(
            dimension_semantics=("parallel", "parallel", "arbitrary"),
            vmem_limit_bytes=48 * 1024 * 1024,
        ),
        cost_estimate=pl.CostEstimate(
            flops=flops,
            transcendentals=seq_count * local_len * seq_len * width // HD,
            bytes_accessed=4 * query.size + 2 * keys.size * 2 * (local_len // block_q) + 16 * keys.size,
        ),
    )(query, keys, values, grad_out, *codes)


def mask_codes(starts, query_position, key_position, segment_offsets, dilation_offsets, seq_len):
    heads = segment_offsets.shape[0]
    query_codes = []
    key_codes = []
    for pattern in range(len(span_parts)):
        span = seq_len * span_parts[pattern] // 8
        rate = dilation_rates[pattern]
        shift = (segment_offsets[:, pattern] % span)[:, None]
        phase = (dilation_offsets[:, pattern] % rate)[:, None]
        query_at = query_position[None, :] + shift
        key_at = key_position[None, :] + shift
        query_codes.append(jnp.where(query_at % rate == phase, query_at // span, -1))
        key_codes.append(jnp.where(key_at % rate == phase, key_at // span, -2))
    patterns = len(span_parts)
    query_codes.append(jnp.broadcast_to(query_position[None, :], (heads, query_position.shape[0])))
    key_codes.append(jnp.broadcast_to(key_position[None, :], (heads, key_position.shape[0])))
    filler = CODE_WIDTH - patterns - 1
    query_codes += [jnp.zeros((heads, query_position.shape[0]), jnp.int32)] * filler
    key_codes += [jnp.zeros((heads, key_position.shape[0]), jnp.int32)] * filler
    patq = jnp.stack(query_codes, 2).astype(jnp.int32)
    patk = jnp.stack(key_codes, 1).astype(jnp.int32)
    query_pic = picture_index(starts, query_position)
    key_pic = picture_index(starts, key_position)
    pcq = jnp.where(query_pic > 0, query_pic, -1)[:, :, None]
    pcq = jnp.pad(pcq, ((0, 0), (0, 0), (0, CODE_WIDTH - 1)))
    pck = jnp.where(key_pic > 0, key_pic, -2)[:, None, :]
    pck = jnp.pad(pck, ((0, 0), (0, CODE_WIDTH - 1), (0, 0)))
    return (patq, patk, pcq.astype(jnp.int32), pck.astype(jnp.int32))


def code_part(codes, begin, end, key_end):
    patq, patk, pcq, pck = codes
    return (patq[:, begin:end], patk[:, :, :key_end], pcq[:, begin:end], pck[:, :, :key_end])


def split_attention_forward(query, keys, values, codes, span):
    if span is None:
        return attention_forward(query, keys, values, codes)
    head = attention_forward(
        query[:, :span], keys[:, :span], values[:, :span], code_part(codes, 0, span, span)
    )
    seq_len = keys.shape[1]
    tail = attention_forward(
        query[:, span:], keys, values, code_part(codes, span, query.shape[1], seq_len)
    )
    return jnp.concatenate([head, tail], 1)


def split_attention_backward(query, keys, values, grad_out, codes, span):
    if span is None:
        return attention_backward(query, keys, values, grad_out, codes)
    seq_len = keys.shape[1]
    head_q, head_k, head_v = attention_backward(
        query[:, :span],
        keys[:, :span],
        values[:, :span],
        grad_out[:, :span],
        code_part(codes, 0, span, span),
    )
    tail_q, tail_k, tail_v = attention_backward(
        query[:, span:],
        keys,
        values,
        grad_out[:, span:],
        code_part(codes, span, query.shape[1], seq_len),
    )
    padding = ((0, 0), (0, seq_len - span), (0, 0))
    return (
        jnp.concatenate([head_q, tail_q], 1),
        tail_k + jnp.pad(head_k, padding),
        tail_v + jnp.pad(head_v, padding),
    )


def spread_sequence(block, local_len):
    me_c = lax.axis_index("context")
    me_t = lax.axis_index("tensor")
    swap = [(0, 1), (1, 0)]
    kept = lax.dynamic_slice_in_dim(block, me_c * local_len, local_len, 1)
    other = lax.dynamic_slice_in_dim(block, (1 - me_c) * local_len, local_len, 1)
    from_context = lax.ppermute(other, "context", perm=swap)
    from_tensor = lax.ppermute(kept, "tensor", perm=swap)
    from_corner = lax.ppermute(other, ("context", "tensor"), perm=[(0, 3), (3, 0), (1, 2), (2, 1)])
    first_c = me_c == 0
    own_pair = jnp.where(
        first_c,
        jnp.concatenate([kept, from_context], 0),
        jnp.concatenate([from_context, kept], 0),
    )
    far_pair = jnp.where(
        first_c,
        jnp.concatenate([from_tensor, from_corner], 0),
        jnp.concatenate([from_corner, from_tensor], 0),
    )
    return jnp.where(
        me_t == 0,
        jnp.concatenate([own_pair, far_pair], 0),
        jnp.concatenate([far_pair, own_pair], 0),
    )


def assemble(stacked, shard_dim, tensor_dim):
    ns, nt = stacked.shape[0], stacked.shape[1]
    if shard_dim is None:
        stacked = stacked[:1]
    if tensor_dim is None:
        stacked = stacked[:, :1]
    local_shape = stacked.shape[2:]
    order = []
    for dim in range(len(local_shape)):
        if dim == shard_dim:
            order.append(0)
        if dim == tensor_dim:
            order.append(1)
        order.append(dim + 2)
    if shard_dim is None:
        order = [0] + order
    if tensor_dim is None:
        order = [1] + order
    moved = stacked.transpose(order)
    full_shape = list(local_shape)
    if shard_dim is not None:
        full_shape[shard_dim] *= ns
    if tensor_dim is not None:
        full_shape[tensor_dim] *= nt
    return moved.reshape(full_shape)


def gather_weight(local_block, shard_dim, tensor_dim):
    ns = lax.axis_size("shard")
    nt = lax.axis_size("tensor")
    stacked = lax.all_gather(local_block, ("shard", "tensor"), axis=0, tiled=False)
    return assemble(stacked.reshape((ns, nt) + local_block.shape), shard_dim, tensor_dim)


def gather_packed(blocks):
    ns = lax.axis_size("shard")
    nt = lax.axis_size("tensor")
    flat = jnp.concatenate([block.reshape(-1) for block, _, _ in blocks])
    padded = -flat.size % 2048
    flat = jnp.pad(flat, (0, padded)).reshape(-1, 128)
    stacked = lax.all_gather(flat, ("shard", "tensor"), axis=0, tiled=False).reshape(ns, nt, -1)
    pieces = []
    offset = 0
    for block, shard_dim, tensor_dim in blocks:
        part = stacked[:, :, offset : offset + block.size].reshape((ns, nt) + block.shape)
        pieces.append(assemble(part, shard_dim, tensor_dim))
        offset += block.size
    return pieces


def pair_gather(block, axis_name, dim):
    if lax.axis_size(axis_name) != 2:
        return lax.all_gather(block, axis_name, axis=dim, tiled=True)
    other = lax.ppermute(block, axis_name, perm=[(0, 1), (1, 0)])
    first = lax.axis_index(axis_name) == 0
    return jnp.where(
        first, jnp.concatenate([block, other], dim), jnp.concatenate([other, block], dim)
    )


def pair_reduce(full, axis_name, dim):
    if lax.axis_size(axis_name) != 2:
        return lax.psum_scatter(
            full.astype(jnp.bfloat16), axis_name, scatter_dimension=dim, tiled=True
        ).astype(jnp.float32)
    half = full.shape[dim] // 2
    me = lax.axis_index(axis_name)
    kept = lax.dynamic_slice_in_dim(full, me * half, half, dim)
    sent = lax.dynamic_slice_in_dim(full, (1 - me) * half, half, dim).astype(jnp.bfloat16)
    received = lax.ppermute(sent, axis_name, perm=[(0, 1), (1, 0)])
    return kept + received.astype(jnp.float32)


def pair_sum(share, axis_name):
    if lax.axis_size(axis_name) != 2:
        return lax.psum(share, axis_name).astype(jnp.float32)
    received = lax.ppermute(share, axis_name, perm=[(0, 1), (1, 0)])
    return share.astype(jnp.float32) + received.astype(jnp.float32)


def disassemble(full, shard_dim, tensor_dim):
    ns = lax.axis_size("shard")
    nt = lax.axis_size("tensor")
    split_shape = []
    positions = {}
    for dim, size in enumerate(full.shape):
        if dim == shard_dim:
            positions["s"] = len(split_shape)
            split_shape += [ns, size // ns]
        elif dim == tensor_dim:
            positions["t"] = len(split_shape)
            split_shape += [nt, size // nt]
        else:
            split_shape.append(size)
    pieces = full.reshape(split_shape)
    lead = [positions[key] for key in ("s", "t") if key in positions]
    rest = [d for d in range(len(split_shape)) if d not in lead]
    pieces = pieces.transpose(lead + rest)
    if "s" not in positions:
        pieces = jnp.broadcast_to(pieces[None], (ns,) + pieces.shape)
    if "t" not in positions:
        pieces = jnp.broadcast_to(pieces[:, None], (ns, nt) + pieces.shape[1:])
    return pieces.reshape(ns * nt, -1)


def pack_rows(terms):
    rows = jnp.concatenate(
        [disassemble(full.astype(jnp.bfloat16), shard_dim, tensor_dim) for full, shard_dim, tensor_dim in terms],
        1,
    )
    width = rows.shape[1]
    return jnp.pad(rows, ((0, 0), (0, -width % 1024))).reshape(rows.shape[0], -1, 128)


def scatter_rows(rows):
    return lax.psum_scatter(rows, ("shard", "tensor"), scatter_dimension=0, tiled=False)


def unpack_share(share, terms):
    total = pair_sum(share, "context").reshape(-1)
    pieces = []
    offset = 0
    ns = lax.axis_size("shard")
    nt = lax.axis_size("tensor")
    for full, shard_dim, tensor_dim in terms:
        local_shape = list(full.shape)
        if shard_dim is not None:
            local_shape[shard_dim] //= ns
        if tensor_dim is not None:
            local_shape[tensor_dim] //= nt
        count = 1
        for size in local_shape:
            count *= size
        pieces.append(total[offset : offset + count].reshape(local_shape))
        offset += count
    return pieces


def shard_stage(grad, dim):
    return lax.psum_scatter(grad.astype(jnp.bfloat16), "shard", scatter_dimension=dim, tiled=True)


def finish_stage(share, tensor_dim):
    summed = pair_reduce(share, "tensor", tensor_dim)
    return pair_sum(summed.astype(jnp.bfloat16), "context")


def forward_pass(block_in, codes, weights, span):
    w_qkv, w_out, w_up, w_down, norm_gains, out_biases, head_biases, head_gain, unit_bias, unit_gain = weights
    seq_count, local_len, model_width = block_in.shape
    row_count = seq_count * local_len
    flattened_input = block_in.reshape(row_count, model_width).astype(jnp.float32)
    first_normed, first_inv, first_out = norm_rows(flattened_input, norm_gains[0])
    attn_in = first_out.astype(jnp.bfloat16)
    projected = jnp.einsum("rd,jde->jre", attn_in, w_qkv, preferred_element_type=jnp.float32)
    query_matrix = (projected[0] + head_biases[0]).astype(jnp.bfloat16)
    keys_local = projected[1].astype(jnp.bfloat16).reshape(seq_count, local_len, model_width)
    values_local = (projected[2] + head_biases[1]).astype(jnp.bfloat16).reshape(
        seq_count, local_len, model_width
    )
    if span is None:
        key_all = pair_gather(keys_local, "context", 1)
        value_all = pair_gather(values_local, "context", 1)
    else:
        key_all, value_all = keys_local, values_local
    attended = split_attention_forward(
        query_matrix.reshape(seq_count, local_len, model_width), key_all, value_all, codes, span
    ).reshape(row_count, model_width)
    sub_normed, sub_inv, sub_out = norm_rows(attended, head_gain)
    sub_in = sub_out.astype(jnp.bfloat16)
    middle = flattened_input + (
        jnp.dot(sub_in, w_out, preferred_element_type=jnp.float32) + out_biases[0]
    )
    second_normed, second_inv, second_out = norm_rows(middle, norm_gains[1])
    ffn_in = second_out.astype(jnp.bfloat16)
    hidden = jnp.dot(ffn_in, w_up, preferred_element_type=jnp.float32) + unit_bias
    activated = jax.nn.gelu(hidden, approximate=True)
    unit_normed, unit_inv, unit_out = norm_rows(activated, unit_gain)
    ffn_mid = unit_out.astype(jnp.bfloat16)
    layer_out = (
        middle + (jnp.dot(ffn_mid, w_down, preferred_element_type=jnp.float32) + out_biases[1])
    ).astype(jnp.bfloat16)
    kept_state = (
        attn_in,
        first_normed,
        first_inv,
        query_matrix,
        key_all,
        value_all,
        codes,
        sub_normed,
        sub_inv,
        sub_in,
        second_normed,
        second_inv,
        ffn_in,
        hidden,
        unit_normed,
        unit_inv,
        ffn_mid,
    )
    return (kept_state, layer_out.reshape(seq_count, local_len, model_width))


def backward_pass(kept_state, block_grad, weights, span, carried):
    w_qkv, w_out, w_up, w_down, norm_gains, out_biases, head_biases, head_gain, unit_bias, unit_gain = weights
    (
        attn_in,
        first_normed,
        first_inv,
        query_matrix,
        key_all,
        value_all,
        codes,
        sub_normed,
        sub_inv,
        sub_in,
        second_normed,
        second_inv,
        ffn_in,
        hidden,
        unit_normed,
        unit_inv,
        ffn_mid,
    ) = kept_state
    seq_count, local_len, model_width = block_grad.shape
    row_count = seq_count * local_len
    seq_len = key_all.shape[1]
    grad_low = block_grad.reshape(row_count, model_width)
    grad_full = grad_low.astype(jnp.float32)
    down_grad = outer_sum(grad_low, ffn_mid)
    last_bias_grad = jnp.sum(grad_full, 0)
    unit_grad = back_dot(grad_low, w_down)
    activated_grad, unit_gain_grad = norm_back(unit_normed, unit_inv, unit_gain, unit_grad)
    gelu_value, gelu_pull = jax.vjp(partial(jax.nn.gelu, approximate=True), hidden)
    hidden_low = gelu_pull(activated_grad)[0].astype(jnp.bfloat16)
    up_grad = outer_sum(ffn_in, hidden_low)
    unit_bias_grad = jnp.sum(hidden_low, 0, dtype=jnp.float32)
    ffn_in_grad = back_dot(hidden_low, w_up)
    middle_part, second_gain_grad = norm_back(second_normed, second_inv, norm_gains[1], ffn_in_grad)
    middle_grad = grad_full + middle_part
    middle_low = middle_grad.astype(jnp.bfloat16)
    out_weight_grad = outer_sum(middle_low, sub_in)
    first_bias_grad = jnp.sum(middle_low, 0, dtype=jnp.float32)
    sub_grad = back_dot(middle_low, w_out)
    attended_grad, head_gain_grad = norm_back(sub_normed, sub_inv, head_gain, sub_grad)
    attended_low = attended_grad.astype(jnp.bfloat16)
    down_grad, up_grad, out_weight_grad, attended_low, carried = lax.optimization_barrier(
        (
            down_grad.astype(jnp.bfloat16),
            up_grad.astype(jnp.bfloat16),
            out_weight_grad.astype(jnp.bfloat16),
            attended_low,
            carried,
        )
    )
    tensor_count = lax.axis_size("tensor")
    early_widths = (down_grad.shape[1], up_grad.shape[1], out_weight_grad.shape[1])
    early_share = shard_stage(
        jnp.concatenate(
            [
                part.reshape(part.shape[0], tensor_count, part.shape[1] // tensor_count)
                for part in (down_grad, up_grad, out_weight_grad)
            ],
            2,
        ),
        0,
    )
    query_grad, key_part, value_part = split_attention_backward(
        query_matrix.reshape(seq_count, local_len, model_width),
        key_all,
        value_all,
        attended_low.reshape(seq_count, local_len, model_width),
        codes,
        span,
    )
    if span is not None:
        key_part = key_part.reshape(row_count, model_width)
        value_part = value_part.reshape(row_count, model_width)
    query_low = query_grad.reshape(row_count, model_width)
    if span is None:
        key_part = pair_reduce(key_part, "context", 1)
        value_part = pair_reduce(value_part, "context", 1)
    key_low = key_part.astype(jnp.bfloat16).reshape(row_count, model_width)
    value_low = value_part.astype(jnp.bfloat16).reshape(row_count, model_width)
    stacked = jnp.stack([query_low, key_low, value_low])
    early_share, stacked = lax.optimization_barrier((early_share, stacked))
    qkv_grad = jnp.einsum("rd,jre->dje", attn_in, stacked, preferred_element_type=jnp.float32)
    head_bias_grad = jnp.stack(
        [jnp.sum(query_low, 0, dtype=jnp.float32), jnp.sum(value_low, 0, dtype=jnp.float32)]
    )
    qkv_grad, stacked = lax.optimization_barrier((qkv_grad, stacked))
    attn_in_grad = jnp.einsum("jre,jde->rd", stacked, w_qkv, preferred_element_type=jnp.float32)
    early_total = finish_stage(early_share, 1).reshape(early_share.shape[0], -1)
    early_total, attn_in_grad = lax.optimization_barrier((early_total, attn_in_grad))
    input_part, first_gain_grad = norm_back(first_normed, first_inv, norm_gains[0], attn_in_grad)
    input_low = (middle_grad + input_part).astype(jnp.bfloat16)
    heads = model_width // HD
    unit_rows = unit_bias_grad.shape[0] // HD
    small_terms = (
        (jnp.stack([first_gain_grad, second_gain_grad]), 1, None),
        (jnp.stack([first_bias_grad, last_bias_grad]), 1, None),
        (head_bias_grad.reshape(2, heads, HD), 2, 1),
        (head_gain_grad.reshape(heads, HD), 1, 0),
        (unit_bias_grad.reshape(unit_rows, HD), 1, 0),
        (unit_gain_grad.reshape(unit_rows, HD), 1, 0),
    )
    ns = lax.axis_size("shard")
    nt = lax.axis_size("tensor")
    small_rows = jnp.concatenate(
        [disassemble(full, shard_dim, tensor_dim) for full, shard_dim, tensor_dim in small_terms], 1
    )
    small_width = small_rows.shape[1]
    block_rows = model_width // ns
    extra_rows = 8
    planes = qkv_grad.shape[1]
    slots = extra_rows * planes * (model_width // nt)
    small_block = (
        jnp.pad(small_rows, ((0, 0), (0, slots - small_width)))
        .reshape(ns, nt, extra_rows, planes, model_width // nt)
        .transpose(0, 2, 3, 1, 4)
        .reshape(ns, extra_rows, planes, model_width)
    )
    widened = jnp.concatenate(
        [qkv_grad.reshape(ns, block_rows, planes, model_width), small_block.astype(qkv_grad.dtype)], 1
    ).reshape(ns * (block_rows + extra_rows), planes, model_width)
    qkv_share = shard_stage(widened, 0)
    qkv_total = finish_stage(qkv_share, 2)
    small_total = qkv_total[block_rows:].reshape(-1)[:small_width]
    small_pieces = []
    offset = 0
    for full, shard_dim, tensor_dim in small_terms:
        local_shape = list(full.shape)
        if shard_dim is not None:
            local_shape[shard_dim] //= ns
        if tensor_dim is not None:
            local_shape[tensor_dim] //= nt
        count = 1
        for size in local_shape:
            count *= size
        small_pieces.append(small_total[offset : offset + count].reshape(local_shape))
        offset += count
    down_width = early_widths[0] // nt
    up_width = early_widths[1] // nt
    grad_shares = (
        early_total[:, :down_width].transpose(1, 0),
        early_total[:, down_width : down_width + up_width],
        early_total[:, down_width + up_width :].transpose(1, 0),
        qkv_total[:block_rows].transpose(1, 0, 2),
    ) + tuple(small_pieces)
    return (grad_shares, input_low.reshape(seq_count, local_len, model_width), carried)


def local(
    inputs,
    out_grad,
    picture_starts,
    segment_offsets,
    dilation_offsets,
    norm_gains,
    w_qkv,
    head_biases,
    head_gain,
    w_out,
    out_biases,
    w_up,
    unit_bias,
    unit_gain,
    w_down,
):
    local_seqs, local_len, model_width = inputs.shape
    tensor_count = lax.axis_size("tensor")
    context_count = lax.axis_size("context")
    seq_len = local_len * context_count
    key_position = jnp.arange(seq_len, dtype=jnp.int32)
    whole = context_count == 2 and tensor_count == 2 and local_seqs == 4
    if whole:
        span = seq_len // PIECES
        me_c = lax.axis_index("context")
        own_seq = lax.axis_index("tensor") * context_count + me_c
        partner_seq = lax.axis_index("tensor") * context_count + 1 - me_c
        swap = [(0, 1), (1, 0)]

        def own_sequence(rows):
            kept = lax.dynamic_slice_in_dim(rows, own_seq, 1, 0)
            sent = lax.dynamic_slice_in_dim(rows, partner_seq, 1, 0)
            received = lax.ppermute(sent, "context", perm=swap)
            return jnp.where(
                me_c == 0,
                jnp.concatenate([kept, received], 1),
                jnp.concatenate([received, kept], 1),
            )

        block_in = own_sequence(inputs)
        block_grad = own_sequence(out_grad)
        starts = lax.dynamic_slice_in_dim(picture_starts, own_seq, 1, 0)
        query_position = key_position
    else:
        span = None
        mine = local_seqs // tensor_count
        first_seq = lax.axis_index("tensor") * mine
        block_in = lax.dynamic_slice_in_dim(inputs, first_seq, mine, 0)
        block_grad = lax.dynamic_slice_in_dim(out_grad, first_seq, mine, 0)
        starts = lax.dynamic_slice_in_dim(picture_starts, first_seq, mine, 0)
        query_position = lax.axis_index("context") * local_len + jnp.arange(
            local_len, dtype=jnp.int32
        )
    spans = jnp.array([seq_len * part // 8 for part in span_parts], jnp.int32)
    rates = jnp.array(dilation_rates, jnp.int32)
    segment_kept = segment_offsets % spans
    dilation_kept = dilation_offsets % rates
    offset_digits = jnp.concatenate(
        [segment_kept // 32, segment_kept % 32, dilation_kept], 1
    ).astype(jnp.bfloat16)
    f32 = jnp.float32
    (
        w_qkv_full,
        gains_full,
        out_bias_full,
        head_bias_full,
        head_gain_full,
        unit_bias_full,
        unit_gain_full,
        digits_full,
    ) = gather_packed(
        (
            (w_qkv, 1, 2),
            (norm_gains, 1, None),
            (out_biases, 1, None),
            (head_biases, 2, 1),
            (head_gain, 1, 0),
            (unit_bias, 1, 0),
            (unit_gain, 1, 0),
            (offset_digits, None, 0),
        )
    )
    patterns = len(span_parts)
    digits_full = digits_full.astype(jnp.int32)
    all_segments = digits_full[:, :patterns] * 32 + digits_full[:, patterns : 2 * patterns]
    all_dilations = digits_full[:, 2 * patterns :]
    codes = mask_codes(starts, query_position, key_position, all_segments, all_dilations, seq_len)
    w_out, w_up, w_down, w_qkv_full = lax.optimization_barrier((w_out, w_up, w_down, w_qkv_full))
    weights = (
        w_qkv_full,
        gather_weight(w_out, 1, 0),
        gather_weight(w_up, 0, 1),
        gather_weight(w_down, 1, 0),
        gains_full.astype(f32),
        out_bias_full.astype(f32),
        head_bias_full.reshape(2, model_width).astype(f32),
        head_gain_full.reshape(model_width).astype(f32),
        unit_bias_full.reshape(-1).astype(f32),
        unit_gain_full.reshape(-1).astype(f32),
    )
    kept_state, layer_block = forward_pass(block_in, codes, weights, span)
    if whole:
        layer_out = spread_sequence(layer_block, local_len)
    else:
        layer_out = pair_gather(layer_block, "tensor", 0)
    grad_shares, input_block, layer_out = backward_pass(
        kept_state, block_grad, weights, span, layer_out
    )
    if whole:
        input_grad = spread_sequence(input_block, local_len)
    else:
        input_grad = pair_gather(input_block, "tensor", 0)
    (
        down_share,
        up_share,
        out_share,
        qkv_share,
        gains_share,
        out_bias_share,
        head_bias_share,
        head_gain_share,
        unit_bias_share,
        unit_gain_share,
    ) = grad_shares
    return (
        layer_out,
        input_grad,
        gains_share,
        qkv_share,
        head_bias_share,
        head_gain_share,
        out_share,
        out_bias_share,
        up_share,
        unit_bias_share,
        unit_gain_share,
        down_share,
    )


def solution(mesh):
    placed = (
        P("shard", "context", None),
        P("shard", "context", None),
        P("shard", None),
        P("tensor", None),
        P("tensor", None),
        P(None, "shard"),
        P(None, "shard", "tensor"),
        P(None, "tensor", "shard"),
        P("tensor", "shard"),
        P("tensor", "shard"),
        P(None, "shard"),
        P("shard", "tensor"),
        P("tensor", "shard"),
        P("tensor", "shard"),
        P("tensor", "shard"),
    )
    return jax.shard_map(
        local,
        mesh=mesh,
        in_specs=placed,
        out_specs=(
            P("shard", "context", None),
            P("shard", "context", None),
            P(None, "shard"),
            P(None, "shard", "tensor"),
            P(None, "tensor", "shard"),
            P("tensor", "shard"),
            P("tensor", "shard"),
            P(None, "shard"),
            P("shard", "tensor"),
            P("tensor", "shard"),
            P("tensor", "shard"),
            P("tensor", "shard"),
        ),
        check_vma=False,
    )
```

```python
from functools import partial

import jax
import jax.numpy as jnp
from jax import lax
from jax.experimental import pallas as pl
from jax.experimental.pallas import tpu as pltpu
from jax.sharding import PartitionSpec as P

HD = 64
FF = 3072
PIECE = 256
PIECES = 2


epsilon = 1e-05
span_parts = (1, 2, 4, 6, 8)
dilation_rates = (1, 2, 4, 6, 12)


def pattern_total(query_position, key_position, segmented_offsets, dilated_offsets, token_length):
    tallied_total = jnp.zeros(
        (segmented_offsets.shape[0], query_position.shape[0], key_position.shape[0]), jnp.float32
    )
    for item_number in range(len(span_parts)):
        segmented_span = token_length * span_parts[item_number] // 8
        dilated_stride = dilation_rates[item_number]
        seg_shift = (segmented_offsets[:, item_number] % segmented_span)[:, None, None]
        dilated_phase = (dilated_offsets[:, item_number] % dilated_stride)[:, None, None]
        query_lookup = query_position[None, :, None] + seg_shift
        key_lookup = key_position[None, None, :] + seg_shift
        merged_heads = (
            (query_lookup // segmented_span == key_lookup // segmented_span)
            & (query_lookup % dilated_stride == dilated_phase)
            & (key_lookup % dilated_stride == dilated_phase)
        )
        tallied_total = tallied_total + merged_heads.astype(jnp.float32)
    return tallied_total


def picture_index(starts, token_positions):
    marked = jnp.zeros((starts.shape[0], token_positions.shape[0]), jnp.int32)
    for piece_number in range(starts.shape[1]):
        begin_at = starts[:, piece_number][:, None]
        inside = (token_positions[None, :] >= begin_at) & (
            token_positions[None, :] < begin_at + PIECE
        )
        marked = marked + (piece_number + 1) * inside.astype(jnp.int32)
    return marked


def allowed_keys(query_pic, key_pic, query_position, key_position):
    causal_ok = key_position[None, None, :] <= query_position[None, :, None]
    same_piece = (query_pic[:, :, None] == key_pic[:, None, :]) & (query_pic[:, :, None] > 0)
    return (causal_ok | same_piece).astype(jnp.float32)


def outer_sum(left_rows, right_rows):
    return lax.dot_general(
        left_rows, right_rows, (((0,), (0,)), ((), ())), preferred_element_type=jnp.float32
    )


def back_dot(left_rows, weight_rows):
    return lax.dot_general(
        left_rows, weight_rows, (((1,), (1,)), ((), ())), preferred_element_type=jnp.float32
    )


def norm_rows(values, scale_row):
    mean_row = jnp.mean(values, -1, keepdims=True)
    centered = values - mean_row
    inv_std = lax.rsqrt(jnp.mean(centered * centered, -1, keepdims=True) + epsilon)
    normed = centered * inv_std
    return (normed, inv_std, normed * scale_row)


def norm_back(normed, inv_std, scale_row, grad_rows):
    scaled = grad_rows * scale_row
    mean_plain = jnp.mean(scaled, -1, keepdims=True)
    mean_cross = jnp.mean(scaled * normed, -1, keepdims=True)
    return (inv_std * (scaled - mean_plain - normed * mean_cross), jnp.sum(grad_rows * normed, 0))


def probabilities(query_heads, key_heads, mask_table):
    raw_scores = jnp.einsum(
        "sqhd,skhd->shqk", query_heads, key_heads, preferred_element_type=jnp.float32
    ) * HD ** (-0.5)
    masked = jnp.where(mask_table > 0, raw_scores, -1000000000.0)
    row_top = jnp.max(masked, -1, keepdims=True)
    exponent = mask_table * jnp.exp(masked - row_top)
    row_total = jnp.sum(exponent, -1, keepdims=True)
    return (exponent / row_total, row_top, row_total)


SCALE = HD ** (-0.5)
HIDDEN = -1000000000.0
PAIR = 2
CODE_WIDTH = 8


def pair_masks(patq_ref, patk_ref, pcq_ref, pck_ref):
    first_q = patq_ref[0]
    first_k = patk_ref[0]
    row = first_q[:, 5:6]
    col = first_k[5:6, :]
    piece_q = pcq_ref[0][:, 0:1]
    piece_k = pck_ref[0][0:1, :]
    allowed = (col <= row) | (piece_q == piece_k)
    masks = []
    for head in range(PAIR):
        codes_q = patq_ref[head]
        codes_k = patk_ref[head]
        tally = (codes_q[:, 0:1] == codes_k[0:1, :]).astype(jnp.float32)
        for pattern in range(1, len(span_parts)):
            tally = tally + (
                codes_q[:, pattern : pattern + 1] == codes_k[pattern : pattern + 1, :]
            ).astype(jnp.float32)
        masks.append(jnp.where(allowed, tally, 0.0))
    return masks


def soft_rows(query_part, key_block, mask):
    scores = (
        lax.dot_general(
            query_part, key_block, (((1,), (1,)), ((), ())), preferred_element_type=jnp.float32
        )
        * SCALE
    )
    masked = jnp.where(mask > 0, scores, HIDDEN)
    top = jnp.max(masked, axis=1, keepdims=True)
    exponent = mask * jnp.exp(masked - top)
    return exponent / jnp.sum(exponent, axis=1, keepdims=True)


def attention_fwd_kernel(q_ref, k_ref, v_ref, patq_ref, patk_ref, pcq_ref, pck_ref, o_ref):
    query = q_ref[0]
    key_block = k_ref[0]
    value_block = v_ref[0]
    first = lax.broadcasted_iota(jnp.int32, query.shape, 1) < HD
    masks = pair_masks(patq_ref, patk_ref, pcq_ref, pck_ref)
    result = None
    for head in range(PAIR):
        keep = first if head == 0 else jnp.logical_not(first)
        query_part = jnp.where(keep, query, jnp.zeros_like(query))
        probs = soft_rows(query_part, key_block, masks[head])
        mixed = jnp.dot(
            probs.astype(jnp.bfloat16), value_block, preferred_element_type=jnp.float32
        )
        result = mixed if result is None else jnp.where(first, result, mixed)
    o_ref[0] = result


def attention_bwd_kernel(
    q_ref, k_ref, v_ref, do_ref, patq_ref, patk_ref, pcq_ref, pck_ref, dq_ref, dk_ref, dv_ref
):
    @pl.when(pl.program_id(2) == 0)
    def _():
        dk_ref[...] = jnp.zeros_like(dk_ref)
        dv_ref[...] = jnp.zeros_like(dv_ref)

    query = q_ref[0]
    key_block = k_ref[0]
    value_block = v_ref[0]
    grad_out = do_ref[0]
    first = lax.broadcasted_iota(jnp.int32, query.shape, 1) < HD
    masks = pair_masks(patq_ref, patk_ref, pcq_ref, pck_ref)
    query_grad = None
    key_grad = dk_ref[0]
    value_grad = dv_ref[0]
    for head in range(PAIR):
        keep = first if head == 0 else jnp.logical_not(first)
        query_part = jnp.where(keep, query, jnp.zeros_like(query))
        grad_part = jnp.where(keep, grad_out, jnp.zeros_like(grad_out))
        probs = soft_rows(query_part, key_block, masks[head])
        prob_grad = lax.dot_general(
            grad_part, value_block, (((1,), (1,)), ((), ())), preferred_element_type=jnp.float32
        )
        inner = jnp.sum(probs * prob_grad, axis=1, keepdims=True)
        score_low = (probs * (prob_grad - inner)).astype(jnp.bfloat16)
        part = jnp.dot(score_low, key_block, preferred_element_type=jnp.float32)
        query_grad = part if query_grad is None else jnp.where(first, query_grad, part)
        key_grad = key_grad + SCALE * lax.dot_general(
            score_low, query_part, (((0,), (0,)), ((), ())), preferred_element_type=jnp.float32
        )
        value_grad = value_grad + lax.dot_general(
            probs.astype(jnp.bfloat16),
            grad_part,
            (((0,), (0,)), ((), ())),
            preferred_element_type=jnp.float32,
        )
    dq_ref[0] = (query_grad * SCALE).astype(jnp.bfloat16)
    dk_ref[0] = key_grad
    dv_ref[0] = value_grad


def attention_specs(seq_count, local_len, seq_len, block_q):
    lanes = PAIR * HD
    query_spec = pl.BlockSpec((1, block_q, lanes), lambda s, g, b: (s, b, g))
    key_spec = pl.BlockSpec((1, seq_len, lanes), lambda s, g, b: (s, 0, g))
    patq_spec = pl.BlockSpec((PAIR, block_q, CODE_WIDTH), lambda s, g, b: (g, b, 0))
    patk_spec = pl.BlockSpec((PAIR, CODE_WIDTH, seq_len), lambda s, g, b: (g, 0, 0))
    pcq_spec = pl.BlockSpec((1, block_q, CODE_WIDTH), lambda s, g, b: (s, b, 0))
    pck_spec = pl.BlockSpec((1, CODE_WIDTH, seq_len), lambda s, g, b: (s, 0, 0))
    return query_spec, key_spec, patq_spec, patk_spec, pcq_spec, pck_spec


def attention_forward(query, keys, values, codes):
    seq_count, local_len, width = query.shape
    seq_len = keys.shape[1]
    block_q = min(256, local_len)
    grid = (seq_count, width // (PAIR * HD), local_len // block_q)
    query_spec, key_spec, patq_spec, patk_spec, pcq_spec, pck_spec = attention_specs(
        seq_count, local_len, seq_len, block_q
    )
    flops = 8 * seq_count * local_len * seq_len * width
    return pl.pallas_call(
        attention_fwd_kernel,
        grid=grid,
        in_specs=[query_spec, key_spec, key_spec, patq_spec, patk_spec, pcq_spec, pck_spec],
        out_specs=query_spec,
        out_shape=jax.ShapeDtypeStruct((seq_count, local_len, width), jnp.float32),
        compiler_params=pltpu.CompilerParams(
            dimension_semantics=("parallel", "parallel", "arbitrary"),
            vmem_limit_bytes=48 * 1024 * 1024,
        ),
        cost_estimate=pl.CostEstimate(
            flops=flops,
            transcendentals=seq_count * local_len * seq_len * width // HD,
            bytes_accessed=2 * query.size + 2 * keys.size * 2 * (local_len // block_q) + 4 * query.size,
        ),
    )(query, keys, values, *codes)


def attention_backward(query, keys, values, grad_out, codes):
    seq_count, local_len, width = query.shape
    seq_len = keys.shape[1]
    block_q = min(256, local_len)
    grid = (seq_count, width // (PAIR * HD), local_len // block_q)
    query_spec, key_spec, patq_spec, patk_spec, pcq_spec, pck_spec = attention_specs(
        seq_count, local_len, seq_len, block_q
    )
    flops = 20 * seq_count * local_len * seq_len * width
    return pl.pallas_call(
        attention_bwd_kernel,
        grid=grid,
        in_specs=[
            query_spec,
            key_spec,
            key_spec,
            query_spec,
            patq_spec,
            patk_spec,
            pcq_spec,
            pck_spec,
        ],
        out_specs=[query_spec, key_spec, key_spec],
        out_shape=[
            jax.ShapeDtypeStruct((seq_count, local_len, width), jnp.bfloat16),
            jax.ShapeDtypeStruct((seq_count, seq_len, width), jnp.float32),
            jax.ShapeDtypeStruct((seq_count, seq_len, width), jnp.float32),
        ],
        compiler_params=pltpu.CompilerParams(
            dimension_semantics=("parallel", "parallel", "arbitrary"),
            vmem_limit_bytes=48 * 1024 * 1024,
        ),
        cost_estimate=pl.CostEstimate(
            flops=flops,
            transcendentals=seq_count * local_len * seq_len * width // HD,
            bytes_accessed=4 * query.size + 2 * keys.size * 2 * (local_len // block_q) + 16 * keys.size,
        ),
    )(query, keys, values, grad_out, *codes)


def mask_codes(starts, query_position, key_position, segment_offsets, dilation_offsets, seq_len):
    heads = segment_offsets.shape[0]
    query_codes = []
    key_codes = []
    for pattern in range(len(span_parts)):
        span = seq_len * span_parts[pattern] // 8
        rate = dilation_rates[pattern]
        shift = (segment_offsets[:, pattern] % span)[:, None]
        phase = (dilation_offsets[:, pattern] % rate)[:, None]
        query_at = query_position[None, :] + shift
        key_at = key_position[None, :] + shift
        query_codes.append(jnp.where(query_at % rate == phase, query_at // span, -1))
        key_codes.append(jnp.where(key_at % rate == phase, key_at // span, -2))
    patterns = len(span_parts)
    query_codes.append(jnp.broadcast_to(query_position[None, :], (heads, query_position.shape[0])))
    key_codes.append(jnp.broadcast_to(key_position[None, :], (heads, key_position.shape[0])))
    filler = CODE_WIDTH - patterns - 1
    query_codes += [jnp.zeros((heads, query_position.shape[0]), jnp.int32)] * filler
    key_codes += [jnp.zeros((heads, key_position.shape[0]), jnp.int32)] * filler
    patq = jnp.stack(query_codes, 2).astype(jnp.int32)
    patk = jnp.stack(key_codes, 1).astype(jnp.int32)
    query_pic = picture_index(starts, query_position)
    key_pic = picture_index(starts, key_position)
    pcq = jnp.where(query_pic > 0, query_pic, -1)[:, :, None]
    pcq = jnp.pad(pcq, ((0, 0), (0, 0), (0, CODE_WIDTH - 1)))
    pck = jnp.where(key_pic > 0, key_pic, -2)[:, None, :]
    pck = jnp.pad(pck, ((0, 0), (0, CODE_WIDTH - 1), (0, 0)))
    return (patq, patk, pcq.astype(jnp.int32), pck.astype(jnp.int32))


def code_part(codes, begin, end, key_end):
    patq, patk, pcq, pck = codes
    return (patq[:, begin:end], patk[:, :, :key_end], pcq[:, begin:end], pck[:, :, :key_end])


def split_attention_forward(query, keys, values, codes, span):
    if span is None:
        return attention_forward(query, keys, values, codes)
    head = attention_forward(
        query[:, :span], keys[:, :span], values[:, :span], code_part(codes, 0, span, span)
    )
    seq_len = keys.shape[1]
    tail = attention_forward(
        query[:, span:], keys, values, code_part(codes, span, query.shape[1], seq_len)
    )
    return jnp.concatenate([head, tail], 1)


def split_attention_backward(query, keys, values, grad_out, codes, span):
    if span is None:
        return attention_backward(query, keys, values, grad_out, codes)
    seq_len = keys.shape[1]
    head_q, head_k, head_v = attention_backward(
        query[:, :span],
        keys[:, :span],
        values[:, :span],
        grad_out[:, :span],
        code_part(codes, 0, span, span),
    )
    tail_q, tail_k, tail_v = attention_backward(
        query[:, span:],
        keys,
        values,
        grad_out[:, span:],
        code_part(codes, span, query.shape[1], seq_len),
    )
    padding = ((0, 0), (0, seq_len - span), (0, 0))
    return (
        jnp.concatenate([head_q, tail_q], 1),
        tail_k + jnp.pad(head_k, padding),
        tail_v + jnp.pad(head_v, padding),
    )


def spread_sequence(block, local_len):
    me_c = lax.axis_index("context")
    me_t = lax.axis_index("tensor")
    swap = [(0, 1), (1, 0)]
    kept = lax.dynamic_slice_in_dim(block, me_c * local_len, local_len, 1)
    other = lax.dynamic_slice_in_dim(block, (1 - me_c) * local_len, local_len, 1)
    from_context = lax.ppermute(other, "context", perm=swap)
    from_tensor = lax.ppermute(kept, "tensor", perm=swap)
    from_corner = lax.ppermute(other, ("context", "tensor"), perm=[(0, 3), (3, 0), (1, 2), (2, 1)])
    first_c = me_c == 0
    own_pair = jnp.where(
        first_c,
        jnp.concatenate([kept, from_context], 0),
        jnp.concatenate([from_context, kept], 0),
    )
    far_pair = jnp.where(
        first_c,
        jnp.concatenate([from_tensor, from_corner], 0),
        jnp.concatenate([from_corner, from_tensor], 0),
    )
    return jnp.where(
        me_t == 0,
        jnp.concatenate([own_pair, far_pair], 0),
        jnp.concatenate([far_pair, own_pair], 0),
    )


def assemble(stacked, shard_dim, tensor_dim):
    ns, nt = stacked.shape[0], stacked.shape[1]
    if shard_dim is None:
        stacked = stacked[:1]
    if tensor_dim is None:
        stacked = stacked[:, :1]
    local_shape = stacked.shape[2:]
    order = []
    for dim in range(len(local_shape)):
        if dim == shard_dim:
            order.append(0)
        if dim == tensor_dim:
            order.append(1)
        order.append(dim + 2)
    if shard_dim is None:
        order = [0] + order
    if tensor_dim is None:
        order = [1] + order
    moved = stacked.transpose(order)
    full_shape = list(local_shape)
    if shard_dim is not None:
        full_shape[shard_dim] *= ns
    if tensor_dim is not None:
        full_shape[tensor_dim] *= nt
    return moved.reshape(full_shape)


def gather_weight(local_block, shard_dim, tensor_dim):
    ns = lax.axis_size("shard")
    nt = lax.axis_size("tensor")
    stacked = lax.all_gather(local_block, ("shard", "tensor"), axis=0, tiled=False)
    return assemble(stacked.reshape((ns, nt) + local_block.shape), shard_dim, tensor_dim)


def gather_packed(blocks):
    ns = lax.axis_size("shard")
    nt = lax.axis_size("tensor")
    flat = jnp.concatenate([block.reshape(-1) for block, _, _ in blocks])
    padded = -flat.size % 2048
    flat = jnp.pad(flat, (0, padded)).reshape(-1, 128)
    stacked = lax.all_gather(flat, ("shard", "tensor"), axis=0, tiled=False).reshape(ns, nt, -1)
    pieces = []
    offset = 0
    for block, shard_dim, tensor_dim in blocks:
        part = stacked[:, :, offset : offset + block.size].reshape((ns, nt) + block.shape)
        pieces.append(assemble(part, shard_dim, tensor_dim))
        offset += block.size
    return pieces


def pair_gather(block, axis_name, dim):
    if lax.axis_size(axis_name) != 2:
        return lax.all_gather(block, axis_name, axis=dim, tiled=True)
    other = lax.ppermute(block, axis_name, perm=[(0, 1), (1, 0)])
    first = lax.axis_index(axis_name) == 0
    return jnp.where(
        first, jnp.concatenate([block, other], dim), jnp.concatenate([other, block], dim)
    )


def pair_reduce(full, axis_name, dim):
    if lax.axis_size(axis_name) != 2:
        return lax.psum_scatter(
            full.astype(jnp.bfloat16), axis_name, scatter_dimension=dim, tiled=True
        ).astype(jnp.float32)
    half = full.shape[dim] // 2
    me = lax.axis_index(axis_name)
    kept = lax.dynamic_slice_in_dim(full, me * half, half, dim)
    sent = lax.dynamic_slice_in_dim(full, (1 - me) * half, half, dim).astype(jnp.bfloat16)
    received = lax.ppermute(sent, axis_name, perm=[(0, 1), (1, 0)])
    return kept + received.astype(jnp.float32)


def pair_sum(share, axis_name):
    if lax.axis_size(axis_name) != 2:
        return lax.psum(share, axis_name).astype(jnp.float32)
    received = lax.ppermute(share, axis_name, perm=[(0, 1), (1, 0)])
    return share.astype(jnp.float32) + received.astype(jnp.float32)


def disassemble(full, shard_dim, tensor_dim):
    ns = lax.axis_size("shard")
    nt = lax.axis_size("tensor")
    split_shape = []
    positions = {}
    for dim, size in enumerate(full.shape):
        if dim == shard_dim:
            positions["s"] = len(split_shape)
            split_shape += [ns, size // ns]
        elif dim == tensor_dim:
            positions["t"] = len(split_shape)
            split_shape += [nt, size // nt]
        else:
            split_shape.append(size)
    pieces = full.reshape(split_shape)
    lead = [positions[key] for key in ("s", "t") if key in positions]
    rest = [d for d in range(len(split_shape)) if d not in lead]
    pieces = pieces.transpose(lead + rest)
    if "s" not in positions:
        pieces = jnp.broadcast_to(pieces[None], (ns,) + pieces.shape)
    if "t" not in positions:
        pieces = jnp.broadcast_to(pieces[:, None], (ns, nt) + pieces.shape[1:])
    return pieces.reshape(ns * nt, -1)


def pack_rows(terms):
    rows = jnp.concatenate(
        [disassemble(full.astype(jnp.bfloat16), shard_dim, tensor_dim) for full, shard_dim, tensor_dim in terms],
        1,
    )
    width = rows.shape[1]
    return jnp.pad(rows, ((0, 0), (0, -width % 1024))).reshape(rows.shape[0], -1, 128)


def scatter_rows(rows):
    return lax.psum_scatter(rows, ("shard", "tensor"), scatter_dimension=0, tiled=False)


def unpack_share(share, terms):
    total = pair_sum(share, "context").reshape(-1)
    pieces = []
    offset = 0
    ns = lax.axis_size("shard")
    nt = lax.axis_size("tensor")
    for full, shard_dim, tensor_dim in terms:
        local_shape = list(full.shape)
        if shard_dim is not None:
            local_shape[shard_dim] //= ns
        if tensor_dim is not None:
            local_shape[tensor_dim] //= nt
        count = 1
        for size in local_shape:
            count *= size
        pieces.append(total[offset : offset + count].reshape(local_shape))
        offset += count
    return pieces


def shard_stage(grad, dim):
    return lax.psum_scatter(grad.astype(jnp.bfloat16), "shard", scatter_dimension=dim, tiled=True)


def finish_stage(share, tensor_dim):
    summed = pair_reduce(share, "tensor", tensor_dim)
    return pair_sum(summed.astype(jnp.bfloat16), "context")


def forward_pass(block_in, codes, weights, span):
    w_qkv, w_out, w_up, w_down, norm_gains, out_biases, head_biases, head_gain, unit_bias, unit_gain = weights
    seq_count, local_len, model_width = block_in.shape
    row_count = seq_count * local_len
    flattened_input = block_in.reshape(row_count, model_width).astype(jnp.float32)
    first_normed, first_inv, first_out = norm_rows(flattened_input, norm_gains[0])
    attn_in = first_out.astype(jnp.bfloat16)
    projected = jnp.einsum("rd,jde->jre", attn_in, w_qkv, preferred_element_type=jnp.float32)
    query_matrix = (projected[0] + head_biases[0]).astype(jnp.bfloat16)
    keys_local = projected[1].astype(jnp.bfloat16).reshape(seq_count, local_len, model_width)
    values_local = (projected[2] + head_biases[1]).astype(jnp.bfloat16).reshape(
        seq_count, local_len, model_width
    )
    if span is None:
        key_all = pair_gather(keys_local, "context", 1)
        value_all = pair_gather(values_local, "context", 1)
    else:
        key_all, value_all = keys_local, values_local
    attended = split_attention_forward(
        query_matrix.reshape(seq_count, local_len, model_width), key_all, value_all, codes, span
    ).reshape(row_count, model_width)
    sub_normed, sub_inv, sub_out = norm_rows(attended, head_gain)
    sub_in = sub_out.astype(jnp.bfloat16)
    middle = flattened_input + (
        jnp.dot(sub_in, w_out, preferred_element_type=jnp.float32) + out_biases[0]
    )
    second_normed, second_inv, second_out = norm_rows(middle, norm_gains[1])
    ffn_in = second_out.astype(jnp.bfloat16)
    hidden = jnp.dot(ffn_in, w_up, preferred_element_type=jnp.float32) + unit_bias
    activated = jax.nn.gelu(hidden, approximate=True)
    unit_normed, unit_inv, unit_out = norm_rows(activated, unit_gain)
    ffn_mid = unit_out.astype(jnp.bfloat16)
    layer_out = (
        middle + (jnp.dot(ffn_mid, w_down, preferred_element_type=jnp.float32) + out_biases[1])
    ).astype(jnp.bfloat16)
    kept_state = (
        attn_in,
        first_normed,
        first_inv,
        query_matrix,
        key_all,
        value_all,
        codes,
        sub_normed,
        sub_inv,
        sub_in,
        second_normed,
        second_inv,
        ffn_in,
        hidden,
        unit_normed,
        unit_inv,
        ffn_mid,
    )
    return (kept_state, layer_out.reshape(seq_count, local_len, model_width))


def backward_pass(kept_state, block_grad, weights, span):
    w_qkv, w_out, w_up, w_down, norm_gains, out_biases, head_biases, head_gain, unit_bias, unit_gain = weights
    (
        attn_in,
        first_normed,
        first_inv,
        query_matrix,
        key_all,
        value_all,
        codes,
        sub_normed,
        sub_inv,
        sub_in,
        second_normed,
        second_inv,
        ffn_in,
        hidden,
        unit_normed,
        unit_inv,
        ffn_mid,
    ) = kept_state
    seq_count, local_len, model_width = block_grad.shape
    row_count = seq_count * local_len
    seq_len = key_all.shape[1]
    grad_low = block_grad.reshape(row_count, model_width)
    grad_full = grad_low.astype(jnp.float32)
    down_grad = outer_sum(grad_low, ffn_mid)
    last_bias_grad = jnp.sum(grad_full, 0)
    unit_grad = back_dot(grad_low, w_down)
    activated_grad, unit_gain_grad = norm_back(unit_normed, unit_inv, unit_gain, unit_grad)
    gelu_value, gelu_pull = jax.vjp(partial(jax.nn.gelu, approximate=True), hidden)
    hidden_low = gelu_pull(activated_grad)[0].astype(jnp.bfloat16)
    up_grad = outer_sum(ffn_in, hidden_low)
    unit_bias_grad = jnp.sum(hidden_low, 0, dtype=jnp.float32)
    ffn_in_grad = back_dot(hidden_low, w_up)
    middle_part, second_gain_grad = norm_back(second_normed, second_inv, norm_gains[1], ffn_in_grad)
    middle_grad = grad_full + middle_part
    middle_low = middle_grad.astype(jnp.bfloat16)
    out_weight_grad = outer_sum(middle_low, sub_in)
    first_bias_grad = jnp.sum(middle_low, 0, dtype=jnp.float32)
    sub_grad = back_dot(middle_low, w_out)
    attended_grad, head_gain_grad = norm_back(sub_normed, sub_inv, head_gain, sub_grad)
    attended_low = attended_grad.astype(jnp.bfloat16)
    down_grad, up_grad, out_weight_grad, attended_low = lax.optimization_barrier(
        (
            down_grad.astype(jnp.bfloat16),
            up_grad.astype(jnp.bfloat16),
            out_weight_grad.astype(jnp.bfloat16),
            attended_low,
        )
    )
    tensor_count = lax.axis_size("tensor")
    early_widths = (down_grad.shape[1], up_grad.shape[1], out_weight_grad.shape[1])
    early_share = shard_stage(
        jnp.concatenate(
            [
                part.reshape(part.shape[0], tensor_count, part.shape[1] // tensor_count)
                for part in (down_grad, up_grad, out_weight_grad)
            ],
            2,
        ),
        0,
    )
    query_grad, key_part, value_part = split_attention_backward(
        query_matrix.reshape(seq_count, local_len, model_width),
        key_all,
        value_all,
        attended_low.reshape(seq_count, local_len, model_width),
        codes,
        span,
    )
    if span is not None:
        key_part = key_part.reshape(row_count, model_width)
        value_part = value_part.reshape(row_count, model_width)
    query_low = query_grad.reshape(row_count, model_width)
    if span is None:
        key_part = pair_reduce(key_part, "context", 1)
        value_part = pair_reduce(value_part, "context", 1)
    key_low = key_part.astype(jnp.bfloat16).reshape(row_count, model_width)
    value_low = value_part.astype(jnp.bfloat16).reshape(row_count, model_width)
    stacked = jnp.stack([query_low, key_low, value_low])
    early_share, stacked = lax.optimization_barrier((early_share, stacked))
    qkv_grad = jnp.einsum("rd,jre->dje", attn_in, stacked, preferred_element_type=jnp.float32)
    head_bias_grad = jnp.stack(
        [jnp.sum(query_low, 0, dtype=jnp.float32), jnp.sum(value_low, 0, dtype=jnp.float32)]
    )
    qkv_grad, stacked = lax.optimization_barrier((qkv_grad, stacked))
    attn_in_grad = jnp.einsum("jre,jde->rd", stacked, w_qkv, preferred_element_type=jnp.float32)
    early_total = finish_stage(early_share, 1).reshape(early_share.shape[0], -1)
    early_total, attn_in_grad = lax.optimization_barrier((early_total, attn_in_grad))
    input_part, first_gain_grad = norm_back(first_normed, first_inv, norm_gains[0], attn_in_grad)
    input_low = (middle_grad + input_part).astype(jnp.bfloat16)
    heads = model_width // HD
    unit_rows = unit_bias_grad.shape[0] // HD
    small_terms = (
        (jnp.stack([first_gain_grad, second_gain_grad]), 1, None),
        (jnp.stack([first_bias_grad, last_bias_grad]), 1, None),
        (head_bias_grad.reshape(2, heads, HD), 2, 1),
        (head_gain_grad.reshape(heads, HD), 1, 0),
        (unit_bias_grad.reshape(unit_rows, HD), 1, 0),
        (unit_gain_grad.reshape(unit_rows, HD), 1, 0),
    )
    ns = lax.axis_size("shard")
    nt = lax.axis_size("tensor")
    small_rows = jnp.concatenate(
        [disassemble(full, shard_dim, tensor_dim) for full, shard_dim, tensor_dim in small_terms], 1
    )
    small_width = small_rows.shape[1]
    block_rows = model_width // ns
    extra_rows = 8
    planes = qkv_grad.shape[1]
    slots = extra_rows * planes * (model_width // nt)
    small_block = (
        jnp.pad(small_rows, ((0, 0), (0, slots - small_width)))
        .reshape(ns, nt, extra_rows, planes, model_width // nt)
        .transpose(0, 2, 3, 1, 4)
        .reshape(ns, extra_rows, planes, model_width)
    )
    widened = jnp.concatenate(
        [qkv_grad.reshape(ns, block_rows, planes, model_width), small_block.astype(qkv_grad.dtype)], 1
    ).reshape(ns * (block_rows + extra_rows), planes, model_width)
    qkv_share = shard_stage(widened, 0)
    qkv_total = finish_stage(qkv_share, 2)
    small_total = qkv_total[block_rows:].reshape(-1)[:small_width]
    small_pieces = []
    offset = 0
    for full, shard_dim, tensor_dim in small_terms:
        local_shape = list(full.shape)
        if shard_dim is not None:
            local_shape[shard_dim] //= ns
        if tensor_dim is not None:
            local_shape[tensor_dim] //= nt
        count = 1
        for size in local_shape:
            count *= size
        small_pieces.append(small_total[offset : offset + count].reshape(local_shape))
        offset += count
    down_width = early_widths[0] // nt
    up_width = early_widths[1] // nt
    grad_shares = (
        early_total[:, :down_width].transpose(1, 0),
        early_total[:, down_width : down_width + up_width],
        early_total[:, down_width + up_width :].transpose(1, 0),
        qkv_total[:block_rows].transpose(1, 0, 2),
    ) + tuple(small_pieces)
    return (grad_shares, input_low.reshape(seq_count, local_len, model_width))


def local(
    inputs,
    out_grad,
    picture_starts,
    segment_offsets,
    dilation_offsets,
    norm_gains,
    w_qkv,
    head_biases,
    head_gain,
    w_out,
    out_biases,
    w_up,
    unit_bias,
    unit_gain,
    w_down,
):
    local_seqs, local_len, model_width = inputs.shape
    tensor_count = lax.axis_size("tensor")
    context_count = lax.axis_size("context")
    seq_len = local_len * context_count
    key_position = jnp.arange(seq_len, dtype=jnp.int32)
    whole = context_count == 2 and tensor_count == 2 and local_seqs == 4
    if whole:
        span = seq_len // PIECES
        me_c = lax.axis_index("context")
        own_seq = lax.axis_index("tensor") * context_count + me_c
        partner_seq = lax.axis_index("tensor") * context_count + 1 - me_c
        swap = [(0, 1), (1, 0)]

        def own_sequence(rows):
            kept = lax.dynamic_slice_in_dim(rows, own_seq, 1, 0)
            sent = lax.dynamic_slice_in_dim(rows, partner_seq, 1, 0)
            received = lax.ppermute(sent, "context", perm=swap)
            return jnp.where(
                me_c == 0,
                jnp.concatenate([kept, received], 1),
                jnp.concatenate([received, kept], 1),
            )

        block_in = own_sequence(inputs)
        block_grad = own_sequence(out_grad)
        starts = lax.dynamic_slice_in_dim(picture_starts, own_seq, 1, 0)
        query_position = key_position
    else:
        span = None
        mine = local_seqs // tensor_count
        first_seq = lax.axis_index("tensor") * mine
        block_in = lax.dynamic_slice_in_dim(inputs, first_seq, mine, 0)
        block_grad = lax.dynamic_slice_in_dim(out_grad, first_seq, mine, 0)
        starts = lax.dynamic_slice_in_dim(picture_starts, first_seq, mine, 0)
        query_position = lax.axis_index("context") * local_len + jnp.arange(
            local_len, dtype=jnp.int32
        )
    spans = jnp.array([seq_len * part // 8 for part in span_parts], jnp.int32)
    rates = jnp.array(dilation_rates, jnp.int32)
    segment_kept = segment_offsets % spans
    dilation_kept = dilation_offsets % rates
    offset_digits = jnp.concatenate(
        [segment_kept // 32, segment_kept % 32, dilation_kept], 1
    ).astype(jnp.bfloat16)
    f32 = jnp.float32
    (
        w_qkv_full,
        gains_full,
        out_bias_full,
        head_bias_full,
        head_gain_full,
        unit_bias_full,
        unit_gain_full,
        digits_full,
    ) = gather_packed(
        (
            (w_qkv, 1, 2),
            (norm_gains, 1, None),
            (out_biases, 1, None),
            (head_biases, 2, 1),
            (head_gain, 1, 0),
            (unit_bias, 1, 0),
            (unit_gain, 1, 0),
            (offset_digits, None, 0),
        )
    )
    patterns = len(span_parts)
    digits_full = digits_full.astype(jnp.int32)
    all_segments = digits_full[:, :patterns] * 32 + digits_full[:, patterns : 2 * patterns]
    all_dilations = digits_full[:, 2 * patterns :]
    codes = mask_codes(starts, query_position, key_position, all_segments, all_dilations, seq_len)
    w_out, w_up, w_down, w_qkv_full = lax.optimization_barrier((w_out, w_up, w_down, w_qkv_full))
    weights = (
        w_qkv_full,
        gather_weight(w_out, 1, 0),
        gather_weight(w_up, 0, 1),
        gather_weight(w_down, 1, 0),
        gains_full.astype(f32),
        out_bias_full.astype(f32),
        head_bias_full.reshape(2, model_width).astype(f32),
        head_gain_full.reshape(model_width).astype(f32),
        unit_bias_full.reshape(-1).astype(f32),
        unit_gain_full.reshape(-1).astype(f32),
    )
    kept_state, layer_block = forward_pass(block_in, codes, weights, span)
    if whole:
        layer_out = spread_sequence(layer_block, local_len)
    else:
        layer_out = pair_gather(layer_block, "tensor", 0)
    grad_shares, input_block = backward_pass(kept_state, block_grad, weights, span)
    if whole:
        input_grad = spread_sequence(input_block, local_len)
    else:
        input_grad = pair_gather(input_block, "tensor", 0)
    (
        down_share,
        up_share,
        out_share,
        qkv_share,
        gains_share,
        out_bias_share,
        head_bias_share,
        head_gain_share,
        unit_bias_share,
        unit_gain_share,
    ) = grad_shares
    return (
        layer_out,
        input_grad,
        gains_share,
        qkv_share,
        head_bias_share,
        head_gain_share,
        out_share,
        out_bias_share,
        up_share,
        unit_bias_share,
        unit_gain_share,
        down_share,
    )


def solution(mesh):
    placed = (
        P("shard", "context", None),
        P("shard", "context", None),
        P("shard", None),
        P("tensor", None),
        P("tensor", None),
        P(None, "shard"),
        P(None, "shard", "tensor"),
        P(None, "tensor", "shard"),
        P("tensor", "shard"),
        P("tensor", "shard"),
        P(None, "shard"),
        P("shard", "tensor"),
        P("tensor", "shard"),
        P("tensor", "shard"),
        P("tensor", "shard"),
    )
    return jax.shard_map(
        local,
        mesh=mesh,
        in_specs=placed,
        out_specs=(
            P("shard", "context", None),
            P("shard", "context", None),
            P(None, "shard"),
            P(None, "shard", "tensor"),
            P(None, "tensor", "shard"),
            P("tensor", "shard"),
            P("tensor", "shard"),
            P(None, "shard"),
            P("shard", "tensor"),
            P("tensor", "shard"),
            P("tensor", "shard"),
            P("tensor", "shard"),
        ),
        check_vma=False,
    )
```

```python
from functools import partial

import jax
import jax.numpy as jnp
from jax import lax
from jax.experimental import pallas as pl
from jax.experimental.pallas import tpu as pltpu
from jax.sharding import PartitionSpec as P

HD = 64
FF = 3072
PIECE = 256
PIECES = 2


epsilon = 1e-05
span_parts = (1, 2, 4, 6, 8)
dilation_rates = (1, 2, 4, 6, 12)


def pattern_total(query_position, key_position, segmented_offsets, dilated_offsets, token_length):
    tallied_total = jnp.zeros(
        (segmented_offsets.shape[0], query_position.shape[0], key_position.shape[0]), jnp.float32
    )
    for item_number in range(len(span_parts)):
        segmented_span = token_length * span_parts[item_number] // 8
        dilated_stride = dilation_rates[item_number]
        seg_shift = (segmented_offsets[:, item_number] % segmented_span)[:, None, None]
        dilated_phase = (dilated_offsets[:, item_number] % dilated_stride)[:, None, None]
        query_lookup = query_position[None, :, None] + seg_shift
        key_lookup = key_position[None, None, :] + seg_shift
        merged_heads = (
            (query_lookup // segmented_span == key_lookup // segmented_span)
            & (query_lookup % dilated_stride == dilated_phase)
            & (key_lookup % dilated_stride == dilated_phase)
        )
        tallied_total = tallied_total + merged_heads.astype(jnp.float32)
    return tallied_total


def picture_index(starts, token_positions):
    marked = jnp.zeros((starts.shape[0], token_positions.shape[0]), jnp.int32)
    for piece_number in range(starts.shape[1]):
        begin_at = starts[:, piece_number][:, None]
        inside = (token_positions[None, :] >= begin_at) & (
            token_positions[None, :] < begin_at + PIECE
        )
        marked = marked + (piece_number + 1) * inside.astype(jnp.int32)
    return marked


def allowed_keys(query_pic, key_pic, query_position, key_position):
    causal_ok = key_position[None, None, :] <= query_position[None, :, None]
    same_piece = (query_pic[:, :, None] == key_pic[:, None, :]) & (query_pic[:, :, None] > 0)
    return (causal_ok | same_piece).astype(jnp.float32)


def outer_sum(left_rows, right_rows):
    return lax.dot_general(
        left_rows, right_rows, (((0,), (0,)), ((), ())), preferred_element_type=jnp.float32
    )


def back_dot(left_rows, weight_rows):
    return lax.dot_general(
        left_rows, weight_rows, (((1,), (1,)), ((), ())), preferred_element_type=jnp.float32
    )


def norm_rows(values, scale_row):
    mean_row = jnp.mean(values, -1, keepdims=True)
    centered = values - mean_row
    inv_std = lax.rsqrt(jnp.mean(centered * centered, -1, keepdims=True) + epsilon)
    normed = centered * inv_std
    return (normed, inv_std, normed * scale_row)


def norm_back(normed, inv_std, scale_row, grad_rows):
    scaled = grad_rows * scale_row
    mean_plain = jnp.mean(scaled, -1, keepdims=True)
    mean_cross = jnp.mean(scaled * normed, -1, keepdims=True)
    return (inv_std * (scaled - mean_plain - normed * mean_cross), jnp.sum(grad_rows * normed, 0))


def probabilities(query_heads, key_heads, mask_table):
    raw_scores = jnp.einsum(
        "sqhd,skhd->shqk", query_heads, key_heads, preferred_element_type=jnp.float32
    ) * HD ** (-0.5)
    masked = jnp.where(mask_table > 0, raw_scores, -1000000000.0)
    row_top = jnp.max(masked, -1, keepdims=True)
    exponent = mask_table * jnp.exp(masked - row_top)
    row_total = jnp.sum(exponent, -1, keepdims=True)
    return (exponent / row_total, row_top, row_total)


SCALE = HD ** (-0.5)
HIDDEN = -1000000000.0
PAIR = 2
CODE_WIDTH = 8


def pair_masks(patq_ref, patk_ref, pcq_ref, pck_ref):
    first_q = patq_ref[0]
    first_k = patk_ref[0]
    row = first_q[:, 5:6]
    col = first_k[5:6, :]
    piece_q = pcq_ref[0][:, 0:1]
    piece_k = pck_ref[0][0:1, :]
    allowed = (col <= row) | (piece_q == piece_k)
    masks = []
    for head in range(PAIR):
        codes_q = patq_ref[head]
        codes_k = patk_ref[head]
        tally = (codes_q[:, 0:1] == codes_k[0:1, :]).astype(jnp.float32)
        for pattern in range(1, len(span_parts)):
            tally = tally + (
                codes_q[:, pattern : pattern + 1] == codes_k[pattern : pattern + 1, :]
            ).astype(jnp.float32)
        masks.append(jnp.where(allowed, tally, 0.0))
    return masks


def soft_rows(query_part, key_block, mask):
    scores = (
        lax.dot_general(
            query_part, key_block, (((1,), (1,)), ((), ())), preferred_element_type=jnp.float32
        )
        * SCALE
    )
    masked = jnp.where(mask > 0, scores, HIDDEN)
    top = jnp.max(masked, axis=1, keepdims=True)
    exponent = mask * jnp.exp(masked - top)
    return exponent / jnp.sum(exponent, axis=1, keepdims=True)


def attention_fwd_kernel(q_ref, k_ref, v_ref, patq_ref, patk_ref, pcq_ref, pck_ref, o_ref):
    query = q_ref[0]
    key_block = k_ref[0]
    value_block = v_ref[0]
    first = lax.broadcasted_iota(jnp.int32, query.shape, 1) < HD
    masks = pair_masks(patq_ref, patk_ref, pcq_ref, pck_ref)
    result = None
    for head in range(PAIR):
        keep = first if head == 0 else jnp.logical_not(first)
        query_part = jnp.where(keep, query, jnp.zeros_like(query))
        probs = soft_rows(query_part, key_block, masks[head])
        mixed = jnp.dot(
            probs.astype(jnp.bfloat16), value_block, preferred_element_type=jnp.float32
        )
        result = mixed if result is None else jnp.where(first, result, mixed)
    o_ref[0] = result


def attention_bwd_kernel(
    q_ref, k_ref, v_ref, do_ref, patq_ref, patk_ref, pcq_ref, pck_ref, dq_ref, dk_ref, dv_ref
):
    @pl.when(pl.program_id(2) == 0)
    def _():
        dk_ref[...] = jnp.zeros_like(dk_ref)
        dv_ref[...] = jnp.zeros_like(dv_ref)

    query = q_ref[0]
    key_block = k_ref[0]
    value_block = v_ref[0]
    grad_out = do_ref[0]
    first = lax.broadcasted_iota(jnp.int32, query.shape, 1) < HD
    masks = pair_masks(patq_ref, patk_ref, pcq_ref, pck_ref)
    query_grad = None
    key_grad = dk_ref[0]
    value_grad = dv_ref[0]
    for head in range(PAIR):
        keep = first if head == 0 else jnp.logical_not(first)
        query_part = jnp.where(keep, query, jnp.zeros_like(query))
        grad_part = jnp.where(keep, grad_out, jnp.zeros_like(grad_out))
        probs = soft_rows(query_part, key_block, masks[head])
        prob_grad = lax.dot_general(
            grad_part, value_block, (((1,), (1,)), ((), ())), preferred_element_type=jnp.float32
        )
        inner = jnp.sum(probs * prob_grad, axis=1, keepdims=True)
        score_low = (probs * (prob_grad - inner)).astype(jnp.bfloat16)
        part = jnp.dot(score_low, key_block, preferred_element_type=jnp.float32)
        query_grad = part if query_grad is None else jnp.where(first, query_grad, part)
        key_grad = key_grad + SCALE * lax.dot_general(
            score_low, query_part, (((0,), (0,)), ((), ())), preferred_element_type=jnp.float32
        )
        value_grad = value_grad + lax.dot_general(
            probs.astype(jnp.bfloat16),
            grad_part,
            (((0,), (0,)), ((), ())),
            preferred_element_type=jnp.float32,
        )
    dq_ref[0] = (query_grad * SCALE).astype(jnp.bfloat16)
    dk_ref[0] = key_grad
    dv_ref[0] = value_grad


def attention_specs(seq_count, local_len, seq_len, block_q):
    lanes = PAIR * HD
    query_spec = pl.BlockSpec((1, block_q, lanes), lambda s, g, b: (s, b, g))
    key_spec = pl.BlockSpec((1, seq_len, lanes), lambda s, g, b: (s, 0, g))
    patq_spec = pl.BlockSpec((PAIR, block_q, CODE_WIDTH), lambda s, g, b: (g, b, 0))
    patk_spec = pl.BlockSpec((PAIR, CODE_WIDTH, seq_len), lambda s, g, b: (g, 0, 0))
    pcq_spec = pl.BlockSpec((1, block_q, CODE_WIDTH), lambda s, g, b: (s, b, 0))
    pck_spec = pl.BlockSpec((1, CODE_WIDTH, seq_len), lambda s, g, b: (s, 0, 0))
    return query_spec, key_spec, patq_spec, patk_spec, pcq_spec, pck_spec


def attention_forward(query, keys, values, codes):
    seq_count, local_len, width = query.shape
    seq_len = keys.shape[1]
    block_q = min(256, local_len)
    grid = (seq_count, width // (PAIR * HD), local_len // block_q)
    query_spec, key_spec, patq_spec, patk_spec, pcq_spec, pck_spec = attention_specs(
        seq_count, local_len, seq_len, block_q
    )
    flops = 8 * seq_count * local_len * seq_len * width
    return pl.pallas_call(
        attention_fwd_kernel,
        grid=grid,
        in_specs=[query_spec, key_spec, key_spec, patq_spec, patk_spec, pcq_spec, pck_spec],
        out_specs=query_spec,
        out_shape=jax.ShapeDtypeStruct((seq_count, local_len, width), jnp.float32),
        compiler_params=pltpu.CompilerParams(
            dimension_semantics=("parallel", "parallel", "arbitrary"),
            vmem_limit_bytes=48 * 1024 * 1024,
        ),
        cost_estimate=pl.CostEstimate(
            flops=flops,
            transcendentals=seq_count * local_len * seq_len * width // HD,
            bytes_accessed=2 * query.size + 2 * keys.size * 2 * (local_len // block_q) + 4 * query.size,
        ),
    )(query, keys, values, *codes)


def attention_backward(query, keys, values, grad_out, codes):
    seq_count, local_len, width = query.shape
    seq_len = keys.shape[1]
    block_q = min(256, local_len)
    grid = (seq_count, width // (PAIR * HD), local_len // block_q)
    query_spec, key_spec, patq_spec, patk_spec, pcq_spec, pck_spec = attention_specs(
        seq_count, local_len, seq_len, block_q
    )
    flops = 20 * seq_count * local_len * seq_len * width
    return pl.pallas_call(
        attention_bwd_kernel,
        grid=grid,
        in_specs=[
            query_spec,
            key_spec,
            key_spec,
            query_spec,
            patq_spec,
            patk_spec,
            pcq_spec,
            pck_spec,
        ],
        out_specs=[query_spec, key_spec, key_spec],
        out_shape=[
            jax.ShapeDtypeStruct((seq_count, local_len, width), jnp.bfloat16),
            jax.ShapeDtypeStruct((seq_count, seq_len, width), jnp.float32),
            jax.ShapeDtypeStruct((seq_count, seq_len, width), jnp.float32),
        ],
        compiler_params=pltpu.CompilerParams(
            dimension_semantics=("parallel", "parallel", "arbitrary"),
            vmem_limit_bytes=48 * 1024 * 1024,
        ),
        cost_estimate=pl.CostEstimate(
            flops=flops,
            transcendentals=seq_count * local_len * seq_len * width // HD,
            bytes_accessed=4 * query.size + 2 * keys.size * 2 * (local_len // block_q) + 16 * keys.size,
        ),
    )(query, keys, values, grad_out, *codes)


def mask_codes(starts, query_position, key_position, segment_offsets, dilation_offsets, seq_len):
    heads = segment_offsets.shape[0]
    query_codes = []
    key_codes = []
    for pattern in range(len(span_parts)):
        span = seq_len * span_parts[pattern] // 8
        rate = dilation_rates[pattern]
        shift = (segment_offsets[:, pattern] % span)[:, None]
        phase = (dilation_offsets[:, pattern] % rate)[:, None]
        query_at = query_position[None, :] + shift
        key_at = key_position[None, :] + shift
        query_codes.append(jnp.where(query_at % rate == phase, query_at // span, -1))
        key_codes.append(jnp.where(key_at % rate == phase, key_at // span, -2))
    patterns = len(span_parts)
    query_codes.append(jnp.broadcast_to(query_position[None, :], (heads, query_position.shape[0])))
    key_codes.append(jnp.broadcast_to(key_position[None, :], (heads, key_position.shape[0])))
    filler = CODE_WIDTH - patterns - 1
    query_codes += [jnp.zeros((heads, query_position.shape[0]), jnp.int32)] * filler
    key_codes += [jnp.zeros((heads, key_position.shape[0]), jnp.int32)] * filler
    patq = jnp.stack(query_codes, 2).astype(jnp.int32)
    patk = jnp.stack(key_codes, 1).astype(jnp.int32)
    query_pic = picture_index(starts, query_position)
    key_pic = picture_index(starts, key_position)
    pcq = jnp.where(query_pic > 0, query_pic, -1)[:, :, None]
    pcq = jnp.pad(pcq, ((0, 0), (0, 0), (0, CODE_WIDTH - 1)))
    pck = jnp.where(key_pic > 0, key_pic, -2)[:, None, :]
    pck = jnp.pad(pck, ((0, 0), (0, CODE_WIDTH - 1), (0, 0)))
    return (patq, patk, pcq.astype(jnp.int32), pck.astype(jnp.int32))


def code_part(codes, begin, end, key_end):
    patq, patk, pcq, pck = codes
    return (patq[:, begin:end], patk[:, :, :key_end], pcq[:, begin:end], pck[:, :, :key_end])


def split_attention_forward(query, keys, values, codes, span):
    if span is None:
        return attention_forward(query, keys, values, codes)
    head = attention_forward(
        query[:, :span], keys[:, :span], values[:, :span], code_part(codes, 0, span, span)
    )
    seq_len = keys.shape[1]
    tail = attention_forward(
        query[:, span:], keys, values, code_part(codes, span, query.shape[1], seq_len)
    )
    return jnp.concatenate([head, tail], 1)


def split_attention_backward(query, keys, values, grad_out, codes, span):
    if span is None:
        return attention_backward(query, keys, values, grad_out, codes)
    seq_len = keys.shape[1]
    head_q, head_k, head_v = attention_backward(
        query[:, :span],
        keys[:, :span],
        values[:, :span],
        grad_out[:, :span],
        code_part(codes, 0, span, span),
    )
    tail_q, tail_k, tail_v = attention_backward(
        query[:, span:],
        keys,
        values,
        grad_out[:, span:],
        code_part(codes, span, query.shape[1], seq_len),
    )
    padding = ((0, 0), (0, seq_len - span), (0, 0))
    return (
        jnp.concatenate([head_q, tail_q], 1),
        tail_k + jnp.pad(head_k, padding),
        tail_v + jnp.pad(head_v, padding),
    )


def spread_sequence(block, local_len):
    me_c = lax.axis_index("context")
    me_t = lax.axis_index("tensor")
    swap = [(0, 1), (1, 0)]
    kept = lax.dynamic_slice_in_dim(block, me_c * local_len, local_len, 1)
    other = lax.dynamic_slice_in_dim(block, (1 - me_c) * local_len, local_len, 1)
    from_context = lax.ppermute(other, "context", perm=swap)
    from_tensor = lax.ppermute(kept, "tensor", perm=swap)
    from_corner = lax.ppermute(other, ("context", "tensor"), perm=[(0, 3), (3, 0), (1, 2), (2, 1)])
    first_c = me_c == 0
    own_pair = jnp.where(
        first_c,
        jnp.concatenate([kept, from_context], 0),
        jnp.concatenate([from_context, kept], 0),
    )
    far_pair = jnp.where(
        first_c,
        jnp.concatenate([from_tensor, from_corner], 0),
        jnp.concatenate([from_corner, from_tensor], 0),
    )
    return jnp.where(
        me_t == 0,
        jnp.concatenate([own_pair, far_pair], 0),
        jnp.concatenate([far_pair, own_pair], 0),
    )


def assemble(stacked, shard_dim, tensor_dim):
    ns, nt = stacked.shape[0], stacked.shape[1]
    if shard_dim is None:
        stacked = stacked[:1]
    if tensor_dim is None:
        stacked = stacked[:, :1]
    local_shape = stacked.shape[2:]
    order = []
    for dim in range(len(local_shape)):
        if dim == shard_dim:
            order.append(0)
        if dim == tensor_dim:
            order.append(1)
        order.append(dim + 2)
    if shard_dim is None:
        order = [0] + order
    if tensor_dim is None:
        order = [1] + order
    moved = stacked.transpose(order)
    full_shape = list(local_shape)
    if shard_dim is not None:
        full_shape[shard_dim] *= ns
    if tensor_dim is not None:
        full_shape[tensor_dim] *= nt
    return moved.reshape(full_shape)


def gather_weight(local_block, shard_dim, tensor_dim):
    ns = lax.axis_size("shard")
    nt = lax.axis_size("tensor")
    stacked = lax.all_gather(local_block, ("shard", "tensor"), axis=0, tiled=False)
    return assemble(stacked.reshape((ns, nt) + local_block.shape), shard_dim, tensor_dim)


def gather_packed(blocks):
    ns = lax.axis_size("shard")
    nt = lax.axis_size("tensor")
    flat = jnp.concatenate([block.reshape(-1) for block, _, _ in blocks])
    padded = -flat.size % 2048
    flat = jnp.pad(flat, (0, padded)).reshape(-1, 128)
    stacked = lax.all_gather(flat, ("shard", "tensor"), axis=0, tiled=False).reshape(ns, nt, -1)
    pieces = []
    offset = 0
    for block, shard_dim, tensor_dim in blocks:
        part = stacked[:, :, offset : offset + block.size].reshape((ns, nt) + block.shape)
        pieces.append(assemble(part, shard_dim, tensor_dim))
        offset += block.size
    return pieces


def pair_gather(block, axis_name, dim):
    if lax.axis_size(axis_name) != 2:
        return lax.all_gather(block, axis_name, axis=dim, tiled=True)
    other = lax.ppermute(block, axis_name, perm=[(0, 1), (1, 0)])
    first = lax.axis_index(axis_name) == 0
    return jnp.where(
        first, jnp.concatenate([block, other], dim), jnp.concatenate([other, block], dim)
    )


def pair_reduce(full, axis_name, dim):
    if lax.axis_size(axis_name) != 2:
        return lax.psum_scatter(
            full.astype(jnp.bfloat16), axis_name, scatter_dimension=dim, tiled=True
        ).astype(jnp.float32)
    half = full.shape[dim] // 2
    me = lax.axis_index(axis_name)
    kept = lax.dynamic_slice_in_dim(full, me * half, half, dim)
    sent = lax.dynamic_slice_in_dim(full, (1 - me) * half, half, dim).astype(jnp.bfloat16)
    received = lax.ppermute(sent, axis_name, perm=[(0, 1), (1, 0)])
    return kept + received.astype(jnp.float32)


def pair_sum(share, axis_name):
    if lax.axis_size(axis_name) != 2:
        return lax.psum(share, axis_name).astype(jnp.float32)
    received = lax.ppermute(share, axis_name, perm=[(0, 1), (1, 0)])
    return share.astype(jnp.float32) + received.astype(jnp.float32)


def disassemble(full, shard_dim, tensor_dim):
    ns = lax.axis_size("shard")
    nt = lax.axis_size("tensor")
    split_shape = []
    positions = {}
    for dim, size in enumerate(full.shape):
        if dim == shard_dim:
            positions["s"] = len(split_shape)
            split_shape += [ns, size // ns]
        elif dim == tensor_dim:
            positions["t"] = len(split_shape)
            split_shape += [nt, size // nt]
        else:
            split_shape.append(size)
    pieces = full.reshape(split_shape)
    lead = [positions[key] for key in ("s", "t") if key in positions]
    rest = [d for d in range(len(split_shape)) if d not in lead]
    pieces = pieces.transpose(lead + rest)
    if "s" not in positions:
        pieces = jnp.broadcast_to(pieces[None], (ns,) + pieces.shape)
    if "t" not in positions:
        pieces = jnp.broadcast_to(pieces[:, None], (ns, nt) + pieces.shape[1:])
    return pieces.reshape(ns * nt, -1)


def pack_rows(terms):
    rows = jnp.concatenate(
        [disassemble(full.astype(jnp.bfloat16), shard_dim, tensor_dim) for full, shard_dim, tensor_dim in terms],
        1,
    )
    width = rows.shape[1]
    return jnp.pad(rows, ((0, 0), (0, -width % 1024))).reshape(rows.shape[0], -1, 128)


def scatter_rows(rows):
    return lax.psum_scatter(rows, ("shard", "tensor"), scatter_dimension=0, tiled=False)


def unpack_share(share, terms):
    total = pair_sum(share, "context").reshape(-1)
    pieces = []
    offset = 0
    ns = lax.axis_size("shard")
    nt = lax.axis_size("tensor")
    for full, shard_dim, tensor_dim in terms:
        local_shape = list(full.shape)
        if shard_dim is not None:
            local_shape[shard_dim] //= ns
        if tensor_dim is not None:
            local_shape[tensor_dim] //= nt
        count = 1
        for size in local_shape:
            count *= size
        pieces.append(total[offset : offset + count].reshape(local_shape))
        offset += count
    return pieces


def shard_stage(grad, dim):
    return lax.psum_scatter(grad.astype(jnp.bfloat16), "shard", scatter_dimension=dim, tiled=True)


def finish_stage(share, tensor_dim):
    summed = pair_reduce(share, "tensor", tensor_dim)
    return pair_sum(summed.astype(jnp.bfloat16), "context")


def forward_pass(block_in, codes, weights, span):
    w_qkv, w_out, w_up, w_down, norm_gains, out_biases, head_biases, head_gain, unit_bias, unit_gain = weights
    seq_count, local_len, model_width = block_in.shape
    row_count = seq_count * local_len
    flattened_input = block_in.reshape(row_count, model_width).astype(jnp.float32)
    first_normed, first_inv, first_out = norm_rows(flattened_input, norm_gains[0])
    attn_in = first_out.astype(jnp.bfloat16)
    projected = jnp.einsum("rd,jde->jre", attn_in, w_qkv, preferred_element_type=jnp.float32)
    query_matrix = (projected[0] + head_biases[0]).astype(jnp.bfloat16)
    keys_local = projected[1].astype(jnp.bfloat16).reshape(seq_count, local_len, model_width)
    values_local = (projected[2] + head_biases[1]).astype(jnp.bfloat16).reshape(
        seq_count, local_len, model_width
    )
    if span is None:
        key_all = pair_gather(keys_local, "context", 1)
        value_all = pair_gather(values_local, "context", 1)
    else:
        key_all, value_all = keys_local, values_local
    attended = split_attention_forward(
        query_matrix.reshape(seq_count, local_len, model_width), key_all, value_all, codes, span
    ).reshape(row_count, model_width)
    sub_normed, sub_inv, sub_out = norm_rows(attended, head_gain)
    sub_in = sub_out.astype(jnp.bfloat16)
    middle = flattened_input + (
        jnp.dot(sub_in, w_out, preferred_element_type=jnp.float32) + out_biases[0]
    )
    second_normed, second_inv, second_out = norm_rows(middle, norm_gains[1])
    ffn_in = second_out.astype(jnp.bfloat16)
    hidden = jnp.dot(ffn_in, w_up, preferred_element_type=jnp.float32) + unit_bias
    activated = jax.nn.gelu(hidden, approximate=True)
    unit_normed, unit_inv, unit_out = norm_rows(activated, unit_gain)
    ffn_mid = unit_out.astype(jnp.bfloat16)
    layer_out = (
        middle + (jnp.dot(ffn_mid, w_down, preferred_element_type=jnp.float32) + out_biases[1])
    ).astype(jnp.bfloat16)
    kept_state = (
        attn_in,
        first_normed,
        first_inv,
        query_matrix,
        key_all,
        value_all,
        codes,
        sub_normed,
        sub_inv,
        sub_in,
        second_normed,
        second_inv,
        ffn_in,
        hidden,
        unit_normed,
        unit_inv,
        ffn_mid,
    )
    return (kept_state, layer_out.reshape(seq_count, local_len, model_width))


def backward_pass(kept_state, block_grad, weights, span, carried):
    w_qkv, w_out, w_up, w_down, norm_gains, out_biases, head_biases, head_gain, unit_bias, unit_gain = weights
    (
        attn_in,
        first_normed,
        first_inv,
        query_matrix,
        key_all,
        value_all,
        codes,
        sub_normed,
        sub_inv,
        sub_in,
        second_normed,
        second_inv,
        ffn_in,
        hidden,
        unit_normed,
        unit_inv,
        ffn_mid,
    ) = kept_state
    seq_count, local_len, model_width = block_grad.shape
    row_count = seq_count * local_len
    seq_len = key_all.shape[1]
    grad_low = block_grad.reshape(row_count, model_width)
    grad_full = grad_low.astype(jnp.float32)
    down_grad = outer_sum(grad_low, ffn_mid)
    last_bias_grad = jnp.sum(grad_full, 0)
    unit_grad = back_dot(grad_low, w_down)
    activated_grad, unit_gain_grad = norm_back(unit_normed, unit_inv, unit_gain, unit_grad)
    gelu_value, gelu_pull = jax.vjp(partial(jax.nn.gelu, approximate=True), hidden)
    hidden_low = gelu_pull(activated_grad)[0].astype(jnp.bfloat16)
    up_grad = outer_sum(ffn_in, hidden_low)
    unit_bias_grad = jnp.sum(hidden_low, 0, dtype=jnp.float32)
    ffn_in_grad = back_dot(hidden_low, w_up)
    middle_part, second_gain_grad = norm_back(second_normed, second_inv, norm_gains[1], ffn_in_grad)
    middle_grad = grad_full + middle_part
    middle_low = middle_grad.astype(jnp.bfloat16)
    out_weight_grad = outer_sum(middle_low, sub_in)
    first_bias_grad = jnp.sum(middle_low, 0, dtype=jnp.float32)
    sub_grad = back_dot(middle_low, w_out)
    attended_grad, head_gain_grad = norm_back(sub_normed, sub_inv, head_gain, sub_grad)
    attended_low = attended_grad.astype(jnp.bfloat16)
    down_grad, up_grad, out_weight_grad, attended_low = lax.optimization_barrier(
        (
            down_grad.astype(jnp.bfloat16),
            up_grad.astype(jnp.bfloat16),
            out_weight_grad.astype(jnp.bfloat16),
            attended_low,
        )
    )
    tensor_count = lax.axis_size("tensor")
    early_widths = (down_grad.shape[1], up_grad.shape[1], out_weight_grad.shape[1])
    early_share = shard_stage(
        jnp.concatenate(
            [
                part.reshape(part.shape[0], tensor_count, part.shape[1] // tensor_count)
                for part in (down_grad, up_grad, out_weight_grad)
            ],
            2,
        ),
        0,
    )
    query_grad, key_part, value_part = split_attention_backward(
        query_matrix.reshape(seq_count, local_len, model_width),
        key_all,
        value_all,
        attended_low.reshape(seq_count, local_len, model_width),
        codes,
        span,
    )
    if span is not None:
        key_part = key_part.reshape(row_count, model_width)
        value_part = value_part.reshape(row_count, model_width)
    query_low = query_grad.reshape(row_count, model_width)
    if span is None:
        key_part = pair_reduce(key_part, "context", 1)
        value_part = pair_reduce(value_part, "context", 1)
    key_low = key_part.astype(jnp.bfloat16).reshape(row_count, model_width)
    value_low = value_part.astype(jnp.bfloat16).reshape(row_count, model_width)
    stacked = jnp.stack([query_low, key_low, value_low])
    early_share, stacked, carried = lax.optimization_barrier((early_share, stacked, carried))
    qkv_grad = jnp.einsum("rd,jre->dje", attn_in, stacked, preferred_element_type=jnp.float32)
    head_bias_grad = jnp.stack(
        [jnp.sum(query_low, 0, dtype=jnp.float32), jnp.sum(value_low, 0, dtype=jnp.float32)]
    )
    qkv_grad, stacked = lax.optimization_barrier((qkv_grad, stacked))
    attn_in_grad = jnp.einsum("jre,jde->rd", stacked, w_qkv, preferred_element_type=jnp.float32)
    input_part, first_gain_grad = norm_back(first_normed, first_inv, norm_gains[0], attn_in_grad)
    input_low = (middle_grad + input_part).astype(jnp.bfloat16)
    heads = model_width // HD
    unit_rows = unit_bias_grad.shape[0] // HD
    small_terms = (
        (jnp.stack([first_gain_grad, second_gain_grad]), 1, None),
        (jnp.stack([first_bias_grad, last_bias_grad]), 1, None),
        (head_bias_grad.reshape(2, heads, HD), 2, 1),
        (head_gain_grad.reshape(heads, HD), 1, 0),
        (unit_bias_grad.reshape(unit_rows, HD), 1, 0),
        (unit_gain_grad.reshape(unit_rows, HD), 1, 0),
    )
    ns = lax.axis_size("shard")
    nt = lax.axis_size("tensor")
    small_rows = jnp.concatenate(
        [disassemble(full, shard_dim, tensor_dim) for full, shard_dim, tensor_dim in small_terms], 1
    )
    small_width = small_rows.shape[1]
    block_rows = model_width // ns
    extra_rows = 8
    planes = qkv_grad.shape[1]
    slots = extra_rows * planes * (model_width // nt)
    small_block = (
        jnp.pad(small_rows, ((0, 0), (0, slots - small_width)))
        .reshape(ns, nt, extra_rows, planes, model_width // nt)
        .transpose(0, 2, 3, 1, 4)
        .reshape(ns, extra_rows, planes, model_width)
    )
    widened = jnp.concatenate(
        [qkv_grad.reshape(ns, block_rows, planes, model_width), small_block.astype(qkv_grad.dtype)], 1
    ).reshape(ns * (block_rows + extra_rows), planes, model_width)
    qkv_share = shard_stage(widened, 0)
    qkv_total = finish_stage(qkv_share, 2)
    small_total = qkv_total[block_rows:].reshape(-1)[:small_width]
    small_pieces = []
    offset = 0
    for full, shard_dim, tensor_dim in small_terms:
        local_shape = list(full.shape)
        if shard_dim is not None:
            local_shape[shard_dim] //= ns
        if tensor_dim is not None:
            local_shape[tensor_dim] //= nt
        count = 1
        for size in local_shape:
            count *= size
        small_pieces.append(small_total[offset : offset + count].reshape(local_shape))
        offset += count
    early_total = finish_stage(early_share, 1).reshape(early_share.shape[0], -1)
    down_width = early_widths[0] // nt
    up_width = early_widths[1] // nt
    grad_shares = (
        early_total[:, :down_width].transpose(1, 0),
        early_total[:, down_width : down_width + up_width],
        early_total[:, down_width + up_width :].transpose(1, 0),
        qkv_total[:block_rows].transpose(1, 0, 2),
    ) + tuple(small_pieces)
    return (grad_shares, input_low.reshape(seq_count, local_len, model_width), carried)


def local(
    inputs,
    out_grad,
    picture_starts,
    segment_offsets,
    dilation_offsets,
    norm_gains,
    w_qkv,
    head_biases,
    head_gain,
    w_out,
    out_biases,
    w_up,
    unit_bias,
    unit_gain,
    w_down,
):
    local_seqs, local_len, model_width = inputs.shape
    tensor_count = lax.axis_size("tensor")
    context_count = lax.axis_size("context")
    seq_len = local_len * context_count
    key_position = jnp.arange(seq_len, dtype=jnp.int32)
    whole = context_count == 2 and tensor_count == 2 and local_seqs == 4
    if whole:
        span = seq_len // PIECES
        me_c = lax.axis_index("context")
        own_seq = lax.axis_index("tensor") * context_count + me_c
        partner_seq = lax.axis_index("tensor") * context_count + 1 - me_c
        swap = [(0, 1), (1, 0)]

        def own_sequence(rows):
            kept = lax.dynamic_slice_in_dim(rows, own_seq, 1, 0)
            sent = lax.dynamic_slice_in_dim(rows, partner_seq, 1, 0)
            received = lax.ppermute(sent, "context", perm=swap)
            return jnp.where(
                me_c == 0,
                jnp.concatenate([kept, received], 1),
                jnp.concatenate([received, kept], 1),
            )

        block_in = own_sequence(inputs)
        block_grad = own_sequence(out_grad)
        starts = lax.dynamic_slice_in_dim(picture_starts, own_seq, 1, 0)
        query_position = key_position
    else:
        span = None
        mine = local_seqs // tensor_count
        first_seq = lax.axis_index("tensor") * mine
        block_in = lax.dynamic_slice_in_dim(inputs, first_seq, mine, 0)
        block_grad = lax.dynamic_slice_in_dim(out_grad, first_seq, mine, 0)
        starts = lax.dynamic_slice_in_dim(picture_starts, first_seq, mine, 0)
        query_position = lax.axis_index("context") * local_len + jnp.arange(
            local_len, dtype=jnp.int32
        )
    spans = jnp.array([seq_len * part // 8 for part in span_parts], jnp.int32)
    rates = jnp.array(dilation_rates, jnp.int32)
    segment_kept = segment_offsets % spans
    dilation_kept = dilation_offsets % rates
    offset_digits = jnp.concatenate(
        [segment_kept // 32, segment_kept % 32, dilation_kept], 1
    ).astype(jnp.bfloat16)
    f32 = jnp.float32
    (
        w_qkv_full,
        gains_full,
        out_bias_full,
        head_bias_full,
        head_gain_full,
        unit_bias_full,
        unit_gain_full,
        digits_full,
    ) = gather_packed(
        (
            (w_qkv, 1, 2),
            (norm_gains, 1, None),
            (out_biases, 1, None),
            (head_biases, 2, 1),
            (head_gain, 1, 0),
            (unit_bias, 1, 0),
            (unit_gain, 1, 0),
            (offset_digits, None, 0),
        )
    )
    patterns = len(span_parts)
    digits_full = digits_full.astype(jnp.int32)
    all_segments = digits_full[:, :patterns] * 32 + digits_full[:, patterns : 2 * patterns]
    all_dilations = digits_full[:, 2 * patterns :]
    codes = mask_codes(starts, query_position, key_position, all_segments, all_dilations, seq_len)
    w_out, w_up, w_down, w_qkv_full = lax.optimization_barrier((w_out, w_up, w_down, w_qkv_full))
    weights = (
        w_qkv_full,
        gather_weight(w_out, 1, 0),
        gather_weight(w_up, 0, 1),
        gather_weight(w_down, 1, 0),
        gains_full.astype(f32),
        out_bias_full.astype(f32),
        head_bias_full.reshape(2, model_width).astype(f32),
        head_gain_full.reshape(model_width).astype(f32),
        unit_bias_full.reshape(-1).astype(f32),
        unit_gain_full.reshape(-1).astype(f32),
    )
    kept_state, layer_block = forward_pass(block_in, codes, weights, span)
    if whole:
        layer_out = spread_sequence(layer_block, local_len)
    else:
        layer_out = pair_gather(layer_block, "tensor", 0)
    grad_shares, input_block, layer_out = backward_pass(
        kept_state, block_grad, weights, span, layer_out
    )
    if whole:
        input_grad = spread_sequence(input_block, local_len)
    else:
        input_grad = pair_gather(input_block, "tensor", 0)
    (
        down_share,
        up_share,
        out_share,
        qkv_share,
        gains_share,
        out_bias_share,
        head_bias_share,
        head_gain_share,
        unit_bias_share,
        unit_gain_share,
    ) = grad_shares
    return (
        layer_out,
        input_grad,
        gains_share,
        qkv_share,
        head_bias_share,
        head_gain_share,
        out_share,
        out_bias_share,
        up_share,
        unit_bias_share,
        unit_gain_share,
        down_share,
    )


def solution(mesh):
    placed = (
        P("shard", "context", None),
        P("shard", "context", None),
        P("shard", None),
        P("tensor", None),
        P("tensor", None),
        P(None, "shard"),
        P(None, "shard", "tensor"),
        P(None, "tensor", "shard"),
        P("tensor", "shard"),
        P("tensor", "shard"),
        P(None, "shard"),
        P("shard", "tensor"),
        P("tensor", "shard"),
        P("tensor", "shard"),
        P("tensor", "shard"),
    )
    return jax.shard_map(
        local,
        mesh=mesh,
        in_specs=placed,
        out_specs=(
            P("shard", "context", None),
            P("shard", "context", None),
            P(None, "shard"),
            P(None, "shard", "tensor"),
            P(None, "tensor", "shard"),
            P("tensor", "shard"),
            P("tensor", "shard"),
            P(None, "shard"),
            P("shard", "tensor"),
            P("tensor", "shard"),
            P("tensor", "shard"),
            P("tensor", "shard"),
        ),
        check_vma=False,
    )
```

```python
from functools import partial

import jax
import jax.numpy as jnp
from jax import lax
from jax.experimental import pallas as pl
from jax.experimental.pallas import tpu as pltpu
from jax.sharding import PartitionSpec as P

HD = 64
FF = 3072
PIECE = 256
PIECES = 2


epsilon = 1e-05
span_parts = (1, 2, 4, 6, 8)
dilation_rates = (1, 2, 4, 6, 12)


def pattern_total(query_position, key_position, segmented_offsets, dilated_offsets, token_length):
    tallied_total = jnp.zeros(
        (segmented_offsets.shape[0], query_position.shape[0], key_position.shape[0]), jnp.float32
    )
    for item_number in range(len(span_parts)):
        segmented_span = token_length * span_parts[item_number] // 8
        dilated_stride = dilation_rates[item_number]
        seg_shift = (segmented_offsets[:, item_number] % segmented_span)[:, None, None]
        dilated_phase = (dilated_offsets[:, item_number] % dilated_stride)[:, None, None]
        query_lookup = query_position[None, :, None] + seg_shift
        key_lookup = key_position[None, None, :] + seg_shift
        merged_heads = (
            (query_lookup // segmented_span == key_lookup // segmented_span)
            & (query_lookup % dilated_stride == dilated_phase)
            & (key_lookup % dilated_stride == dilated_phase)
        )
        tallied_total = tallied_total + merged_heads.astype(jnp.float32)
    return tallied_total


def picture_index(starts, token_positions):
    marked = jnp.zeros((starts.shape[0], token_positions.shape[0]), jnp.int32)
    for piece_number in range(starts.shape[1]):
        begin_at = starts[:, piece_number][:, None]
        inside = (token_positions[None, :] >= begin_at) & (
            token_positions[None, :] < begin_at + PIECE
        )
        marked = marked + (piece_number + 1) * inside.astype(jnp.int32)
    return marked


def allowed_keys(query_pic, key_pic, query_position, key_position):
    causal_ok = key_position[None, None, :] <= query_position[None, :, None]
    same_piece = (query_pic[:, :, None] == key_pic[:, None, :]) & (query_pic[:, :, None] > 0)
    return (causal_ok | same_piece).astype(jnp.float32)


def outer_sum(left_rows, right_rows):
    return lax.dot_general(
        left_rows, right_rows, (((0,), (0,)), ((), ())), preferred_element_type=jnp.float32
    )


def back_dot(left_rows, weight_rows):
    return lax.dot_general(
        left_rows, weight_rows, (((1,), (1,)), ((), ())), preferred_element_type=jnp.float32
    )


def norm_rows(values, scale_row):
    mean_row = jnp.mean(values, -1, keepdims=True)
    centered = values - mean_row
    inv_std = lax.rsqrt(jnp.mean(centered * centered, -1, keepdims=True) + epsilon)
    normed = centered * inv_std
    return (normed, inv_std, normed * scale_row)


def norm_back(normed, inv_std, scale_row, grad_rows):
    scaled = grad_rows * scale_row
    mean_plain = jnp.mean(scaled, -1, keepdims=True)
    mean_cross = jnp.mean(scaled * normed, -1, keepdims=True)
    return (inv_std * (scaled - mean_plain - normed * mean_cross), jnp.sum(grad_rows * normed, 0))


def probabilities(query_heads, key_heads, mask_table):
    raw_scores = jnp.einsum(
        "sqhd,skhd->shqk", query_heads, key_heads, preferred_element_type=jnp.float32
    ) * HD ** (-0.5)
    masked = jnp.where(mask_table > 0, raw_scores, -1000000000.0)
    row_top = jnp.max(masked, -1, keepdims=True)
    exponent = mask_table * jnp.exp(masked - row_top)
    row_total = jnp.sum(exponent, -1, keepdims=True)
    return (exponent / row_total, row_top, row_total)


SCALE = HD ** (-0.5)
HIDDEN = -1000000000.0
PAIR = 2
CODE_WIDTH = 8


def pair_masks(patq_ref, patk_ref, pcq_ref, pck_ref):
    first_q = patq_ref[0]
    first_k = patk_ref[0]
    row = first_q[:, 5:6]
    col = first_k[5:6, :]
    piece_q = pcq_ref[0][:, 0:1]
    piece_k = pck_ref[0][0:1, :]
    allowed = (col <= row) | (piece_q == piece_k)
    masks = []
    for head in range(PAIR):
        codes_q = patq_ref[head]
        codes_k = patk_ref[head]
        tally = (codes_q[:, 0:1] == codes_k[0:1, :]).astype(jnp.float32)
        for pattern in range(1, len(span_parts)):
            tally = tally + (
                codes_q[:, pattern : pattern + 1] == codes_k[pattern : pattern + 1, :]
            ).astype(jnp.float32)
        masks.append(jnp.where(allowed, tally, 0.0))
    return masks


def soft_rows(query_part, key_block, mask):
    scores = (
        lax.dot_general(
            query_part, key_block, (((1,), (1,)), ((), ())), preferred_element_type=jnp.float32
        )
        * SCALE
    )
    masked = jnp.where(mask > 0, scores, HIDDEN)
    top = jnp.max(masked, axis=1, keepdims=True)
    exponent = mask * jnp.exp(masked - top)
    return exponent / jnp.sum(exponent, axis=1, keepdims=True)


def attention_fwd_kernel(q_ref, k_ref, v_ref, patq_ref, patk_ref, pcq_ref, pck_ref, o_ref):
    query = q_ref[0]
    key_block = k_ref[0]
    value_block = v_ref[0]
    first = lax.broadcasted_iota(jnp.int32, query.shape, 1) < HD
    masks = pair_masks(patq_ref, patk_ref, pcq_ref, pck_ref)
    result = None
    for head in range(PAIR):
        keep = first if head == 0 else jnp.logical_not(first)
        query_part = jnp.where(keep, query, jnp.zeros_like(query))
        probs = soft_rows(query_part, key_block, masks[head])
        mixed = jnp.dot(
            probs.astype(jnp.bfloat16), value_block, preferred_element_type=jnp.float32
        )
        result = mixed if result is None else jnp.where(first, result, mixed)
    o_ref[0] = result


def attention_bwd_kernel(
    q_ref, k_ref, v_ref, do_ref, patq_ref, patk_ref, pcq_ref, pck_ref, dq_ref, dk_ref, dv_ref
):
    @pl.when(pl.program_id(2) == 0)
    def _():
        dk_ref[...] = jnp.zeros_like(dk_ref)
        dv_ref[...] = jnp.zeros_like(dv_ref)

    query = q_ref[0]
    key_block = k_ref[0]
    value_block = v_ref[0]
    grad_out = do_ref[0]
    first = lax.broadcasted_iota(jnp.int32, query.shape, 1) < HD
    masks = pair_masks(patq_ref, patk_ref, pcq_ref, pck_ref)
    query_grad = None
    key_grad = dk_ref[0]
    value_grad = dv_ref[0]
    for head in range(PAIR):
        keep = first if head == 0 else jnp.logical_not(first)
        query_part = jnp.where(keep, query, jnp.zeros_like(query))
        grad_part = jnp.where(keep, grad_out, jnp.zeros_like(grad_out))
        probs = soft_rows(query_part, key_block, masks[head])
        prob_grad = lax.dot_general(
            grad_part, value_block, (((1,), (1,)), ((), ())), preferred_element_type=jnp.float32
        )
        inner = jnp.sum(probs * prob_grad, axis=1, keepdims=True)
        score_low = (probs * (prob_grad - inner)).astype(jnp.bfloat16)
        part = jnp.dot(score_low, key_block, preferred_element_type=jnp.float32)
        query_grad = part if query_grad is None else jnp.where(first, query_grad, part)
        key_grad = key_grad + SCALE * lax.dot_general(
            score_low, query_part, (((0,), (0,)), ((), ())), preferred_element_type=jnp.float32
        )
        value_grad = value_grad + lax.dot_general(
            probs.astype(jnp.bfloat16),
            grad_part,
            (((0,), (0,)), ((), ())),
            preferred_element_type=jnp.float32,
        )
    dq_ref[0] = (query_grad * SCALE).astype(jnp.bfloat16)
    dk_ref[0] = key_grad
    dv_ref[0] = value_grad


def attention_specs(seq_count, local_len, seq_len, block_q):
    lanes = PAIR * HD
    query_spec = pl.BlockSpec((1, block_q, lanes), lambda s, g, b: (s, b, g))
    key_spec = pl.BlockSpec((1, seq_len, lanes), lambda s, g, b: (s, 0, g))
    patq_spec = pl.BlockSpec((PAIR, block_q, CODE_WIDTH), lambda s, g, b: (g, b, 0))
    patk_spec = pl.BlockSpec((PAIR, CODE_WIDTH, seq_len), lambda s, g, b: (g, 0, 0))
    pcq_spec = pl.BlockSpec((1, block_q, CODE_WIDTH), lambda s, g, b: (s, b, 0))
    pck_spec = pl.BlockSpec((1, CODE_WIDTH, seq_len), lambda s, g, b: (s, 0, 0))
    return query_spec, key_spec, patq_spec, patk_spec, pcq_spec, pck_spec


def attention_forward(query, keys, values, codes):
    seq_count, local_len, width = query.shape
    seq_len = keys.shape[1]
    block_q = min(256, local_len)
    grid = (seq_count, width // (PAIR * HD), local_len // block_q)
    query_spec, key_spec, patq_spec, patk_spec, pcq_spec, pck_spec = attention_specs(
        seq_count, local_len, seq_len, block_q
    )
    flops = 8 * seq_count * local_len * seq_len * width
    return pl.pallas_call(
        attention_fwd_kernel,
        grid=grid,
        in_specs=[query_spec, key_spec, key_spec, patq_spec, patk_spec, pcq_spec, pck_spec],
        out_specs=query_spec,
        out_shape=jax.ShapeDtypeStruct((seq_count, local_len, width), jnp.float32),
        compiler_params=pltpu.CompilerParams(
            dimension_semantics=("parallel", "parallel", "arbitrary"),
            vmem_limit_bytes=48 * 1024 * 1024,
        ),
        cost_estimate=pl.CostEstimate(
            flops=flops,
            transcendentals=seq_count * local_len * seq_len * width // HD,
            bytes_accessed=2 * query.size + 2 * keys.size * 2 * (local_len // block_q) + 4 * query.size,
        ),
    )(query, keys, values, *codes)


def attention_backward(query, keys, values, grad_out, codes):
    seq_count, local_len, width = query.shape
    seq_len = keys.shape[1]
    block_q = min(256, local_len)
    grid = (seq_count, width // (PAIR * HD), local_len // block_q)
    query_spec, key_spec, patq_spec, patk_spec, pcq_spec, pck_spec = attention_specs(
        seq_count, local_len, seq_len, block_q
    )
    flops = 20 * seq_count * local_len * seq_len * width
    return pl.pallas_call(
        attention_bwd_kernel,
        grid=grid,
        in_specs=[
            query_spec,
            key_spec,
            key_spec,
            query_spec,
            patq_spec,
            patk_spec,
            pcq_spec,
            pck_spec,
        ],
        out_specs=[query_spec, key_spec, key_spec],
        out_shape=[
            jax.ShapeDtypeStruct((seq_count, local_len, width), jnp.bfloat16),
            jax.ShapeDtypeStruct((seq_count, seq_len, width), jnp.float32),
            jax.ShapeDtypeStruct((seq_count, seq_len, width), jnp.float32),
        ],
        compiler_params=pltpu.CompilerParams(
            dimension_semantics=("parallel", "parallel", "arbitrary"),
            vmem_limit_bytes=48 * 1024 * 1024,
        ),
        cost_estimate=pl.CostEstimate(
            flops=flops,
            transcendentals=seq_count * local_len * seq_len * width // HD,
            bytes_accessed=4 * query.size + 2 * keys.size * 2 * (local_len // block_q) + 16 * keys.size,
        ),
    )(query, keys, values, grad_out, *codes)


def mask_codes(starts, query_position, key_position, segment_offsets, dilation_offsets, seq_len):
    heads = segment_offsets.shape[0]
    query_codes = []
    key_codes = []
    for pattern in range(len(span_parts)):
        span = seq_len * span_parts[pattern] // 8
        rate = dilation_rates[pattern]
        shift = (segment_offsets[:, pattern] % span)[:, None]
        phase = (dilation_offsets[:, pattern] % rate)[:, None]
        query_at = query_position[None, :] + shift
        key_at = key_position[None, :] + shift
        query_codes.append(jnp.where(query_at % rate == phase, query_at // span, -1))
        key_codes.append(jnp.where(key_at % rate == phase, key_at // span, -2))
    patterns = len(span_parts)
    query_codes.append(jnp.broadcast_to(query_position[None, :], (heads, query_position.shape[0])))
    key_codes.append(jnp.broadcast_to(key_position[None, :], (heads, key_position.shape[0])))
    filler = CODE_WIDTH - patterns - 1
    query_codes += [jnp.zeros((heads, query_position.shape[0]), jnp.int32)] * filler
    key_codes += [jnp.zeros((heads, key_position.shape[0]), jnp.int32)] * filler
    patq = jnp.stack(query_codes, 2).astype(jnp.int32)
    patk = jnp.stack(key_codes, 1).astype(jnp.int32)
    query_pic = picture_index(starts, query_position)
    key_pic = picture_index(starts, key_position)
    pcq = jnp.where(query_pic > 0, query_pic, -1)[:, :, None]
    pcq = jnp.pad(pcq, ((0, 0), (0, 0), (0, CODE_WIDTH - 1)))
    pck = jnp.where(key_pic > 0, key_pic, -2)[:, None, :]
    pck = jnp.pad(pck, ((0, 0), (0, CODE_WIDTH - 1), (0, 0)))
    return (patq, patk, pcq.astype(jnp.int32), pck.astype(jnp.int32))


def code_part(codes, begin, end, key_end):
    patq, patk, pcq, pck = codes
    return (patq[:, begin:end], patk[:, :, :key_end], pcq[:, begin:end], pck[:, :, :key_end])


def split_attention_forward(query, keys, values, codes, span):
    if span is None:
        return attention_forward(query, keys, values, codes)
    head = attention_forward(
        query[:, :span], keys[:, :span], values[:, :span], code_part(codes, 0, span, span)
    )
    seq_len = keys.shape[1]
    tail = attention_forward(
        query[:, span:], keys, values, code_part(codes, span, query.shape[1], seq_len)
    )
    return jnp.concatenate([head, tail], 1)


def split_attention_backward(query, keys, values, grad_out, codes, span):
    if span is None:
        return attention_backward(query, keys, values, grad_out, codes)
    seq_len = keys.shape[1]
    head_q, head_k, head_v = attention_backward(
        query[:, :span],
        keys[:, :span],
        values[:, :span],
        grad_out[:, :span],
        code_part(codes, 0, span, span),
    )
    tail_q, tail_k, tail_v = attention_backward(
        query[:, span:],
        keys,
        values,
        grad_out[:, span:],
        code_part(codes, span, query.shape[1], seq_len),
    )
    padding = ((0, 0), (0, seq_len - span), (0, 0))
    return (
        jnp.concatenate([head_q, tail_q], 1),
        tail_k + jnp.pad(head_k, padding),
        tail_v + jnp.pad(head_v, padding),
    )


def spread_sequence(block, local_len):
    me_c = lax.axis_index("context")
    me_t = lax.axis_index("tensor")
    swap = [(0, 1), (1, 0)]
    kept = lax.dynamic_slice_in_dim(block, me_c * local_len, local_len, 1)
    other = lax.dynamic_slice_in_dim(block, (1 - me_c) * local_len, local_len, 1)
    from_context = lax.ppermute(other, "context", perm=swap)
    from_tensor = lax.ppermute(kept, "tensor", perm=swap)
    from_corner = lax.ppermute(other, ("context", "tensor"), perm=[(0, 3), (3, 0), (1, 2), (2, 1)])
    first_c = me_c == 0
    own_pair = jnp.where(
        first_c,
        jnp.concatenate([kept, from_context], 0),
        jnp.concatenate([from_context, kept], 0),
    )
    far_pair = jnp.where(
        first_c,
        jnp.concatenate([from_tensor, from_corner], 0),
        jnp.concatenate([from_corner, from_tensor], 0),
    )
    return jnp.where(
        me_t == 0,
        jnp.concatenate([own_pair, far_pair], 0),
        jnp.concatenate([far_pair, own_pair], 0),
    )


def assemble(stacked, shard_dim, tensor_dim):
    ns, nt = stacked.shape[0], stacked.shape[1]
    if shard_dim is None:
        stacked = stacked[:1]
    if tensor_dim is None:
        stacked = stacked[:, :1]
    local_shape = stacked.shape[2:]
    order = []
    for dim in range(len(local_shape)):
        if dim == shard_dim:
            order.append(0)
        if dim == tensor_dim:
            order.append(1)
        order.append(dim + 2)
    if shard_dim is None:
        order = [0] + order
    if tensor_dim is None:
        order = [1] + order
    moved = stacked.transpose(order)
    full_shape = list(local_shape)
    if shard_dim is not None:
        full_shape[shard_dim] *= ns
    if tensor_dim is not None:
        full_shape[tensor_dim] *= nt
    return moved.reshape(full_shape)


def gather_weight(local_block, shard_dim, tensor_dim):
    ns = lax.axis_size("shard")
    nt = lax.axis_size("tensor")
    stacked = lax.all_gather(local_block, ("shard", "tensor"), axis=0, tiled=False)
    return assemble(stacked.reshape((ns, nt) + local_block.shape), shard_dim, tensor_dim)


def gather_packed(blocks):
    ns = lax.axis_size("shard")
    nt = lax.axis_size("tensor")
    flat = jnp.concatenate([block.reshape(-1) for block, _, _ in blocks])
    padded = -flat.size % 2048
    flat = jnp.pad(flat, (0, padded)).reshape(-1, 128)
    stacked = lax.all_gather(flat, ("shard", "tensor"), axis=0, tiled=False).reshape(ns, nt, -1)
    pieces = []
    offset = 0
    for block, shard_dim, tensor_dim in blocks:
        part = stacked[:, :, offset : offset + block.size].reshape((ns, nt) + block.shape)
        pieces.append(assemble(part, shard_dim, tensor_dim))
        offset += block.size
    return pieces


def pair_gather(block, axis_name, dim):
    if lax.axis_size(axis_name) != 2:
        return lax.all_gather(block, axis_name, axis=dim, tiled=True)
    other = lax.ppermute(block, axis_name, perm=[(0, 1), (1, 0)])
    first = lax.axis_index(axis_name) == 0
    return jnp.where(
        first, jnp.concatenate([block, other], dim), jnp.concatenate([other, block], dim)
    )


def pair_reduce(full, axis_name, dim):
    if lax.axis_size(axis_name) != 2:
        return lax.psum_scatter(
            full.astype(jnp.bfloat16), axis_name, scatter_dimension=dim, tiled=True
        ).astype(jnp.float32)
    half = full.shape[dim] // 2
    me = lax.axis_index(axis_name)
    kept = lax.dynamic_slice_in_dim(full, me * half, half, dim)
    sent = lax.dynamic_slice_in_dim(full, (1 - me) * half, half, dim).astype(jnp.bfloat16)
    received = lax.ppermute(sent, axis_name, perm=[(0, 1), (1, 0)])
    return kept + received.astype(jnp.float32)


def pair_sum(share, axis_name):
    if lax.axis_size(axis_name) != 2:
        return lax.psum(share, axis_name).astype(jnp.float32)
    received = lax.ppermute(share, axis_name, perm=[(0, 1), (1, 0)])
    return share.astype(jnp.float32) + received.astype(jnp.float32)


def disassemble(full, shard_dim, tensor_dim):
    ns = lax.axis_size("shard")
    nt = lax.axis_size("tensor")
    split_shape = []
    positions = {}
    for dim, size in enumerate(full.shape):
        if dim == shard_dim:
            positions["s"] = len(split_shape)
            split_shape += [ns, size // ns]
        elif dim == tensor_dim:
            positions["t"] = len(split_shape)
            split_shape += [nt, size // nt]
        else:
            split_shape.append(size)
    pieces = full.reshape(split_shape)
    lead = [positions[key] for key in ("s", "t") if key in positions]
    rest = [d for d in range(len(split_shape)) if d not in lead]
    pieces = pieces.transpose(lead + rest)
    if "s" not in positions:
        pieces = jnp.broadcast_to(pieces[None], (ns,) + pieces.shape)
    if "t" not in positions:
        pieces = jnp.broadcast_to(pieces[:, None], (ns, nt) + pieces.shape[1:])
    return pieces.reshape(ns * nt, -1)


def pack_rows(terms):
    rows = jnp.concatenate(
        [disassemble(full.astype(jnp.bfloat16), shard_dim, tensor_dim) for full, shard_dim, tensor_dim in terms],
        1,
    )
    width = rows.shape[1]
    return jnp.pad(rows, ((0, 0), (0, -width % 1024))).reshape(rows.shape[0], -1, 128)


def scatter_rows(rows):
    return lax.psum_scatter(rows, ("shard", "tensor"), scatter_dimension=0, tiled=False)


def unpack_share(share, terms):
    total = pair_sum(share, "context").reshape(-1)
    pieces = []
    offset = 0
    ns = lax.axis_size("shard")
    nt = lax.axis_size("tensor")
    for full, shard_dim, tensor_dim in terms:
        local_shape = list(full.shape)
        if shard_dim is not None:
            local_shape[shard_dim] //= ns
        if tensor_dim is not None:
            local_shape[tensor_dim] //= nt
        count = 1
        for size in local_shape:
            count *= size
        pieces.append(total[offset : offset + count].reshape(local_shape))
        offset += count
    return pieces


def shard_stage(grad, dim):
    return lax.psum_scatter(grad.astype(jnp.bfloat16), "shard", scatter_dimension=dim, tiled=True)


def finish_stage(share, tensor_dim):
    summed = pair_reduce(share, "tensor", tensor_dim)
    return pair_sum(summed.astype(jnp.bfloat16), "context")


def forward_pass(block_in, codes, weights, span):
    w_qkv, w_out, w_up, w_down, norm_gains, out_biases, head_biases, head_gain, unit_bias, unit_gain = weights
    seq_count, local_len, model_width = block_in.shape
    row_count = seq_count * local_len
    flattened_input = block_in.reshape(row_count, model_width).astype(jnp.float32)
    first_normed, first_inv, first_out = norm_rows(flattened_input, norm_gains[0])
    attn_in = first_out.astype(jnp.bfloat16)
    projected = jnp.einsum("rd,jde->jre", attn_in, w_qkv, preferred_element_type=jnp.float32)
    query_matrix = (projected[0] + head_biases[0]).astype(jnp.bfloat16)
    keys_local = projected[1].astype(jnp.bfloat16).reshape(seq_count, local_len, model_width)
    values_local = (projected[2] + head_biases[1]).astype(jnp.bfloat16).reshape(
        seq_count, local_len, model_width
    )
    if span is None:
        key_all = pair_gather(keys_local, "context", 1)
        value_all = pair_gather(values_local, "context", 1)
    else:
        key_all, value_all = keys_local, values_local
    attended = split_attention_forward(
        query_matrix.reshape(seq_count, local_len, model_width), key_all, value_all, codes, span
    ).reshape(row_count, model_width)
    sub_normed, sub_inv, sub_out = norm_rows(attended, head_gain)
    sub_in = sub_out.astype(jnp.bfloat16)
    middle = flattened_input + (
        jnp.dot(sub_in, w_out, preferred_element_type=jnp.float32) + out_biases[0]
    )
    second_normed, second_inv, second_out = norm_rows(middle, norm_gains[1])
    ffn_in = second_out.astype(jnp.bfloat16)
    hidden = jnp.dot(ffn_in, w_up, preferred_element_type=jnp.float32) + unit_bias
    activated = jax.nn.gelu(hidden, approximate=True)
    unit_normed, unit_inv, unit_out = norm_rows(activated, unit_gain)
    ffn_mid = unit_out.astype(jnp.bfloat16)
    layer_out = (
        middle + (jnp.dot(ffn_mid, w_down, preferred_element_type=jnp.float32) + out_biases[1])
    ).astype(jnp.bfloat16)
    kept_state = (
        attn_in,
        first_normed,
        first_inv,
        query_matrix,
        key_all,
        value_all,
        codes,
        sub_normed,
        sub_inv,
        sub_in,
        second_normed,
        second_inv,
        ffn_in,
        hidden,
        unit_normed,
        unit_inv,
        ffn_mid,
    )
    return (kept_state, layer_out.reshape(seq_count, local_len, model_width))


def backward_pass(kept_state, block_grad, weights, span, carried):
    w_qkv, w_out, w_up, w_down, norm_gains, out_biases, head_biases, head_gain, unit_bias, unit_gain = weights
    (
        attn_in,
        first_normed,
        first_inv,
        query_matrix,
        key_all,
        value_all,
        codes,
        sub_normed,
        sub_inv,
        sub_in,
        second_normed,
        second_inv,
        ffn_in,
        hidden,
        unit_normed,
        unit_inv,
        ffn_mid,
    ) = kept_state
    seq_count, local_len, model_width = block_grad.shape
    row_count = seq_count * local_len
    seq_len = key_all.shape[1]
    grad_low = block_grad.reshape(row_count, model_width)
    grad_full = grad_low.astype(jnp.float32)
    down_grad = outer_sum(grad_low, ffn_mid)
    last_bias_grad = jnp.sum(grad_full, 0)
    unit_grad = back_dot(grad_low, w_down)
    activated_grad, unit_gain_grad = norm_back(unit_normed, unit_inv, unit_gain, unit_grad)
    gelu_value, gelu_pull = jax.vjp(partial(jax.nn.gelu, approximate=True), hidden)
    hidden_low = gelu_pull(activated_grad)[0].astype(jnp.bfloat16)
    up_grad = outer_sum(ffn_in, hidden_low)
    unit_bias_grad = jnp.sum(hidden_low, 0, dtype=jnp.float32)
    ffn_in_grad = back_dot(hidden_low, w_up)
    middle_part, second_gain_grad = norm_back(second_normed, second_inv, norm_gains[1], ffn_in_grad)
    middle_grad = grad_full + middle_part
    middle_low = middle_grad.astype(jnp.bfloat16)
    out_weight_grad = outer_sum(middle_low, sub_in)
    first_bias_grad = jnp.sum(middle_low, 0, dtype=jnp.float32)
    sub_grad = back_dot(middle_low, w_out)
    attended_grad, head_gain_grad = norm_back(sub_normed, sub_inv, head_gain, sub_grad)
    attended_low = attended_grad.astype(jnp.bfloat16)
    down_grad, up_grad, out_weight_grad, attended_low = lax.optimization_barrier(
        (
            down_grad.astype(jnp.bfloat16),
            up_grad.astype(jnp.bfloat16),
            out_weight_grad.astype(jnp.bfloat16),
            attended_low,
        )
    )
    tensor_count = lax.axis_size("tensor")
    early_widths = (down_grad.shape[1], up_grad.shape[1], out_weight_grad.shape[1])
    early_share = shard_stage(
        jnp.concatenate(
            [
                part.reshape(part.shape[0], tensor_count, part.shape[1] // tensor_count)
                for part in (down_grad, up_grad, out_weight_grad)
            ],
            2,
        ),
        0,
    )
    query_grad, key_part, value_part = split_attention_backward(
        query_matrix.reshape(seq_count, local_len, model_width),
        key_all,
        value_all,
        attended_low.reshape(seq_count, local_len, model_width),
        codes,
        span,
    )
    if span is not None:
        key_part = key_part.reshape(row_count, model_width)
        value_part = value_part.reshape(row_count, model_width)
    query_low = query_grad.reshape(row_count, model_width)
    if span is None:
        key_part = pair_reduce(key_part, "context", 1)
        value_part = pair_reduce(value_part, "context", 1)
    key_low = key_part.astype(jnp.bfloat16).reshape(row_count, model_width)
    value_low = value_part.astype(jnp.bfloat16).reshape(row_count, model_width)
    stacked = jnp.stack([query_low, key_low, value_low])
    early_share, stacked, carried = lax.optimization_barrier((early_share, stacked, carried))
    qkv_grad = jnp.einsum("rd,jre->dje", attn_in, stacked, preferred_element_type=jnp.float32)
    head_bias_grad = jnp.stack(
        [jnp.sum(query_low, 0, dtype=jnp.float32), jnp.sum(value_low, 0, dtype=jnp.float32)]
    )
    qkv_grad, stacked = lax.optimization_barrier((qkv_grad, stacked))
    attn_in_grad = jnp.einsum("jre,jde->rd", stacked, w_qkv, preferred_element_type=jnp.float32)
    first_gain_grad = jnp.sum(attn_in_grad * first_normed, 0)
    heads = model_width // HD
    unit_rows = unit_bias_grad.shape[0] // HD
    small_terms = (
        (jnp.stack([first_gain_grad, second_gain_grad]), 1, None),
        (jnp.stack([first_bias_grad, last_bias_grad]), 1, None),
        (head_bias_grad.reshape(2, heads, HD), 2, 1),
        (head_gain_grad.reshape(heads, HD), 1, 0),
        (unit_bias_grad.reshape(unit_rows, HD), 1, 0),
        (unit_gain_grad.reshape(unit_rows, HD), 1, 0),
    )
    ns = lax.axis_size("shard")
    nt = lax.axis_size("tensor")
    small_rows = jnp.concatenate(
        [disassemble(full, shard_dim, tensor_dim) for full, shard_dim, tensor_dim in small_terms], 1
    )
    small_width = small_rows.shape[1]
    block_rows = model_width // ns
    extra_rows = 8
    planes = qkv_grad.shape[1]
    slots = extra_rows * planes * (model_width // nt)
    small_block = (
        jnp.pad(small_rows, ((0, 0), (0, slots - small_width)))
        .reshape(ns, nt, extra_rows, planes, model_width // nt)
        .transpose(0, 2, 3, 1, 4)
        .reshape(ns, extra_rows, planes, model_width)
    )
    widened = jnp.concatenate(
        [qkv_grad.reshape(ns, block_rows, planes, model_width), small_block.astype(qkv_grad.dtype)], 1
    ).reshape(ns * (block_rows + extra_rows), planes, model_width)
    widened, attn_in_grad = lax.optimization_barrier((widened, attn_in_grad))
    qkv_share = shard_stage(widened, 0)
    input_part = norm_back(first_normed, first_inv, norm_gains[0], attn_in_grad)[0]
    input_low = (middle_grad + input_part).astype(jnp.bfloat16)
    qkv_total = finish_stage(qkv_share, 2)
    small_total = qkv_total[block_rows:].reshape(-1)[:small_width]
    small_pieces = []
    offset = 0
    for full, shard_dim, tensor_dim in small_terms:
        local_shape = list(full.shape)
        if shard_dim is not None:
            local_shape[shard_dim] //= ns
        if tensor_dim is not None:
            local_shape[tensor_dim] //= nt
        count = 1
        for size in local_shape:
            count *= size
        small_pieces.append(small_total[offset : offset + count].reshape(local_shape))
        offset += count
    early_total = finish_stage(early_share, 1).reshape(early_share.shape[0], -1)
    down_width = early_widths[0] // nt
    up_width = early_widths[1] // nt
    grad_shares = (
        early_total[:, :down_width].transpose(1, 0),
        early_total[:, down_width : down_width + up_width],
        early_total[:, down_width + up_width :].transpose(1, 0),
        qkv_total[:block_rows].transpose(1, 0, 2),
    ) + tuple(small_pieces)
    return (grad_shares, input_low.reshape(seq_count, local_len, model_width), carried)


def local(
    inputs,
    out_grad,
    picture_starts,
    segment_offsets,
    dilation_offsets,
    norm_gains,
    w_qkv,
    head_biases,
    head_gain,
    w_out,
    out_biases,
    w_up,
    unit_bias,
    unit_gain,
    w_down,
):
    local_seqs, local_len, model_width = inputs.shape
    tensor_count = lax.axis_size("tensor")
    context_count = lax.axis_size("context")
    seq_len = local_len * context_count
    key_position = jnp.arange(seq_len, dtype=jnp.int32)
    whole = context_count == 2 and tensor_count == 2 and local_seqs == 4
    if whole:
        span = seq_len // PIECES
        me_c = lax.axis_index("context")
        own_seq = lax.axis_index("tensor") * context_count + me_c
        partner_seq = lax.axis_index("tensor") * context_count + 1 - me_c
        swap = [(0, 1), (1, 0)]

        def own_sequence(rows):
            kept = lax.dynamic_slice_in_dim(rows, own_seq, 1, 0)
            sent = lax.dynamic_slice_in_dim(rows, partner_seq, 1, 0)
            received = lax.ppermute(sent, "context", perm=swap)
            return jnp.where(
                me_c == 0,
                jnp.concatenate([kept, received], 1),
                jnp.concatenate([received, kept], 1),
            )

        block_in = own_sequence(inputs)
        block_grad = own_sequence(out_grad)
        starts = lax.dynamic_slice_in_dim(picture_starts, own_seq, 1, 0)
        query_position = key_position
    else:
        span = None
        mine = local_seqs // tensor_count
        first_seq = lax.axis_index("tensor") * mine
        block_in = lax.dynamic_slice_in_dim(inputs, first_seq, mine, 0)
        block_grad = lax.dynamic_slice_in_dim(out_grad, first_seq, mine, 0)
        starts = lax.dynamic_slice_in_dim(picture_starts, first_seq, mine, 0)
        query_position = lax.axis_index("context") * local_len + jnp.arange(
            local_len, dtype=jnp.int32
        )
    spans = jnp.array([seq_len * part // 8 for part in span_parts], jnp.int32)
    rates = jnp.array(dilation_rates, jnp.int32)
    segment_kept = segment_offsets % spans
    dilation_kept = dilation_offsets % rates
    offset_digits = jnp.concatenate(
        [segment_kept // 32, segment_kept % 32, dilation_kept], 1
    ).astype(jnp.bfloat16)
    f32 = jnp.float32
    (
        w_qkv_full,
        gains_full,
        out_bias_full,
        head_bias_full,
        head_gain_full,
        unit_bias_full,
        unit_gain_full,
        digits_full,
    ) = gather_packed(
        (
            (w_qkv, 1, 2),
            (norm_gains, 1, None),
            (out_biases, 1, None),
            (head_biases, 2, 1),
            (head_gain, 1, 0),
            (unit_bias, 1, 0),
            (unit_gain, 1, 0),
            (offset_digits, None, 0),
        )
    )
    patterns = len(span_parts)
    digits_full = digits_full.astype(jnp.int32)
    all_segments = digits_full[:, :patterns] * 32 + digits_full[:, patterns : 2 * patterns]
    all_dilations = digits_full[:, 2 * patterns :]
    codes = mask_codes(starts, query_position, key_position, all_segments, all_dilations, seq_len)
    w_out, w_up, w_down, w_qkv_full = lax.optimization_barrier((w_out, w_up, w_down, w_qkv_full))
    weights = (
        w_qkv_full,
        gather_weight(w_out, 1, 0),
        gather_weight(w_up, 0, 1),
        gather_weight(w_down, 1, 0),
        gains_full.astype(f32),
        out_bias_full.astype(f32),
        head_bias_full.reshape(2, model_width).astype(f32),
        head_gain_full.reshape(model_width).astype(f32),
        unit_bias_full.reshape(-1).astype(f32),
        unit_gain_full.reshape(-1).astype(f32),
    )
    kept_state, layer_block = forward_pass(block_in, codes, weights, span)
    if whole:
        layer_out = spread_sequence(layer_block, local_len)
    else:
        layer_out = pair_gather(layer_block, "tensor", 0)
    grad_shares, input_block, layer_out = backward_pass(
        kept_state, block_grad, weights, span, layer_out
    )
    if whole:
        input_grad = spread_sequence(input_block, local_len)
    else:
        input_grad = pair_gather(input_block, "tensor", 0)
    (
        down_share,
        up_share,
        out_share,
        qkv_share,
        gains_share,
        out_bias_share,
        head_bias_share,
        head_gain_share,
        unit_bias_share,
        unit_gain_share,
    ) = grad_shares
    return (
        layer_out,
        input_grad,
        gains_share,
        qkv_share,
        head_bias_share,
        head_gain_share,
        out_share,
        out_bias_share,
        up_share,
        unit_bias_share,
        unit_gain_share,
        down_share,
    )


def solution(mesh):
    placed = (
        P("shard", "context", None),
        P("shard", "context", None),
        P("shard", None),
        P("tensor", None),
        P("tensor", None),
        P(None, "shard"),
        P(None, "shard", "tensor"),
        P(None, "tensor", "shard"),
        P("tensor", "shard"),
        P("tensor", "shard"),
        P(None, "shard"),
        P("shard", "tensor"),
        P("tensor", "shard"),
        P("tensor", "shard"),
        P("tensor", "shard"),
    )
    return jax.shard_map(
        local,
        mesh=mesh,
        in_specs=placed,
        out_specs=(
            P("shard", "context", None),
            P("shard", "context", None),
            P(None, "shard"),
            P(None, "shard", "tensor"),
            P(None, "tensor", "shard"),
            P("tensor", "shard"),
            P("tensor", "shard"),
            P(None, "shard"),
            P("shard", "tensor"),
            P("tensor", "shard"),
            P("tensor", "shard"),
            P("tensor", "shard"),
        ),
        check_vma=False,
    )
```

```python
from functools import partial

import jax
import jax.numpy as jnp
from jax import lax
from jax.experimental import pallas as pl
from jax.experimental.pallas import tpu as pltpu
from jax.sharding import PartitionSpec as P

HD = 64
FF = 3072
PIECE = 256
PIECES = 2


epsilon = 1e-05
span_parts = (1, 2, 4, 6, 8)
dilation_rates = (1, 2, 4, 6, 12)


def pattern_total(query_position, key_position, segmented_offsets, dilated_offsets, token_length):
    tallied_total = jnp.zeros(
        (segmented_offsets.shape[0], query_position.shape[0], key_position.shape[0]), jnp.float32
    )
    for item_number in range(len(span_parts)):
        segmented_span = token_length * span_parts[item_number] // 8
        dilated_stride = dilation_rates[item_number]
        seg_shift = (segmented_offsets[:, item_number] % segmented_span)[:, None, None]
        dilated_phase = (dilated_offsets[:, item_number] % dilated_stride)[:, None, None]
        query_lookup = query_position[None, :, None] + seg_shift
        key_lookup = key_position[None, None, :] + seg_shift
        merged_heads = (
            (query_lookup // segmented_span == key_lookup // segmented_span)
            & (query_lookup % dilated_stride == dilated_phase)
            & (key_lookup % dilated_stride == dilated_phase)
        )
        tallied_total = tallied_total + merged_heads.astype(jnp.float32)
    return tallied_total


def picture_index(starts, token_positions):
    marked = jnp.zeros((starts.shape[0], token_positions.shape[0]), jnp.int32)
    for piece_number in range(starts.shape[1]):
        begin_at = starts[:, piece_number][:, None]
        inside = (token_positions[None, :] >= begin_at) & (
            token_positions[None, :] < begin_at + PIECE
        )
        marked = marked + (piece_number + 1) * inside.astype(jnp.int32)
    return marked


def allowed_keys(query_pic, key_pic, query_position, key_position):
    causal_ok = key_position[None, None, :] <= query_position[None, :, None]
    same_piece = (query_pic[:, :, None] == key_pic[:, None, :]) & (query_pic[:, :, None] > 0)
    return (causal_ok | same_piece).astype(jnp.float32)


def outer_sum(left_rows, right_rows):
    return lax.dot_general(
        left_rows, right_rows, (((0,), (0,)), ((), ())), preferred_element_type=jnp.float32
    )


def back_dot(left_rows, weight_rows):
    return lax.dot_general(
        left_rows, weight_rows, (((1,), (1,)), ((), ())), preferred_element_type=jnp.float32
    )


def norm_rows(values, scale_row):
    mean_row = jnp.mean(values, -1, keepdims=True)
    centered = values - mean_row
    inv_std = lax.rsqrt(jnp.mean(centered * centered, -1, keepdims=True) + epsilon)
    normed = centered * inv_std
    return (normed, inv_std, normed * scale_row)


def norm_back(normed, inv_std, scale_row, grad_rows):
    scaled = grad_rows * scale_row
    mean_plain = jnp.mean(scaled, -1, keepdims=True)
    mean_cross = jnp.mean(scaled * normed, -1, keepdims=True)
    return (inv_std * (scaled - mean_plain - normed * mean_cross), jnp.sum(grad_rows * normed, 0))


def probabilities(query_heads, key_heads, mask_table):
    raw_scores = jnp.einsum(
        "sqhd,skhd->shqk", query_heads, key_heads, preferred_element_type=jnp.float32
    ) * HD ** (-0.5)
    masked = jnp.where(mask_table > 0, raw_scores, -1000000000.0)
    row_top = jnp.max(masked, -1, keepdims=True)
    exponent = mask_table * jnp.exp(masked - row_top)
    row_total = jnp.sum(exponent, -1, keepdims=True)
    return (exponent / row_total, row_top, row_total)


SCALE = HD ** (-0.5)
HIDDEN = -1000000000.0
PAIR = 2
CODE_WIDTH = 8


def pair_masks(patq_ref, patk_ref, pcq_ref, pck_ref):
    first_q = patq_ref[0]
    first_k = patk_ref[0]
    row = first_q[:, 5:6]
    col = first_k[5:6, :]
    piece_q = pcq_ref[0][:, 0:1]
    piece_k = pck_ref[0][0:1, :]
    allowed = (col <= row) | (piece_q == piece_k)
    masks = []
    for head in range(PAIR):
        codes_q = patq_ref[head]
        codes_k = patk_ref[head]
        tally = (codes_q[:, 0:1] == codes_k[0:1, :]).astype(jnp.float32)
        for pattern in range(1, len(span_parts)):
            tally = tally + (
                codes_q[:, pattern : pattern + 1] == codes_k[pattern : pattern + 1, :]
            ).astype(jnp.float32)
        masks.append(jnp.where(allowed, tally, 0.0))
    return masks


def soft_rows(query_part, key_block, mask):
    scores = (
        lax.dot_general(
            query_part, key_block, (((1,), (1,)), ((), ())), preferred_element_type=jnp.float32
        )
        * SCALE
    )
    masked = jnp.where(mask > 0, scores, HIDDEN)
    top = jnp.max(masked, axis=1, keepdims=True)
    exponent = mask * jnp.exp(masked - top)
    return exponent / jnp.sum(exponent, axis=1, keepdims=True)


def attention_fwd_kernel(q_ref, k_ref, v_ref, patq_ref, patk_ref, pcq_ref, pck_ref, o_ref):
    query = q_ref[0]
    key_block = k_ref[0]
    value_block = v_ref[0]
    first = lax.broadcasted_iota(jnp.int32, query.shape, 1) < HD
    masks = pair_masks(patq_ref, patk_ref, pcq_ref, pck_ref)
    result = None
    for head in range(PAIR):
        keep = first if head == 0 else jnp.logical_not(first)
        query_part = jnp.where(keep, query, jnp.zeros_like(query))
        probs = soft_rows(query_part, key_block, masks[head])
        mixed = jnp.dot(
            probs.astype(jnp.bfloat16), value_block, preferred_element_type=jnp.float32
        )
        result = mixed if result is None else jnp.where(first, result, mixed)
    o_ref[0] = result


def attention_bwd_kernel(
    q_ref, k_ref, v_ref, do_ref, patq_ref, patk_ref, pcq_ref, pck_ref, dq_ref, dk_ref, dv_ref
):
    @pl.when(pl.program_id(2) == 0)
    def _():
        dk_ref[...] = jnp.zeros_like(dk_ref)
        dv_ref[...] = jnp.zeros_like(dv_ref)

    query = q_ref[0]
    key_block = k_ref[0]
    value_block = v_ref[0]
    grad_out = do_ref[0]
    first = lax.broadcasted_iota(jnp.int32, query.shape, 1) < HD
    masks = pair_masks(patq_ref, patk_ref, pcq_ref, pck_ref)
    query_grad = None
    key_grad = dk_ref[0]
    value_grad = dv_ref[0]
    for head in range(PAIR):
        keep = first if head == 0 else jnp.logical_not(first)
        query_part = jnp.where(keep, query, jnp.zeros_like(query))
        grad_part = jnp.where(keep, grad_out, jnp.zeros_like(grad_out))
        probs = soft_rows(query_part, key_block, masks[head])
        prob_grad = lax.dot_general(
            grad_part, value_block, (((1,), (1,)), ((), ())), preferred_element_type=jnp.float32
        )
        inner = jnp.sum(probs * prob_grad, axis=1, keepdims=True)
        score_low = (probs * (prob_grad - inner)).astype(jnp.bfloat16)
        part = jnp.dot(score_low, key_block, preferred_element_type=jnp.float32)
        query_grad = part if query_grad is None else jnp.where(first, query_grad, part)
        key_grad = key_grad + SCALE * lax.dot_general(
            score_low, query_part, (((0,), (0,)), ((), ())), preferred_element_type=jnp.float32
        )
        value_grad = value_grad + lax.dot_general(
            probs.astype(jnp.bfloat16),
            grad_part,
            (((0,), (0,)), ((), ())),
            preferred_element_type=jnp.float32,
        )
    dq_ref[0] = (query_grad * SCALE).astype(jnp.bfloat16)
    dk_ref[0] = key_grad
    dv_ref[0] = value_grad


def attention_specs(seq_count, local_len, seq_len, block_q):
    lanes = PAIR * HD
    query_spec = pl.BlockSpec((1, block_q, lanes), lambda s, g, b: (s, b, g))
    key_spec = pl.BlockSpec((1, seq_len, lanes), lambda s, g, b: (s, 0, g))
    patq_spec = pl.BlockSpec((PAIR, block_q, CODE_WIDTH), lambda s, g, b: (g, b, 0))
    patk_spec = pl.BlockSpec((PAIR, CODE_WIDTH, seq_len), lambda s, g, b: (g, 0, 0))
    pcq_spec = pl.BlockSpec((1, block_q, CODE_WIDTH), lambda s, g, b: (s, b, 0))
    pck_spec = pl.BlockSpec((1, CODE_WIDTH, seq_len), lambda s, g, b: (s, 0, 0))
    return query_spec, key_spec, patq_spec, patk_spec, pcq_spec, pck_spec


def attention_forward(query, keys, values, codes):
    seq_count, local_len, width = query.shape
    seq_len = keys.shape[1]
    block_q = min(256, local_len)
    grid = (seq_count, width // (PAIR * HD), local_len // block_q)
    query_spec, key_spec, patq_spec, patk_spec, pcq_spec, pck_spec = attention_specs(
        seq_count, local_len, seq_len, block_q
    )
    flops = 8 * seq_count * local_len * seq_len * width
    return pl.pallas_call(
        attention_fwd_kernel,
        grid=grid,
        in_specs=[query_spec, key_spec, key_spec, patq_spec, patk_spec, pcq_spec, pck_spec],
        out_specs=query_spec,
        out_shape=jax.ShapeDtypeStruct((seq_count, local_len, width), jnp.float32),
        compiler_params=pltpu.CompilerParams(
            dimension_semantics=("parallel", "parallel", "arbitrary"),
            vmem_limit_bytes=48 * 1024 * 1024,
        ),
        cost_estimate=pl.CostEstimate(
            flops=flops,
            transcendentals=seq_count * local_len * seq_len * width // HD,
            bytes_accessed=2 * query.size + 2 * keys.size * 2 * (local_len // block_q) + 4 * query.size,
        ),
    )(query, keys, values, *codes)


def attention_backward(query, keys, values, grad_out, codes):
    seq_count, local_len, width = query.shape
    seq_len = keys.shape[1]
    block_q = min(256, local_len)
    grid = (seq_count, width // (PAIR * HD), local_len // block_q)
    query_spec, key_spec, patq_spec, patk_spec, pcq_spec, pck_spec = attention_specs(
        seq_count, local_len, seq_len, block_q
    )
    flops = 20 * seq_count * local_len * seq_len * width
    return pl.pallas_call(
        attention_bwd_kernel,
        grid=grid,
        in_specs=[
            query_spec,
            key_spec,
            key_spec,
            query_spec,
            patq_spec,
            patk_spec,
            pcq_spec,
            pck_spec,
        ],
        out_specs=[query_spec, key_spec, key_spec],
        out_shape=[
            jax.ShapeDtypeStruct((seq_count, local_len, width), jnp.bfloat16),
            jax.ShapeDtypeStruct((seq_count, seq_len, width), jnp.float32),
            jax.ShapeDtypeStruct((seq_count, seq_len, width), jnp.float32),
        ],
        compiler_params=pltpu.CompilerParams(
            dimension_semantics=("parallel", "parallel", "arbitrary"),
            vmem_limit_bytes=48 * 1024 * 1024,
        ),
        cost_estimate=pl.CostEstimate(
            flops=flops,
            transcendentals=seq_count * local_len * seq_len * width // HD,
            bytes_accessed=4 * query.size + 2 * keys.size * 2 * (local_len // block_q) + 16 * keys.size,
        ),
    )(query, keys, values, grad_out, *codes)


def mask_codes(starts, query_position, key_position, segment_offsets, dilation_offsets, seq_len):
    heads = segment_offsets.shape[0]
    query_codes = []
    key_codes = []
    for pattern in range(len(span_parts)):
        span = seq_len * span_parts[pattern] // 8
        rate = dilation_rates[pattern]
        shift = (segment_offsets[:, pattern] % span)[:, None]
        phase = (dilation_offsets[:, pattern] % rate)[:, None]
        query_at = query_position[None, :] + shift
        key_at = key_position[None, :] + shift
        query_codes.append(jnp.where(query_at % rate == phase, query_at // span, -1))
        key_codes.append(jnp.where(key_at % rate == phase, key_at // span, -2))
    patterns = len(span_parts)
    query_codes.append(jnp.broadcast_to(query_position[None, :], (heads, query_position.shape[0])))
    key_codes.append(jnp.broadcast_to(key_position[None, :], (heads, key_position.shape[0])))
    filler = CODE_WIDTH - patterns - 1
    query_codes += [jnp.zeros((heads, query_position.shape[0]), jnp.int32)] * filler
    key_codes += [jnp.zeros((heads, key_position.shape[0]), jnp.int32)] * filler
    patq = jnp.stack(query_codes, 2).astype(jnp.int32)
    patk = jnp.stack(key_codes, 1).astype(jnp.int32)
    query_pic = picture_index(starts, query_position)
    key_pic = picture_index(starts, key_position)
    pcq = jnp.where(query_pic > 0, query_pic, -1)[:, :, None]
    pcq = jnp.pad(pcq, ((0, 0), (0, 0), (0, CODE_WIDTH - 1)))
    pck = jnp.where(key_pic > 0, key_pic, -2)[:, None, :]
    pck = jnp.pad(pck, ((0, 0), (0, CODE_WIDTH - 1), (0, 0)))
    return (patq, patk, pcq.astype(jnp.int32), pck.astype(jnp.int32))


def code_part(codes, begin, end, key_end):
    patq, patk, pcq, pck = codes
    return (patq[:, begin:end], patk[:, :, :key_end], pcq[:, begin:end], pck[:, :, :key_end])


def split_attention_forward(query, keys, values, codes, span):
    if span is None:
        return attention_forward(query, keys, values, codes)
    head = attention_forward(
        query[:, :span], keys[:, :span], values[:, :span], code_part(codes, 0, span, span)
    )
    seq_len = keys.shape[1]
    tail = attention_forward(
        query[:, span:], keys, values, code_part(codes, span, query.shape[1], seq_len)
    )
    return jnp.concatenate([head, tail], 1)


def split_attention_backward(query, keys, values, grad_out, codes, span):
    if span is None:
        return attention_backward(query, keys, values, grad_out, codes)
    seq_len = keys.shape[1]
    head_q, head_k, head_v = attention_backward(
        query[:, :span],
        keys[:, :span],
        values[:, :span],
        grad_out[:, :span],
        code_part(codes, 0, span, span),
    )
    tail_q, tail_k, tail_v = attention_backward(
        query[:, span:],
        keys,
        values,
        grad_out[:, span:],
        code_part(codes, span, query.shape[1], seq_len),
    )
    padding = ((0, 0), (0, seq_len - span), (0, 0))
    return (
        jnp.concatenate([head_q, tail_q], 1),
        tail_k + jnp.pad(head_k, padding),
        tail_v + jnp.pad(head_v, padding),
    )


def spread_sequence(block, local_len):
    me_c = lax.axis_index("context")
    me_t = lax.axis_index("tensor")
    swap = [(0, 1), (1, 0)]
    kept = lax.dynamic_slice_in_dim(block, me_c * local_len, local_len, 1)
    other = lax.dynamic_slice_in_dim(block, (1 - me_c) * local_len, local_len, 1)
    from_context = lax.ppermute(other, "context", perm=swap)
    from_tensor = lax.ppermute(kept, "tensor", perm=swap)
    from_corner = lax.ppermute(other, ("context", "tensor"), perm=[(0, 3), (3, 0), (1, 2), (2, 1)])
    first_c = me_c == 0
    own_pair = jnp.where(
        first_c,
        jnp.concatenate([kept, from_context], 0),
        jnp.concatenate([from_context, kept], 0),
    )
    far_pair = jnp.where(
        first_c,
        jnp.concatenate([from_tensor, from_corner], 0),
        jnp.concatenate([from_corner, from_tensor], 0),
    )
    return jnp.where(
        me_t == 0,
        jnp.concatenate([own_pair, far_pair], 0),
        jnp.concatenate([far_pair, own_pair], 0),
    )


def assemble(stacked, shard_dim, tensor_dim):
    ns, nt = stacked.shape[0], stacked.shape[1]
    if shard_dim is None:
        stacked = stacked[:1]
    if tensor_dim is None:
        stacked = stacked[:, :1]
    local_shape = stacked.shape[2:]
    order = []
    for dim in range(len(local_shape)):
        if dim == shard_dim:
            order.append(0)
        if dim == tensor_dim:
            order.append(1)
        order.append(dim + 2)
    if shard_dim is None:
        order = [0] + order
    if tensor_dim is None:
        order = [1] + order
    moved = stacked.transpose(order)
    full_shape = list(local_shape)
    if shard_dim is not None:
        full_shape[shard_dim] *= ns
    if tensor_dim is not None:
        full_shape[tensor_dim] *= nt
    return moved.reshape(full_shape)


def gather_weight(local_block, shard_dim, tensor_dim):
    ns = lax.axis_size("shard")
    nt = lax.axis_size("tensor")
    stacked = lax.all_gather(local_block, ("shard", "tensor"), axis=0, tiled=False)
    return assemble(stacked.reshape((ns, nt) + local_block.shape), shard_dim, tensor_dim)


def gather_packed(blocks):
    ns = lax.axis_size("shard")
    nt = lax.axis_size("tensor")
    flat = jnp.concatenate([block.reshape(-1) for block, _, _ in blocks])
    padded = -flat.size % 2048
    flat = jnp.pad(flat, (0, padded)).reshape(-1, 128)
    stacked = lax.all_gather(flat, ("shard", "tensor"), axis=0, tiled=False).reshape(ns, nt, -1)
    pieces = []
    offset = 0
    for block, shard_dim, tensor_dim in blocks:
        part = stacked[:, :, offset : offset + block.size].reshape((ns, nt) + block.shape)
        pieces.append(assemble(part, shard_dim, tensor_dim))
        offset += block.size
    return pieces


def pair_gather(block, axis_name, dim):
    if lax.axis_size(axis_name) != 2:
        return lax.all_gather(block, axis_name, axis=dim, tiled=True)
    other = lax.ppermute(block, axis_name, perm=[(0, 1), (1, 0)])
    first = lax.axis_index(axis_name) == 0
    return jnp.where(
        first, jnp.concatenate([block, other], dim), jnp.concatenate([other, block], dim)
    )


def pair_reduce(full, axis_name, dim):
    if lax.axis_size(axis_name) != 2:
        return lax.psum_scatter(
            full.astype(jnp.bfloat16), axis_name, scatter_dimension=dim, tiled=True
        ).astype(jnp.float32)
    half = full.shape[dim] // 2
    me = lax.axis_index(axis_name)
    kept = lax.dynamic_slice_in_dim(full, me * half, half, dim)
    sent = lax.dynamic_slice_in_dim(full, (1 - me) * half, half, dim).astype(jnp.bfloat16)
    received = lax.ppermute(sent, axis_name, perm=[(0, 1), (1, 0)])
    return kept + received.astype(jnp.float32)


def pair_sum(share, axis_name):
    if lax.axis_size(axis_name) != 2:
        return lax.psum(share, axis_name).astype(jnp.float32)
    received = lax.ppermute(share, axis_name, perm=[(0, 1), (1, 0)])
    return share.astype(jnp.float32) + received.astype(jnp.float32)


def disassemble(full, shard_dim, tensor_dim):
    ns = lax.axis_size("shard")
    nt = lax.axis_size("tensor")
    split_shape = []
    positions = {}
    for dim, size in enumerate(full.shape):
        if dim == shard_dim:
            positions["s"] = len(split_shape)
            split_shape += [ns, size // ns]
        elif dim == tensor_dim:
            positions["t"] = len(split_shape)
            split_shape += [nt, size // nt]
        else:
            split_shape.append(size)
    pieces = full.reshape(split_shape)
    lead = [positions[key] for key in ("s", "t") if key in positions]
    rest = [d for d in range(len(split_shape)) if d not in lead]
    pieces = pieces.transpose(lead + rest)
    if "s" not in positions:
        pieces = jnp.broadcast_to(pieces[None], (ns,) + pieces.shape)
    if "t" not in positions:
        pieces = jnp.broadcast_to(pieces[:, None], (ns, nt) + pieces.shape[1:])
    return pieces.reshape(ns * nt, -1)


def pack_rows(terms):
    rows = jnp.concatenate(
        [disassemble(full.astype(jnp.bfloat16), shard_dim, tensor_dim) for full, shard_dim, tensor_dim in terms],
        1,
    )
    width = rows.shape[1]
    return jnp.pad(rows, ((0, 0), (0, -width % 1024))).reshape(rows.shape[0], -1, 128)


def scatter_rows(rows):
    return lax.psum_scatter(rows, ("shard", "tensor"), scatter_dimension=0, tiled=False)


def unpack_share(share, terms):
    total = pair_sum(share, "context").reshape(-1)
    pieces = []
    offset = 0
    ns = lax.axis_size("shard")
    nt = lax.axis_size("tensor")
    for full, shard_dim, tensor_dim in terms:
        local_shape = list(full.shape)
        if shard_dim is not None:
            local_shape[shard_dim] //= ns
        if tensor_dim is not None:
            local_shape[tensor_dim] //= nt
        count = 1
        for size in local_shape:
            count *= size
        pieces.append(total[offset : offset + count].reshape(local_shape))
        offset += count
    return pieces


def shard_stage(grad, dim):
    return lax.psum_scatter(grad.astype(jnp.bfloat16), "shard", scatter_dimension=dim, tiled=True)


def finish_stage(share, tensor_dim):
    summed = pair_reduce(share, "tensor", tensor_dim)
    return pair_sum(summed.astype(jnp.bfloat16), "context")


def forward_pass(block_in, codes, weights, span):
    w_qkv, w_out, w_up, w_down, norm_gains, out_biases, head_biases, head_gain, unit_bias, unit_gain = weights
    seq_count, local_len, model_width = block_in.shape
    row_count = seq_count * local_len
    flattened_input = block_in.reshape(row_count, model_width).astype(jnp.float32)
    first_normed, first_inv, first_out = norm_rows(flattened_input, norm_gains[0])
    attn_in = first_out.astype(jnp.bfloat16)
    projected = jnp.einsum("rd,jde->jre", attn_in, w_qkv, preferred_element_type=jnp.float32)
    query_matrix = (projected[0] + head_biases[0]).astype(jnp.bfloat16)
    keys_local = projected[1].astype(jnp.bfloat16).reshape(seq_count, local_len, model_width)
    values_local = (projected[2] + head_biases[1]).astype(jnp.bfloat16).reshape(
        seq_count, local_len, model_width
    )
    if span is None:
        key_all = pair_gather(keys_local, "context", 1)
        value_all = pair_gather(values_local, "context", 1)
    else:
        key_all, value_all = keys_local, values_local
    attended = split_attention_forward(
        query_matrix.reshape(seq_count, local_len, model_width), key_all, value_all, codes, span
    ).reshape(row_count, model_width)
    sub_normed, sub_inv, sub_out = norm_rows(attended, head_gain)
    sub_in = sub_out.astype(jnp.bfloat16)
    middle = flattened_input + (
        jnp.dot(sub_in, w_out, preferred_element_type=jnp.float32) + out_biases[0]
    )
    second_normed, second_inv, second_out = norm_rows(middle, norm_gains[1])
    ffn_in = second_out.astype(jnp.bfloat16)
    hidden = jnp.dot(ffn_in, w_up, preferred_element_type=jnp.float32) + unit_bias
    activated = jax.nn.gelu(hidden, approximate=True)
    unit_normed, unit_inv, unit_out = norm_rows(activated, unit_gain)
    ffn_mid = unit_out.astype(jnp.bfloat16)
    layer_out = (
        middle + (jnp.dot(ffn_mid, w_down, preferred_element_type=jnp.float32) + out_biases[1])
    ).astype(jnp.bfloat16)
    kept_state = (
        attn_in,
        first_normed,
        first_inv,
        query_matrix,
        key_all,
        value_all,
        codes,
        sub_normed,
        sub_inv,
        sub_in,
        second_normed,
        second_inv,
        ffn_in,
        hidden,
        unit_normed,
        unit_inv,
        ffn_mid,
    )
    return (kept_state, layer_out.reshape(seq_count, local_len, model_width))


def backward_pass(kept_state, block_grad, weights, span, carried):
    w_qkv, w_out, w_up, w_down, norm_gains, out_biases, head_biases, head_gain, unit_bias, unit_gain = weights
    (
        attn_in,
        first_normed,
        first_inv,
        query_matrix,
        key_all,
        value_all,
        codes,
        sub_normed,
        sub_inv,
        sub_in,
        second_normed,
        second_inv,
        ffn_in,
        hidden,
        unit_normed,
        unit_inv,
        ffn_mid,
    ) = kept_state
    seq_count, local_len, model_width = block_grad.shape
    row_count = seq_count * local_len
    seq_len = key_all.shape[1]
    grad_low = block_grad.reshape(row_count, model_width)
    grad_full = grad_low.astype(jnp.float32)
    down_grad = outer_sum(grad_low, ffn_mid)
    last_bias_grad = jnp.sum(grad_full, 0)
    unit_grad = back_dot(grad_low, w_down)
    activated_grad, unit_gain_grad = norm_back(unit_normed, unit_inv, unit_gain, unit_grad)
    gelu_value, gelu_pull = jax.vjp(partial(jax.nn.gelu, approximate=True), hidden)
    hidden_low = gelu_pull(activated_grad)[0].astype(jnp.bfloat16)
    up_grad = outer_sum(ffn_in, hidden_low)
    unit_bias_grad = jnp.sum(hidden_low, 0, dtype=jnp.float32)
    ffn_in_grad = back_dot(hidden_low, w_up)
    middle_part, second_gain_grad = norm_back(second_normed, second_inv, norm_gains[1], ffn_in_grad)
    middle_grad = grad_full + middle_part
    middle_low = middle_grad.astype(jnp.bfloat16)
    out_weight_grad = outer_sum(middle_low, sub_in)
    first_bias_grad = jnp.sum(middle_low, 0, dtype=jnp.float32)
    sub_grad = back_dot(middle_low, w_out)
    attended_grad, head_gain_grad = norm_back(sub_normed, sub_inv, head_gain, sub_grad)
    attended_low = attended_grad.astype(jnp.bfloat16)
    down_grad, up_grad, out_weight_grad, attended_low = lax.optimization_barrier(
        (
            down_grad.astype(jnp.bfloat16),
            up_grad.astype(jnp.bfloat16),
            out_weight_grad.astype(jnp.bfloat16),
            attended_low,
        )
    )
    tensor_count = lax.axis_size("tensor")
    early_widths = (down_grad.shape[1], up_grad.shape[1], out_weight_grad.shape[1])
    early_share = shard_stage(
        jnp.concatenate(
            [
                part.reshape(part.shape[0], tensor_count, part.shape[1] // tensor_count)
                for part in (down_grad, up_grad, out_weight_grad)
            ],
            2,
        ),
        0,
    )
    query_grad, key_part, value_part = split_attention_backward(
        query_matrix.reshape(seq_count, local_len, model_width),
        key_all,
        value_all,
        attended_low.reshape(seq_count, local_len, model_width),
        codes,
        span,
    )
    if span is not None:
        key_part = key_part.reshape(row_count, model_width)
        value_part = value_part.reshape(row_count, model_width)
    query_low = query_grad.reshape(row_count, model_width)
    if span is None:
        key_part = pair_reduce(key_part, "context", 1)
        value_part = pair_reduce(value_part, "context", 1)
    key_low = key_part.astype(jnp.bfloat16).reshape(row_count, model_width)
    value_low = value_part.astype(jnp.bfloat16).reshape(row_count, model_width)
    stacked = jnp.stack([query_low, key_low, value_low])
    early_share, stacked, carried = lax.optimization_barrier((early_share, stacked, carried))
    qkv_grad = jnp.einsum("rd,jre->dje", attn_in, stacked, preferred_element_type=jnp.float32)
    head_bias_grad = jnp.stack(
        [jnp.sum(query_low, 0, dtype=jnp.float32), jnp.sum(value_low, 0, dtype=jnp.float32)]
    )
    qkv_grad, stacked = lax.optimization_barrier((qkv_grad, stacked))
    attn_in_grad = jnp.einsum("jre,jde->rd", stacked, w_qkv, preferred_element_type=jnp.float32)
    first_gain_grad = jnp.sum(attn_in_grad * first_normed, 0)
    heads = model_width // HD
    unit_rows = unit_bias_grad.shape[0] // HD
    small_terms = (
        (jnp.stack([first_gain_grad, second_gain_grad]), 1, None),
        (jnp.stack([first_bias_grad, last_bias_grad]), 1, None),
        (head_bias_grad.reshape(2, heads, HD), 2, 1),
        (head_gain_grad.reshape(heads, HD), 1, 0),
        (unit_bias_grad.reshape(unit_rows, HD), 1, 0),
        (unit_gain_grad.reshape(unit_rows, HD), 1, 0),
    )
    ns = lax.axis_size("shard")
    nt = lax.axis_size("tensor")
    small_rows = jnp.concatenate(
        [disassemble(full, shard_dim, tensor_dim) for full, shard_dim, tensor_dim in small_terms], 1
    )
    small_width = small_rows.shape[1]
    block_rows = model_width // ns
    extra_rows = 8
    planes = qkv_grad.shape[1]
    slots = extra_rows * planes * (model_width // nt)
    small_block = (
        jnp.pad(small_rows, ((0, 0), (0, slots - small_width)))
        .reshape(ns, nt, extra_rows, planes, model_width // nt)
        .transpose(0, 2, 3, 1, 4)
        .reshape(ns, extra_rows, planes, model_width)
    )
    widened = jnp.concatenate(
        [qkv_grad.reshape(ns, block_rows, planes, model_width), small_block.astype(qkv_grad.dtype)], 1
    ).reshape(ns * (block_rows + extra_rows), planes, model_width)
    widened, attn_in_grad = lax.optimization_barrier((widened, attn_in_grad))
    qkv_share = shard_stage(widened, 0)
    early_total = finish_stage(early_share, 1).reshape(early_share.shape[0], -1)
    early_total, attn_in_grad = lax.optimization_barrier((early_total, attn_in_grad))
    input_part = norm_back(first_normed, first_inv, norm_gains[0], attn_in_grad)[0]
    input_low = (middle_grad + input_part).astype(jnp.bfloat16)
    qkv_total = finish_stage(qkv_share, 2)
    small_total = qkv_total[block_rows:].reshape(-1)[:small_width]
    small_pieces = []
    offset = 0
    for full, shard_dim, tensor_dim in small_terms:
        local_shape = list(full.shape)
        if shard_dim is not None:
            local_shape[shard_dim] //= ns
        if tensor_dim is not None:
            local_shape[tensor_dim] //= nt
        count = 1
        for size in local_shape:
            count *= size
        small_pieces.append(small_total[offset : offset + count].reshape(local_shape))
        offset += count
    down_width = early_widths[0] // nt
    up_width = early_widths[1] // nt
    grad_shares = (
        early_total[:, :down_width].transpose(1, 0),
        early_total[:, down_width : down_width + up_width],
        early_total[:, down_width + up_width :].transpose(1, 0),
        qkv_total[:block_rows].transpose(1, 0, 2),
    ) + tuple(small_pieces)
    return (grad_shares, input_low.reshape(seq_count, local_len, model_width), carried)


def local(
    inputs,
    out_grad,
    picture_starts,
    segment_offsets,
    dilation_offsets,
    norm_gains,
    w_qkv,
    head_biases,
    head_gain,
    w_out,
    out_biases,
    w_up,
    unit_bias,
    unit_gain,
    w_down,
):
    local_seqs, local_len, model_width = inputs.shape
    tensor_count = lax.axis_size("tensor")
    context_count = lax.axis_size("context")
    seq_len = local_len * context_count
    key_position = jnp.arange(seq_len, dtype=jnp.int32)
    whole = context_count == 2 and tensor_count == 2 and local_seqs == 4
    if whole:
        span = seq_len // PIECES
        me_c = lax.axis_index("context")
        own_seq = lax.axis_index("tensor") * context_count + me_c
        partner_seq = lax.axis_index("tensor") * context_count + 1 - me_c
        swap = [(0, 1), (1, 0)]

        def own_sequence(rows):
            kept = lax.dynamic_slice_in_dim(rows, own_seq, 1, 0)
            sent = lax.dynamic_slice_in_dim(rows, partner_seq, 1, 0)
            received = lax.ppermute(sent, "context", perm=swap)
            return jnp.where(
                me_c == 0,
                jnp.concatenate([kept, received], 1),
                jnp.concatenate([received, kept], 1),
            )

        block_in = own_sequence(inputs)
        block_grad = own_sequence(out_grad)
        starts = lax.dynamic_slice_in_dim(picture_starts, own_seq, 1, 0)
        query_position = key_position
    else:
        span = None
        mine = local_seqs // tensor_count
        first_seq = lax.axis_index("tensor") * mine
        block_in = lax.dynamic_slice_in_dim(inputs, first_seq, mine, 0)
        block_grad = lax.dynamic_slice_in_dim(out_grad, first_seq, mine, 0)
        starts = lax.dynamic_slice_in_dim(picture_starts, first_seq, mine, 0)
        query_position = lax.axis_index("context") * local_len + jnp.arange(
            local_len, dtype=jnp.int32
        )
    spans = jnp.array([seq_len * part // 8 for part in span_parts], jnp.int32)
    rates = jnp.array(dilation_rates, jnp.int32)
    segment_kept = segment_offsets % spans
    dilation_kept = dilation_offsets % rates
    offset_digits = jnp.concatenate(
        [segment_kept // 32, segment_kept % 32, dilation_kept], 1
    ).astype(jnp.bfloat16)
    f32 = jnp.float32
    (
        w_qkv_full,
        gains_full,
        out_bias_full,
        head_bias_full,
        head_gain_full,
        unit_bias_full,
        unit_gain_full,
        digits_full,
    ) = gather_packed(
        (
            (w_qkv, 1, 2),
            (norm_gains, 1, None),
            (out_biases, 1, None),
            (head_biases, 2, 1),
            (head_gain, 1, 0),
            (unit_bias, 1, 0),
            (unit_gain, 1, 0),
            (offset_digits, None, 0),
        )
    )
    patterns = len(span_parts)
    digits_full = digits_full.astype(jnp.int32)
    all_segments = digits_full[:, :patterns] * 32 + digits_full[:, patterns : 2 * patterns]
    all_dilations = digits_full[:, 2 * patterns :]
    codes = mask_codes(starts, query_position, key_position, all_segments, all_dilations, seq_len)
    w_out, w_up, w_down, w_qkv_full = lax.optimization_barrier((w_out, w_up, w_down, w_qkv_full))
    weights = (
        w_qkv_full,
        gather_weight(w_out, 1, 0),
        gather_weight(w_up, 0, 1),
        gather_weight(w_down, 1, 0),
        gains_full.astype(f32),
        out_bias_full.astype(f32),
        head_bias_full.reshape(2, model_width).astype(f32),
        head_gain_full.reshape(model_width).astype(f32),
        unit_bias_full.reshape(-1).astype(f32),
        unit_gain_full.reshape(-1).astype(f32),
    )
    kept_state, layer_block = forward_pass(block_in, codes, weights, span)
    if whole:
        layer_out = spread_sequence(layer_block, local_len)
    else:
        layer_out = pair_gather(layer_block, "tensor", 0)
    grad_shares, input_block, layer_out = backward_pass(
        kept_state, block_grad, weights, span, layer_out
    )
    if whole:
        input_grad = spread_sequence(input_block, local_len)
    else:
        input_grad = pair_gather(input_block, "tensor", 0)
    (
        down_share,
        up_share,
        out_share,
        qkv_share,
        gains_share,
        out_bias_share,
        head_bias_share,
        head_gain_share,
        unit_bias_share,
        unit_gain_share,
    ) = grad_shares
    return (
        layer_out,
        input_grad,
        gains_share,
        qkv_share,
        head_bias_share,
        head_gain_share,
        out_share,
        out_bias_share,
        up_share,
        unit_bias_share,
        unit_gain_share,
        down_share,
    )


def solution(mesh):
    placed = (
        P("shard", "context", None),
        P("shard", "context", None),
        P("shard", None),
        P("tensor", None),
        P("tensor", None),
        P(None, "shard"),
        P(None, "shard", "tensor"),
        P(None, "tensor", "shard"),
        P("tensor", "shard"),
        P("tensor", "shard"),
        P(None, "shard"),
        P("shard", "tensor"),
        P("tensor", "shard"),
        P("tensor", "shard"),
        P("tensor", "shard"),
    )
    return jax.shard_map(
        local,
        mesh=mesh,
        in_specs=placed,
        out_specs=(
            P("shard", "context", None),
            P("shard", "context", None),
            P(None, "shard"),
            P(None, "shard", "tensor"),
            P(None, "tensor", "shard"),
            P("tensor", "shard"),
            P("tensor", "shard"),
            P(None, "shard"),
            P("shard", "tensor"),
            P("tensor", "shard"),
            P("tensor", "shard"),
            P("tensor", "shard"),
        ),
        check_vma=False,
    )
```

```python
from functools import partial

import jax
import jax.numpy as jnp
from jax import lax
from jax.experimental import pallas as pl
from jax.experimental.pallas import tpu as pltpu
from jax.sharding import PartitionSpec as P

HD = 64
FF = 3072
PIECE = 256
PIECES = 2


epsilon = 1e-05
span_parts = (1, 2, 4, 6, 8)
dilation_rates = (1, 2, 4, 6, 12)


def pattern_total(query_position, key_position, segmented_offsets, dilated_offsets, token_length):
    tallied_total = jnp.zeros(
        (segmented_offsets.shape[0], query_position.shape[0], key_position.shape[0]), jnp.float32
    )
    for item_number in range(len(span_parts)):
        segmented_span = token_length * span_parts[item_number] // 8
        dilated_stride = dilation_rates[item_number]
        seg_shift = (segmented_offsets[:, item_number] % segmented_span)[:, None, None]
        dilated_phase = (dilated_offsets[:, item_number] % dilated_stride)[:, None, None]
        query_lookup = query_position[None, :, None] + seg_shift
        key_lookup = key_position[None, None, :] + seg_shift
        merged_heads = (
            (query_lookup // segmented_span == key_lookup // segmented_span)
            & (query_lookup % dilated_stride == dilated_phase)
            & (key_lookup % dilated_stride == dilated_phase)
        )
        tallied_total = tallied_total + merged_heads.astype(jnp.float32)
    return tallied_total


def picture_index(starts, token_positions):
    marked = jnp.zeros((starts.shape[0], token_positions.shape[0]), jnp.int32)
    for piece_number in range(starts.shape[1]):
        begin_at = starts[:, piece_number][:, None]
        inside = (token_positions[None, :] >= begin_at) & (
            token_positions[None, :] < begin_at + PIECE
        )
        marked = marked + (piece_number + 1) * inside.astype(jnp.int32)
    return marked


def allowed_keys(query_pic, key_pic, query_position, key_position):
    causal_ok = key_position[None, None, :] <= query_position[None, :, None]
    same_piece = (query_pic[:, :, None] == key_pic[:, None, :]) & (query_pic[:, :, None] > 0)
    return (causal_ok | same_piece).astype(jnp.float32)


def outer_sum(left_rows, right_rows):
    return lax.dot_general(
        left_rows, right_rows, (((0,), (0,)), ((), ())), preferred_element_type=jnp.float32
    )


def back_dot(left_rows, weight_rows):
    return lax.dot_general(
        left_rows, weight_rows, (((1,), (1,)), ((), ())), preferred_element_type=jnp.float32
    )


def norm_rows(values, scale_row):
    mean_row = jnp.mean(values, -1, keepdims=True)
    centered = values - mean_row
    inv_std = lax.rsqrt(jnp.mean(centered * centered, -1, keepdims=True) + epsilon)
    normed = centered * inv_std
    return (normed, inv_std, normed * scale_row)


def norm_back(normed, inv_std, scale_row, grad_rows):
    scaled = grad_rows * scale_row
    mean_plain = jnp.mean(scaled, -1, keepdims=True)
    mean_cross = jnp.mean(scaled * normed, -1, keepdims=True)
    return (inv_std * (scaled - mean_plain - normed * mean_cross), jnp.sum(grad_rows * normed, 0))


def probabilities(query_heads, key_heads, mask_table):
    raw_scores = jnp.einsum(
        "sqhd,skhd->shqk", query_heads, key_heads, preferred_element_type=jnp.float32
    ) * HD ** (-0.5)
    masked = jnp.where(mask_table > 0, raw_scores, -1000000000.0)
    row_top = jnp.max(masked, -1, keepdims=True)
    exponent = mask_table * jnp.exp(masked - row_top)
    row_total = jnp.sum(exponent, -1, keepdims=True)
    return (exponent / row_total, row_top, row_total)


SCALE = HD ** (-0.5)
HIDDEN = -1000000000.0
PAIR = 2
CODE_WIDTH = 8


def pair_masks(patq_ref, patk_ref, pcq_ref, pck_ref):
    first_q = patq_ref[0]
    first_k = patk_ref[0]
    row = first_q[:, 5:6]
    col = first_k[5:6, :]
    piece_q = pcq_ref[0][:, 0:1]
    piece_k = pck_ref[0][0:1, :]
    allowed = (col <= row) | (piece_q == piece_k)
    masks = []
    for head in range(PAIR):
        codes_q = patq_ref[head]
        codes_k = patk_ref[head]
        tally = (codes_q[:, 0:1] == codes_k[0:1, :]).astype(jnp.float32)
        for pattern in range(1, len(span_parts)):
            tally = tally + (
                codes_q[:, pattern : pattern + 1] == codes_k[pattern : pattern + 1, :]
            ).astype(jnp.float32)
        masks.append(jnp.where(allowed, tally, 0.0))
    return masks


def soft_rows(query_part, key_block, mask):
    scores = (
        lax.dot_general(
            query_part, key_block, (((1,), (1,)), ((), ())), preferred_element_type=jnp.float32
        )
        * SCALE
    )
    masked = jnp.where(mask > 0, scores, HIDDEN)
    top = jnp.max(masked, axis=1, keepdims=True)
    exponent = mask * jnp.exp(masked - top)
    return exponent / jnp.sum(exponent, axis=1, keepdims=True)


def attention_fwd_kernel(q_ref, k_ref, v_ref, patq_ref, patk_ref, pcq_ref, pck_ref, o_ref):
    query = q_ref[0]
    key_block = k_ref[0]
    value_block = v_ref[0]
    first = lax.broadcasted_iota(jnp.int32, query.shape, 1) < HD
    masks = pair_masks(patq_ref, patk_ref, pcq_ref, pck_ref)
    result = None
    for head in range(PAIR):
        keep = first if head == 0 else jnp.logical_not(first)
        query_part = jnp.where(keep, query, jnp.zeros_like(query))
        probs = soft_rows(query_part, key_block, masks[head])
        mixed = jnp.dot(
            probs.astype(jnp.bfloat16), value_block, preferred_element_type=jnp.float32
        )
        result = mixed if result is None else jnp.where(first, result, mixed)
    o_ref[0] = result


def attention_bwd_kernel(
    q_ref, k_ref, v_ref, do_ref, patq_ref, patk_ref, pcq_ref, pck_ref, dq_ref, dk_ref, dv_ref
):
    @pl.when(pl.program_id(2) == 0)
    def _():
        dk_ref[...] = jnp.zeros_like(dk_ref)
        dv_ref[...] = jnp.zeros_like(dv_ref)

    query = q_ref[0]
    key_block = k_ref[0]
    value_block = v_ref[0]
    grad_out = do_ref[0]
    first = lax.broadcasted_iota(jnp.int32, query.shape, 1) < HD
    masks = pair_masks(patq_ref, patk_ref, pcq_ref, pck_ref)
    query_grad = None
    key_grad = dk_ref[0]
    value_grad = dv_ref[0]
    for head in range(PAIR):
        keep = first if head == 0 else jnp.logical_not(first)
        query_part = jnp.where(keep, query, jnp.zeros_like(query))
        grad_part = jnp.where(keep, grad_out, jnp.zeros_like(grad_out))
        probs = soft_rows(query_part, key_block, masks[head])
        prob_grad = lax.dot_general(
            grad_part, value_block, (((1,), (1,)), ((), ())), preferred_element_type=jnp.float32
        )
        inner = jnp.sum(probs * prob_grad, axis=1, keepdims=True)
        score_low = (probs * (prob_grad - inner)).astype(jnp.bfloat16)
        part = jnp.dot(score_low, key_block, preferred_element_type=jnp.float32)
        query_grad = part if query_grad is None else jnp.where(first, query_grad, part)
        key_grad = key_grad + SCALE * lax.dot_general(
            score_low, query_part, (((0,), (0,)), ((), ())), preferred_element_type=jnp.float32
        )
        value_grad = value_grad + lax.dot_general(
            probs.astype(jnp.bfloat16),
            grad_part,
            (((0,), (0,)), ((), ())),
            preferred_element_type=jnp.float32,
        )
    dq_ref[0] = (query_grad * SCALE).astype(jnp.bfloat16)
    dk_ref[0] = key_grad
    dv_ref[0] = value_grad


def attention_specs(seq_count, local_len, seq_len, block_q):
    lanes = PAIR * HD
    query_spec = pl.BlockSpec((1, block_q, lanes), lambda s, g, b: (s, b, g))
    key_spec = pl.BlockSpec((1, seq_len, lanes), lambda s, g, b: (s, 0, g))
    patq_spec = pl.BlockSpec((PAIR, block_q, CODE_WIDTH), lambda s, g, b: (g, b, 0))
    patk_spec = pl.BlockSpec((PAIR, CODE_WIDTH, seq_len), lambda s, g, b: (g, 0, 0))
    pcq_spec = pl.BlockSpec((1, block_q, CODE_WIDTH), lambda s, g, b: (s, b, 0))
    pck_spec = pl.BlockSpec((1, CODE_WIDTH, seq_len), lambda s, g, b: (s, 0, 0))
    return query_spec, key_spec, patq_spec, patk_spec, pcq_spec, pck_spec


def attention_forward(query, keys, values, codes):
    seq_count, local_len, width = query.shape
    seq_len = keys.shape[1]
    block_q = min(128, local_len)
    grid = (seq_count, width // (PAIR * HD), local_len // block_q)
    query_spec, key_spec, patq_spec, patk_spec, pcq_spec, pck_spec = attention_specs(
        seq_count, local_len, seq_len, block_q
    )
    flops = 8 * seq_count * local_len * seq_len * width
    return pl.pallas_call(
        attention_fwd_kernel,
        grid=grid,
        in_specs=[query_spec, key_spec, key_spec, patq_spec, patk_spec, pcq_spec, pck_spec],
        out_specs=query_spec,
        out_shape=jax.ShapeDtypeStruct((seq_count, local_len, width), jnp.float32),
        compiler_params=pltpu.CompilerParams(
            dimension_semantics=("parallel", "parallel", "arbitrary"),
            vmem_limit_bytes=48 * 1024 * 1024,
        ),
        cost_estimate=pl.CostEstimate(
            flops=flops,
            transcendentals=seq_count * local_len * seq_len * width // HD,
            bytes_accessed=2 * query.size + 2 * keys.size * 2 * (local_len // block_q) + 4 * query.size,
        ),
    )(query, keys, values, *codes)


def attention_backward(query, keys, values, grad_out, codes):
    seq_count, local_len, width = query.shape
    seq_len = keys.shape[1]
    block_q = min(128, local_len)
    grid = (seq_count, width // (PAIR * HD), local_len // block_q)
    query_spec, key_spec, patq_spec, patk_spec, pcq_spec, pck_spec = attention_specs(
        seq_count, local_len, seq_len, block_q
    )
    flops = 20 * seq_count * local_len * seq_len * width
    return pl.pallas_call(
        attention_bwd_kernel,
        grid=grid,
        in_specs=[
            query_spec,
            key_spec,
            key_spec,
            query_spec,
            patq_spec,
            patk_spec,
            pcq_spec,
            pck_spec,
        ],
        out_specs=[query_spec, key_spec, key_spec],
        out_shape=[
            jax.ShapeDtypeStruct((seq_count, local_len, width), jnp.bfloat16),
            jax.ShapeDtypeStruct((seq_count, seq_len, width), jnp.float32),
            jax.ShapeDtypeStruct((seq_count, seq_len, width), jnp.float32),
        ],
        compiler_params=pltpu.CompilerParams(
            dimension_semantics=("parallel", "parallel", "arbitrary"),
            vmem_limit_bytes=48 * 1024 * 1024,
        ),
        cost_estimate=pl.CostEstimate(
            flops=flops,
            transcendentals=seq_count * local_len * seq_len * width // HD,
            bytes_accessed=4 * query.size + 2 * keys.size * 2 * (local_len // block_q) + 16 * keys.size,
        ),
    )(query, keys, values, grad_out, *codes)


def mask_codes(starts, query_position, key_position, segment_offsets, dilation_offsets, seq_len):
    heads = segment_offsets.shape[0]
    query_codes = []
    key_codes = []
    for pattern in range(len(span_parts)):
        span = seq_len * span_parts[pattern] // 8
        rate = dilation_rates[pattern]
        shift = (segment_offsets[:, pattern] % span)[:, None]
        phase = (dilation_offsets[:, pattern] % rate)[:, None]
        query_at = query_position[None, :] + shift
        key_at = key_position[None, :] + shift
        query_codes.append(jnp.where(query_at % rate == phase, query_at // span, -1))
        key_codes.append(jnp.where(key_at % rate == phase, key_at // span, -2))
    patterns = len(span_parts)
    query_codes.append(jnp.broadcast_to(query_position[None, :], (heads, query_position.shape[0])))
    key_codes.append(jnp.broadcast_to(key_position[None, :], (heads, key_position.shape[0])))
    filler = CODE_WIDTH - patterns - 1
    query_codes += [jnp.zeros((heads, query_position.shape[0]), jnp.int32)] * filler
    key_codes += [jnp.zeros((heads, key_position.shape[0]), jnp.int32)] * filler
    patq = jnp.stack(query_codes, 2).astype(jnp.int32)
    patk = jnp.stack(key_codes, 1).astype(jnp.int32)
    query_pic = picture_index(starts, query_position)
    key_pic = picture_index(starts, key_position)
    pcq = jnp.where(query_pic > 0, query_pic, -1)[:, :, None]
    pcq = jnp.pad(pcq, ((0, 0), (0, 0), (0, CODE_WIDTH - 1)))
    pck = jnp.where(key_pic > 0, key_pic, -2)[:, None, :]
    pck = jnp.pad(pck, ((0, 0), (0, CODE_WIDTH - 1), (0, 0)))
    return (patq, patk, pcq.astype(jnp.int32), pck.astype(jnp.int32))


def code_part(codes, begin, end, key_end):
    patq, patk, pcq, pck = codes
    return (patq[:, begin:end], patk[:, :, :key_end], pcq[:, begin:end], pck[:, :, :key_end])


def split_attention_forward(query, keys, values, codes, span):
    if span is None:
        return attention_forward(query, keys, values, codes)
    head = attention_forward(
        query[:, :span], keys[:, :span], values[:, :span], code_part(codes, 0, span, span)
    )
    seq_len = keys.shape[1]
    tail = attention_forward(
        query[:, span:], keys, values, code_part(codes, span, query.shape[1], seq_len)
    )
    return jnp.concatenate([head, tail], 1)


def split_attention_backward(query, keys, values, grad_out, codes, span):
    if span is None:
        return attention_backward(query, keys, values, grad_out, codes)
    seq_len = keys.shape[1]
    head_q, head_k, head_v = attention_backward(
        query[:, :span],
        keys[:, :span],
        values[:, :span],
        grad_out[:, :span],
        code_part(codes, 0, span, span),
    )
    tail_q, tail_k, tail_v = attention_backward(
        query[:, span:],
        keys,
        values,
        grad_out[:, span:],
        code_part(codes, span, query.shape[1], seq_len),
    )
    padding = ((0, 0), (0, seq_len - span), (0, 0))
    return (
        jnp.concatenate([head_q, tail_q], 1),
        tail_k + jnp.pad(head_k, padding),
        tail_v + jnp.pad(head_v, padding),
    )


def spread_sequence(block, local_len):
    me_c = lax.axis_index("context")
    me_t = lax.axis_index("tensor")
    swap = [(0, 1), (1, 0)]
    kept = lax.dynamic_slice_in_dim(block, me_c * local_len, local_len, 1)
    other = lax.dynamic_slice_in_dim(block, (1 - me_c) * local_len, local_len, 1)
    from_context = lax.ppermute(other, "context", perm=swap)
    from_tensor = lax.ppermute(kept, "tensor", perm=swap)
    from_corner = lax.ppermute(other, ("context", "tensor"), perm=[(0, 3), (3, 0), (1, 2), (2, 1)])
    first_c = me_c == 0
    own_pair = jnp.where(
        first_c,
        jnp.concatenate([kept, from_context], 0),
        jnp.concatenate([from_context, kept], 0),
    )
    far_pair = jnp.where(
        first_c,
        jnp.concatenate([from_tensor, from_corner], 0),
        jnp.concatenate([from_corner, from_tensor], 0),
    )
    return jnp.where(
        me_t == 0,
        jnp.concatenate([own_pair, far_pair], 0),
        jnp.concatenate([far_pair, own_pair], 0),
    )


def assemble(stacked, shard_dim, tensor_dim):
    ns, nt = stacked.shape[0], stacked.shape[1]
    if shard_dim is None:
        stacked = stacked[:1]
    if tensor_dim is None:
        stacked = stacked[:, :1]
    local_shape = stacked.shape[2:]
    order = []
    for dim in range(len(local_shape)):
        if dim == shard_dim:
            order.append(0)
        if dim == tensor_dim:
            order.append(1)
        order.append(dim + 2)
    if shard_dim is None:
        order = [0] + order
    if tensor_dim is None:
        order = [1] + order
    moved = stacked.transpose(order)
    full_shape = list(local_shape)
    if shard_dim is not None:
        full_shape[shard_dim] *= ns
    if tensor_dim is not None:
        full_shape[tensor_dim] *= nt
    return moved.reshape(full_shape)


def gather_weight(local_block, shard_dim, tensor_dim):
    ns = lax.axis_size("shard")
    nt = lax.axis_size("tensor")
    stacked = lax.all_gather(local_block, ("shard", "tensor"), axis=0, tiled=False)
    return assemble(stacked.reshape((ns, nt) + local_block.shape), shard_dim, tensor_dim)


def gather_packed(blocks):
    ns = lax.axis_size("shard")
    nt = lax.axis_size("tensor")
    flat = jnp.concatenate([block.reshape(-1) for block, _, _ in blocks])
    padded = -flat.size % 2048
    flat = jnp.pad(flat, (0, padded)).reshape(-1, 128)
    stacked = lax.all_gather(flat, ("shard", "tensor"), axis=0, tiled=False).reshape(ns, nt, -1)
    pieces = []
    offset = 0
    for block, shard_dim, tensor_dim in blocks:
        part = stacked[:, :, offset : offset + block.size].reshape((ns, nt) + block.shape)
        pieces.append(assemble(part, shard_dim, tensor_dim))
        offset += block.size
    return pieces


def pair_gather(block, axis_name, dim):
    if lax.axis_size(axis_name) != 2:
        return lax.all_gather(block, axis_name, axis=dim, tiled=True)
    other = lax.ppermute(block, axis_name, perm=[(0, 1), (1, 0)])
    first = lax.axis_index(axis_name) == 0
    return jnp.where(
        first, jnp.concatenate([block, other], dim), jnp.concatenate([other, block], dim)
    )


def pair_reduce(full, axis_name, dim):
    if lax.axis_size(axis_name) != 2:
        return lax.psum_scatter(
            full.astype(jnp.bfloat16), axis_name, scatter_dimension=dim, tiled=True
        ).astype(jnp.float32)
    half = full.shape[dim] // 2
    me = lax.axis_index(axis_name)
    kept = lax.dynamic_slice_in_dim(full, me * half, half, dim)
    sent = lax.dynamic_slice_in_dim(full, (1 - me) * half, half, dim).astype(jnp.bfloat16)
    received = lax.ppermute(sent, axis_name, perm=[(0, 1), (1, 0)])
    return kept + received.astype(jnp.float32)


def pair_sum(share, axis_name):
    if lax.axis_size(axis_name) != 2:
        return lax.psum(share, axis_name).astype(jnp.float32)
    received = lax.ppermute(share, axis_name, perm=[(0, 1), (1, 0)])
    return share.astype(jnp.float32) + received.astype(jnp.float32)


def disassemble(full, shard_dim, tensor_dim):
    ns = lax.axis_size("shard")
    nt = lax.axis_size("tensor")
    split_shape = []
    positions = {}
    for dim, size in enumerate(full.shape):
        if dim == shard_dim:
            positions["s"] = len(split_shape)
            split_shape += [ns, size // ns]
        elif dim == tensor_dim:
            positions["t"] = len(split_shape)
            split_shape += [nt, size // nt]
        else:
            split_shape.append(size)
    pieces = full.reshape(split_shape)
    lead = [positions[key] for key in ("s", "t") if key in positions]
    rest = [d for d in range(len(split_shape)) if d not in lead]
    pieces = pieces.transpose(lead + rest)
    if "s" not in positions:
        pieces = jnp.broadcast_to(pieces[None], (ns,) + pieces.shape)
    if "t" not in positions:
        pieces = jnp.broadcast_to(pieces[:, None], (ns, nt) + pieces.shape[1:])
    return pieces.reshape(ns * nt, -1)


def pack_rows(terms):
    rows = jnp.concatenate(
        [disassemble(full.astype(jnp.bfloat16), shard_dim, tensor_dim) for full, shard_dim, tensor_dim in terms],
        1,
    )
    width = rows.shape[1]
    return jnp.pad(rows, ((0, 0), (0, -width % 1024))).reshape(rows.shape[0], -1, 128)


def scatter_rows(rows):
    return lax.psum_scatter(rows, ("shard", "tensor"), scatter_dimension=0, tiled=False)


def unpack_share(share, terms):
    total = pair_sum(share, "context").reshape(-1)
    pieces = []
    offset = 0
    ns = lax.axis_size("shard")
    nt = lax.axis_size("tensor")
    for full, shard_dim, tensor_dim in terms:
        local_shape = list(full.shape)
        if shard_dim is not None:
            local_shape[shard_dim] //= ns
        if tensor_dim is not None:
            local_shape[tensor_dim] //= nt
        count = 1
        for size in local_shape:
            count *= size
        pieces.append(total[offset : offset + count].reshape(local_shape))
        offset += count
    return pieces


def shard_stage(grad, dim):
    return lax.psum_scatter(grad.astype(jnp.bfloat16), "shard", scatter_dimension=dim, tiled=True)


def finish_stage(share, tensor_dim):
    summed = pair_reduce(share, "tensor", tensor_dim)
    return pair_sum(summed.astype(jnp.bfloat16), "context")


def forward_pass(block_in, codes, weights, span):
    w_qkv, w_out, w_up, w_down, norm_gains, out_biases, head_biases, head_gain, unit_bias, unit_gain = weights
    seq_count, local_len, model_width = block_in.shape
    row_count = seq_count * local_len
    flattened_input = block_in.reshape(row_count, model_width).astype(jnp.float32)
    first_normed, first_inv, first_out = norm_rows(flattened_input, norm_gains[0])
    attn_in = first_out.astype(jnp.bfloat16)
    projected = jnp.einsum("rd,jde->jre", attn_in, w_qkv, preferred_element_type=jnp.float32)
    query_matrix = (projected[0] + head_biases[0]).astype(jnp.bfloat16)
    keys_local = projected[1].astype(jnp.bfloat16).reshape(seq_count, local_len, model_width)
    values_local = (projected[2] + head_biases[1]).astype(jnp.bfloat16).reshape(
        seq_count, local_len, model_width
    )
    if span is None:
        key_all = pair_gather(keys_local, "context", 1)
        value_all = pair_gather(values_local, "context", 1)
    else:
        key_all, value_all = keys_local, values_local
    attended = split_attention_forward(
        query_matrix.reshape(seq_count, local_len, model_width), key_all, value_all, codes, span
    ).reshape(row_count, model_width)
    sub_normed, sub_inv, sub_out = norm_rows(attended, head_gain)
    sub_in = sub_out.astype(jnp.bfloat16)
    middle = flattened_input + (
        jnp.dot(sub_in, w_out, preferred_element_type=jnp.float32) + out_biases[0]
    )
    second_normed, second_inv, second_out = norm_rows(middle, norm_gains[1])
    ffn_in = second_out.astype(jnp.bfloat16)
    hidden = jnp.dot(ffn_in, w_up, preferred_element_type=jnp.float32) + unit_bias
    activated = jax.nn.gelu(hidden, approximate=True)
    unit_normed, unit_inv, unit_out = norm_rows(activated, unit_gain)
    ffn_mid = unit_out.astype(jnp.bfloat16)
    layer_out = (
        middle + (jnp.dot(ffn_mid, w_down, preferred_element_type=jnp.float32) + out_biases[1])
    ).astype(jnp.bfloat16)
    kept_state = (
        attn_in,
        first_normed,
        first_inv,
        query_matrix,
        key_all,
        value_all,
        codes,
        sub_normed,
        sub_inv,
        sub_in,
        second_normed,
        second_inv,
        ffn_in,
        hidden,
        unit_normed,
        unit_inv,
        ffn_mid,
    )
    return (kept_state, layer_out.reshape(seq_count, local_len, model_width))


def backward_pass(kept_state, block_grad, weights, span, carried):
    w_qkv, w_out, w_up, w_down, norm_gains, out_biases, head_biases, head_gain, unit_bias, unit_gain = weights
    (
        attn_in,
        first_normed,
        first_inv,
        query_matrix,
        key_all,
        value_all,
        codes,
        sub_normed,
        sub_inv,
        sub_in,
        second_normed,
        second_inv,
        ffn_in,
        hidden,
        unit_normed,
        unit_inv,
        ffn_mid,
    ) = kept_state
    seq_count, local_len, model_width = block_grad.shape
    row_count = seq_count * local_len
    seq_len = key_all.shape[1]
    grad_low = block_grad.reshape(row_count, model_width)
    grad_full = grad_low.astype(jnp.float32)
    down_grad = outer_sum(grad_low, ffn_mid)
    last_bias_grad = jnp.sum(grad_full, 0)
    unit_grad = back_dot(grad_low, w_down)
    activated_grad, unit_gain_grad = norm_back(unit_normed, unit_inv, unit_gain, unit_grad)
    gelu_value, gelu_pull = jax.vjp(partial(jax.nn.gelu, approximate=True), hidden)
    hidden_low = gelu_pull(activated_grad)[0].astype(jnp.bfloat16)
    up_grad = outer_sum(ffn_in, hidden_low)
    unit_bias_grad = jnp.sum(hidden_low, 0, dtype=jnp.float32)
    ffn_in_grad = back_dot(hidden_low, w_up)
    middle_part, second_gain_grad = norm_back(second_normed, second_inv, norm_gains[1], ffn_in_grad)
    middle_grad = grad_full + middle_part
    middle_low = middle_grad.astype(jnp.bfloat16)
    out_weight_grad = outer_sum(middle_low, sub_in)
    first_bias_grad = jnp.sum(middle_low, 0, dtype=jnp.float32)
    sub_grad = back_dot(middle_low, w_out)
    attended_grad, head_gain_grad = norm_back(sub_normed, sub_inv, head_gain, sub_grad)
    attended_low = attended_grad.astype(jnp.bfloat16)
    down_grad, up_grad, out_weight_grad, attended_low = lax.optimization_barrier(
        (
            down_grad.astype(jnp.bfloat16),
            up_grad.astype(jnp.bfloat16),
            out_weight_grad.astype(jnp.bfloat16),
            attended_low,
        )
    )
    tensor_count = lax.axis_size("tensor")
    early_widths = (down_grad.shape[1], up_grad.shape[1], out_weight_grad.shape[1])
    early_share = shard_stage(
        jnp.concatenate(
            [
                part.reshape(part.shape[0], tensor_count, part.shape[1] // tensor_count)
                for part in (down_grad, up_grad, out_weight_grad)
            ],
            2,
        ),
        0,
    )
    query_grad, key_part, value_part = split_attention_backward(
        query_matrix.reshape(seq_count, local_len, model_width),
        key_all,
        value_all,
        attended_low.reshape(seq_count, local_len, model_width),
        codes,
        span,
    )
    if span is not None:
        key_part = key_part.reshape(row_count, model_width)
        value_part = value_part.reshape(row_count, model_width)
    query_low = query_grad.reshape(row_count, model_width)
    if span is None:
        key_part = pair_reduce(key_part, "context", 1)
        value_part = pair_reduce(value_part, "context", 1)
    key_low = key_part.astype(jnp.bfloat16).reshape(row_count, model_width)
    value_low = value_part.astype(jnp.bfloat16).reshape(row_count, model_width)
    stacked = jnp.stack([query_low, key_low, value_low])
    early_share, stacked, carried = lax.optimization_barrier((early_share, stacked, carried))
    qkv_grad = jnp.einsum("rd,jre->dje", attn_in, stacked, preferred_element_type=jnp.float32)
    head_bias_grad = jnp.stack(
        [jnp.sum(query_low, 0, dtype=jnp.float32), jnp.sum(value_low, 0, dtype=jnp.float32)]
    )
    qkv_grad, stacked = lax.optimization_barrier((qkv_grad, stacked))
    attn_in_grad = jnp.einsum("jre,jde->rd", stacked, w_qkv, preferred_element_type=jnp.float32)
    input_part, first_gain_grad = norm_back(first_normed, first_inv, norm_gains[0], attn_in_grad)
    input_low = (middle_grad + input_part).astype(jnp.bfloat16)
    heads = model_width // HD
    unit_rows = unit_bias_grad.shape[0] // HD
    small_terms = (
        (jnp.stack([first_gain_grad, second_gain_grad]), 1, None),
        (jnp.stack([first_bias_grad, last_bias_grad]), 1, None),
        (head_bias_grad.reshape(2, heads, HD), 2, 1),
        (head_gain_grad.reshape(heads, HD), 1, 0),
        (unit_bias_grad.reshape(unit_rows, HD), 1, 0),
        (unit_gain_grad.reshape(unit_rows, HD), 1, 0),
    )
    ns = lax.axis_size("shard")
    nt = lax.axis_size("tensor")
    small_rows = jnp.concatenate(
        [disassemble(full, shard_dim, tensor_dim) for full, shard_dim, tensor_dim in small_terms], 1
    )
    small_width = small_rows.shape[1]
    block_rows = model_width // ns
    extra_rows = 8
    planes = qkv_grad.shape[1]
    slots = extra_rows * planes * (model_width // nt)
    small_block = (
        jnp.pad(small_rows, ((0, 0), (0, slots - small_width)))
        .reshape(ns, nt, extra_rows, planes, model_width // nt)
        .transpose(0, 2, 3, 1, 4)
        .reshape(ns, extra_rows, planes, model_width)
    )
    widened = jnp.concatenate(
        [qkv_grad.reshape(ns, block_rows, planes, model_width), small_block.astype(qkv_grad.dtype)], 1
    ).reshape(ns * (block_rows + extra_rows), planes, model_width)
    qkv_share = shard_stage(widened, 0)
    qkv_total = finish_stage(qkv_share, 2)
    small_total = qkv_total[block_rows:].reshape(-1)[:small_width]
    small_pieces = []
    offset = 0
    for full, shard_dim, tensor_dim in small_terms:
        local_shape = list(full.shape)
        if shard_dim is not None:
            local_shape[shard_dim] //= ns
        if tensor_dim is not None:
            local_shape[tensor_dim] //= nt
        count = 1
        for size in local_shape:
            count *= size
        small_pieces.append(small_total[offset : offset + count].reshape(local_shape))
        offset += count
    early_total = finish_stage(early_share, 1).reshape(early_share.shape[0], -1)
    down_width = early_widths[0] // nt
    up_width = early_widths[1] // nt
    grad_shares = (
        early_total[:, :down_width].transpose(1, 0),
        early_total[:, down_width : down_width + up_width],
        early_total[:, down_width + up_width :].transpose(1, 0),
        qkv_total[:block_rows].transpose(1, 0, 2),
    ) + tuple(small_pieces)
    return (grad_shares, input_low.reshape(seq_count, local_len, model_width), carried)


def local(
    inputs,
    out_grad,
    picture_starts,
    segment_offsets,
    dilation_offsets,
    norm_gains,
    w_qkv,
    head_biases,
    head_gain,
    w_out,
    out_biases,
    w_up,
    unit_bias,
    unit_gain,
    w_down,
):
    local_seqs, local_len, model_width = inputs.shape
    tensor_count = lax.axis_size("tensor")
    context_count = lax.axis_size("context")
    seq_len = local_len * context_count
    key_position = jnp.arange(seq_len, dtype=jnp.int32)
    whole = context_count == 2 and tensor_count == 2 and local_seqs == 4
    if whole:
        span = seq_len // PIECES
        me_c = lax.axis_index("context")
        own_seq = lax.axis_index("tensor") * context_count + me_c
        partner_seq = lax.axis_index("tensor") * context_count + 1 - me_c
        swap = [(0, 1), (1, 0)]

        def own_sequence(rows):
            kept = lax.dynamic_slice_in_dim(rows, own_seq, 1, 0)
            sent = lax.dynamic_slice_in_dim(rows, partner_seq, 1, 0)
            received = lax.ppermute(sent, "context", perm=swap)
            return jnp.where(
                me_c == 0,
                jnp.concatenate([kept, received], 1),
                jnp.concatenate([received, kept], 1),
            )

        block_in = own_sequence(inputs)
        block_grad = own_sequence(out_grad)
        starts = lax.dynamic_slice_in_dim(picture_starts, own_seq, 1, 0)
        query_position = key_position
    else:
        span = None
        mine = local_seqs // tensor_count
        first_seq = lax.axis_index("tensor") * mine
        block_in = lax.dynamic_slice_in_dim(inputs, first_seq, mine, 0)
        block_grad = lax.dynamic_slice_in_dim(out_grad, first_seq, mine, 0)
        starts = lax.dynamic_slice_in_dim(picture_starts, first_seq, mine, 0)
        query_position = lax.axis_index("context") * local_len + jnp.arange(
            local_len, dtype=jnp.int32
        )
    spans = jnp.array([seq_len * part // 8 for part in span_parts], jnp.int32)
    rates = jnp.array(dilation_rates, jnp.int32)
    segment_kept = segment_offsets % spans
    dilation_kept = dilation_offsets % rates
    offset_digits = jnp.concatenate(
        [segment_kept // 32, segment_kept % 32, dilation_kept], 1
    ).astype(jnp.bfloat16)
    f32 = jnp.float32
    (
        w_qkv_full,
        gains_full,
        out_bias_full,
        head_bias_full,
        head_gain_full,
        unit_bias_full,
        unit_gain_full,
        digits_full,
    ) = gather_packed(
        (
            (w_qkv, 1, 2),
            (norm_gains, 1, None),
            (out_biases, 1, None),
            (head_biases, 2, 1),
            (head_gain, 1, 0),
            (unit_bias, 1, 0),
            (unit_gain, 1, 0),
            (offset_digits, None, 0),
        )
    )
    patterns = len(span_parts)
    digits_full = digits_full.astype(jnp.int32)
    all_segments = digits_full[:, :patterns] * 32 + digits_full[:, patterns : 2 * patterns]
    all_dilations = digits_full[:, 2 * patterns :]
    codes = mask_codes(starts, query_position, key_position, all_segments, all_dilations, seq_len)
    w_out, w_up, w_down, w_qkv_full = lax.optimization_barrier((w_out, w_up, w_down, w_qkv_full))
    weights = (
        w_qkv_full,
        gather_weight(w_out, 1, 0),
        gather_weight(w_up, 0, 1),
        gather_weight(w_down, 1, 0),
        gains_full.astype(f32),
        out_bias_full.astype(f32),
        head_bias_full.reshape(2, model_width).astype(f32),
        head_gain_full.reshape(model_width).astype(f32),
        unit_bias_full.reshape(-1).astype(f32),
        unit_gain_full.reshape(-1).astype(f32),
    )
    kept_state, layer_block = forward_pass(block_in, codes, weights, span)
    if whole:
        layer_out = spread_sequence(layer_block, local_len)
    else:
        layer_out = pair_gather(layer_block, "tensor", 0)
    grad_shares, input_block, layer_out = backward_pass(
        kept_state, block_grad, weights, span, layer_out
    )
    if whole:
        input_grad = spread_sequence(input_block, local_len)
    else:
        input_grad = pair_gather(input_block, "tensor", 0)
    (
        down_share,
        up_share,
        out_share,
        qkv_share,
        gains_share,
        out_bias_share,
        head_bias_share,
        head_gain_share,
        unit_bias_share,
        unit_gain_share,
    ) = grad_shares
    return (
        layer_out,
        input_grad,
        gains_share,
        qkv_share,
        head_bias_share,
        head_gain_share,
        out_share,
        out_bias_share,
        up_share,
        unit_bias_share,
        unit_gain_share,
        down_share,
    )


def solution(mesh):
    placed = (
        P("shard", "context", None),
        P("shard", "context", None),
        P("shard", None),
        P("tensor", None),
        P("tensor", None),
        P(None, "shard"),
        P(None, "shard", "tensor"),
        P(None, "tensor", "shard"),
        P("tensor", "shard"),
        P("tensor", "shard"),
        P(None, "shard"),
        P("shard", "tensor"),
        P("tensor", "shard"),
        P("tensor", "shard"),
        P("tensor", "shard"),
    )
    return jax.shard_map(
        local,
        mesh=mesh,
        in_specs=placed,
        out_specs=(
            P("shard", "context", None),
            P("shard", "context", None),
            P(None, "shard"),
            P(None, "shard", "tensor"),
            P(None, "tensor", "shard"),
            P("tensor", "shard"),
            P("tensor", "shard"),
            P(None, "shard"),
            P("shard", "tensor"),
            P("tensor", "shard"),
            P("tensor", "shard"),
            P("tensor", "shard"),
        ),
        check_vma=False,
    )
```
